128 devices in a mesh: gp: 128 (over z, y, x, core).
Axes of the slice: x: 4, y: 4, z: 4, core: 2. Of those that a mesh axis runs over, the one named last changes fastest.
Arguments:
- features: bfloat16 [1572864, 128], P('gp')
- labels: int32 [1572864], P('gp')
- train_mask: float32 [1572864], P('gp')
- send_idx: int32 [16384, 64], P('gp')
- src_idx: int32 [3145728], P('gp')
- dst_idx: int32 [3145728], P('gp')
- inv_deg: float32 [1572864], P('gp')
- w_self_1: bfloat16 [128, 256], replicated
- w_neigh_1: bfloat16 [128, 256], replicated
- bias_1: float32 [256], replicated
- w_self_2: bfloat16 [256, 256], replicated
- w_neigh_2: bfloat16 [256, 256], replicated
- bias_2: float32 [256], replicated
- w_self_3: bfloat16 [256, 40], replicated
- w_neigh_3: bfloat16 [256, 40], replicated
- bias_3: float32 [40], replicated
Outputs:
- output 1: float32 [], replicated
- output 2: float32 [128, 256], replicated
- output 3: float32 [128, 256], replicated
- output 4: float32 [256], replicated
- output 5: float32 [256, 256], replicated
- output 6: float32 [256, 256], replicated
- output 7: float32 [256], replicated
- output 8: float32 [256, 40], replicated
- output 9: float32 [256, 40], replicated
- output 10: float32 [40], replicated
All inputs are finite; a program needn't handle non-finite values.
Results may differ from the reference program's by a relative error of at most 0.00569115.
Values are sent between devices in bfloat16 or wider.
A program may use at most 1 GiB of HBM per device.

```python
import jax
import jax.numpy as jnp
from jax import lax

GROUP = 128
N_DEV = 12288
HALO_DEV = 8192
DEG = 2
F_IN = 128
HIDDEN = 256
CLASSES = 40
SEND = HALO_DEV // GROUP
EDGES = N_DEV * DEG
NODES = GROUP * N_DEV
TABLE_ROWS = N_DEV + HALO_DEV


def draw_graph(key):
    keys = jax.random.split(key, 8)
    send_idx = jax.random.randint(keys[0], (GROUP * GROUP, SEND), 0, N_DEV, jnp.int32)
    hub_weight = jax.random.randint(keys[1], (GROUP, 1), 1, 5, jnp.int32)
    counts = jax.random.randint(keys[2], (GROUP, GROUP), 1, SEND + 1, jnp.int32)
    counts = jnp.clip((counts * hub_weight) // 4, 1, SEND)
    dst_idx = jnp.sort(jax.random.randint(keys[3], (GROUP, EDGES), 0, N_DEV, jnp.int32), axis=1)
    from_halo = jax.random.randint(keys[4], (GROUP, EDGES), 0, 2, jnp.int32)
    local_src = jax.random.randint(keys[5], (GROUP, EDGES), 0, N_DEV, jnp.int32)
    owner = jnp.arange(GROUP, dtype=jnp.int32)[:, None]
    peer = (owner + 1 + jax.random.randint(keys[6], (GROUP, EDGES), 0, GROUP - 1, jnp.int32)) % GROUP
    slot = jax.random.randint(keys[7], (GROUP, EDGES), 0, counts[peer, owner], jnp.int32)
    src_idx = jnp.where(from_halo == 1, N_DEV + peer * SEND + slot, local_src)
    ones_row = jnp.ones((EDGES,), jnp.float32)
    degree = jax.vmap(lambda dst_row: jax.ops.segment_sum(ones_row, dst_row, num_segments=N_DEV))(dst_idx)
    inv_deg = 1.0 / jnp.maximum(degree, 1.0)
    return send_idx, src_idx.reshape(-1), dst_idx.reshape(-1), inv_deg.reshape(-1)


def draw_weight(key, fan_in, fan_out):
    normal = jax.random.normal(key, (fan_in, fan_out), jnp.float32)
    return (normal * fan_in ** -0.5).astype(jnp.bfloat16)


def setup_inputs(seed: int = 0) -> dict:
    keys = jax.random.split(jax.random.key(seed), 13)
    send_idx, src_idx, dst_idx, inv_deg = draw_graph(keys[0])
    return {
        'features': jax.random.normal(keys[1], (NODES, F_IN), jnp.float32).astype(jnp.bfloat16),
        'labels': jax.random.randint(keys[2], (NODES,), 0, CLASSES, jnp.int32),
        'train_mask': jax.random.randint(keys[3], (NODES,), 0, 2, jnp.int32).astype(jnp.float32),
        'send_idx': send_idx,
        'src_idx': src_idx,
        'dst_idx': dst_idx,
        'inv_deg': inv_deg,
        'w_self_1': draw_weight(keys[4], F_IN, HIDDEN),
        'w_neigh_1': draw_weight(keys[5], F_IN, HIDDEN),
        'bias_1': 0.5 * jax.random.normal(keys[6], (HIDDEN,), jnp.float32),
        'w_self_2': draw_weight(keys[7], HIDDEN, HIDDEN),
        'w_neigh_2': draw_weight(keys[8], HIDDEN, HIDDEN),
        'bias_2': 0.5 * jax.random.normal(keys[9], (HIDDEN,), jnp.float32),
        'w_self_3': draw_weight(keys[10], HIDDEN, CLASSES),
        'w_neigh_3': draw_weight(keys[11], HIDDEN, CLASSES),
        'bias_3': 0.5 * jax.random.normal(keys[12], (CLASSES,), jnp.float32),
    }


def reference(features, labels, train_mask, send_idx, src_idx, dst_idx, inv_deg,
              w_self_1, w_neigh_1, bias_1, w_self_2, w_neigh_2, bias_2,
              w_self_3, w_neigh_3, bias_3):
    base = jnp.arange(GROUP, dtype=jnp.int32) * N_DEV
    halo_global = (send_idx.reshape(GROUP, GROUP, SEND) + base[:, None, None]).transpose(1, 0, 2).reshape(-1)
    src_groups = src_idx.reshape(GROUP, EDGES)
    dst_groups = dst_idx.reshape(GROUP, EDGES)
    inv_groups = inv_deg.reshape(GROUP, N_DEV, 1)

    def aggregate(hidden):
        width = hidden.shape[1]
        halo = hidden[halo_global].reshape(GROUP, HALO_DEV, width)

        def one_group(pieces):
            own_rows, halo_rows, src_row, dst_row, inv_row = pieces
            table = jnp.concatenate([own_rows, halo_rows], axis=0)
            summed = jax.ops.segment_sum(table[src_row].astype(jnp.float32), dst_row, num_segments=N_DEV)
            return (summed * inv_row).astype(jnp.bfloat16)

        pieces = (hidden.reshape(GROUP, N_DEV, width), halo, src_groups, dst_groups, inv_groups)
        return lax.map(one_group, pieces).reshape(NODES, width)

    def layer(hidden, w_self, w_neigh, bias):
        neigh_mean = aggregate(hidden)
        return (jnp.dot(hidden, w_self, preferred_element_type=jnp.float32)
                + jnp.dot(neigh_mean, w_neigh, preferred_element_type=jnp.float32) + bias)

    def loss_of(params):
        hidden_1 = jax.nn.relu(layer(features, params[0], params[1], params[2])).astype(jnp.bfloat16)
        hidden_2 = jax.nn.relu(layer(hidden_1, params[3], params[4], params[5])).astype(jnp.bfloat16)
        logits = layer(hidden_2, params[6], params[7], params[8])
        log_prob = jax.nn.log_softmax(logits, axis=-1)
        picked = jnp.take_along_axis(log_prob, labels[:, None], axis=1)[:, 0]
        return jnp.sum(train_mask * -picked) / jnp.sum(train_mask)

    params = (w_self_1, w_neigh_1, bias_1, w_self_2, w_neigh_2, bias_2, w_self_3, w_neigh_3, bias_3)
    loss, grads = jax.value_and_grad(loss_of)(params)
    return (loss,
            grads[0].astype(jnp.float32), grads[1].astype(jnp.float32), grads[2].astype(jnp.float32),
            grads[3].astype(jnp.float32), grads[4].astype(jnp.float32), grads[5].astype(jnp.float32),
            grads[6].astype(jnp.float32), grads[7].astype(jnp.float32), grads[8].astype(jnp.float32))
```

```python
import math

import jax
import jax.numpy as jnp
from jax import lax
from jax.experimental import pallas as pl
from jax.experimental.pallas import tpu as pltpu
from jax.sharding import PartitionSpec as P

GROUP_AXIS = 'gp'
LANES = 128
SPREAD = 40
BLOCK = 128
TAIL = 8
F32 = jnp.float32
BF16 = jnp.bfloat16
VMEM_LIMIT = 60 * 2 ** 20

SMEM_SPEC = pl.BlockSpec(memory_space=pltpu.SMEM)
HBM_SPEC = pl.BlockSpec(memory_space=pltpu.HBM)


def whole_spec(shape):
    return pl.BlockSpec(shape, lambda i: (0,) * len(shape))


def row_spec(rows, width):
    return pl.BlockSpec((rows, width), lambda i: (i, 0))


def params():
    return pltpu.CompilerParams(vmem_limit_bytes=VMEM_LIMIT, dimension_semantics=('arbitrary',))


def cost(micros):
    return pl.CostEstimate(flops=int(micros * 4e6), bytes_accessed=int(micros * 1e6), transcendentals=0)


def chunk_of(*sizes):
    common = math.gcd(*sizes)
    return max(d for d in range(1, min(common, 1024) + 1) if common % d == 0)


def mm(a, b):
    return jnp.dot(a, b, preferred_element_type=F32)


def tile_linear(row):
    return ((row >> 3) << 4) | (row & 7)


def stream(steps, copies, body):
    for c in copies(0, 0):
        c.start()

    def step(k, carry):
        slot = lax.rem(k, 2)

        @pl.when(k + 1 < steps)
        def _():
            for c in copies(k + 1, 1 - slot):
                c.start()
        for c in copies(k, slot):
            c.wait()
        body(k, slot)
        return carry
    lax.fori_loop(0, steps, step, 0)


def put_rows(tab, row0, x, nc):
    rows = x.shape[0]
    if nc == 1:
        tab[pl.ds(pl.multiple_of(row0, 8), rows), :] = x
    else:
        for g in range(rows // 8):
            for c in range(nc):
                at = pl.multiple_of((row0 + g * 8) * nc + c * 8, 8)
                tab[pl.ds(at, 8), :] = x[g * 8:g * 8 + 8, c * LANES:(c + 1) * LANES]


def load_table(src, tab, row0, stage, sem, nc):
    chunk = stage.shape[1]
    total = src.shape[0]

    def copies(k, slot):
        return [pltpu.make_async_copy(src.at[pl.ds(pl.multiple_of(k * chunk, chunk), chunk), :],
                                      stage.at[slot], sem.at[slot])]

    def body(k, slot):
        step = min(chunk, 128)
        for j in range(chunk // step):
            put_rows(tab, row0 + k * chunk + j * step, stage[slot, j * step:(j + 1) * step, :].astype(F32), nc)
    stream(total // chunk, copies, body)


def zero_rows(acc):
    rows = acc.shape[0]
    step = next(s for s in (256, 128, 64, 32, 16, 8) if rows % s == 0)

    def body(k, carry):
        acc[pl.ds(pl.multiple_of(k * step, step), step), :] = jnp.zeros((step, acc.shape[1]), F32)
        return carry
    lax.fori_loop(0, rows // step, body, 0)


def gather_16(idx, first, tab, nc):
    sub = lax.broadcasted_iota(jnp.int32, (8, LANES), 0)
    halves = [[None, None] for _ in range(nc)]
    for h in range(2):
        for k in range(8):
            at = idx[first + h * 8 + k]
            for c in range(nc):
                row = jnp.broadcast_to(tab[pl.ds(at + 8 * c, 1), :], (8, LANES))
                halves[c][h] = row if k == 0 else jnp.where(sub == k, row, halves[c][h])
    return [jnp.concatenate(halves[c], axis=0).astype(BF16) for c in range(nc)]


def segment_sums(meta, idx, seg, tab, acc, buf, nc, window, blocks):
    first_block, end_block, most = meta[2 * blocks], meta[2 * blocks + 1], meta[2 * blocks + 2]

    def fill(b):
        for g in range(BLOCK // 16):
            parts = gather_16(idx, b * BLOCK + g * 16, tab, nc)
            for c in range(nc):
                buf[g * 16:g * 16 + 16, c * LANES:(c + 1) * LANES] = parts[c]

    def add(b, at):
        at = pl.multiple_of(at, 8)
        rows = lax.broadcasted_iota(jnp.int32, (window, BLOCK), 0) + at
        hot = jnp.where(rows == seg[b], 1.0, 0.0).astype(BF16)
        acc[pl.ds(at, window), :] += mm(hot, buf[...])

    def body(b, carry):
        fill(b)
        add(b, meta[b])
        return carry
    lax.fori_loop(first_block, end_block, body, 0)

    @pl.when(most > 1)
    def _():
        def again(b, carry):
            count = meta[blocks + b]

            @pl.when(count > 1)
            def _():
                fill(b)

                def more(w, c):
                    add(b, meta[b] + w * window)
                    return c
                lax.fori_loop(1, count, more, 0)
            return carry
        lax.fori_loop(first_block, end_block, again, 0)


def spread_lanes():
    return lax.broadcasted_iota(jnp.int32, (1, LANES), 1)


def split3(x):
    hi = x.astype(BF16).astype(F32)
    rest = x - hi
    mid = rest.astype(BF16).astype(F32)
    low = rest - mid
    lane = spread_lanes()
    out = jnp.where(lane < SPREAD, hi, jnp.where(lane < 2 * SPREAD, mid, low))
    return jnp.where(lane < 3 * SPREAD, out, 0.0).astype(BF16)


def fold3(a):
    lane = spread_lanes()
    s = SPREAD
    one = jnp.where(lane < 2 * s, pltpu.roll(a, LANES - s, 1), pltpu.roll(a, 2 * s, 1))
    two = jnp.where(lane < s, pltpu.roll(a, LANES - 2 * s, 1), pltpu.roll(a, s, 1))
    return a + one + two


def add_rows(ref, x):
    ref[...] += jnp.sum(x.reshape(x.shape[0] // 8, 8, x.shape[1]), axis=0)


def pick_rows(name, src, idx, peers, slots, tail):
    n = src.shape[0]
    per = 8
    extra = 0 if tail is None else TAIL
    chunk = chunk_of(n)

    def kern(idx_ref, src_ref, *refs):
        if extra:
            tail_ref, out, tab, stage, sem = refs
        else:
            out, tab, stage, sem = refs

        @pl.when(pl.program_id(0) == 0)
        def _():
            load_table(src_ref, tab, 0, stage, sem, 1)
        first = pl.program_id(0) * (per * slots)

        def body(p, carry):
            for g in range(slots // 16):
                out[p, g * 16:g * 16 + 16, :] = gather_16(idx_ref, first + p * slots + g * 16, tab, 1)[0]
            if extra:
                out[p, slots:slots + extra, :] = tail_ref[...]
            return carry
        lax.fori_loop(0, per, body, 0)

    operands = [idx, src] + ([tail] if extra else [])
    specs = [SMEM_SPEC, HBM_SPEC] + ([whole_spec((TAIL, LANES))] if extra else [])
    return pl.pallas_call(
        kern, name=name, grid=(peers // per,),
        out_shape=jax.ShapeDtypeStruct((peers, slots + extra, LANES), BF16),
        in_specs=specs,
        out_specs=pl.BlockSpec((per, slots + extra, LANES), lambda i: (i, 0, 0)),
        scratch_shapes=[pltpu.VMEM((n, LANES), F32), pltpu.VMEM((2, chunk, LANES), BF16), pltpu.SemaphoreType.DMA((2,))],
        compiler_params=params(), cost_estimate=cost(10))(*operands)


def edge_call(name, edges, nc, table_rows, acc_rows, window, build, hbm_in, blocked, fixed, outs, rows_out, tile,
              epilogue, micros, stage_rows, init=None, extra_scratch=()):
    meta, idx, seg = edges
    blocks = seg.shape[0]
    width = nc * LANES
    steps = rows_out // tile
    nh, nb, nf, no = len(hbm_in), len(blocked), len(fixed), len(outs)
    acc_total = -(-(acc_rows + window) // 256) * 256

    def kern(meta_ref, idx_ref, seg_ref, *refs):
        hb, refs = refs[:nh], refs[nh:]
        bl, refs = refs[:nb], refs[nb:]
        fx, refs = refs[:nf], refs[nf:]
        out, refs = refs[:no], refs[no:]
        tab, acc, buf, stage, sem, isem = refs[:6]
        more = refs[6:]

        @pl.when(pl.program_id(0) == 0)
        def _():
            if init is None:
                zero_rows(acc)
            else:
                start = pltpu.make_async_copy(hb[init], acc.at[pl.ds(0, acc_rows), :], isem)
                start.start()
            build(tab, hb, fx, stage, sem, more)
            if init is not None:
                start.wait()
            segment_sums(meta_ref, idx_ref, seg_ref, tab, acc, buf, nc, window, blocks)
        i = pl.program_id(0)
        at = pl.multiple_of(i * tile, tile)
        epilogue(i, acc[pl.ds(at, tile), :], bl, fx, out)

    out_shape, out_specs = [], []
    for shape, dtype, sums in outs:
        out_shape.append(jax.ShapeDtypeStruct(shape, dtype))
        out_specs.append(whole_spec(shape) if sums else row_spec(tile, shape[1]))
    return pl.pallas_call(
        kern, name=name, grid=(steps,), out_shape=out_shape,
        in_specs=([SMEM_SPEC, SMEM_SPEC, whole_spec(seg.shape)] + [HBM_SPEC] * nh
                  + [row_spec(tile, x.shape[1]) for x in blocked] + [whole_spec(x.shape) for x in fixed]),
        out_specs=out_specs,
        scratch_shapes=[pltpu.VMEM((table_rows * nc, LANES), F32), pltpu.VMEM((acc_total, width), F32),
                        pltpu.VMEM((BLOCK, width), BF16), pltpu.VMEM((2, stage_rows, width), BF16),
                        pltpu.SemaphoreType.DMA((2,)), pltpu.SemaphoreType.DMA(())] + list(extra_scratch),
        compiler_params=params(), cost_estimate=cost(micros))(meta, idx, seg, *hbm_in, *blocked, *fixed)


def edge_meta(seg_first, seg_last, window, first_block, end_block):
    base = seg_first & ~7
    count = (seg_last - base) // window + 1
    tail = jnp.stack([first_block, end_block, jnp.max(count)])
    return jnp.concatenate([base, count, tail]).astype(jnp.int32)


def bits_for(n):
    return max(1, (n - 1).bit_length())


def spread3(w):
    w = jnp.pad(w, ((0, 0), (0, SPREAD - w.shape[1])))
    return jnp.pad(jnp.concatenate([w, w, w], axis=1), ((0, 0), (0, LANES - 3 * SPREAD)))


def lanes_pad(w):
    return jnp.pad(w, ((0, 0), (0, LANES - w.shape[1])))


def solution(mesh):
    peers = mesh.shape[GROUP_AXIS]

    def exchange(x):
        return lax.all_to_all(x, GROUP_AXIS, 0, 0, tiled=True)

    def device_step(features, labels, train_mask, send_idx, src_idx, dst_idx, inv_deg,
                    w_self_1, w_neigh_1, bias_1, w_self_2, w_neigh_2, bias_2,
                    w_self_3, w_neigh_3, bias_3):
        n = features.shape[0]
        slots = send_idx.shape[1]
        halo = peers * slots
        edges = src_idx.shape[0]
        hidden = w_self_1.shape[1]
        classes = w_self_3.shape[1]
        send_flat = send_idx.reshape(-1)
        tile = min(1024, n)
        stage_own = chunk_of(n)
        stage_halo = chunk_of(halo)
        slot_bits = bits_for(halo)
        dst_bits = bits_for(n)
        table = n + halo

        key_src = (src_idx << dst_bits) | dst_idx
        key_send = (send_flat << slot_bits) | jnp.arange(halo, dtype=jnp.int32)
        key_send = jnp.concatenate([key_send, jnp.full((edges - halo,), jnp.iinfo(jnp.int32).max, jnp.int32)])
        ordered = lax.sort(jnp.stack([key_src, key_send]), dimension=1, is_stable=False)
        src_s = ordered[0] >> dst_bits
        dst_s = ordered[0] & ((1 << dst_bits) - 1)
        row_s = ordered[1, :halo] >> slot_bits
        slot_s = ordered[1, :halo] & ((1 << slot_bits) - 1)
        blocks = edges // BLOCK
        halo_blocks = halo // BLOCK
        zero = jnp.int32(0)

        win_f, win_o, win_h, win_r = 128, 176, 176, 240
        far = src_idx - n
        idx_1 = jnp.where(src_idx < n, src_idx, src_idx + TAIL * (far // slots))
        meta_f = edge_meta(dst_idx[::BLOCK], dst_idx[BLOCK - 1::BLOCK], win_f, zero, jnp.int32(blocks))
        seg_f = dst_idx.reshape(blocks, 1, BLOCK)
        fwd_1 = (meta_f, idx_1, seg_f)
        fwd_2 = (meta_f, tile_linear(src_idx), seg_f)
        fwd_3 = (meta_f, src_idx, seg_f)

        owned = jnp.sum((src_idx < n).astype(jnp.int32))
        first, last = src_s[::BLOCK], src_s[BLOCK - 1::BLOCK]
        meta_o = edge_meta(jnp.minimum(first, n - 1), jnp.minimum(last, n - 1), win_o, zero,
                           (owned + BLOCK - 1) // BLOCK)
        meta_h = edge_meta(jnp.maximum(first - n, 0), jnp.maximum(last - n, 0), win_h, owned // BLOCK,
                           jnp.int32(blocks))
        seg_o = src_s.reshape(blocks, 1, BLOCK)
        seg_h = seg_o - n
        meta_r = edge_meta(row_s[::BLOCK], row_s[BLOCK - 1::BLOCK], win_r, zero, jnp.int32(halo_blocks))
        seg_r = row_s.reshape(halo_blocks, 1, BLOCK)
        dst_wide = tile_linear(dst_s)

        inv = jnp.broadcast_to(inv_deg[:, None], (n, LANES))
        b1 = bias_1.reshape(1, -1)
        b2 = bias_2.reshape(1, -1)
        lane = jnp.arange(LANES, dtype=jnp.int32)
        b3 = jnp.where(lane < 3 * SPREAD, spread3(bias_3.reshape(1, -1)), -1e30)
        if classes < SPREAD:
            b3 = jnp.where(lane % SPREAD < classes, b3, -1e30)
        target = jnp.where(lane[None, :] < 3 * SPREAD,
                           train_mask[:, None] * (1.0 + (labels[:, None] == lane[None, :] % SPREAD)), 0.0).astype(BF16)
        ws3, wn3 = spread3(w_self_3), spread3(w_neigh_3)
        ws3_t, wn3_t = lanes_pad(w_self_3).T, lanes_pad(w_neigh_3).T

        marked = jnp.sum(train_mask).astype(jnp.int32)
        digits = jnp.stack([marked // LANES, marked % LANES]).astype(BF16)
        tail = jnp.pad(digits.reshape(1, 2), ((0, TAIL - 1), (0, LANES - 2)))
        out_1 = pick_rows('send_1', features, send_flat, peers, slots, tail)
        got_1 = exchange(out_1)
        counts = got_1[:, slots, :2].astype(F32)
        total = jnp.sum(counts[:, 0]) * LANES + jnp.sum(counts[:, 1])
        got_1_rows = got_1.reshape(peers * (slots + TAIL), LANES)
        rows_1 = got_1_rows.shape[0]

        def own_and_halo(nc, rows_own):
            def build(tab, hb, fx, stage, sem, more):
                load_table(hb[0], tab, 0, stage, sem, nc)
                load_table(hb[1], tab, rows_own, stage, sem, nc)
            return build

        def only(nc):
            def build(tab, hb, fx, stage, sem, more):
                load_table(hb[0], tab, 0, stage, sem, nc)
            return build

        def epi_1(i, a, bl, fx, out):
            mean = (a * bl[1][...]).astype(BF16)
            z = mm(bl[0][...], fx[0][...]) + mm(mean, fx[1][...]) + fx[2][...]
            out[0][...] = mean
            out[1][...] = jnp.maximum(z, 0.0).astype(BF16)

        mean_1, hidden_1 = edge_call(
            'layer_1', fwd_1, 1, n + rows_1, n, win_f, own_and_halo(1, n), [features, got_1_rows],
            [features, inv], [w_self_1, w_neigh_1, b1],
            [((n, LANES), BF16, False), ((n, hidden), BF16, False)], n, tile, epi_1, 40,
            stage_rows=chunk_of(n, rows_1))

        out_2 = pick_rows('send_2', mean_1, send_flat, peers, slots, None)
        got_2 = exchange(out_2)
        group = 8

        def build_2(tab, hb, fx, stage, sem, more):
            load_table(hb[0], tab, 0, stage, sem, 2)
            hb_f, hb_m, sem_m = more

            def copies(k, slot):
                at = pl.ds(k * group, group)
                return [pltpu.make_async_copy(hb[1].at[at], hb_f.at[slot], sem.at[slot]),
                        pltpu.make_async_copy(hb[2].at[at], hb_m.at[slot], sem_m.at[slot])]

            def body(k, slot):
                def one(p, carry):
                    z = (mm(hb_f[slot, p, :slots, :], fx[3][...]) + mm(hb_m[slot, p], fx[4][...]) + fx[5][...])
                    h = jnp.maximum(z, 0.0).astype(BF16).astype(F32)
                    put_rows(tab, n + (k * group + p) * slots, h, 2)
                    return carry
                lax.fori_loop(0, group, one, 0)
            stream(peers // group, copies, body)

        def epi_2(i, a, bl, fx, out):
            scale = bl[1][...]
            mean = (a * jnp.concatenate([scale, scale], axis=1)).astype(BF16)
            z = mm(bl[0][...], fx[0][...]) + mm(mean, fx[1][...]) + fx[2][...]
            h = jnp.maximum(z, 0.0).astype(BF16)
            out[0][...] = mean
            out[1][...] = h
            out[2][...] = split3(mm(h, fx[6][...]))
            out[3][...] = mm(h, fx[7][...])

        mean_2, hidden_2, proj, logits_self = edge_call(
            'layer_2', fwd_2, 2, table, n, win_f, build_2, [hidden_1, got_1, got_2], [hidden_1, inv],
            [w_self_2, w_neigh_2, b2, w_self_1, w_neigh_1, b1, wn3, ws3],
            [((n, hidden), BF16, False), ((n, hidden), BF16, False), ((n, LANES), BF16, False),
             ((n, LANES), F32, False)], n, tile, epi_2, 60, stage_rows=stage_own,
            extra_scratch=[pltpu.VMEM((2, group, slots + TAIL, LANES), BF16), pltpu.VMEM((2, group, slots, LANES), BF16),
                           pltpu.SemaphoreType.DMA((2,))])

        out_3 = pick_rows('send_3', proj, send_flat, peers, slots, None)
        got_3 = exchange(out_3).reshape(halo, LANES)
        inv_total = (1.0 / total).reshape(1, 1)

        def epi_3(i, a, bl, fx, out):
            scale = bl[1][...]
            z = bl[0][...] + fold3(a * scale) + fx[0][...]
            lane = spread_lanes()
            z = jnp.where(lane < 3 * SPREAD, z, -1e30)
            top = jnp.max(z, axis=1, keepdims=True)
            e = jnp.where(lane < SPREAD, jnp.exp(z - top), 0.0)
            lse = top + jnp.log(jnp.sum(e, axis=1, keepdims=True))
            t = bl[2][...].astype(F32)
            hit = t > 1.5
            d = jnp.where(t > 0.5, jnp.exp(z - lse) - jnp.where(hit, 1.0, 0.0), 0.0) * fx[1][...]
            db = d.astype(BF16)
            out[0][...] = db
            out[1][...] = split3(db.astype(F32) * scale)

            @pl.when(i == 0)
            def _():
                out[2][...] = jnp.zeros_like(out[2])
                out[3][...] = jnp.zeros_like(out[3])
            add_rows(out[2], d)
            add_rows(out[3], jnp.where(hit & (lane < SPREAD), lse - z, 0.0))

        d_bf_3, scaled_3, g_b3, loss_parts = edge_call(
            'layer_3', fwd_3, 1, table, n, win_f, own_and_halo(1, n), [proj, got_3],
            [logits_self, inv, target], [b3, jnp.broadcast_to(inv_total, (1, LANES))],
            [((n, LANES), BF16, False), ((n, LANES), BF16, False), ((8, LANES), F32, True), ((8, LANES), F32, True)],
            n, tile, epi_3, 40, stage_rows=chunk_of(n, halo))

        def epi_b3h(i, a, bl, fx, out):
            out[0][...] = split3(fold3(a))

        def epi_plain(i, a, bl, fx, out):
            out[0][...] = a

        tile_h = min(1024, halo)
        back_3 = edge_call('back_3_halo', (meta_h, dst_s, seg_h), 1, n, halo, win_h, only(1), [scaled_3], [], [],
                           [((halo, LANES), BF16, False)], halo, tile_h, epi_b3h, 15, stage_rows=stage_own)[0]
        ret_3 = exchange(back_3.reshape(peers, slots, LANES)).reshape(halo, LANES)
        own_3 = edge_call('back_3_own', (meta_o, dst_s, seg_o), 1, n, n, win_o, only(1), [scaled_3], [], [],
                          [((n, LANES), F32, False)], n, tile, epi_plain, 20, stage_rows=stage_own)[0]

        def epi_o3(i, a, bl, fx, out):
            tb = fold3(a).astype(BF16)
            d_h = mm(bl[0][...], fx[0][...]) + mm(tb, fx[1][...])
            d_pre = jnp.where(bl[1][...] > 0, d_h, 0.0)
            db = d_pre.astype(BF16)
            scale = bl[2][...]
            out[0][...] = tb
            out[1][...] = db
            out[2][...] = (mm(db, fx[2][...]) * jnp.concatenate([scale, scale], axis=1)).astype(BF16)

            @pl.when(i == 0)
            def _():
                out[3][...] = jnp.zeros_like(out[3])
            add_rows(out[3], d_pre)

        tb_3, d_bf_2, scaled_2, g_b2 = edge_call(
            'owner_3', (meta_r, slot_s, seg_r), 1, halo, n, win_r, only(1), [ret_3, own_3],
            [d_bf_3, hidden_2, inv], [ws3_t, wn3_t, w_neigh_2.T],
            [((n, LANES), BF16, False), ((n, hidden), BF16, False), ((n, hidden), BF16, False), ((8, hidden), F32, True)],
            n, tile, epi_o3, 30, init=1, stage_rows=stage_halo)

        def epi_b2h(i, a, bl, fx, out):
            out[0][...] = a.astype(BF16)

        def epi_b2o(i, a, bl, fx, out):
            out[0][...] = a + mm(bl[0][...], fx[0][...])

        back_2 = edge_call('back_2_halo', (meta_h, dst_wide, seg_h), 2, n, halo, win_h, only(2), [scaled_2], [], [],
                           [((halo, hidden), BF16, False)], halo, tile_h, epi_b2h, 20, stage_rows=stage_own)[0]
        ret_2 = exchange(back_2.reshape(peers, slots, hidden)).reshape(halo, hidden)
        own_2 = edge_call('back_2_own', (meta_o, dst_wide, seg_o), 2, n, n, win_o, only(2), [scaled_2], [d_bf_2],
                          [w_self_2.T], [((n, hidden), F32, False)], n, tile, epi_b2o, 30, stage_rows=stage_own)[0]

        def epi_o2(i, a, bl, fx, out):
            d_pre = jnp.where(bl[0][...] > 0, a, 0.0)
            out[0][...] = d_pre.astype(BF16)

            @pl.when(i == 0)
            def _():
                out[1][...] = jnp.zeros_like(out[1])
            add_rows(out[1], d_pre)

        d_bf_1, g_b1 = edge_call(
            'owner_2', (meta_r, tile_linear(slot_s), seg_r), 2, halo, n, win_r, only(2), [ret_2, own_2],
            [hidden_1], [], [((n, hidden), BF16, False), ((8, hidden), F32, True)], n, tile, epi_o2, 25, init=1,
            stage_rows=stage_halo)

        def contract(a, b):
            return jnp.einsum('nd,ne->de', a, b, preferred_element_type=F32)

        parts = [contract(features, d_bf_1), contract(mean_1, d_bf_1), jnp.sum(g_b1, axis=0),
                 contract(hidden_1, d_bf_2), contract(mean_2, d_bf_2), jnp.sum(g_b2, axis=0),
                 contract(hidden_2, d_bf_3)[:, :classes], contract(hidden_2, tb_3)[:, :classes],
                 jnp.sum(g_b3, axis=0)[:classes], jnp.sum(loss_parts).reshape(1)]
        sizes = [p.size for p in parts]
        whole = sum(sizes)
        share = -(-whole // (peers * LANES)) * LANES
        flat = jnp.concatenate([p.reshape(-1) for p in parts] + [jnp.zeros((share * peers - whole,), F32)])
        mine = jnp.sum(exchange(flat.reshape(peers, share)), axis=0)
        full = exchange(jnp.broadcast_to(mine, (peers, share))).reshape(-1)
        outs, at = [], 0
        for p, size in zip(parts, sizes):
            outs.append(full[at:at + size].reshape(p.shape))
            at += size
        return (outs[-1][0] / total,) + tuple(outs[:-1])

    sharded = P(GROUP_AXIS)
    whole = P()
    return jax.shard_map(device_step, mesh=mesh,
                         in_specs=(sharded,) * 7 + (whole,) * 9,
                         out_specs=(whole,) * 10, check_vma=False)
```

```python
import math

import jax
import jax.numpy as jnp
from jax import lax
from jax.experimental import pallas as pl
from jax.experimental.pallas import tpu as pltpu
from jax.sharding import PartitionSpec as P

GROUP_AXIS = 'gp'
LANES = 128
SPREAD = 40
BLOCK = 128
GROUP = 8
TAIL = 8
F32 = jnp.float32
BF16 = jnp.bfloat16
VMEM_LIMIT = 60 * 2 ** 20

SMEM_SPEC = pl.BlockSpec(memory_space=pltpu.SMEM)
HBM_SPEC = pl.BlockSpec(memory_space=pltpu.HBM)


def whole_spec(shape):
    return pl.BlockSpec(shape, lambda i: (0,) * len(shape))


def row_spec(rows, width):
    return pl.BlockSpec((rows, width), lambda i: (i, 0))


def params():
    return pltpu.CompilerParams(vmem_limit_bytes=VMEM_LIMIT, dimension_semantics=('arbitrary',))


def cost(micros):
    return pl.CostEstimate(flops=int(micros * 4e6), bytes_accessed=int(micros * 1e6), transcendentals=0)


def mm(a, b):
    return jnp.dot(a, b, preferred_element_type=F32)


def tile_linear(row):
    return ((row >> 3) << 4) | (row & 7)


def put_rows(tab, row0, x, nc):
    rows = x.shape[0]
    if nc == 1:
        tab[pl.ds(pl.multiple_of(row0, 8), rows), :] = x
    else:
        for g in range(rows // 8):
            for c in range(nc):
                at = pl.multiple_of((row0 + g * 8) * nc + c * 8, 8)
                tab[pl.ds(at, 8), :] = x[g * 8:g * 8 + 8, c * LANES:(c + 1) * LANES]


def fetch(src, stage, sem, parts):
    rows = src.shape[0] // parts
    copies = [pltpu.make_async_copy(src.at[pl.ds(k * rows, rows)], stage.at[pl.ds(k * rows, rows)], sem.at[k])
              for k in range(parts)]
    for c in copies:
        c.start()
    return copies


def unpack(copies, stage, tab, row0, nc):
    rows = stage.shape[0] // len(copies)
    step = next(d for d in (128, 96, 64, 32, 16) if rows % d == 0)
    for p, c in enumerate(copies):
        c.wait()

        def body(k, carry):
            at = pl.multiple_of(p * rows + k * step, step)
            put_rows(tab, row0 + at, stage[pl.ds(at, step), :].astype(F32), nc)
            return carry
        lax.fori_loop(0, rows // step, body, 0)


def group_of(blocks):
    return next(u for u in (GROUP, 4, 2) if blocks % u == 0)


def zero_rows(acc):
    rows = acc.shape[0]
    step = next(s for s in (256, 128, 64, 32, 16, 8) if rows % s == 0)

    def body(k, carry):
        acc[pl.ds(pl.multiple_of(k * step, step), step), :] = jnp.zeros((step, acc.shape[1]), F32)
        return carry
    lax.fori_loop(0, rows // step, body, 0)


def gather_16(idx, first, tab, nc):
    sub = lax.broadcasted_iota(jnp.int32, (8, LANES), 0)
    halves = [[None, None] for _ in range(nc)]
    for h in range(2):
        for k in range(8):
            at = idx[first + h * 8 + k]
            for c in range(nc):
                row = jnp.broadcast_to(tab[pl.ds(at + 8 * c, 1), :], (8, LANES))
                halves[c][h] = row if k == 0 else jnp.where(sub == k, row, halves[c][h])
    return [jnp.concatenate(halves[c], axis=0).astype(BF16) for c in range(nc)]


def segment_sums(meta, idx, seg, tab, acc, bufs, nc, window, blocks):
    unroll = group_of(blocks)
    first_trip, end_trip, most = meta[2 * blocks], meta[2 * blocks + 1], meta[2 * blocks + 2]

    def fill(b, buf):
        for g in range(BLOCK // 16):
            parts = gather_16(idx, b * BLOCK + g * 16, tab, nc)
            for c in range(nc):
                buf[g * 16:g * 16 + 16, c * LANES:(c + 1) * LANES] = parts[c]

    def sums(b, at, buf):
        rows = lax.broadcasted_iota(jnp.int32, (window, BLOCK), 0) + at
        return mm(jnp.where(rows == seg[b], 1.0, 0.0).astype(BF16), buf[...])

    def add(at, x):
        acc[pl.ds(pl.multiple_of(at, 8), window), :] += x

    fill(jnp.minimum(first_trip * unroll, blocks - 1), bufs[0])

    def body(t, carry):
        before = None
        for u in range(unroll):
            b = t * unroll + u
            now = (meta[b], sums(b, meta[b], bufs[u % 2]))
            fill(jnp.minimum(b + 1, blocks - 1), bufs[(u + 1) % 2])
            if before is not None:
                add(*before)
            before = now
        add(*before)
        return carry
    lax.fori_loop(first_trip, end_trip, body, 0)

    @pl.when(most > 1)
    def _():
        def again(b, carry):
            count = meta[blocks + b]

            @pl.when(count > 1)
            def _():
                fill(b, bufs[0])

                def more(w, c):
                    at = meta[b] + w * window
                    add(at, sums(b, at, bufs[0]))
                    return c
                lax.fori_loop(1, count, more, 0)
            return carry
        lax.fori_loop(first_trip * unroll, end_trip * unroll, again, 0)


def spread_lanes():
    return lax.broadcasted_iota(jnp.int32, (1, LANES), 1)


def split3(x):
    hi = x.astype(BF16).astype(F32)
    rest = x - hi
    mid = rest.astype(BF16).astype(F32)
    low = rest - mid
    lane = spread_lanes()
    out = jnp.where(lane < SPREAD, hi, jnp.where(lane < 2 * SPREAD, mid, low))
    return jnp.where(lane < 3 * SPREAD, out, 0.0).astype(BF16)


def fold3(a):
    lane = spread_lanes()
    s = SPREAD
    one = jnp.where(lane < 2 * s, pltpu.roll(a, LANES - s, 1), pltpu.roll(a, 2 * s, 1))
    two = jnp.where(lane < s, pltpu.roll(a, LANES - 2 * s, 1), pltpu.roll(a, s, 1))
    return a + one + two


def add_rows(ref, x):
    ref[...] += jnp.sum(x.reshape(x.shape[0] // 8, 8, x.shape[1]), axis=0)


def pick_rows(name, src, idx, peers, slots, tail):
    n = src.shape[0]
    per = math.gcd(peers, 32)
    extra = 0 if tail is None else TAIL
    parts = math.gcd(n // 128, 4)

    def kern(idx_ref, src_ref, *refs):
        if extra:
            tail_ref, out, tab, stage, sem = refs
        else:
            out, tab, stage, sem = refs

        @pl.when(pl.program_id(0) == 0)
        def _():
            unpack(fetch(src_ref, stage, sem, parts), stage, tab, 0, 1)
        first = pl.program_id(0) * (per * slots)

        def body(p, carry):
            for g in range(slots // 16):
                out[p, g * 16:g * 16 + 16, :] = gather_16(idx_ref, first + p * slots + g * 16, tab, 1)[0]
            if extra:
                out[p, slots:slots + extra, :] = tail_ref[...]
            return carry
        lax.fori_loop(0, per, body, 0)

    operands = [idx, src] + ([tail] if extra else [])
    specs = [SMEM_SPEC, HBM_SPEC] + ([whole_spec((TAIL, LANES))] if extra else [])
    return pl.pallas_call(
        kern, name=name, grid=(peers // per,),
        out_shape=jax.ShapeDtypeStruct((peers, slots + extra, LANES), BF16),
        in_specs=specs,
        out_specs=pl.BlockSpec((per, slots + extra, LANES), lambda i: (i, 0, 0)),
        scratch_shapes=[pltpu.VMEM((n, LANES), F32), pltpu.VMEM((n, LANES), BF16), pltpu.SemaphoreType.DMA((parts,))],
        compiler_params=params(), cost_estimate=cost(10))(*operands)


def edge_call(name, edges, nc, table_rows, acc_rows, window, sources, build, hbm_in, blocked, fixed, outs, rows_out,
              tile, epilogue, micros, init=None):
    meta, idx, seg = edges
    blocks = seg.shape[0]
    width = nc * LANES
    nh, nb, nf, no, ns = len(hbm_in), len(blocked), len(fixed), len(outs), len(sources)
    acc_total = -(-(acc_rows + window) // 256) * 256
    parts = 4

    def kern(meta_ref, idx_ref, seg_ref, *refs):
        hb, refs = refs[:nh], refs[nh:]
        bl, refs = refs[:nb], refs[nb:]
        fx, refs = refs[:nf], refs[nf:]
        out, refs = refs[:no], refs[no:]
        tab, acc, buf_0, buf_1, isem = refs[:5]
        stages, sems = refs[5:5 + ns], refs[5 + ns:]

        @pl.when(pl.program_id(0) == 0)
        def _():
            copies = [fetch(h, st, sm, parts) for h, st, sm in zip(hb, stages, sems)]
            if init is None:
                zero_rows(acc)
            else:
                start = pltpu.make_async_copy(hb[init], acc.at[pl.ds(0, acc_rows), :], isem)
                start.start()
            build(copies, stages, tab, fx)
            if init is not None:
                start.wait()
            segment_sums(meta_ref, idx_ref, seg_ref, tab, acc, (buf_0, buf_1), nc, window, blocks)
        i = pl.program_id(0)
        epilogue(i, acc[pl.ds(pl.multiple_of(i * tile, tile), tile), :], bl, fx, out)

    out_shape, out_specs = [], []
    for shape, dtype, sums in outs:
        out_shape.append(jax.ShapeDtypeStruct(shape, dtype))
        out_specs.append(whole_spec(shape) if sums else row_spec(tile, shape[1]))
    return pl.pallas_call(
        kern, name=name, grid=(rows_out // tile,), out_shape=out_shape,
        in_specs=([SMEM_SPEC, SMEM_SPEC, whole_spec(seg.shape)] + [HBM_SPEC] * nh
                  + [row_spec(tile, x.shape[1]) for x in blocked] + [whole_spec(x.shape) for x in fixed]),
        out_specs=out_specs,
        scratch_shapes=([pltpu.VMEM((table_rows * nc, LANES), F32), pltpu.VMEM((acc_total, width), F32),
                         pltpu.VMEM((BLOCK, width), BF16), pltpu.VMEM((BLOCK, width), BF16),
                         pltpu.SemaphoreType.DMA(())]
                        + [pltpu.VMEM(shape, BF16) for shape in sources]
                        + [pltpu.SemaphoreType.DMA((parts,)) for _ in sources]),
        compiler_params=params(), cost_estimate=cost(micros))(meta, idx, seg, *hbm_in, *blocked, *fixed)


def edge_meta(seg_first, seg_last, window, first_block, end_block):
    unroll = group_of(seg_first.shape[0])
    base = seg_first & ~7
    count = (seg_last - base) // window + 1
    tail = jnp.stack([first_block // unroll, (end_block + unroll - 1) // unroll, jnp.max(count)])
    return jnp.concatenate([base, count, tail]).astype(jnp.int32)


def bits_for(n):
    return max(1, (n - 1).bit_length())


def spread3(w):
    w = jnp.pad(w, ((0, 0), (0, SPREAD - w.shape[1])))
    return jnp.pad(jnp.concatenate([w, w, w], axis=1), ((0, 0), (0, LANES - 3 * SPREAD)))


def lanes_pad(w):
    return jnp.pad(w, ((0, 0), (0, LANES - w.shape[1])))


def solution(mesh):
    peers = mesh.shape[GROUP_AXIS]

    def exchange(x):
        return lax.all_to_all(x, GROUP_AXIS, 0, 0, tiled=True)

    def device_step(features, labels, train_mask, send_idx, src_idx, dst_idx, inv_deg,
                    w_self_1, w_neigh_1, bias_1, w_self_2, w_neigh_2, bias_2,
                    w_self_3, w_neigh_3, bias_3):
        n = features.shape[0]
        slots = send_idx.shape[1]
        halo = peers * slots
        edges = src_idx.shape[0]
        hidden = w_self_1.shape[1]
        classes = w_self_3.shape[1]
        send_flat = send_idx.reshape(-1)
        tile = min(1024, n)
        slot_bits = bits_for(halo)
        dst_bits = bits_for(n)
        table = n + halo

        key_src = (src_idx << dst_bits) | dst_idx
        key_send = (send_flat << slot_bits) | jnp.arange(halo, dtype=jnp.int32)
        by_src = lax.sort(key_src, is_stable=False)
        by_row = lax.sort(key_send, is_stable=False)
        src_s = by_src >> dst_bits
        dst_s = by_src & ((1 << dst_bits) - 1)
        row_s = by_row >> slot_bits
        slot_s = by_row & ((1 << slot_bits) - 1)
        blocks = edges // BLOCK
        halo_blocks = halo // BLOCK
        zero = jnp.int32(0)

        win_f, win_o, win_h, win_r = 128, 176, 144, 240
        far = src_idx - n
        idx_1 = jnp.where(src_idx < n, src_idx, src_idx + TAIL * (far // slots))
        meta_f = edge_meta(dst_idx[::BLOCK], dst_idx[BLOCK - 1::BLOCK], win_f, zero, jnp.int32(blocks))
        seg_f = dst_idx.reshape(blocks, 1, BLOCK)
        fwd_1 = (meta_f, idx_1, seg_f)
        fwd_2 = (meta_f, tile_linear(src_idx), seg_f)
        fwd_3 = (meta_f, src_idx, seg_f)

        owned = jnp.sum((src_idx < n).astype(jnp.int32))
        first, last = src_s[::BLOCK], src_s[BLOCK - 1::BLOCK]
        meta_o = edge_meta(jnp.minimum(first, n - 1), jnp.minimum(last, n - 1), win_o, zero,
                           (owned + BLOCK - 1) // BLOCK)
        meta_h = edge_meta(jnp.maximum(first - n, 0), jnp.maximum(last - n, 0), win_h, owned // BLOCK,
                           jnp.int32(blocks))
        seg_o = src_s.reshape(blocks, 1, BLOCK)
        seg_h = seg_o - n
        meta_r = edge_meta(row_s[::BLOCK], row_s[BLOCK - 1::BLOCK], win_r, zero, jnp.int32(halo_blocks))
        seg_r = row_s.reshape(halo_blocks, 1, BLOCK)
        dst_wide = tile_linear(dst_s)

        inv = jnp.broadcast_to(inv_deg[:, None], (n, LANES))
        b1 = bias_1.reshape(1, -1)
        b2 = bias_2.reshape(1, -1)
        lane = jnp.arange(LANES, dtype=jnp.int32)
        b3 = jnp.where(lane < 3 * SPREAD, spread3(bias_3.reshape(1, -1)), -1e30)
        if classes < SPREAD:
            b3 = jnp.where(lane % SPREAD < classes, b3, -1e30)
        target = jnp.where(lane[None, :] < 3 * SPREAD,
                           train_mask[:, None] * (1.0 + (labels[:, None] == lane[None, :] % SPREAD)), 0.0).astype(BF16)
        ws3, wn3 = spread3(w_self_3), spread3(w_neigh_3)
        ws3_t, wn3_t = lanes_pad(w_self_3).T, lanes_pad(w_neigh_3).T

        marked = jnp.sum(train_mask).astype(jnp.int32)
        digits = jnp.stack([marked // LANES, marked % LANES]).astype(BF16)
        tail = jnp.pad(digits.reshape(1, 2), ((0, TAIL - 1), (0, LANES - 2)))
        out_1 = pick_rows('send_1', features, send_flat, peers, slots, tail)
        got_1 = exchange(out_1)
        counts = got_1[:, slots, :2].astype(F32)
        total = jnp.sum(counts[:, 0]) * LANES + jnp.sum(counts[:, 1])
        got_1_rows = got_1.reshape(peers * (slots + TAIL), LANES)
        rows_1 = got_1_rows.shape[0]

        def rows_of(nc, *starts):
            def build(copies, stages, tab, fx):
                for c, st, row0 in zip(copies, stages, starts):
                    unpack(c, st, tab, row0, nc)
            return build

        def epi_1(i, a, bl, fx, out):
            mean = (a * bl[1][...]).astype(BF16)
            z = mm(bl[0][...], fx[0][...]) + mm(mean, fx[1][...]) + fx[2][...]
            out[0][...] = mean
            out[1][...] = jnp.maximum(z, 0.0).astype(BF16)

        mean_1, hidden_1 = edge_call(
            'layer_1', fwd_1, 1, n + rows_1, n, win_f, [(n, LANES), (rows_1, LANES)], rows_of(1, 0, n),
            [features, got_1_rows],
            [features, inv], [w_self_1, w_neigh_1, b1],
            [((n, LANES), BF16, False), ((n, hidden), BF16, False)], n, tile, epi_1, 40)

        out_2 = pick_rows('send_2', mean_1, send_flat, peers, slots, None)
        got_2 = exchange(out_2)

        def build_2(copies, stages, tab, fx):
            unpack(copies[0], stages[0], tab, 0, 2)
            per = peers // len(copies[1])
            some = math.gcd(per, 8)
            for p in range(len(copies[1])):
                copies[1][p].wait()
                copies[2][p].wait()

                def body(k, carry):
                    q = p * per + k * some
                    f = stages[1][pl.ds(q, some), :slots, :].reshape(some * slots, LANES)
                    m = stages[2][pl.ds(q, some)].reshape(some * slots, LANES)
                    z = mm(f, fx[3][...]) + mm(m, fx[4][...]) + fx[5][...]
                    put_rows(tab, n + q * slots, jnp.maximum(z, 0.0).astype(BF16).astype(F32), 2)
                    return carry
                lax.fori_loop(0, per // some, body, 0)

        def epi_2(i, a, bl, fx, out):
            scale = bl[1][...]
            mean = (a * jnp.concatenate([scale, scale], axis=1)).astype(BF16)
            z = mm(bl[0][...], fx[0][...]) + mm(mean, fx[1][...]) + fx[2][...]
            h = jnp.maximum(z, 0.0).astype(BF16)
            out[0][...] = mean
            out[1][...] = h
            out[2][...] = split3(mm(h, fx[6][...]))
            out[3][...] = mm(h, fx[7][...])

        mean_2, hidden_2, proj, logits_self = edge_call(
            'layer_2', fwd_2, 2, table, n, win_f,
            [(n, hidden), (peers, slots + TAIL, LANES), (peers, slots, LANES)], build_2, [hidden_1, got_1, got_2],
            [hidden_1, inv], [w_self_2, w_neigh_2, b2, w_self_1, w_neigh_1, b1, wn3, ws3],
            [((n, hidden), BF16, False), ((n, hidden), BF16, False), ((n, LANES), BF16, False),
             ((n, LANES), F32, False)], n, tile, epi_2, 60)

        out_3 = pick_rows('send_3', proj, send_flat, peers, slots, None)
        got_3 = exchange(out_3).reshape(halo, LANES)
        inv_total = (1.0 / total).reshape(1, 1)

        def epi_3(i, a, bl, fx, out):
            scale = bl[1][...]
            z = bl[0][...] + fold3(a * scale) + fx[0][...]
            lane = spread_lanes()
            z = jnp.where(lane < 3 * SPREAD, z, -1e30)
            top = jnp.max(z, axis=1, keepdims=True)
            e = jnp.where(lane < SPREAD, jnp.exp(z - top), 0.0)
            lse = top + jnp.log(jnp.sum(e, axis=1, keepdims=True))
            t = bl[2][...].astype(F32)
            hit = t > 1.5
            d = jnp.where(t > 0.5, jnp.exp(z - lse) - jnp.where(hit, 1.0, 0.0), 0.0) * fx[1][...]
            db = d.astype(BF16)
            out[0][...] = db
            out[1][...] = split3(db.astype(F32) * scale)

            @pl.when(i == 0)
            def _():
                out[2][...] = jnp.zeros_like(out[2])
                out[3][...] = jnp.zeros_like(out[3])
            add_rows(out[2], d)
            add_rows(out[3], jnp.where(hit & (lane < SPREAD), lse - z, 0.0))

        d_bf_3, scaled_3, g_b3, loss_parts = edge_call(
            'layer_3', fwd_3, 1, table, n, win_f, [(n, LANES), (halo, LANES)], rows_of(1, 0, n), [proj, got_3],
            [logits_self, inv, target], [b3, jnp.broadcast_to(inv_total, (1, LANES))],
            [((n, LANES), BF16, False), ((n, LANES), BF16, False), ((8, LANES), F32, True), ((8, LANES), F32, True)],
            n, tile, epi_3, 40)

        def epi_b3h(i, a, bl, fx, out):
            out[0][...] = split3(fold3(a))

        def epi_plain(i, a, bl, fx, out):
            out[0][...] = a

        tile_h = min(1024, halo)
        back_3 = edge_call('back_3_halo', (meta_h, dst_s, seg_h), 1, n, halo, win_h, [(n, LANES)], rows_of(1, 0), [scaled_3], [], [],
                           [((halo, LANES), BF16, False)], halo, tile_h, epi_b3h, 15)[0]
        ret_3 = exchange(back_3.reshape(peers, slots, LANES)).reshape(halo, LANES)
        own_3 = edge_call('back_3_own', (meta_o, dst_s, seg_o), 1, n, n, win_o, [(n, LANES)], rows_of(1, 0), [scaled_3], [], [],
                          [((n, LANES), F32, False)], n, tile, epi_plain, 20)[0]

        def epi_o3(i, a, bl, fx, out):
            tb = fold3(a).astype(BF16)
            d_h = mm(bl[0][...], fx[0][...]) + mm(tb, fx[1][...])
            d_pre = jnp.where(bl[1][...] > 0, d_h, 0.0)
            db = d_pre.astype(BF16)
            scale = bl[2][...]
            out[0][...] = tb
            out[1][...] = db
            out[2][...] = (mm(db, fx[2][...]) * jnp.concatenate([scale, scale], axis=1)).astype(BF16)

            @pl.when(i == 0)
            def _():
                out[3][...] = jnp.zeros_like(out[3])
            add_rows(out[3], d_pre)

        tb_3, d_bf_2, scaled_2, g_b2 = edge_call(
            'owner_3', (meta_r, slot_s, seg_r), 1, halo, n, win_r, [(halo, LANES)], rows_of(1, 0), [ret_3, own_3],
            [d_bf_3, hidden_2, inv], [ws3_t, wn3_t, w_neigh_2.T],
            [((n, LANES), BF16, False), ((n, hidden), BF16, False), ((n, hidden), BF16, False), ((8, hidden), F32, True)],
            n, tile, epi_o3, 30, init=1)

        def epi_b2h(i, a, bl, fx, out):
            out[0][...] = a.astype(BF16)

        def epi_b2o(i, a, bl, fx, out):
            out[0][...] = a + mm(bl[0][...], fx[0][...])

        back_2 = edge_call('back_2_halo', (meta_h, dst_wide, seg_h), 2, n, halo, win_h, [(n, hidden)], rows_of(2, 0), [scaled_2], [], [],
                           [((halo, hidden), BF16, False)], halo, tile_h, epi_b2h, 20)[0]
        ret_2 = exchange(back_2.reshape(peers, slots, hidden)).reshape(halo, hidden)
        own_2 = edge_call('back_2_own', (meta_o, dst_wide, seg_o), 2, n, n, win_o, [(n, hidden)], rows_of(2, 0), [scaled_2], [d_bf_2],
                          [w_self_2.T], [((n, hidden), F32, False)], n, tile, epi_b2o, 30)[0]

        def epi_o2(i, a, bl, fx, out):
            d_pre = jnp.where(bl[0][...] > 0, a, 0.0)
            out[0][...] = d_pre.astype(BF16)

            @pl.when(i == 0)
            def _():
                out[1][...] = jnp.zeros_like(out[1])
            add_rows(out[1], d_pre)

        d_bf_1, g_b1 = edge_call(
            'owner_2', (meta_r, tile_linear(slot_s), seg_r), 2, halo, n, win_r, [(halo, hidden)], rows_of(2, 0), [ret_2, own_2],
            [hidden_1], [], [((n, hidden), BF16, False), ((8, hidden), F32, True)], n, tile, epi_o2, 25, init=1)

        def contract(a, b):
            return jnp.einsum('nd,ne->de', a, b, preferred_element_type=F32)

        parts = [contract(features, d_bf_1), contract(mean_1, d_bf_1), jnp.sum(g_b1, axis=0),
                 contract(hidden_1, d_bf_2), contract(mean_2, d_bf_2), jnp.sum(g_b2, axis=0),
                 contract(hidden_2, d_bf_3)[:, :classes], contract(hidden_2, tb_3)[:, :classes],
                 jnp.sum(g_b3, axis=0)[:classes], jnp.sum(loss_parts).reshape(1)]
        sizes = [p.size for p in parts]
        whole = sum(sizes)
        share = -(-whole // (peers * LANES)) * LANES
        flat = jnp.concatenate([p.reshape(-1) for p in parts] + [jnp.zeros((share * peers - whole,), F32)])
        mine = jnp.sum(exchange(flat.reshape(peers, share)), axis=0)
        full = exchange(jnp.broadcast_to(mine, (peers, share))).reshape(-1)
        outs, at = [], 0
        for p, size in zip(parts, sizes):
            outs.append(full[at:at + size].reshape(p.shape))
            at += size
        return (outs[-1][0] / total,) + tuple(outs[:-1])

    sharded = P(GROUP_AXIS)
    whole = P()
    return jax.shard_map(device_step, mesh=mesh,
                         in_specs=(sharded,) * 7 + (whole,) * 9,
                         out_specs=(whole,) * 10, check_vma=False)
```

```python
import math

import jax
import jax.numpy as jnp
from jax import lax
from jax.experimental import pallas as pl
from jax.experimental.pallas import tpu as pltpu
from jax.sharding import PartitionSpec as P

GROUP_AXIS = 'gp'
LANES = 128
SPREAD = 40
BLOCK = 128
GROUP = 8
TAIL = 8
F32 = jnp.float32
BF16 = jnp.bfloat16
VMEM_LIMIT = 60 * 2 ** 20

SMEM_SPEC = pl.BlockSpec(memory_space=pltpu.SMEM)
HBM_SPEC = pl.BlockSpec(memory_space=pltpu.HBM)


def whole_spec(shape):
    return pl.BlockSpec(shape, lambda i: (0,) * len(shape))


def row_spec(rows, width):
    return pl.BlockSpec((rows, width), lambda i: (i, 0))


def params(limit=VMEM_LIMIT):
    return pltpu.CompilerParams(vmem_limit_bytes=limit, dimension_semantics=('arbitrary',))


def cost(micros):
    return pl.CostEstimate(flops=int(micros * 4e6), bytes_accessed=int(micros * 1e6), transcendentals=0)


def mm(a, b):
    return jnp.dot(a, b, preferred_element_type=F32)


def tile_linear(row):
    return ((row >> 3) << 4) | (row & 7)


def put_rows(tab, row0, x, nc):
    rows = x.shape[0]
    if nc == 1:
        tab[pl.ds(pl.multiple_of(row0, 8), rows), :] = x
    else:
        for g in range(rows // 8):
            for c in range(nc):
                at = pl.multiple_of((row0 + g * 8) * nc + c * 8, 8)
                tab[pl.ds(at, 8), :] = x[g * 8:g * 8 + 8, c * LANES:(c + 1) * LANES]


def fetch(src, stage, sem, parts):
    rows = src.shape[0] // parts
    copies = [pltpu.make_async_copy(src.at[pl.ds(k * rows, rows)], stage.at[pl.ds(k * rows, rows)], sem.at[k])
              for k in range(parts)]
    for c in copies:
        c.start()
    return copies


def unpack(copies, stage, tab, row0, nc):
    rows = stage.shape[0] // len(copies)
    step = next(d for d in (128, 96, 64, 32, 16) if rows % d == 0)
    for p, c in enumerate(copies):
        c.wait()

        def body(k, carry):
            at = pl.multiple_of(p * rows + k * step, step)
            put_rows(tab, row0 + at, stage[pl.ds(at, step), :].astype(F32), nc)
            return carry
        lax.fori_loop(0, rows // step, body, 0)


def group_of(blocks):
    return next(u for u in (GROUP, 4, 2) if blocks % u == 0)


def zero_rows(acc):
    rows = acc.shape[0]
    step = next(s for s in (256, 128, 64, 32, 16, 8) if rows % s == 0)

    def body(k, carry):
        acc[pl.ds(pl.multiple_of(k * step, step), step), :] = jnp.zeros((step, acc.shape[1]), F32)
        return carry
    lax.fori_loop(0, rows // step, body, 0)


def gather_16(idx, first, tab, nc):
    sub = lax.broadcasted_iota(jnp.int32, (8, LANES), 0)
    halves = [[None, None] for _ in range(nc)]
    for h in range(2):
        for k in range(8):
            at = idx[first + h * 8 + k]
            for c in range(nc):
                row = jnp.broadcast_to(tab[pl.ds(at + 8 * c, 1), :], (8, LANES))
                halves[c][h] = row if k == 0 else jnp.where(sub == k, row, halves[c][h])
    return [jnp.concatenate(halves[c], axis=0).astype(BF16) for c in range(nc)]


def segment_sums(meta, meta_at, idx, seg, tab, acc, bufs, nc, window, blocks):
    unroll = group_of(blocks)
    first_trip, end_trip, most = [meta[meta_at + 2 * blocks + k] for k in range(3)]

    def fill(b, buf):
        for g in range(BLOCK // 16):
            parts = gather_16(idx, b * BLOCK + g * 16, tab, nc)
            for c in range(nc):
                buf[g * 16:g * 16 + 16, c * LANES:(c + 1) * LANES] = parts[c]

    def sums(b, at, buf):
        rows = lax.broadcasted_iota(jnp.int32, (window, BLOCK), 0) + at
        return mm(jnp.where(rows == seg[b], 1.0, 0.0).astype(BF16), buf[...])

    def add(at, x):
        acc[pl.ds(pl.multiple_of(at, 8), window), :] += x

    fill(jnp.minimum(first_trip * unroll, blocks - 1), bufs[0])

    def body(t, carry):
        before = None
        for u in range(unroll):
            b = t * unroll + u
            now = (meta[meta_at + b], sums(b, meta[meta_at + b], bufs[u % 2]))
            fill(jnp.minimum(b + 1, blocks - 1), bufs[(u + 1) % 2])
            if before is not None:
                add(*before)
            before = now
        add(*before)
        return carry
    lax.fori_loop(first_trip, end_trip, body, 0)

    @pl.when(most > 1)
    def _():
        def again(b, carry):
            count = meta[meta_at + blocks + b]

            @pl.when(count > 1)
            def _():
                fill(b, bufs[0])

                def more(w, c):
                    at = meta[meta_at + b] + w * window
                    add(at, sums(b, at, bufs[0]))
                    return c
                lax.fori_loop(1, count, more, 0)
            return carry
        lax.fori_loop(first_trip * unroll, end_trip * unroll, again, 0)


def spread_lanes():
    return lax.broadcasted_iota(jnp.int32, (1, LANES), 1)


def split3(x):
    hi = x.astype(BF16).astype(F32)
    rest = x - hi
    mid = rest.astype(BF16).astype(F32)
    low = rest - mid
    lane = spread_lanes()
    out = jnp.where(lane < SPREAD, hi, jnp.where(lane < 2 * SPREAD, mid, low))
    return jnp.where(lane < 3 * SPREAD, out, 0.0).astype(BF16)


def pieces3(a):
    hi = a.astype(BF16)
    rest = a - hi.astype(F32)
    mid = rest.astype(BF16)
    low = (rest - mid.astype(F32)).astype(BF16)
    return jnp.concatenate([hi, mid, low], axis=1)


def fold3(a, folder):
    return mm(pieces3(a), folder)


def add_rows(ref, x):
    ref[...] += jnp.sum(x.reshape(x.shape[0] // 8, 8, x.shape[1]), axis=0)


def pick_rows(name, src, idx, peers, slots, mask):
    n = src.shape[0]
    per = math.gcd(peers, 32)
    extra = 0 if mask is None else TAIL
    parts = math.gcd(n // 128, 4)

    def kern(idx_ref, src_ref, *refs):
        if extra:
            mask_ref, out, tab, stage, sem, tail = refs
        else:
            out, tab, stage, sem = refs

        @pl.when(pl.program_id(0) == 0)
        def _():
            copies = fetch(src_ref, stage, sem, parts)
            if extra:
                total = jnp.sum(mask_ref[...], axis=(0, 1), keepdims=True)
                high = jnp.floor(total * (1.0 / LANES))
                first = lax.broadcasted_iota(jnp.int32, (TAIL, LANES), 0) == 0
                lane = lax.broadcasted_iota(jnp.int32, (TAIL, LANES), 1)
                digits = jnp.where(lane == 0, high, jnp.where(lane == 1, total - high * LANES, 0.0))
                tail[...] = jnp.where(first, digits, 0.0).astype(BF16)
            unpack(copies, stage, tab, 0, 1)
        first = pl.program_id(0) * (per * slots)

        def body(p, carry):
            for g in range(slots // 16):
                out[p, g * 16:g * 16 + 16, :] = gather_16(idx_ref, first + p * slots + g * 16, tab, 1)[0]
            if extra:
                out[p, slots:slots + extra, :] = tail[...]
            return carry
        lax.fori_loop(0, per, body, 0)

    operands = [idx, src] + ([mask] if extra else [])
    specs = [SMEM_SPEC, HBM_SPEC] + ([whole_spec(mask.shape)] if extra else [])
    return pl.pallas_call(
        kern, name=name, grid=(peers // per,),
        out_shape=jax.ShapeDtypeStruct((peers, slots + extra, LANES), BF16),
        in_specs=specs,
        out_specs=pl.BlockSpec((per, slots + extra, LANES), lambda i: (i, 0, 0)),
        scratch_shapes=([pltpu.VMEM((n, LANES), F32), pltpu.VMEM((n, LANES), BF16), pltpu.SemaphoreType.DMA((parts,))]
                        + ([pltpu.VMEM((TAIL, LANES), BF16)] if extra else [])),
        compiler_params=params(), cost_estimate=cost(10))(*operands)


def edge_call(name, edges, nc, table_rows, acc_rows, window, sources, build, hbm_in, blocked, fixed, outs, rows_out,
              tile, epilogue, micros, init=None, sub=256, limit=VMEM_LIMIT):
    meta, meta_at, idx, seg = edges
    blocks = seg.shape[0]
    width = nc * LANES
    nh, nb, nf, no, ns = len(hbm_in), len(blocked), len(fixed), len(outs), len(sources)
    acc_total = -(-(acc_rows + window) // 256) * 256
    parts = 4
    sub = math.gcd(sub, tile)

    def kern(meta_ref, idx_ref, seg_ref, *refs):
        hb, refs = refs[:nh], refs[nh:]
        bl, refs = refs[:nb], refs[nb:]
        fx, refs = refs[:nf], refs[nf:]
        out, refs = refs[:no], refs[no:]
        tab, acc, buf_0, buf_1, isem = refs[:5]
        stages, sems = refs[5:5 + ns], refs[5 + ns:]
        i = pl.program_id(0)

        @pl.when(i == 0)
        def _():
            copies = [fetch(h, st, sm, parts) for h, st, sm in zip(hb, stages, sems)]
            if init is None:
                zero_rows(acc)
            else:
                start = pltpu.make_async_copy(hb[init], acc.at[pl.ds(0, acc_rows), :], isem)
                start.start()
            for o, (_, _, sums) in zip(out, outs):
                if sums:
                    o[...] = jnp.zeros_like(o)
            build(copies, stages, tab, fx)
            if init is not None:
                start.wait()
            segment_sums(meta_ref, meta_at, idx_ref, seg_ref, tab, acc, (buf_0, buf_1), nc, window, blocks)
        for j in range(tile // sub):
            at = j * sub
            epilogue(acc[pl.ds(pl.multiple_of(i * tile + at, sub), sub), :], [r.at[pl.ds(at, sub), :] for r in bl], fx,
                     [o if sums else o.at[pl.ds(at, sub), :] for o, (_, _, sums) in zip(out, outs)])

    out_shape, out_specs = [], []
    for shape, dtype, sums in outs:
        out_shape.append(jax.ShapeDtypeStruct(shape, dtype))
        out_specs.append(whole_spec(shape) if sums else row_spec(tile, shape[1]))
    return pl.pallas_call(
        kern, name=name, grid=(rows_out // tile,), out_shape=out_shape,
        in_specs=([SMEM_SPEC, SMEM_SPEC, whole_spec(seg.shape)] + [HBM_SPEC] * nh
                  + [row_spec(tile, x.shape[1]) for x in blocked] + [whole_spec(x.shape) for x in fixed]),
        out_specs=out_specs,
        scratch_shapes=([pltpu.VMEM((table_rows * nc, LANES), F32), pltpu.VMEM((acc_total, width), F32),
                         pltpu.VMEM((BLOCK, width), BF16), pltpu.VMEM((BLOCK, width), BF16),
                         pltpu.SemaphoreType.DMA(())]
                        + [pltpu.VMEM(shape, BF16) for shape in sources]
                        + [pltpu.SemaphoreType.DMA((parts,)) for _ in sources]),
        compiler_params=params(limit), cost_estimate=cost(micros))(meta, idx, seg, *hbm_in, *blocked, *fixed)


def edge_meta(seg_first, seg_last, window, first_block, end_block):
    blocks = seg_first.shape[0]
    unroll = group_of(blocks)
    at = jnp.arange(blocks, dtype=jnp.int32)
    base = seg_first & ~7
    count = jnp.where((at >= first_block) & (at < end_block), (seg_last - base) // window + 1, 1)
    tail = jnp.stack([first_block // unroll, (end_block + unroll - 1) // unroll, jnp.max(count)])
    return [base, count, tail]


def join_meta(*metas):
    offsets, at = [], 0
    for m in metas:
        offsets.append(at)
        at += sum(x.shape[0] for x in m)
    return jnp.concatenate([x for m in metas for x in m]).astype(jnp.int32), offsets


def bits_for(n):
    return max(1, (n - 1).bit_length())


def spread3(w):
    w = jnp.pad(w, ((0, 0), (0, SPREAD - w.shape[1])))
    return jnp.pad(jnp.concatenate([w, w, w], axis=1), ((0, 0), (0, LANES - 3 * SPREAD)))


def lanes_pad(w):
    return jnp.pad(w, ((0, 0), (0, LANES - w.shape[1])))


def solution(mesh):
    peers = mesh.shape[GROUP_AXIS]

    def exchange(x):
        return lax.all_to_all(x, GROUP_AXIS, 0, 0, tiled=True)

    def device_step(features, labels, train_mask, send_idx, src_idx, dst_idx, inv_deg,
                    w_self_1, w_neigh_1, bias_1, w_self_2, w_neigh_2, bias_2,
                    w_self_3, w_neigh_3, bias_3):
        n = features.shape[0]
        slots = send_idx.shape[1]
        halo = peers * slots
        edges = src_idx.shape[0]
        hidden = w_self_1.shape[1]
        classes = w_self_3.shape[1]
        send_flat = send_idx.reshape(-1)
        tile = min(1024, n)
        slot_bits = bits_for(halo)
        dst_bits = bits_for(n)
        table = n + halo

        blocks = edges // BLOCK
        halo_blocks = halo // BLOCK
        zero = jnp.int32(0)
        win_e, win_h, win_r = 176, 144, 240
        owned = jnp.sum((src_idx < n).astype(jnp.int32))
        near_end = (owned + BLOCK - 1) // BLOCK
        far_start = owned // BLOCK

        src_bits = bits_for(table)
        far_bit = dst_bits + src_bits
        by_dst = lax.sort(((src_idx >= n).astype(jnp.int32) << far_bit) | (dst_idx << src_bits) | src_idx, is_stable=False)
        src_f = by_dst & ((1 << src_bits) - 1)
        dst_f = (by_dst >> src_bits) & ((1 << dst_bits) - 1)
        is_far = src_f >= n
        src_near = jnp.minimum(src_f, n - 1)
        src_far = jnp.maximum(src_f - n, 0)
        seg_near = jnp.where(is_far, -1, dst_f).reshape(blocks, 1, BLOCK)
        seg_far = jnp.where(is_far, dst_f, -1).reshape(blocks, 1, BLOCK)
        first, last = dst_f[::BLOCK], dst_f[BLOCK - 1::BLOCK]
        meta_f, (near_at, far_at) = join_meta(
            edge_meta(first, jnp.where(is_far[BLOCK - 1::BLOCK], n - 1, last), win_e, zero, near_end),
            edge_meta(jnp.where(is_far[::BLOCK], first, 0), last, win_e, far_start, jnp.int32(blocks)))

        keys = jnp.concatenate([(src_idx << dst_bits) | dst_idx,
                                (1 << 30) | (send_flat << slot_bits) | jnp.arange(halo, dtype=jnp.int32)])
        ordered = lax.sort(keys, is_stable=False)
        by_src, by_row = ordered[:edges], ordered[edges:] & ((1 << 30) - 1)
        src_s = by_src >> dst_bits
        dst_s = by_src & ((1 << dst_bits) - 1)
        row_s = by_row >> slot_bits
        slot_s = by_row & ((1 << slot_bits) - 1)
        first, last = src_s[::BLOCK], src_s[BLOCK - 1::BLOCK]
        meta_b, (own_at, halo_at, owner_at) = join_meta(
            edge_meta(jnp.minimum(first, n - 1), jnp.minimum(last, n - 1), win_e, zero, near_end),
            edge_meta(jnp.maximum(first - n, 0), jnp.maximum(last - n, 0), win_h, far_start, jnp.int32(blocks)),
            edge_meta(row_s[::BLOCK], row_s[BLOCK - 1::BLOCK], win_r, zero, jnp.int32(halo_blocks)))
        seg_o = src_s.reshape(blocks, 1, BLOCK)
        seg_h = seg_o - n
        seg_r = row_s.reshape(halo_blocks, 1, BLOCK)
        dst_wide = tile_linear(dst_s)

        inv = jnp.broadcast_to(inv_deg[:, None], (n, LANES))
        b1 = bias_1.reshape(1, -1)
        b2 = bias_2.reshape(1, -1)
        lane = jnp.arange(LANES, dtype=jnp.int32)
        used = lane < 3 * SPREAD
        folder = jnp.tile(((lane[:, None] % SPREAD == lane[None, :] % SPREAD) & used[:, None] & used[None, :]).astype(BF16),
                          (3, 1))
        b3 = jnp.where(lane < 3 * SPREAD, spread3(bias_3.reshape(1, -1)), -1e30)
        if classes < SPREAD:
            b3 = jnp.where(lane % SPREAD < classes, b3, -1e30)
        target = jnp.where(lane[None, :] < 3 * SPREAD,
                           train_mask[:, None] * (1.0 + (labels[:, None] == lane[None, :] % SPREAD)), 0.0).astype(BF16)
        ws3, wn3 = spread3(w_self_3), spread3(w_neigh_3)
        ws3_t, wn3_t = lanes_pad(w_self_3).T, lanes_pad(w_neigh_3).T

        def rows_of(nc):
            def build(copies, stages, tab, fx):
                unpack(copies[0], stages[0], tab, 0, nc)
            return build

        def epi_plain(a, bl, fx, out):
            out[0][...] = a

        def near_sums(name, nc, idx, rows, also):
            return edge_call(name, (meta_f, near_at, idx, seg_near), nc, n, n, win_e, [rows.shape], rows_of(nc),
                             [rows] + also, [], [], [((n, nc * LANES), F32, False)], n, tile, epi_plain, 20, sub=tile)[0]

        out_1 = pick_rows('send_1', features, send_flat, peers, slots, train_mask.reshape(-1, LANES))
        got_1 = exchange(out_1)
        near_1 = near_sums('near_1', 1, src_near, features, [inv])
        counts = got_1[:, slots, :2].astype(F32)
        total = jnp.sum(counts[:, 0]) * LANES + jnp.sum(counts[:, 1])

        def build_1(copies, stages, tab, fx):
            per = peers // len(copies[0])
            some = math.gcd(per, 8)
            for p in range(len(copies[0])):
                copies[0][p].wait()

                def body(k, carry):
                    q = p * per + k * some
                    rows = stages[0][pl.ds(q, some), :slots, :].reshape(some * slots, LANES)
                    put_rows(tab, q * slots, rows.astype(F32), 1)
                    return carry
                lax.fori_loop(0, per // some, body, 0)

        def epi_1(a, bl, fx, out):
            mean = (a * bl[1][...]).astype(BF16)
            z = mm(bl[0][...], fx[0][...]) + mm(mean, fx[1][...]) + fx[2][...]
            out[0][...] = mean
            out[1][...] = jnp.maximum(z, 0.0).astype(BF16)

        mean_1, hidden_1 = edge_call(
            'layer_1', (meta_f, far_at, src_far, seg_far), 1, halo, n, win_e, [(peers, slots + TAIL, LANES)], build_1,
            [got_1, near_1], [features, inv], [w_self_1, w_neigh_1, b1],
            [((n, LANES), BF16, False), ((n, hidden), BF16, False)], n, tile, epi_1, 25, init=1)

        out_2 = pick_rows('send_2', mean_1, send_flat, peers, slots, None)
        got_2 = exchange(out_2)
        near_2 = near_sums('near_2', 2, tile_linear(src_near), hidden_1, [])

        def build_2(copies, stages, tab, fx):
            per = peers // len(copies[0])
            some = math.gcd(per, 8)
            for p in range(len(copies[0])):
                copies[0][p].wait()
                copies[1][p].wait()

                def body(k, carry):
                    q = p * per + k * some
                    f = stages[0][pl.ds(q, some), :slots, :].reshape(some * slots, LANES)
                    m = stages[1][pl.ds(q, some)].reshape(some * slots, LANES)
                    z = mm(f, fx[3][...]) + mm(m, fx[4][...]) + fx[5][...]
                    put_rows(tab, q * slots, jnp.maximum(z, 0.0).astype(BF16).astype(F32), 2)
                    return carry
                lax.fori_loop(0, per // some, body, 0)

        def epi_2(a, bl, fx, out):
            scale = bl[1][...]
            mean = (a * jnp.concatenate([scale, scale], axis=1)).astype(BF16)
            z = mm(bl[0][...], fx[0][...]) + mm(mean, fx[1][...]) + fx[2][...]
            h = jnp.maximum(z, 0.0).astype(BF16)
            out[0][...] = mean
            out[1][...] = h
            both = mm(h, fx[6][...])
            out[2][...] = split3(both[:, :LANES])
            out[3][...] = both[:, LANES:]

        mean_2, hidden_2, proj, logits_self = edge_call(
            'layer_2', (meta_f, far_at, tile_linear(src_far), seg_far), 2, halo, n, win_e,
            [(peers, slots + TAIL, LANES), (peers, slots, LANES)], build_2, [got_1, got_2, near_2],
            [hidden_1, inv], [w_self_2, w_neigh_2, b2, w_self_1, w_neigh_1, b1, jnp.concatenate([wn3, ws3], axis=1)],
            [((n, hidden), BF16, False), ((n, hidden), BF16, False), ((n, LANES), BF16, False),
             ((n, LANES), F32, False)], n, tile, epi_2, 40, init=2, sub=1024)

        out_3 = pick_rows('send_3', proj, send_flat, peers, slots, None)
        got_3 = exchange(out_3).reshape(halo, LANES)
        near_3 = near_sums('near_3', 1, src_near, proj, [target])
        inv_total = (1.0 / total).reshape(1, 1)

        def epi_3(a, bl, fx, out):
            scale = bl[1][...]
            z = bl[0][...] + fold3(a * scale, fx[2][...]) + fx[0][...]
            lane = spread_lanes()
            z = jnp.where(lane < 3 * SPREAD, z, -1e30)
            top = jnp.max(z, axis=1, keepdims=True)
            e = jnp.where(lane < SPREAD, jnp.exp(z - top), 0.0)
            lse = top + jnp.log(jnp.sum(e, axis=1, keepdims=True))
            t = bl[2][...].astype(F32)
            hit = t > 1.5
            d = jnp.where(t > 0.5, jnp.exp(z - lse) - jnp.where(hit, 1.0, 0.0), 0.0) * fx[1][...]
            db = d.astype(BF16)
            out[0][...] = db
            out[1][...] = split3(db.astype(F32) * scale)
            add_rows(out[2], d)
            add_rows(out[3], jnp.where(hit & (lane < SPREAD), lse - z, 0.0))

        d_bf_3, scaled_3, g_b3, loss_parts = edge_call(
            'layer_3', (meta_f, far_at, src_far, seg_far), 1, halo, n, win_e, [(halo, LANES)], rows_of(1), [got_3, near_3],
            [logits_self, inv, target], [b3, jnp.broadcast_to(inv_total, (1, LANES)), folder],
            [((n, LANES), BF16, False), ((n, LANES), BF16, False), ((8, LANES), F32, True), ((8, LANES), F32, True)],
            n, tile, epi_3, 30, init=1, sub=1024)

        def epi_b3h(a, bl, fx, out):
            out[0][...] = split3(fold3(a, fx[0][...]))

        tile_h = min(1024, halo)
        back_3 = edge_call('back_3_halo', (meta_b, halo_at, dst_s, seg_h), 1, n, halo, win_h, [(n, LANES)], rows_of(1),
                           [scaled_3], [], [folder], [((halo, LANES), BF16, False)], halo, tile_h, epi_b3h, 15, sub=1024)[0]
        ret_3 = exchange(back_3.reshape(peers, slots, LANES)).reshape(halo, LANES)
        own_3 = edge_call('back_3_own', (meta_b, own_at, dst_s, seg_o), 1, n, n, win_e, [(n, LANES)], rows_of(1),
                          [scaled_3], [], [], [((n, LANES), F32, False)], n, tile, epi_plain, 20, sub=tile)[0]

        def epi_o3(a, bl, fx, out):
            tb = fold3(a, fx[2][...]).astype(BF16)
            d_h = mm(jnp.concatenate([bl[0][...], tb], axis=1), fx[0][...])
            d_pre = jnp.where(bl[1][...].astype(F32) > 0, d_h, 0.0)
            db = d_pre.astype(BF16)
            scale = bl[2][...]
            out[0][...] = tb
            out[1][...] = db
            out[2][...] = (mm(db, fx[1][...]) * jnp.concatenate([scale, scale], axis=1)).astype(BF16)
            add_rows(out[3], d_pre)

        tb_3, d_bf_2, scaled_2, g_b2 = edge_call(
            'owner_3', (meta_b, owner_at, slot_s, seg_r), 1, halo, n, win_r, [(halo, LANES)], rows_of(1), [ret_3, own_3],
            [d_bf_3, hidden_2, inv], [jnp.concatenate([ws3_t, wn3_t], axis=0), w_neigh_2.T, folder],
            [((n, LANES), BF16, False), ((n, hidden), BF16, False), ((n, hidden), BF16, False), ((8, hidden), F32, True)],
            n, tile, epi_o3, 30, init=1, sub=512)

        def epi_b2h(a, bl, fx, out):
            out[0][...] = a.astype(BF16)

        def epi_b2o(a, bl, fx, out):
            out[0][...] = a + mm(bl[0][...], fx[0][...])

        back_2 = edge_call('back_2_halo', (meta_b, halo_at, dst_wide, seg_h), 2, n, halo, win_h, [(n, hidden)], rows_of(2),
                           [scaled_2], [], [], [((halo, hidden), BF16, False)], halo, tile_h, epi_b2h, 20)[0]
        ret_2 = exchange(back_2.reshape(peers, slots, hidden)).reshape(halo, hidden)
        own_2 = edge_call('back_2_own', (meta_b, own_at, dst_wide, seg_o), 2, n, n, win_e, [(n, hidden)], rows_of(2),
                          [scaled_2], [d_bf_2], [w_self_2.T], [((n, hidden), F32, False)], n, tile, epi_b2o, 30)[0]

        def epi_o2(a, bl, fx, out):
            d_pre = jnp.where(bl[0][...].astype(F32) > 0, a, 0.0)
            out[0][...] = d_pre.astype(BF16)
            add_rows(out[1], d_pre)

        d_bf_1, g_b1 = edge_call(
            'owner_2', (meta_b, owner_at, tile_linear(slot_s), seg_r), 2, halo, n, win_r, [(halo, hidden)], rows_of(2),
            [ret_2, own_2], [hidden_1], [], [((n, hidden), BF16, False), ((8, hidden), F32, True)], n, tile, epi_o2, 25,
            init=1)

        def contract(a, b):
            return jnp.einsum('nd,ne->de', a, b, preferred_element_type=F32)

        parts = [contract(features, d_bf_1), contract(mean_1, d_bf_1), jnp.sum(g_b1, axis=0),
                 contract(hidden_1, d_bf_2), contract(mean_2, d_bf_2), jnp.sum(g_b2, axis=0),
                 contract(hidden_2, d_bf_3)[:, :classes], contract(hidden_2, tb_3)[:, :classes],
                 jnp.sum(g_b3, axis=0)[:classes], jnp.sum(loss_parts).reshape(1)]
        sizes = [p.size for p in parts]
        whole = sum(sizes)
        share = -(-whole // (peers * LANES)) * LANES
        flat = jnp.concatenate([p.reshape(-1) for p in parts] + [jnp.zeros((share * peers - whole,), F32)])
        mine = jnp.sum(exchange(flat.reshape(peers, share)), axis=0)
        full = exchange(jnp.broadcast_to(mine, (peers, share))).reshape(-1)
        outs, at = [], 0
        for p, size in zip(parts, sizes):
            outs.append(full[at:at + size].reshape(p.shape))
            at += size
        return (outs[-1][0] / total,) + tuple(outs[:-1])

    sharded = P(GROUP_AXIS)
    whole = P()
    return jax.shard_map(device_step, mesh=mesh,
                         in_specs=(sharded,) * 7 + (whole,) * 9,
                         out_specs=(whole,) * 10, check_vma=False)
```

```python
import math

import jax
import jax.numpy as jnp
from jax import lax
from jax.experimental import pallas as pl
from jax.experimental.pallas import tpu as pltpu
from jax.sharding import PartitionSpec as P

GROUP_AXIS = 'gp'
LANES = 128
SPREAD = 40
BLOCK = 128
GROUP = 8
RING = 3
TAIL = 8
F32 = jnp.float32
BF16 = jnp.bfloat16
VMEM_LIMIT = 60 * 2 ** 20

SMEM_SPEC = pl.BlockSpec(memory_space=pltpu.SMEM)
HBM_SPEC = pl.BlockSpec(memory_space=pltpu.HBM)


def whole_spec(shape):
    return pl.BlockSpec(shape, lambda i: (0,) * len(shape))


def row_spec(rows, width):
    return pl.BlockSpec((rows, width), lambda i: (i, 0))


def params(limit=VMEM_LIMIT):
    return pltpu.CompilerParams(vmem_limit_bytes=limit, dimension_semantics=('arbitrary',))


def cost(micros):
    return pl.CostEstimate(flops=int(micros * 4e6), bytes_accessed=int(micros * 1e6), transcendentals=0)


def mm(a, b):
    return jnp.dot(a, b, preferred_element_type=F32)


def tile_linear(row):
    return ((row >> 3) << 4) | (row & 7)


def put_rows(tab, row0, x, nc):
    rows = x.shape[0]
    if nc == 1:
        tab[pl.ds(pl.multiple_of(row0, 8), rows), :] = x
    else:
        for g in range(rows // 8):
            for c in range(nc):
                at = pl.multiple_of((row0 + g * 8) * nc + c * 8, 8)
                tab[pl.ds(at, 8), :] = x[g * 8:g * 8 + 8, c * LANES:(c + 1) * LANES]


def fetch(src, stage, sem, parts):
    rows = src.shape[0] // parts
    copies = [pltpu.make_async_copy(src.at[pl.ds(k * rows, rows)], stage.at[pl.ds(k * rows, rows)], sem.at[k])
              for k in range(parts)]
    for c in copies:
        c.start()
    return copies


def unpack(copies, stage, tab, row0, nc):
    rows = stage.shape[0] // len(copies)
    step = next(d for d in (128, 96, 64, 32, 16) if rows % d == 0)
    for p, c in enumerate(copies):
        c.wait()

        def body(k, carry):
            at = pl.multiple_of(p * rows + k * step, step)
            put_rows(tab, row0 + at, stage[pl.ds(at, step), :].astype(F32), nc)
            return carry
        lax.fori_loop(0, rows // step, body, 0)


def group_of(blocks):
    return next(u for u in (GROUP, 4, 2) if blocks % u == 0)


def zero_rows(acc):
    rows = acc.shape[0]
    step = next(s for s in (256, 128, 64, 32, 16, 8) if rows % s == 0)

    def body(k, carry):
        acc[pl.ds(pl.multiple_of(k * step, step), step), :] = jnp.zeros((step, acc.shape[1]), F32)
        return carry
    lax.fori_loop(0, rows // step, body, 0)


def gather_16(idx, first, tab, nc):
    sub = lax.broadcasted_iota(jnp.int32, (8, LANES), 0)
    halves = [[None, None] for _ in range(nc)]
    for h in range(2):
        for k in range(8):
            at = idx[first + h * 8 + k]
            for c in range(nc):
                row = jnp.broadcast_to(tab[pl.ds(at + 8 * c, 1), :], (8, LANES))
                halves[c][h] = row if k == 0 else jnp.where(sub == k, row, halves[c][h])
    return [jnp.concatenate(halves[c], axis=0).astype(BF16) for c in range(nc)]


def index_copy(idx, ring, sem, t):
    span = ring.shape[0] // RING
    slot = lax.rem(t, RING)
    return pltpu.make_async_copy(idx.at[pl.ds(pl.multiple_of(t * span, span), span)],
                                 ring.at[pl.ds(pl.multiple_of(slot * span, span), span)], sem.at[slot])


def segment_sums(meta, meta_at, idx, ring, ring_sem, seg, tab, acc, bufs, nc, window, blocks):
    unroll = group_of(blocks)
    span = unroll * BLOCK
    first_trip, end_trip, most = [meta[meta_at + 2 * blocks + k] for k in range(3)]

    def fill(place, buf):
        for g in range(BLOCK // 16):
            parts = gather_16(ring, place + g * 16, tab, nc)
            for c in range(nc):
                buf[g * 16:g * 16 + 16, c * LANES:(c + 1) * LANES] = parts[c]

    def sums(b, at, buf):
        rows = lax.broadcasted_iota(jnp.int32, (window, BLOCK), 0) + at
        return mm(jnp.where(rows == seg[b], 1.0, 0.0).astype(BF16), buf[...])

    def add(at, x):
        acc[pl.ds(pl.multiple_of(at, 8), window), :] += x

    @pl.when(first_trip < end_trip)
    def _():
        index_copy(idx, ring, ring_sem, first_trip).wait()
        fill(lax.rem(first_trip, RING) * span, bufs[0])

    def body(t, carry):
        @pl.when(t + 1 < end_trip)
        def _():
            index_copy(idx, ring, ring_sem, t + 1).wait()

        @pl.when(t + 2 < end_trip)
        def _():
            index_copy(idx, ring, ring_sem, t + 2).start()
        here = lax.rem(t, RING) * span
        after = jnp.where(t + 1 < end_trip, lax.rem(t + 1, RING) * span, here)
        before = None
        for u in range(unroll):
            b = t * unroll + u
            now = (meta[meta_at + b], sums(b, meta[meta_at + b], bufs[u % 2]))
            fill(here + (u + 1) * BLOCK if u + 1 < unroll else after, bufs[(u + 1) % 2])
            if before is not None:
                add(*before)
            before = now
        add(*before)
        return carry
    lax.fori_loop(first_trip, end_trip, body, 0)

    @pl.when(most > 1)
    def _():
        def again(t, carry):
            copy = index_copy(idx, ring, ring_sem, t)
            copy.start()
            copy.wait()

            def one(u, c):
                b = t * unroll + u
                count = meta[meta_at + blocks + b]

                @pl.when(count > 1)
                def _():
                    fill(lax.rem(t, RING) * span + u * BLOCK, bufs[0])

                    def more(w, x):
                        at = meta[meta_at + b] + w * window
                        add(at, sums(b, at, bufs[0]))
                        return x
                    lax.fori_loop(1, count, more, 0)
                return c
            lax.fori_loop(0, unroll, one, 0)
            return carry
        lax.fori_loop(first_trip, end_trip, again, 0)


def first_indices(meta, meta_at, idx, ring, ring_sem, blocks):
    first_trip, end_trip = meta[meta_at + 2 * blocks], meta[meta_at + 2 * blocks + 1]
    for k in range(2):
        @pl.when(first_trip + k < end_trip)
        def _():
            index_copy(idx, ring, ring_sem, first_trip + k).start()


def spread_lanes():
    return lax.broadcasted_iota(jnp.int32, (1, LANES), 1)


def split3(x):
    hi = x.astype(BF16).astype(F32)
    rest = x - hi
    mid = rest.astype(BF16).astype(F32)
    low = rest - mid
    lane = spread_lanes()
    out = jnp.where(lane < SPREAD, hi, jnp.where(lane < 2 * SPREAD, mid, low))
    return jnp.where(lane < 3 * SPREAD, out, 0.0).astype(BF16)


def pieces3(a):
    hi = a.astype(BF16)
    rest = a - hi.astype(F32)
    mid = rest.astype(BF16)
    low = (rest - mid.astype(F32)).astype(BF16)
    return jnp.concatenate([hi, mid, low], axis=1)


def fold3(a, folder):
    return mm(pieces3(a), folder)


def add_rows(ref, x):
    ref[...] += jnp.sum(x.reshape(x.shape[0] // 8, 8, x.shape[1]), axis=0)


def pick_rows(name, src, idx, peers, slots, mask):
    n = src.shape[0]
    per = math.gcd(peers, 16)
    extra = 0 if mask is None else TAIL
    parts = math.gcd(n // 128, 4)

    def kern(idx_ref, src_ref, *refs):
        if extra:
            mask_ref, out, tab, stage, sem, tail = refs
        else:
            out, tab, stage, sem = refs

        @pl.when(pl.program_id(0) == 0)
        def _():
            copies = fetch(src_ref, stage, sem, parts)
            if extra:
                total = jnp.sum(mask_ref[...], axis=(0, 1), keepdims=True)
                high = jnp.floor(total * (1.0 / LANES))
                first = lax.broadcasted_iota(jnp.int32, (TAIL, LANES), 0) == 0
                lane = lax.broadcasted_iota(jnp.int32, (TAIL, LANES), 1)
                digits = jnp.where(lane == 0, high, jnp.where(lane == 1, total - high * LANES, 0.0))
                tail[...] = jnp.where(first, digits, 0.0).astype(BF16)
            unpack(copies, stage, tab, 0, 1)

        def body(p, carry):
            for g in range(slots // 16):
                out[p, g * 16:g * 16 + 16, :] = gather_16(idx_ref, p * slots + g * 16, tab, 1)[0]
            if extra:
                out[p, slots:slots + extra, :] = tail[...]
            return carry
        lax.fori_loop(0, per, body, 0)

    operands = [idx, src] + ([mask] if extra else [])
    specs = [pl.BlockSpec((per * slots,), lambda i: (i,), memory_space=pltpu.SMEM), HBM_SPEC] + ([whole_spec(mask.shape)] if extra else [])
    return pl.pallas_call(
        kern, name=name, grid=(peers // per,),
        out_shape=jax.ShapeDtypeStruct((peers, slots + extra, LANES), BF16),
        in_specs=specs,
        out_specs=pl.BlockSpec((per, slots + extra, LANES), lambda i: (i, 0, 0)),
        scratch_shapes=([pltpu.VMEM((n, LANES), F32), pltpu.VMEM((n, LANES), BF16), pltpu.SemaphoreType.DMA((parts,))]
                        + ([pltpu.VMEM((TAIL, LANES), BF16)] if extra else [])),
        compiler_params=params(), cost_estimate=cost(10))(*operands)


def edge_call(name, edges, nc, table_rows, acc_rows, window, sources, build, hbm_in, blocked, fixed, outs, rows_out,
              tile, epilogue, micros, init=None, sub=256, limit=VMEM_LIMIT):
    meta, meta_at, idx, seg = edges
    blocks = seg.shape[0]
    width = nc * LANES
    nh, nb, nf, no, ns = len(hbm_in), len(blocked), len(fixed), len(outs), len(sources)
    acc_total = -(-(acc_rows + window) // 256) * 256
    parts = 4
    sub = math.gcd(sub, tile)

    def kern(meta_ref, idx_ref, seg_ref, *refs):
        hb, refs = refs[:nh], refs[nh:]
        bl, refs = refs[:nb], refs[nb:]
        fx, refs = refs[:nf], refs[nf:]
        out, refs = refs[:no], refs[no:]
        tab, acc, buf_0, buf_1, isem, ring, ring_sem = refs[:7]
        stages, sems = refs[7:7 + ns], refs[7 + ns:]
        i = pl.program_id(0)

        @pl.when(i == 0)
        def _():
            copies = [fetch(h, st, sm, parts) for h, st, sm in zip(hb, stages, sems)]
            first_indices(meta_ref, meta_at, idx_ref, ring, ring_sem, blocks)
            if init is None:
                zero_rows(acc)
            else:
                start = pltpu.make_async_copy(hb[init], acc.at[pl.ds(0, acc_rows), :], isem)
                start.start()
            for o, (_, _, sums) in zip(out, outs):
                if sums:
                    o[...] = jnp.zeros_like(o)
            build(copies, stages, tab, fx)
            if init is not None:
                start.wait()
            segment_sums(meta_ref, meta_at, idx_ref, ring, ring_sem, seg_ref, tab, acc, (buf_0, buf_1), nc, window,
                         blocks)
        for j in range(tile // sub):
            at = j * sub
            epilogue(acc[pl.ds(pl.multiple_of(i * tile + at, sub), sub), :], [r.at[pl.ds(at, sub), :] for r in bl], fx,
                     [o if sums else o.at[pl.ds(at, sub), :] for o, (_, _, sums) in zip(out, outs)])

    out_shape, out_specs = [], []
    for shape, dtype, sums in outs:
        out_shape.append(jax.ShapeDtypeStruct(shape, dtype))
        out_specs.append(whole_spec(shape) if sums else row_spec(tile, shape[1]))
    return pl.pallas_call(
        kern, name=name, grid=(rows_out // tile,), out_shape=out_shape,
        in_specs=([SMEM_SPEC, HBM_SPEC, whole_spec(seg.shape)] + [HBM_SPEC] * nh
                  + [row_spec(tile, x.shape[1]) for x in blocked] + [whole_spec(x.shape) for x in fixed]),
        out_specs=out_specs,
        scratch_shapes=([pltpu.VMEM((table_rows * nc, LANES), F32), pltpu.VMEM((acc_total, width), F32),
                         pltpu.VMEM((BLOCK, width), BF16), pltpu.VMEM((BLOCK, width), BF16),
                         pltpu.SemaphoreType.DMA(()), pltpu.SMEM((RING * group_of(blocks) * BLOCK,), jnp.int32),
                         pltpu.SemaphoreType.DMA((RING,))]
                        + [pltpu.VMEM(shape, BF16) for shape in sources]
                        + [pltpu.SemaphoreType.DMA((parts,)) for _ in sources]),
        compiler_params=params(limit), cost_estimate=cost(micros))(meta, idx, seg, *hbm_in, *blocked, *fixed)


def edge_meta(seg_first, seg_last, window, first_block, end_block):
    blocks = seg_first.shape[0]
    unroll = group_of(blocks)
    at = jnp.arange(blocks, dtype=jnp.int32)
    base = seg_first & ~7
    count = jnp.where((at >= first_block) & (at < end_block), (seg_last - base) // window + 1, 1)
    tail = jnp.stack([first_block // unroll, (end_block + unroll - 1) // unroll, jnp.max(count)])
    return [base, count, tail]


def join_meta(*metas):
    offsets, at = [], 0
    for m in metas:
        offsets.append(at)
        at += sum(x.shape[0] for x in m)
    return jnp.concatenate([x for m in metas for x in m]).astype(jnp.int32), offsets


def bits_for(n):
    return max(1, (n - 1).bit_length())


def spread3(w):
    w = jnp.pad(w, ((0, 0), (0, SPREAD - w.shape[1])))
    return jnp.pad(jnp.concatenate([w, w, w], axis=1), ((0, 0), (0, LANES - 3 * SPREAD)))


def lanes_pad(w):
    return jnp.pad(w, ((0, 0), (0, LANES - w.shape[1])))


def solution(mesh):
    peers = mesh.shape[GROUP_AXIS]

    def exchange(x):
        return lax.all_to_all(x, GROUP_AXIS, 0, 0, tiled=True)

    def device_step(features, labels, train_mask, send_idx, src_idx, dst_idx, inv_deg,
                    w_self_1, w_neigh_1, bias_1, w_self_2, w_neigh_2, bias_2,
                    w_self_3, w_neigh_3, bias_3):
        n = features.shape[0]
        slots = send_idx.shape[1]
        halo = peers * slots
        edges = src_idx.shape[0]
        hidden = w_self_1.shape[1]
        classes = w_self_3.shape[1]
        send_flat = send_idx.reshape(-1)
        tile = min(1024, n)
        slot_bits = bits_for(halo)
        dst_bits = bits_for(n)
        table = n + halo

        blocks = edges // BLOCK
        halo_blocks = halo // BLOCK
        zero = jnp.int32(0)
        win_e, win_h, win_r = 176, 144, 240
        owned = jnp.sum((src_idx < n).astype(jnp.int32))
        near_end = (owned + BLOCK - 1) // BLOCK
        far_start = owned // BLOCK

        src_bits = bits_for(table)
        far_bit = dst_bits + src_bits
        by_dst = lax.sort(((src_idx >= n).astype(jnp.int32) << far_bit) | (dst_idx << src_bits) | src_idx, is_stable=False)
        src_f = by_dst & ((1 << src_bits) - 1)
        dst_f = (by_dst >> src_bits) & ((1 << dst_bits) - 1)
        is_far = src_f >= n
        src_near = jnp.minimum(src_f, n - 1)
        src_far = jnp.maximum(src_f - n, 0)
        seg_near = jnp.where(is_far, -1, dst_f).reshape(blocks, 1, BLOCK)
        seg_far = jnp.where(is_far, dst_f, -1).reshape(blocks, 1, BLOCK)
        first, last = dst_f[::BLOCK], dst_f[BLOCK - 1::BLOCK]
        meta_f, (near_at, far_at) = join_meta(
            edge_meta(first, jnp.where(is_far[BLOCK - 1::BLOCK], n - 1, last), win_e, zero, near_end),
            edge_meta(jnp.where(is_far[::BLOCK], first, 0), last, win_e, far_start, jnp.int32(blocks)))

        keys = jnp.concatenate([(src_idx << dst_bits) | dst_idx,
                                (1 << 30) | (send_flat << slot_bits) | jnp.arange(halo, dtype=jnp.int32)])
        ordered = lax.sort(keys, is_stable=False)
        by_src, by_row = ordered[:edges], ordered[edges:] & ((1 << 30) - 1)
        src_s = by_src >> dst_bits
        dst_s = by_src & ((1 << dst_bits) - 1)
        row_s = by_row >> slot_bits
        slot_s = by_row & ((1 << slot_bits) - 1)
        first, last = src_s[::BLOCK], src_s[BLOCK - 1::BLOCK]
        meta_b, (own_at, halo_at, owner_at) = join_meta(
            edge_meta(jnp.minimum(first, n - 1), jnp.minimum(last, n - 1), win_e, zero, near_end),
            edge_meta(jnp.maximum(first - n, 0), jnp.maximum(last - n, 0), win_h, far_start, jnp.int32(blocks)),
            edge_meta(row_s[::BLOCK], row_s[BLOCK - 1::BLOCK], win_r, zero, jnp.int32(halo_blocks)))
        seg_o = src_s.reshape(blocks, 1, BLOCK)
        seg_h = seg_o - n
        seg_r = row_s.reshape(halo_blocks, 1, BLOCK)
        dst_wide = tile_linear(dst_s)

        inv = jnp.broadcast_to(inv_deg[:, None], (n, LANES))
        b1 = bias_1.reshape(1, -1)
        b2 = bias_2.reshape(1, -1)
        lane = jnp.arange(LANES, dtype=jnp.int32)
        used = lane < 3 * SPREAD
        folder = jnp.tile(((lane[:, None] % SPREAD == lane[None, :] % SPREAD) & used[:, None] & used[None, :]).astype(BF16),
                          (3, 1))
        b3 = jnp.where(lane < 3 * SPREAD, spread3(bias_3.reshape(1, -1)), -1e30)
        if classes < SPREAD:
            b3 = jnp.where(lane % SPREAD < classes, b3, -1e30)
        target = jnp.where(lane[None, :] < 3 * SPREAD,
                           train_mask[:, None] * (1.0 + (labels[:, None] == lane[None, :] % SPREAD)), 0.0).astype(BF16)
        ws3, wn3 = spread3(w_self_3), spread3(w_neigh_3)
        ws3_t, wn3_t = lanes_pad(w_self_3).T, lanes_pad(w_neigh_3).T

        def rows_of(nc):
            def build(copies, stages, tab, fx):
                unpack(copies[0], stages[0], tab, 0, nc)
            return build

        def epi_plain(a, bl, fx, out):
            out[0][...] = a

        def near_sums(name, nc, idx, rows, also):
            return edge_call(name, (meta_f, near_at, idx, seg_near), nc, n, n, win_e, [rows.shape], rows_of(nc),
                             [rows] + also, [], [], [((n, nc * LANES), F32, False)], n, tile, epi_plain, 20, sub=tile)[0]

        out_1 = pick_rows('send_1', features, send_flat, peers, slots, train_mask.reshape(-1, LANES))
        got_1 = exchange(out_1)
        near_1 = near_sums('near_1', 1, src_near, features, [inv])
        counts = got_1[:, slots, :2].astype(F32)
        total = jnp.sum(counts[:, 0]) * LANES + jnp.sum(counts[:, 1])

        def build_1(copies, stages, tab, fx):
            per = peers // len(copies[0])
            some = math.gcd(per, 8)
            for p in range(len(copies[0])):
                copies[0][p].wait()

                def body(k, carry):
                    q = p * per + k * some
                    rows = stages[0][pl.ds(q, some), :slots, :].reshape(some * slots, LANES)
                    put_rows(tab, q * slots, rows.astype(F32), 1)
                    return carry
                lax.fori_loop(0, per // some, body, 0)

        def epi_1(a, bl, fx, out):
            mean = (a * bl[1][...]).astype(BF16)
            z = mm(bl[0][...], fx[0][...]) + mm(mean, fx[1][...]) + fx[2][...]
            out[0][...] = mean
            out[1][...] = jnp.maximum(z, 0.0).astype(BF16)

        mean_1, hidden_1 = edge_call(
            'layer_1', (meta_f, far_at, src_far, seg_far), 1, halo, n, win_e, [(peers, slots + TAIL, LANES)], build_1,
            [got_1, near_1], [features, inv], [w_self_1, w_neigh_1, b1],
            [((n, LANES), BF16, False), ((n, hidden), BF16, False)], n, tile, epi_1, 25, init=1)

        out_2 = pick_rows('send_2', mean_1, send_flat, peers, slots, None)
        got_2 = exchange(out_2)
        near_2 = near_sums('near_2', 2, tile_linear(src_near), hidden_1, [])

        def build_2(copies, stages, tab, fx):
            per = peers // len(copies[0])
            some = math.gcd(per, 8)
            for p in range(len(copies[0])):
                copies[0][p].wait()
                copies[1][p].wait()

                def body(k, carry):
                    q = p * per + k * some
                    f = stages[0][pl.ds(q, some), :slots, :].reshape(some * slots, LANES)
                    m = stages[1][pl.ds(q, some)].reshape(some * slots, LANES)
                    z = mm(f, fx[3][...]) + mm(m, fx[4][...]) + fx[5][...]
                    put_rows(tab, q * slots, jnp.maximum(z, 0.0).astype(BF16).astype(F32), 2)
                    return carry
                lax.fori_loop(0, per // some, body, 0)

        def epi_2(a, bl, fx, out):
            scale = bl[1][...]
            mean = (a * jnp.concatenate([scale, scale], axis=1)).astype(BF16)
            z = mm(bl[0][...], fx[0][...]) + mm(mean, fx[1][...]) + fx[2][...]
            h = jnp.maximum(z, 0.0).astype(BF16)
            out[0][...] = mean
            out[1][...] = h
            both = mm(h, fx[6][...])
            out[2][...] = split3(both[:, :LANES])
            out[3][...] = both[:, LANES:]

        mean_2, hidden_2, proj, logits_self = edge_call(
            'layer_2', (meta_f, far_at, tile_linear(src_far), seg_far), 2, halo, n, win_e,
            [(peers, slots + TAIL, LANES), (peers, slots, LANES)], build_2, [got_1, got_2, near_2],
            [hidden_1, inv], [w_self_2, w_neigh_2, b2, w_self_1, w_neigh_1, b1, jnp.concatenate([wn3, ws3], axis=1)],
            [((n, hidden), BF16, False), ((n, hidden), BF16, False), ((n, LANES), BF16, False),
             ((n, LANES), F32, False)], n, tile, epi_2, 40, init=2, sub=1024)

        out_3 = pick_rows('send_3', proj, send_flat, peers, slots, None)
        got_3 = exchange(out_3).reshape(halo, LANES)
        near_3 = near_sums('near_3', 1, src_near, proj, [target])
        inv_total = (1.0 / total).reshape(1, 1)

        def epi_3(a, bl, fx, out):
            scale = bl[1][...]
            z = bl[0][...] + fold3(a * scale, fx[2][...]) + fx[0][...]
            lane = spread_lanes()
            z = jnp.where(lane < 3 * SPREAD, z, -1e30)
            top = jnp.max(z, axis=1, keepdims=True)
            e = jnp.where(lane < SPREAD, jnp.exp(z - top), 0.0)
            lse = top + jnp.log(jnp.sum(e, axis=1, keepdims=True))
            t = bl[2][...].astype(F32)
            hit = t > 1.5
            d = jnp.where(t > 0.5, jnp.exp(z - lse) - jnp.where(hit, 1.0, 0.0), 0.0) * fx[1][...]
            db = d.astype(BF16)
            out[0][...] = db
            out[1][...] = split3(db.astype(F32) * scale)
            add_rows(out[2], d)
            add_rows(out[3], jnp.where(hit & (lane < SPREAD), lse - z, 0.0))

        d_bf_3, scaled_3, g_b3, loss_parts = edge_call(
            'layer_3', (meta_f, far_at, src_far, seg_far), 1, halo, n, win_e, [(halo, LANES)], rows_of(1), [got_3, near_3],
            [logits_self, inv, target], [b3, jnp.broadcast_to(inv_total, (1, LANES)), folder],
            [((n, LANES), BF16, False), ((n, LANES), BF16, False), ((8, LANES), F32, True), ((8, LANES), F32, True)],
            n, tile, epi_3, 30, init=1, sub=1024)

        def epi_b3h(a, bl, fx, out):
            out[0][...] = split3(fold3(a, fx[0][...]))

        tile_h = min(1024, halo)
        back_3 = edge_call('back_3_halo', (meta_b, halo_at, dst_s, seg_h), 1, n, halo, win_h, [(n, LANES)], rows_of(1),
                           [scaled_3], [], [folder], [((halo, LANES), BF16, False)], halo, tile_h, epi_b3h, 15, sub=1024)[0]
        ret_3 = exchange(back_3.reshape(peers, slots, LANES)).reshape(halo, LANES)
        own_3 = edge_call('back_3_own', (meta_b, own_at, dst_s, seg_o), 1, n, n, win_e, [(n, LANES)], rows_of(1),
                          [scaled_3], [], [], [((n, LANES), F32, False)], n, tile, epi_plain, 20, sub=tile)[0]

        def epi_o3(a, bl, fx, out):
            tb = fold3(a, fx[2][...]).astype(BF16)
            d_h = mm(jnp.concatenate([bl[0][...], tb], axis=1), fx[0][...])
            d_pre = jnp.where(bl[1][...].astype(F32) > 0, d_h, 0.0)
            db = d_pre.astype(BF16)
            scale = bl[2][...]
            out[0][...] = tb
            out[1][...] = db
            out[2][...] = (mm(db, fx[1][...]) * jnp.concatenate([scale, scale], axis=1)).astype(BF16)
            add_rows(out[3], d_pre)

        tb_3, d_bf_2, scaled_2, g_b2 = edge_call(
            'owner_3', (meta_b, owner_at, slot_s, seg_r), 1, halo, n, win_r, [(halo, LANES)], rows_of(1), [ret_3, own_3],
            [d_bf_3, hidden_2, inv], [jnp.concatenate([ws3_t, wn3_t], axis=0), w_neigh_2.T, folder],
            [((n, LANES), BF16, False), ((n, hidden), BF16, False), ((n, hidden), BF16, False), ((8, hidden), F32, True)],
            n, tile, epi_o3, 30, init=1, sub=512)

        def epi_b2h(a, bl, fx, out):
            out[0][...] = a.astype(BF16)

        def epi_b2o(a, bl, fx, out):
            out[0][...] = a + mm(bl[0][...], fx[0][...])

        back_2 = edge_call('back_2_halo', (meta_b, halo_at, dst_wide, seg_h), 2, n, halo, win_h, [(n, hidden)], rows_of(2),
                           [scaled_2], [], [], [((halo, hidden), BF16, False)], halo, tile_h, epi_b2h, 20)[0]
        ret_2 = exchange(back_2.reshape(peers, slots, hidden)).reshape(halo, hidden)
        own_2 = edge_call('back_2_own', (meta_b, own_at, dst_wide, seg_o), 2, n, n, win_e, [(n, hidden)], rows_of(2),
                          [scaled_2], [d_bf_2], [w_self_2.T], [((n, hidden), F32, False)], n, tile, epi_b2o, 30)[0]

        def epi_o2(a, bl, fx, out):
            d_pre = jnp.where(bl[0][...].astype(F32) > 0, a, 0.0)
            out[0][...] = d_pre.astype(BF16)
            add_rows(out[1], d_pre)

        d_bf_1, g_b1 = edge_call(
            'owner_2', (meta_b, owner_at, tile_linear(slot_s), seg_r), 2, halo, n, win_r, [(halo, hidden)], rows_of(2),
            [ret_2, own_2], [hidden_1], [], [((n, hidden), BF16, False), ((8, hidden), F32, True)], n, tile, epi_o2, 25,
            init=1)

        def contract(a, b):
            return jnp.einsum('nd,ne->de', a, b, preferred_element_type=F32)

        parts = [contract(features, d_bf_1), contract(mean_1, d_bf_1), jnp.sum(g_b1, axis=0),
                 contract(hidden_1, d_bf_2), contract(mean_2, d_bf_2), jnp.sum(g_b2, axis=0),
                 contract(hidden_2, d_bf_3)[:, :classes], contract(hidden_2, tb_3)[:, :classes],
                 jnp.sum(g_b3, axis=0)[:classes], jnp.sum(loss_parts).reshape(1)]
        sizes = [p.size for p in parts]
        whole = sum(sizes)
        share = -(-whole // (peers * LANES)) * LANES
        flat = jnp.concatenate([p.reshape(-1) for p in parts] + [jnp.zeros((share * peers - whole,), F32)])
        mine = jnp.sum(exchange(flat.reshape(peers, share)), axis=0)
        full = exchange(jnp.broadcast_to(mine, (peers, share))).reshape(-1)
        outs, at = [], 0
        for p, size in zip(parts, sizes):
            outs.append(full[at:at + size].reshape(p.shape))
            at += size
        return (outs[-1][0] / total,) + tuple(outs[:-1])

    sharded = P(GROUP_AXIS)
    whole = P()
    return jax.shard_map(device_step, mesh=mesh,
                         in_specs=(sharded,) * 7 + (whole,) * 9,
                         out_specs=(whole,) * 10, check_vma=False)
```

```python
import math

import jax
import jax.numpy as jnp
from jax import lax
from jax.experimental import pallas as pl
from jax.experimental.pallas import tpu as pltpu
from jax.sharding import PartitionSpec as P

GROUP_AXIS = 'gp'
LANES = 128
SPREAD = 40
BLOCK = 128
GROUP = 8
TAIL = 8
F32 = jnp.float32
BF16 = jnp.bfloat16
VMEM_LIMIT = 60 * 2 ** 20

SMEM_SPEC = pl.BlockSpec(memory_space=pltpu.SMEM)
HBM_SPEC = pl.BlockSpec(memory_space=pltpu.HBM)


def whole_spec(shape):
    return pl.BlockSpec(shape, lambda i: (0,) * len(shape))


def row_spec(rows, width):
    return pl.BlockSpec((rows, width), lambda i: (i, 0))


def params():
    return pltpu.CompilerParams(vmem_limit_bytes=VMEM_LIMIT, dimension_semantics=('arbitrary',))


def cost(micros):
    return pl.CostEstimate(flops=int(micros * 4e6), bytes_accessed=int(micros * 1e6), transcendentals=0)


def mm(a, b):
    return jnp.dot(a, b, preferred_element_type=F32)


def tile_linear(row):
    return ((row >> 3) << 4) | (row & 7)


def put_rows(tab, row0, x, nc):
    rows = x.shape[0]
    if nc == 1:
        tab[pl.ds(pl.multiple_of(row0, 8), rows), :] = x
    else:
        for g in range(rows // 8):
            for c in range(nc):
                at = pl.multiple_of((row0 + g * 8) * nc + c * 8, 8)
                tab[pl.ds(at, 8), :] = x[g * 8:g * 8 + 8, c * LANES:(c + 1) * LANES]


def fetch(src, stage, sem, parts):
    rows = src.shape[0] // parts
    copies = [pltpu.make_async_copy(src.at[pl.ds(k * rows, rows)], stage.at[pl.ds(k * rows, rows)], sem.at[k])
              for k in range(parts)]
    for c in copies:
        c.start()
    return copies


def unpack(copies, stage, tab, row0, nc):
    rows = stage.shape[0] // len(copies)
    step = next(d for d in (128, 96, 64, 32, 16) if rows % d == 0)
    for p, c in enumerate(copies):
        c.wait()

        def body(k, carry):
            at = pl.multiple_of(p * rows + k * step, step)
            put_rows(tab, row0 + at, stage[pl.ds(at, step), :].astype(F32), nc)
            return carry
        lax.fori_loop(0, rows // step, body, 0)


def group_of(blocks):
    return next(u for u in (GROUP, 4, 2) if blocks % u == 0)


def zero_rows(acc):
    rows = acc.shape[0]
    step = next(s for s in (256, 128, 64, 32, 16, 8) if rows % s == 0)

    def body(k, carry):
        acc[pl.ds(pl.multiple_of(k * step, step), step), :] = jnp.zeros((step, acc.shape[1]), F32)
        return carry
    lax.fori_loop(0, rows // step, body, 0)


def gather_16(idx, first, tab, nc):
    sub = lax.broadcasted_iota(jnp.int32, (8, LANES), 0)
    halves = [[None, None] for _ in range(nc)]
    for h in range(2):
        for k in range(8):
            at = idx[first + h * 8 + k]
            for c in range(nc):
                row = jnp.broadcast_to(tab[pl.ds(at + 8 * c, 1), :], (8, LANES))
                halves[c][h] = row if k == 0 else jnp.where(sub == k, row, halves[c][h])
    return [jnp.concatenate(halves[c], axis=0).astype(BF16) for c in range(nc)]


def segment_sums(meta, meta_at, idx, seg, tab, acc, bufs, nc, window, blocks):
    unroll = group_of(blocks)
    first_trip, end_trip, most = [meta[meta_at + 2 * blocks + k] for k in range(3)]

    def fill(b, buf):
        for g in range(BLOCK // 16):
            parts = gather_16(idx, b * BLOCK + g * 16, tab, nc)
            for c in range(nc):
                buf[g * 16:g * 16 + 16, c * LANES:(c + 1) * LANES] = parts[c]

    def sums(b, at, buf):
        rows = lax.broadcasted_iota(jnp.int32, (window, BLOCK), 0) + at
        return mm(jnp.where(rows == seg[b], 1.0, 0.0).astype(BF16), buf[...])

    def add(at, x):
        acc[pl.ds(pl.multiple_of(at, 8), window), :] += x

    fill(jnp.minimum(first_trip * unroll, blocks - 1), bufs[0])

    def body(t, carry):
        before = None
        for u in range(unroll):
            b = t * unroll + u
            now = (meta[meta_at + b], sums(b, meta[meta_at + b], bufs[u % 2]))
            fill(jnp.minimum(b + 1, blocks - 1), bufs[(u + 1) % 2])
            if before is not None:
                add(*before)
            before = now
        add(*before)
        return carry
    lax.fori_loop(first_trip, end_trip, body, 0)

    @pl.when(most > 1)
    def _():
        def again(b, carry):
            count = meta[meta_at + blocks + b]

            @pl.when(count > 1)
            def _():
                fill(b, bufs[0])

                def more(w, c):
                    at = meta[meta_at + b] + w * window
                    add(at, sums(b, at, bufs[0]))
                    return c
                lax.fori_loop(1, count, more, 0)
            return carry
        lax.fori_loop(first_trip * unroll, end_trip * unroll, again, 0)


def spread_lanes():
    return lax.broadcasted_iota(jnp.int32, (1, LANES), 1)


def split3(x):
    hi = x.astype(BF16).astype(F32)
    rest = x - hi
    mid = rest.astype(BF16).astype(F32)
    low = rest - mid
    lane = spread_lanes()
    out = jnp.where(lane < SPREAD, hi, jnp.where(lane < 2 * SPREAD, mid, low))
    return jnp.where(lane < 3 * SPREAD, out, 0.0).astype(BF16)


def pieces3(a):
    hi = a.astype(BF16)
    rest = a - hi.astype(F32)
    mid = rest.astype(BF16)
    low = (rest - mid.astype(F32)).astype(BF16)
    return jnp.concatenate([hi, mid, low], axis=1)


def fold3(a, folder):
    return mm(pieces3(a), folder)


def add_rows(ref, x):
    ref[...] += jnp.sum(x.reshape(x.shape[0] // 8, 8, x.shape[1]), axis=0)


def pick_rows(name, src, idx, peers, slots, mask):
    n = src.shape[0]
    per = math.gcd(peers, 16)
    extra = 0 if mask is None else TAIL
    parts = math.gcd(n // 128, 4)

    def kern(idx_ref, src_ref, *refs):
        if extra:
            mask_ref, out, tab, stage, sem, tail = refs
        else:
            out, tab, stage, sem = refs

        @pl.when(pl.program_id(0) == 0)
        def _():
            copies = fetch(src_ref, stage, sem, parts)
            if extra:
                total = jnp.sum(mask_ref[...], axis=(0, 1), keepdims=True)
                high = jnp.floor(total * (1.0 / LANES))
                first = lax.broadcasted_iota(jnp.int32, (TAIL, LANES), 0) == 0
                lane = lax.broadcasted_iota(jnp.int32, (TAIL, LANES), 1)
                digits = jnp.where(lane == 0, high, jnp.where(lane == 1, total - high * LANES, 0.0))
                tail[...] = jnp.where(first, digits, 0.0).astype(BF16)
            unpack(copies, stage, tab, 0, 1)

        def body(p, carry):
            for g in range(slots // 16):
                out[p, g * 16:g * 16 + 16, :] = gather_16(idx_ref, p * slots + g * 16, tab, 1)[0]
            if extra:
                out[p, slots:slots + extra, :] = tail[...]
            return carry
        lax.fori_loop(0, per, body, 0)

    operands = [idx, src] + ([mask] if extra else [])
    specs = [pl.BlockSpec((per * slots,), lambda i: (i,), memory_space=pltpu.SMEM), HBM_SPEC] + ([whole_spec(mask.shape)] if extra else [])
    return pl.pallas_call(
        kern, name=name, grid=(peers // per,),
        out_shape=jax.ShapeDtypeStruct((peers, slots + extra, LANES), BF16),
        in_specs=specs,
        out_specs=pl.BlockSpec((per, slots + extra, LANES), lambda i: (i, 0, 0)),
        scratch_shapes=([pltpu.VMEM((n, LANES), F32), pltpu.VMEM((n, LANES), BF16), pltpu.SemaphoreType.DMA((parts,))]
                        + ([pltpu.VMEM((TAIL, LANES), BF16)] if extra else [])),
        compiler_params=params(), cost_estimate=cost(10))(*operands)


def edge_call(name, edges, nc, table_rows, acc_rows, window, sources, build, hbm_in, blocked, fixed, outs, rows_out,
              tile, epilogue, micros, init=None, sub=1024):
    meta, meta_at, idx, seg = edges
    blocks = seg.shape[0]
    width = nc * LANES
    nh, nb, nf, no, ns = len(hbm_in), len(blocked), len(fixed), len(outs), len(sources)
    acc_total = -(-(acc_rows + window) // 256) * 256
    parts = 4
    sub = math.gcd(sub, tile)

    def kern(meta_ref, idx_ref, seg_ref, *refs):
        hb, refs = refs[:nh], refs[nh:]
        bl, refs = refs[:nb], refs[nb:]
        fx, refs = refs[:nf], refs[nf:]
        out, refs = refs[:no], refs[no:]
        tab, acc, buf_0, buf_1, isem = refs[:5]
        stages, sems = refs[5:5 + ns], refs[5 + ns:]
        i = pl.program_id(0)

        @pl.when(i == 0)
        def _():
            copies = [fetch(h, st, sm, parts) for h, st, sm in zip(hb, stages, sems)]
            if init is None:
                zero_rows(acc)
            else:
                start = pltpu.make_async_copy(hb[init], acc.at[pl.ds(0, acc_rows), :], isem)
                start.start()
            for o, (_, _, sums) in zip(out, outs):
                if sums:
                    o[...] = jnp.zeros_like(o)
            build(copies, stages, tab, fx)
            if init is not None:
                start.wait()
            segment_sums(meta_ref, meta_at, idx_ref, seg_ref, tab, acc, (buf_0, buf_1), nc, window, blocks)
            if epilogue is None:
                done = pltpu.make_async_copy(acc.at[pl.ds(0, acc_rows), :], out[0], isem)
                done.start()
                done.wait()
        if epilogue is not None:
            def part(j, carry):
                at = pl.multiple_of(j * sub, sub)
                epilogue(acc[pl.ds(pl.multiple_of(i * tile + at, sub), sub), :], [r.at[pl.ds(at, sub), :] for r in bl], fx,
                         [o if sums else o.at[pl.ds(at, sub), :] for o, (_, _, sums) in zip(out, outs)])
                return carry
            lax.fori_loop(0, tile // sub, part, 0)

    out_shape, out_specs = [], []
    for shape, dtype, sums in outs:
        out_shape.append(jax.ShapeDtypeStruct(shape, dtype))
        out_specs.append(HBM_SPEC if epilogue is None else whole_spec(shape) if sums else row_spec(tile, shape[1]))
    return pl.pallas_call(
        kern, name=name, grid=(1 if epilogue is None else rows_out // tile,), out_shape=out_shape,
        in_specs=([SMEM_SPEC, SMEM_SPEC, whole_spec(seg.shape)] + [HBM_SPEC] * nh
                  + [row_spec(tile, x.shape[1]) for x in blocked] + [whole_spec(x.shape) for x in fixed]),
        out_specs=out_specs,
        scratch_shapes=([pltpu.VMEM((table_rows * nc, LANES), F32), pltpu.VMEM((acc_total, width), F32),
                         pltpu.VMEM((BLOCK, width), BF16), pltpu.VMEM((BLOCK, width), BF16),
                         pltpu.SemaphoreType.DMA(())]
                        + [pltpu.VMEM(shape, BF16) for shape in sources]
                        + [pltpu.SemaphoreType.DMA((parts,)) for _ in sources]),
        compiler_params=params(), cost_estimate=cost(micros))(meta, idx, seg, *hbm_in, *blocked, *fixed)


def edge_meta(seg_first, seg_last, window, first_block, end_block):
    blocks = seg_first.shape[0]
    unroll = group_of(blocks)
    at = jnp.arange(blocks, dtype=jnp.int32)
    base = seg_first & ~7
    count = jnp.where((at >= first_block) & (at < end_block), (seg_last - base) // window + 1, 1)
    tail = jnp.stack([first_block // unroll, (end_block + unroll - 1) // unroll, jnp.max(count)])
    return [base, count, tail]


def join_meta(*metas):
    offsets, at = [], 0
    for m in metas:
        offsets.append(at)
        at += sum(x.shape[0] for x in m)
    return jnp.concatenate([x for m in metas for x in m]).astype(jnp.int32), offsets


def bits_for(n):
    return max(1, (n - 1).bit_length())


def spread3(w):
    w = jnp.pad(w, ((0, 0), (0, SPREAD - w.shape[1])))
    return jnp.pad(jnp.concatenate([w, w, w], axis=1), ((0, 0), (0, LANES - 3 * SPREAD)))


def lanes_pad(w):
    return jnp.pad(w, ((0, 0), (0, LANES - w.shape[1])))


def solution(mesh):
    peers = mesh.shape[GROUP_AXIS]

    def exchange(x):
        return lax.all_to_all(x, GROUP_AXIS, 0, 0, tiled=True)

    def device_step(features, labels, train_mask, send_idx, src_idx, dst_idx, inv_deg,
                    w_self_1, w_neigh_1, bias_1, w_self_2, w_neigh_2, bias_2,
                    w_self_3, w_neigh_3, bias_3):
        n = features.shape[0]
        slots = send_idx.shape[1]
        halo = peers * slots
        edges = src_idx.shape[0]
        hidden = w_self_1.shape[1]
        classes = w_self_3.shape[1]
        send_flat = send_idx.reshape(-1)
        tile = next(t for t in (4096, 1024) if n % t == 0)
        slot_bits = bits_for(halo)
        dst_bits = bits_for(n)
        table = n + halo

        blocks = edges // BLOCK
        halo_blocks = halo // BLOCK
        zero = jnp.int32(0)
        win_e, win_h, win_r = 176, 192, 240
        owned = jnp.sum((src_idx < n).astype(jnp.int32))
        near_end = (owned + BLOCK - 1) // BLOCK
        far_start = owned // BLOCK

        src_bits = bits_for(table)
        far_bit = dst_bits + src_bits
        by_dst = lax.sort(((src_idx >= n).astype(jnp.int32) << far_bit) | (dst_idx << src_bits) | src_idx, is_stable=False)
        src_f = by_dst & ((1 << src_bits) - 1)
        dst_f = (by_dst >> src_bits) & ((1 << dst_bits) - 1)
        is_far = src_f >= n
        src_near = jnp.minimum(src_f, n - 1)
        src_far = jnp.maximum(src_f - n, 0)
        seg_near = jnp.where(is_far, -1, dst_f).reshape(blocks, 1, BLOCK)
        seg_far = jnp.where(is_far, dst_f, -1).reshape(blocks, 1, BLOCK)
        first, last = dst_f[::BLOCK], dst_f[BLOCK - 1::BLOCK]
        meta_f, (near_at, far_at) = join_meta(
            edge_meta(first, jnp.where(is_far[BLOCK - 1::BLOCK], n - 1, last), win_e, zero, near_end),
            edge_meta(jnp.where(is_far[::BLOCK], first, 0), last, win_e, far_start, jnp.int32(blocks)))

        keys = jnp.concatenate([(src_idx << dst_bits) | dst_idx,
                                (1 << 30) | (send_flat << slot_bits) | jnp.arange(halo, dtype=jnp.int32)])
        ordered = lax.sort(keys, is_stable=False)
        by_src, by_row = ordered[:edges], ordered[edges:] & ((1 << 30) - 1)
        src_s = by_src >> dst_bits
        dst_s = by_src & ((1 << dst_bits) - 1)
        row_s = by_row >> slot_bits
        slot_s = by_row & ((1 << slot_bits) - 1)
        first, last = src_s[::BLOCK], src_s[BLOCK - 1::BLOCK]
        meta_b, (own_at, halo_at, owner_at) = join_meta(
            edge_meta(jnp.minimum(first, n - 1), jnp.minimum(last, n - 1), win_e, zero, near_end),
            edge_meta(jnp.maximum(first - n, 0), jnp.maximum(last - n, 0), win_h, far_start, jnp.int32(blocks)),
            edge_meta(row_s[::BLOCK], row_s[BLOCK - 1::BLOCK], win_r, zero, jnp.int32(halo_blocks)))
        seg_o = src_s.reshape(blocks, 1, BLOCK)
        seg_h = seg_o - n
        seg_r = row_s.reshape(halo_blocks, 1, BLOCK)
        dst_wide = tile_linear(dst_s)

        inv = jnp.broadcast_to(inv_deg[:, None], (n, LANES))
        b1 = bias_1.reshape(1, -1)
        b2 = bias_2.reshape(1, -1)
        lane = jnp.arange(LANES, dtype=jnp.int32)
        used = lane < 3 * SPREAD
        folder = jnp.tile(((lane[:, None] % SPREAD == lane[None, :] % SPREAD) & used[:, None] & used[None, :]).astype(BF16),
                          (3, 1))
        b3 = jnp.where(lane < 3 * SPREAD, spread3(bias_3.reshape(1, -1)), -1e30)
        if classes < SPREAD:
            b3 = jnp.where(lane % SPREAD < classes, b3, -1e30)
        target = jnp.where(lane[None, :] < 3 * SPREAD,
                           train_mask[:, None] * (1.0 + (labels[:, None] == lane[None, :] % SPREAD)), 0.0).astype(BF16)
        ws3, wn3 = spread3(w_self_3), spread3(w_neigh_3)
        ws3_t, wn3_t = lanes_pad(w_self_3).T, lanes_pad(w_neigh_3).T

        def rows_of(nc):
            def build(copies, stages, tab, fx):
                unpack(copies[0], stages[0], tab, 0, nc)
            return build

        def near_sums(name, nc, idx, rows, also):
            return edge_call(name, (meta_f, near_at, idx, seg_near), nc, n, n, win_e, [rows.shape], rows_of(nc),
                             [rows] + also, [], [], [((n, nc * LANES), F32, False)], n, tile, None, 20)[0]

        out_1 = pick_rows('send_1', features, send_flat, peers, slots, train_mask.reshape(-1, LANES))
        got_1 = exchange(out_1)
        near_1 = near_sums('near_1', 1, src_near, features, [inv])
        counts = got_1[:, slots, :2].astype(F32)
        total = jnp.sum(counts[:, 0]) * LANES + jnp.sum(counts[:, 1])

        def build_1(copies, stages, tab, fx):
            per = peers // len(copies[0])
            some = math.gcd(per, 8)
            for p in range(len(copies[0])):
                copies[0][p].wait()

                def body(k, carry):
                    q = p * per + k * some
                    rows = stages[0][pl.ds(q, some), :slots, :].reshape(some * slots, LANES)
                    put_rows(tab, q * slots, rows.astype(F32), 1)
                    return carry
                lax.fori_loop(0, per // some, body, 0)

        def epi_1(a, bl, fx, out):
            mean = (a * bl[1][...]).astype(BF16)
            z = mm(bl[0][...], fx[0][...]) + mm(mean, fx[1][...]) + fx[2][...]
            out[0][...] = mean
            out[1][...] = jnp.maximum(z, 0.0).astype(BF16)

        mean_1, hidden_1 = edge_call(
            'layer_1', (meta_f, far_at, src_far, seg_far), 1, halo, n, win_e, [(peers, slots + TAIL, LANES)], build_1,
            [got_1, near_1], [features, inv], [w_self_1, w_neigh_1, b1],
            [((n, LANES), BF16, False), ((n, hidden), BF16, False)], n, tile, epi_1, 25, init=1)

        out_2 = pick_rows('send_2', mean_1, send_flat, peers, slots, None)
        got_2 = exchange(out_2)
        near_2 = near_sums('near_2', 2, tile_linear(src_near), hidden_1, [])

        def build_2(copies, stages, tab, fx):
            per = peers // len(copies[0])
            some = math.gcd(per, 8)
            for p in range(len(copies[0])):
                copies[0][p].wait()
                copies[1][p].wait()

                def body(k, carry):
                    q = p * per + k * some
                    f = stages[0][pl.ds(q, some), :slots, :].reshape(some * slots, LANES)
                    m = stages[1][pl.ds(q, some)].reshape(some * slots, LANES)
                    z = mm(f, fx[3][...]) + mm(m, fx[4][...]) + fx[5][...]
                    put_rows(tab, q * slots, jnp.maximum(z, 0.0).astype(BF16).astype(F32), 2)
                    return carry
                lax.fori_loop(0, per // some, body, 0)

        def epi_2(a, bl, fx, out):
            scale = bl[1][...]
            mean = (a * jnp.concatenate([scale, scale], axis=1)).astype(BF16)
            z = mm(bl[0][...], fx[0][...]) + mm(mean, fx[1][...]) + fx[2][...]
            h = jnp.maximum(z, 0.0).astype(BF16)
            out[0][...] = mean
            out[1][...] = h
            both = mm(h, fx[6][...])
            out[2][...] = split3(both[:, :LANES])
            out[3][...] = both[:, LANES:]

        mean_2, hidden_2, proj, logits_self = edge_call(
            'layer_2', (meta_f, far_at, tile_linear(src_far), seg_far), 2, halo, n, win_e,
            [(peers, slots + TAIL, LANES), (peers, slots, LANES)], build_2, [got_1, got_2, near_2],
            [hidden_1, inv], [w_self_2, w_neigh_2, b2, w_self_1, w_neigh_1, b1, jnp.concatenate([wn3, ws3], axis=1)],
            [((n, hidden), BF16, False), ((n, hidden), BF16, False), ((n, LANES), BF16, False),
             ((n, LANES), F32, False)], n, tile, epi_2, 40, init=2)

        out_3 = pick_rows('send_3', proj, send_flat, peers, slots, None)
        got_3 = exchange(out_3).reshape(halo, LANES)
        near_3 = near_sums('near_3', 1, src_near, proj, [target])
        inv_total = (1.0 / total).reshape(1, 1)

        def epi_3(a, bl, fx, out):
            scale = bl[1][...]
            z = bl[0][...] + fold3(a * scale, fx[2][...]) + fx[0][...]
            lane = spread_lanes()
            z = jnp.where(lane < 3 * SPREAD, z, -1e30)
            top = jnp.max(z, axis=1, keepdims=True)
            e = jnp.where(lane < SPREAD, jnp.exp(z - top), 0.0)
            lse = top + jnp.log(jnp.sum(e, axis=1, keepdims=True))
            t = bl[2][...].astype(F32)
            hit = t > 1.5
            d = jnp.where(t > 0.5, jnp.exp(z - lse) - jnp.where(hit, 1.0, 0.0), 0.0) * fx[1][...]
            db = d.astype(BF16)
            out[0][...] = db
            out[1][...] = split3(db.astype(F32) * scale)
            add_rows(out[2], d)
            add_rows(out[3], jnp.where(hit & (lane < SPREAD), lse - z, 0.0))

        d_bf_3, scaled_3, g_b3, loss_parts = edge_call(
            'layer_3', (meta_f, far_at, src_far, seg_far), 1, halo, n, win_e, [(halo, LANES)], rows_of(1), [got_3, near_3],
            [logits_self, inv, target], [b3, jnp.broadcast_to(inv_total, (1, LANES)), folder],
            [((n, LANES), BF16, False), ((n, LANES), BF16, False), ((8, LANES), F32, True), ((8, LANES), F32, True)],
            n, tile, epi_3, 30, init=1)

        def epi_b3h(a, bl, fx, out):
            out[0][...] = split3(fold3(a, fx[0][...]))

        tile_h = next(t for t in (4096, 512) if halo % t == 0)
        back_3 = edge_call('back_3_halo', (meta_b, halo_at, dst_s, seg_h), 1, n, halo, win_h, [(n, LANES)], rows_of(1),
                           [scaled_3], [], [folder], [((halo, LANES), BF16, False)], halo, tile_h, epi_b3h, 15)[0]
        ret_3 = exchange(back_3.reshape(peers, slots, LANES)).reshape(halo, LANES)
        own_3 = edge_call('back_3_own', (meta_b, own_at, dst_s, seg_o), 1, n, n, win_e, [(n, LANES)], rows_of(1),
                          [scaled_3], [], [], [((n, LANES), F32, False)], n, tile, None, 20)[0]

        def epi_o3(a, bl, fx, out):
            tb = fold3(a, fx[2][...]).astype(BF16)
            d_h = mm(jnp.concatenate([bl[0][...], tb], axis=1), fx[0][...])
            d_pre = jnp.where(bl[1][...].astype(F32) > 0, d_h, 0.0)
            db = d_pre.astype(BF16)
            scale = bl[2][...]
            out[0][...] = tb
            out[1][...] = db
            out[2][...] = (mm(db, fx[1][...]) * jnp.concatenate([scale, scale], axis=1)).astype(BF16)
            add_rows(out[3], d_pre)

        tb_3, d_bf_2, scaled_2, g_b2 = edge_call(
            'owner_3', (meta_b, owner_at, slot_s, seg_r), 1, halo, n, win_r, [(halo, LANES)], rows_of(1), [ret_3, own_3],
            [d_bf_3, hidden_2, inv], [jnp.concatenate([ws3_t, wn3_t], axis=0), w_neigh_2.T, folder],
            [((n, LANES), BF16, False), ((n, hidden), BF16, False), ((n, hidden), BF16, False), ((8, hidden), F32, True)],
            n, tile, epi_o3, 30, init=1, sub=512)

        def epi_b2h(a, bl, fx, out):
            out[0][...] = a.astype(BF16)

        def epi_b2o(a, bl, fx, out):
            out[0][...] = a + mm(bl[0][...], fx[0][...])

        back_2 = edge_call('back_2_halo', (meta_b, halo_at, dst_wide, seg_h), 2, n, halo, win_h, [(n, hidden)], rows_of(2),
                           [scaled_2], [], [], [((halo, hidden), BF16, False)], halo, tile_h, epi_b2h, 20)[0]
        ret_2 = exchange(back_2.reshape(peers, slots, hidden)).reshape(halo, hidden)
        own_2 = edge_call('back_2_own', (meta_b, own_at, dst_wide, seg_o), 2, n, n, win_e, [(n, hidden)], rows_of(2),
                          [scaled_2], [d_bf_2], [w_self_2.T], [((n, hidden), F32, False)], n, tile, epi_b2o, 30)[0]

        def epi_o2(a, bl, fx, out):
            d_pre = jnp.where(bl[0][...].astype(F32) > 0, a, 0.0)
            out[0][...] = d_pre.astype(BF16)
            add_rows(out[1], d_pre)

        d_bf_1, g_b1 = edge_call(
            'owner_2', (meta_b, owner_at, tile_linear(slot_s), seg_r), 2, halo, n, win_r, [(halo, hidden)], rows_of(2),
            [ret_2, own_2], [hidden_1], [], [((n, hidden), BF16, False), ((8, hidden), F32, True)], n, tile, epi_o2, 25,
            init=1)

        def contract(a, b):
            return jnp.einsum('nd,ne->de', a, b, preferred_element_type=F32)

        parts = [contract(features, d_bf_1), contract(mean_1, d_bf_1), jnp.sum(g_b1, axis=0),
                 contract(hidden_1, d_bf_2), contract(mean_2, d_bf_2), jnp.sum(g_b2, axis=0),
                 contract(hidden_2, d_bf_3)[:, :classes], contract(hidden_2, tb_3)[:, :classes],
                 jnp.sum(g_b3, axis=0)[:classes], jnp.sum(loss_parts).reshape(1)]
        sizes = [p.size for p in parts]
        whole = sum(sizes)
        share = -(-whole // (peers * LANES)) * LANES
        flat = jnp.concatenate([p.reshape(-1) for p in parts] + [jnp.zeros((share * peers - whole,), F32)])
        mine = jnp.sum(exchange(flat.reshape(peers, share)), axis=0)
        full = exchange(jnp.broadcast_to(mine, (peers, share))).reshape(-1)
        outs, at = [], 0
        for p, size in zip(parts, sizes):
            outs.append(full[at:at + size].reshape(p.shape))
            at += size
        return (outs[-1][0] / total,) + tuple(outs[:-1])

    sharded = P(GROUP_AXIS)
    whole = P()
    return jax.shard_map(device_step, mesh=mesh,
                         in_specs=(sharded,) * 7 + (whole,) * 9,
                         out_specs=(whole,) * 10, check_vma=False)
```

```python
import math

import jax
import jax.numpy as jnp
from jax import lax
from jax.experimental import pallas as pl
from jax.experimental.pallas import tpu as pltpu
from jax.sharding import PartitionSpec as P

GROUP_AXIS = 'gp'
LANES = 128
SPREAD = 40
BLOCK = 128
GROUP = 8
TAIL = 8
F32 = jnp.float32
BF16 = jnp.bfloat16
VMEM_LIMIT = 60 * 2 ** 20

SMEM_SPEC = pl.BlockSpec(memory_space=pltpu.SMEM)
HBM_SPEC = pl.BlockSpec(memory_space=pltpu.HBM)


def whole_spec(shape):
    return pl.BlockSpec(shape, lambda i: (0,) * len(shape))


def row_spec(rows, width):
    return pl.BlockSpec((rows, width), lambda i: (i, 0))


def params():
    return pltpu.CompilerParams(vmem_limit_bytes=VMEM_LIMIT, dimension_semantics=('arbitrary',))


def cost(micros):
    return pl.CostEstimate(flops=int(micros * 4e6), bytes_accessed=int(micros * 1e6), transcendentals=0)


def mm(a, b):
    return jnp.dot(a, b, preferred_element_type=F32)


def tile_linear(row):
    return ((row >> 3) << 4) | (row & 7)


def put_rows(tab, row0, x, nc):
    rows = x.shape[0]
    if nc == 1:
        tab[pl.ds(pl.multiple_of(row0, 8), rows), :] = x
    else:
        for g in range(rows // 8):
            for c in range(nc):
                at = pl.multiple_of((row0 + g * 8) * nc + c * 8, 8)
                tab[pl.ds(at, 8), :] = x[g * 8:g * 8 + 8, c * LANES:(c + 1) * LANES]


def fetch(src, stage, sem, parts):
    rows = src.shape[0] // parts
    copies = [pltpu.make_async_copy(src.at[pl.ds(k * rows, rows)], stage.at[pl.ds(k * rows, rows)], sem.at[k])
              for k in range(parts)]
    for c in copies:
        c.start()
    return copies


def unpack(copies, stage, tab, row0, nc):
    rows = stage.shape[0] // len(copies)
    step = next(d for d in (128, 96, 64, 32, 16) if rows % d == 0)
    for p, c in enumerate(copies):
        c.wait()

        def body(k, carry):
            at = pl.multiple_of(p * rows + k * step, step)
            put_rows(tab, row0 + at, stage[pl.ds(at, step), :].astype(F32), nc)
            return carry
        lax.fori_loop(0, rows // step, body, 0)


def group_of(blocks):
    return next(u for u in (GROUP, 4, 2) if blocks % u == 0)


def zero_rows(acc):
    rows = acc.shape[0]
    step = next(s for s in (256, 128, 64, 32, 16, 8) if rows % s == 0)

    def body(k, carry):
        acc[pl.ds(pl.multiple_of(k * step, step), step), :] = jnp.zeros((step, acc.shape[1]), F32)
        return carry
    lax.fori_loop(0, rows // step, body, 0)


def gather_16(idx, first, tab, nc):
    sub = lax.broadcasted_iota(jnp.int32, (8, LANES), 0)
    halves = [[None, None] for _ in range(nc)]
    for h in range(2):
        for k in range(8):
            at = idx[first + h * 8 + k]
            for c in range(nc):
                row = jnp.broadcast_to(tab[pl.ds(at + 8 * c, 1), :], (8, LANES))
                halves[c][h] = row if k == 0 else jnp.where(sub == k, row, halves[c][h])
    return [jnp.concatenate(halves[c], axis=0).astype(BF16) for c in range(nc)]


def segment_sums(meta, meta_at, idx, seg, tab, acc, bufs, nc, window, blocks):
    unroll = group_of(blocks)
    first_trip, end_trip, most = [meta[meta_at + 2 * blocks + k] for k in range(3)]

    def fill(b, buf):
        for g in range(BLOCK // 16):
            parts = gather_16(idx, b * BLOCK + g * 16, tab, nc)
            for c in range(nc):
                buf[g * 16:g * 16 + 16, c * LANES:(c + 1) * LANES] = parts[c]

    def sums(b, at, buf):
        rows = lax.broadcasted_iota(jnp.int32, (window, BLOCK), 0) + at
        return mm(jnp.where(rows == seg[b], 1.0, 0.0).astype(BF16), buf[...])

    def add(at, x):
        acc[pl.ds(pl.multiple_of(at, 8), window), :] += x

    fill(jnp.minimum(first_trip * unroll, blocks - 1), bufs[0])

    def body(t, carry):
        before = None
        for u in range(unroll):
            b = t * unroll + u
            now = (meta[meta_at + b], sums(b, meta[meta_at + b], bufs[u % 2]))
            fill(jnp.minimum(b + 1, blocks - 1), bufs[(u + 1) % 2])
            if before is not None:
                add(*before)
            before = now
        add(*before)
        return carry
    lax.fori_loop(first_trip, end_trip, body, 0)

    @pl.when(most > 1)
    def _():
        def again(b, carry):
            count = meta[meta_at + blocks + b]

            @pl.when(count > 1)
            def _():
                fill(b, bufs[0])

                def more(w, c):
                    at = meta[meta_at + b] + w * window
                    add(at, sums(b, at, bufs[0]))
                    return c
                lax.fori_loop(1, count, more, 0)
            return carry
        lax.fori_loop(first_trip * unroll, end_trip * unroll, again, 0)


def spread_lanes():
    return lax.broadcasted_iota(jnp.int32, (1, LANES), 1)


def split3(x):
    hi = x.astype(BF16).astype(F32)
    rest = x - hi
    mid = rest.astype(BF16).astype(F32)
    low = rest - mid
    lane = spread_lanes()
    out = jnp.where(lane < SPREAD, hi, jnp.where(lane < 2 * SPREAD, mid, low))
    return jnp.where(lane < 3 * SPREAD, out, 0.0).astype(BF16)


def pieces3(a):
    hi = a.astype(BF16)
    rest = a - hi.astype(F32)
    mid = rest.astype(BF16)
    low = (rest - mid.astype(F32)).astype(BF16)
    return jnp.concatenate([hi, mid, low], axis=1)


def fold3(a, folder):
    return mm(pieces3(a), folder)


def add_rows(ref, x):
    ref[...] += jnp.sum(x.reshape(x.shape[0] // 8, 8, x.shape[1]), axis=0)


def pick_rows(name, src, idx, peers, slots, mask):
    n = src.shape[0]
    per = math.gcd(peers, 16)
    extra = 0 if mask is None else TAIL
    parts = math.gcd(n // 128, 4)

    def kern(idx_ref, src_ref, *refs):
        if extra:
            mask_ref, out, tab, stage, sem, tail = refs
        else:
            out, tab, stage, sem = refs

        @pl.when(pl.program_id(0) == 0)
        def _():
            copies = fetch(src_ref, stage, sem, parts)
            if extra:
                total = jnp.sum(mask_ref[...], axis=(0, 1), keepdims=True)
                high = jnp.floor(total * (1.0 / LANES))
                first = lax.broadcasted_iota(jnp.int32, (TAIL, LANES), 0) == 0
                lane = lax.broadcasted_iota(jnp.int32, (TAIL, LANES), 1)
                digits = jnp.where(lane == 0, high, jnp.where(lane == 1, total - high * LANES, 0.0))
                tail[...] = jnp.where(first, digits, 0.0).astype(BF16)
            unpack(copies, stage, tab, 0, 1)

        def body(p, carry):
            for g in range(slots // 16):
                out[p, g * 16:g * 16 + 16, :] = gather_16(idx_ref, p * slots + g * 16, tab, 1)[0]
            if extra:
                out[p, slots:slots + extra, :] = tail[...]
            return carry
        lax.fori_loop(0, per, body, 0)

    operands = [idx, src] + ([mask] if extra else [])
    specs = [pl.BlockSpec((per * slots,), lambda i: (i,), memory_space=pltpu.SMEM), HBM_SPEC] + ([whole_spec(mask.shape)] if extra else [])
    return pl.pallas_call(
        kern, name=name, grid=(peers // per,),
        out_shape=jax.ShapeDtypeStruct((peers, slots + extra, LANES), BF16),
        in_specs=specs,
        out_specs=pl.BlockSpec((per, slots + extra, LANES), lambda i: (i, 0, 0)),
        scratch_shapes=([pltpu.VMEM((n, LANES), F32), pltpu.VMEM((n, LANES), BF16), pltpu.SemaphoreType.DMA((parts,))]
                        + ([pltpu.VMEM((TAIL, LANES), BF16)] if extra else [])),
        compiler_params=params(), cost_estimate=cost(10))(*operands)


def edge_call(name, edges, nc, table_rows, acc_rows, window, sources, build, hbm_in, blocked, fixed, outs, rows_out,
              tile, epilogue, micros, init=None, sub=1024):
    meta, meta_at, idx, seg = edges
    blocks = seg.shape[0]
    width = nc * LANES
    nh, nb, nf, no, ns = len(hbm_in), len(blocked), len(fixed), len(outs), len(sources)
    acc_total = -(-(acc_rows + window) // 256) * 256
    parts = 4
    sub = math.gcd(sub, tile)

    def kern(meta_ref, idx_ref, seg_ref, *refs):
        hb, refs = refs[:nh], refs[nh:]
        bl, refs = refs[:nb], refs[nb:]
        fx, refs = refs[:nf], refs[nf:]
        out, refs = refs[:no], refs[no:]
        tab, acc, buf_0, buf_1, isem = refs[:5]
        stages, sems = refs[5:5 + ns], refs[5 + ns:]
        i = pl.program_id(0)

        @pl.when(i == 0)
        def _():
            copies = [fetch(h, st, sm, parts) for h, st, sm in zip(hb, stages, sems)]
            if init is None:
                zero_rows(acc)
            else:
                start = pltpu.make_async_copy(hb[init], acc.at[pl.ds(0, acc_rows), :], isem)
                start.start()
            for o, (_, _, sums) in zip(out, outs):
                if sums:
                    o[...] = jnp.zeros_like(o)
            build(copies, stages, tab, fx)
            if init is not None:
                start.wait()
            segment_sums(meta_ref, meta_at, idx_ref, seg_ref, tab, acc, (buf_0, buf_1), nc, window, blocks)
            if epilogue is None:
                done = pltpu.make_async_copy(acc.at[pl.ds(0, acc_rows), :], out[0], isem)
                done.start()
                done.wait()
        if epilogue is not None:
            def part(j, carry):
                at = pl.multiple_of(j * sub, sub)
                epilogue(acc[pl.ds(pl.multiple_of(i * tile + at, sub), sub), :], [r.at[pl.ds(at, sub), :] for r in bl], fx,
                         [o if sums else o.at[pl.ds(at, sub), :] for o, (_, _, sums) in zip(out, outs)])
                return carry
            lax.fori_loop(0, tile // sub, part, 0)

    out_shape, out_specs = [], []
    for shape, dtype, sums in outs:
        out_shape.append(jax.ShapeDtypeStruct(shape, dtype))
        out_specs.append(HBM_SPEC if epilogue is None else whole_spec(shape) if sums else row_spec(tile, shape[1]))
    return pl.pallas_call(
        kern, name=name, grid=(1 if epilogue is None else rows_out // tile,), out_shape=out_shape,
        in_specs=([SMEM_SPEC, SMEM_SPEC, whole_spec(seg.shape)] + [HBM_SPEC] * nh
                  + [row_spec(tile, x.shape[1]) for x in blocked] + [whole_spec(x.shape) for x in fixed]),
        out_specs=out_specs,
        scratch_shapes=([pltpu.VMEM((table_rows * nc, LANES), F32), pltpu.VMEM((acc_total, width), F32),
                         pltpu.VMEM((BLOCK, width), BF16), pltpu.VMEM((BLOCK, width), BF16),
                         pltpu.SemaphoreType.DMA(())]
                        + [pltpu.VMEM(shape, BF16) for shape in sources]
                        + [pltpu.SemaphoreType.DMA((parts,)) for _ in sources]),
        compiler_params=params(), cost_estimate=cost(micros))(meta, idx, seg, *hbm_in, *blocked, *fixed)


def sum_over_devices(x, peers):
    _, chips, rows, lanes = x.shape

    def device(chip, core):
        return chip * 2 + core

    def kern(x_ref, out_ref, half, mine, got, pair_sem, send_sem, recv_sem, send_2, recv_2):
        me = lax.axis_index(GROUP_AXIS)
        chip, core = me // 2, me % 2
        mate = device(chip, 1 - core)

        def pair(src, dst, k):
            return pltpu.make_async_remote_copy(src_ref=src, dst_ref=dst, send_sem=pair_sem.at[2 * k],
                                                recv_sem=pair_sem.at[2 * k + 1], device_id=(mate,),
                                                device_id_type=pl.DeviceIdType.MESH)
        first = pair(x_ref.at[1 - core], half, 0)
        first.start()
        first.wait()

        def add(c, carry):
            mine[c] = x_ref[core, c] + half[c]
            return carry
        lax.fori_loop(0, chips, add, 0)

        def share(k):
            to = (chip + k) % chips
            return pltpu.make_async_remote_copy(src_ref=mine.at[to], dst_ref=got.at[chip], send_sem=send_sem.at[k],
                                                recv_sem=recv_sem.at[chip], device_id=(device(to, core),),
                                                device_id_type=pl.DeviceIdType.MESH)

        def landed(k):
            frm = (chip + k) % chips
            return pltpu.make_async_remote_copy(src_ref=mine.at[frm], dst_ref=got.at[frm], send_sem=send_sem.at[k],
                                                recv_sem=recv_sem.at[frm], device_id=(me,),
                                                device_id_type=pl.DeviceIdType.MESH)

        def start(k, carry):
            share(k).start()
            return carry
        lax.fori_loop(1, chips, start, 0)
        got[chip] = mine[chip]

        def settle(k, carry):
            landed(k).wait_recv()
            return carry
        lax.fori_loop(1, chips, settle, 0)

        def more(c, total):
            return total + got[c]
        out_ref[core, chip] = lax.fori_loop(0, chips, more, jnp.zeros((rows, lanes), F32))

        def drain(k, carry):
            share(k).wait_send()
            return carry
        lax.fori_loop(1, chips, drain, 0)

        def give(k):
            return pltpu.make_async_remote_copy(src_ref=out_ref.at[core, chip], dst_ref=out_ref.at[core, chip],
                                                send_sem=send_2.at[k], recv_sem=recv_2.at[chip],
                                                device_id=(device((chip + k) % chips, core),),
                                                device_id_type=pl.DeviceIdType.MESH)

        def given(k):
            frm = (chip + k) % chips
            return pltpu.make_async_remote_copy(src_ref=out_ref.at[core, frm], dst_ref=out_ref.at[core, frm],
                                                send_sem=send_2.at[k], recv_sem=recv_2.at[frm], device_id=(me,),
                                                device_id_type=pl.DeviceIdType.MESH)

        def start_2(k, carry):
            give(k).start()
            return carry
        lax.fori_loop(1, chips, start_2, 0)

        def settle_2(k, carry):
            given(k).wait_recv()
            return carry
        lax.fori_loop(1, chips, settle_2, 0)

        def drain_2(k, carry):
            give(k).wait_send()
            return carry
        lax.fori_loop(1, chips, drain_2, 0)
        last = pair(out_ref.at[core], out_ref.at[core], 1)
        last.start()
        last.wait()

    return pl.pallas_call(
        kern, name='sum_all', out_shape=jax.ShapeDtypeStruct(x.shape, F32),
        in_specs=[pl.BlockSpec(memory_space=pltpu.VMEM)], out_specs=pl.BlockSpec(memory_space=pltpu.VMEM),
        scratch_shapes=[pltpu.VMEM((chips, rows, lanes), F32), pltpu.VMEM((chips, rows, lanes), F32),
                        pltpu.VMEM((chips, rows, lanes), F32), pltpu.SemaphoreType.DMA((4,)),
                        pltpu.SemaphoreType.DMA((chips,)), pltpu.SemaphoreType.DMA((chips,)),
                        pltpu.SemaphoreType.DMA((chips,)), pltpu.SemaphoreType.DMA((chips,))],
        compiler_params=pltpu.CompilerParams(has_side_effects=True), cost_estimate=cost(25))(x)


def edge_meta(seg_first, seg_last, window, first_block, end_block):
    blocks = seg_first.shape[0]
    unroll = group_of(blocks)
    at = jnp.arange(blocks, dtype=jnp.int32)
    base = seg_first & ~7
    count = jnp.where((at >= first_block) & (at < end_block), (seg_last - base) // window + 1, 1)
    tail = jnp.stack([first_block // unroll, (end_block + unroll - 1) // unroll, jnp.max(count)])
    return [base, count, tail]


def join_meta(*metas):
    offsets, at = [], 0
    for m in metas:
        offsets.append(at)
        at += sum(x.shape[0] for x in m)
    return jnp.concatenate([x for m in metas for x in m]).astype(jnp.int32), offsets


def bits_for(n):
    return max(1, (n - 1).bit_length())


def spread3(w):
    w = jnp.pad(w, ((0, 0), (0, SPREAD - w.shape[1])))
    return jnp.pad(jnp.concatenate([w, w, w], axis=1), ((0, 0), (0, LANES - 3 * SPREAD)))


def lanes_pad(w):
    return jnp.pad(w, ((0, 0), (0, LANES - w.shape[1])))


def solution(mesh):
    peers = mesh.shape[GROUP_AXIS]

    def exchange(x):
        return lax.all_to_all(x, GROUP_AXIS, 0, 0, tiled=True)

    def device_step(features, labels, train_mask, send_idx, src_idx, dst_idx, inv_deg,
                    w_self_1, w_neigh_1, bias_1, w_self_2, w_neigh_2, bias_2,
                    w_self_3, w_neigh_3, bias_3):
        n = features.shape[0]
        slots = send_idx.shape[1]
        halo = peers * slots
        edges = src_idx.shape[0]
        hidden = w_self_1.shape[1]
        classes = w_self_3.shape[1]
        send_flat = send_idx.reshape(-1)
        tile = next(t for t in (4096, 1024) if n % t == 0)
        slot_bits = bits_for(halo)
        dst_bits = bits_for(n)
        table = n + halo

        blocks = edges // BLOCK
        halo_blocks = halo // BLOCK
        zero = jnp.int32(0)
        win_e, win_h, win_r = 176, 192, 240
        owned = jnp.sum((src_idx < n).astype(jnp.int32))
        near_end = (owned + BLOCK - 1) // BLOCK
        far_start = owned // BLOCK

        src_bits = bits_for(table)
        far_bit = dst_bits + src_bits
        by_dst = lax.sort(((src_idx >= n).astype(jnp.int32) << far_bit) | (dst_idx << src_bits) | src_idx, is_stable=False)
        src_f = by_dst & ((1 << src_bits) - 1)
        dst_f = (by_dst >> src_bits) & ((1 << dst_bits) - 1)
        is_far = src_f >= n
        src_near = jnp.minimum(src_f, n - 1)
        src_far = jnp.maximum(src_f - n, 0)
        seg_near = jnp.where(is_far, -1, dst_f).reshape(blocks, 1, BLOCK)
        seg_far = jnp.where(is_far, dst_f, -1).reshape(blocks, 1, BLOCK)
        first, last = dst_f[::BLOCK], dst_f[BLOCK - 1::BLOCK]
        meta_f, (near_at, far_at) = join_meta(
            edge_meta(first, jnp.where(is_far[BLOCK - 1::BLOCK], n - 1, last), win_e, zero, near_end),
            edge_meta(jnp.where(is_far[::BLOCK], first, 0), last, win_e, far_start, jnp.int32(blocks)))

        inv = jnp.broadcast_to(inv_deg[:, None], (n, LANES))
        b1 = bias_1.reshape(1, -1)
        b2 = bias_2.reshape(1, -1)
        lane = jnp.arange(LANES, dtype=jnp.int32)
        used = lane < 3 * SPREAD
        folder = jnp.tile(((lane[:, None] % SPREAD == lane[None, :] % SPREAD) & used[:, None] & used[None, :]).astype(BF16),
                          (3, 1))
        b3 = jnp.where(lane < 3 * SPREAD, spread3(bias_3.reshape(1, -1)), -1e30)
        if classes < SPREAD:
            b3 = jnp.where(lane % SPREAD < classes, b3, -1e30)
        target = jnp.where(lane[None, :] < 3 * SPREAD,
                           train_mask[:, None] * (1.0 + (labels[:, None] == lane[None, :] % SPREAD)), 0.0).astype(BF16)
        ws3, wn3 = spread3(w_self_3), spread3(w_neigh_3)
        ws3_t, wn3_t = lanes_pad(w_self_3).T, lanes_pad(w_neigh_3).T

        def rows_of(nc):
            def build(copies, stages, tab, fx):
                unpack(copies[0], stages[0], tab, 0, nc)
            return build

        def near_sums(name, nc, idx, rows, also):
            return edge_call(name, (meta_f, near_at, idx, seg_near), nc, n, n, win_e, [rows.shape], rows_of(nc),
                             [rows] + also, [], [], [((n, nc * LANES), F32, False)], n, tile, None, 20)[0]

        out_1 = pick_rows('send_1', features, send_flat, peers, slots, train_mask.reshape(-1, LANES))
        got_1 = exchange(out_1)
        near_1 = near_sums('near_1', 1, src_near, features, [inv])
        counts = got_1[:, slots, :2].astype(F32)
        total = jnp.sum(counts[:, 0]) * LANES + jnp.sum(counts[:, 1])

        def build_1(copies, stages, tab, fx):
            per = peers // len(copies[0])
            some = math.gcd(per, 8)
            for p in range(len(copies[0])):
                copies[0][p].wait()

                def body(k, carry):
                    q = p * per + k * some
                    rows = stages[0][pl.ds(q, some), :slots, :].reshape(some * slots, LANES)
                    put_rows(tab, q * slots, rows.astype(F32), 1)
                    return carry
                lax.fori_loop(0, per // some, body, 0)

        def epi_1(a, bl, fx, out):
            mean = (a * bl[1][...]).astype(BF16)
            z = mm(bl[0][...], fx[0][...]) + mm(mean, fx[1][...]) + fx[2][...]
            out[0][...] = mean
            out[1][...] = jnp.maximum(z, 0.0).astype(BF16)

        mean_1, hidden_1 = edge_call(
            'layer_1', (meta_f, far_at, src_far, seg_far), 1, halo, n, win_e, [(peers, slots + TAIL, LANES)], build_1,
            [got_1, near_1], [features, inv], [w_self_1, w_neigh_1, b1],
            [((n, LANES), BF16, False), ((n, hidden), BF16, False)], n, tile, epi_1, 25, init=1)

        keys = jnp.concatenate([(src_idx << dst_bits) | dst_idx,
                                (1 << 30) | (send_flat << slot_bits) | jnp.arange(halo, dtype=jnp.int32)])
        keys = lax.optimization_barrier((keys, mean_1))[0]
        ordered = lax.sort(keys, is_stable=False)
        by_src, by_row = ordered[:edges], ordered[edges:] & ((1 << 30) - 1)
        src_s = by_src >> dst_bits
        dst_s = by_src & ((1 << dst_bits) - 1)
        row_s = by_row >> slot_bits
        slot_s = by_row & ((1 << slot_bits) - 1)
        first, last = src_s[::BLOCK], src_s[BLOCK - 1::BLOCK]
        meta_b, (own_at, halo_at, owner_at) = join_meta(
            edge_meta(jnp.minimum(first, n - 1), jnp.minimum(last, n - 1), win_e, zero, near_end),
            edge_meta(jnp.maximum(first - n, 0), jnp.maximum(last - n, 0), win_h, far_start, jnp.int32(blocks)),
            edge_meta(row_s[::BLOCK], row_s[BLOCK - 1::BLOCK], win_r, zero, jnp.int32(halo_blocks)))
        seg_o = src_s.reshape(blocks, 1, BLOCK)
        seg_h = seg_o - n
        seg_r = row_s.reshape(halo_blocks, 1, BLOCK)
        dst_wide = tile_linear(dst_s)

        out_2 = pick_rows('send_2', mean_1, send_flat, peers, slots, None)
        got_2 = exchange(out_2)
        near_2 = near_sums('near_2', 2, tile_linear(src_near), hidden_1, [])

        def build_2(copies, stages, tab, fx):
            per = peers // len(copies[0])
            some = math.gcd(per, 8)
            for p in range(len(copies[0])):
                copies[0][p].wait()
                copies[1][p].wait()

                def body(k, carry):
                    q = p * per + k * some
                    f = stages[0][pl.ds(q, some), :slots, :].reshape(some * slots, LANES)
                    m = stages[1][pl.ds(q, some)].reshape(some * slots, LANES)
                    z = mm(f, fx[3][...]) + mm(m, fx[4][...]) + fx[5][...]
                    put_rows(tab, q * slots, jnp.maximum(z, 0.0).astype(BF16).astype(F32), 2)
                    return carry
                lax.fori_loop(0, per // some, body, 0)

        def epi_2(a, bl, fx, out):
            scale = bl[1][...]
            mean = (a * jnp.concatenate([scale, scale], axis=1)).astype(BF16)
            z = mm(bl[0][...], fx[0][...]) + mm(mean, fx[1][...]) + fx[2][...]
            h = jnp.maximum(z, 0.0).astype(BF16)
            out[0][...] = mean
            out[1][...] = h
            both = mm(h, fx[6][...])
            out[2][...] = split3(both[:, :LANES])
            out[3][...] = both[:, LANES:]

        mean_2, hidden_2, proj, logits_self = edge_call(
            'layer_2', (meta_f, far_at, tile_linear(src_far), seg_far), 2, halo, n, win_e,
            [(peers, slots + TAIL, LANES), (peers, slots, LANES)], build_2, [got_1, got_2, near_2],
            [hidden_1, inv], [w_self_2, w_neigh_2, b2, w_self_1, w_neigh_1, b1, jnp.concatenate([wn3, ws3], axis=1)],
            [((n, hidden), BF16, False), ((n, hidden), BF16, False), ((n, LANES), BF16, False),
             ((n, LANES), F32, False)], n, tile, epi_2, 40, init=2)

        out_3 = pick_rows('send_3', proj, send_flat, peers, slots, None)
        got_3 = exchange(out_3).reshape(halo, LANES)
        near_3 = near_sums('near_3', 1, src_near, proj, [target])
        inv_total = (1.0 / total).reshape(1, 1)

        def epi_3(a, bl, fx, out):
            scale = bl[1][...]
            z = bl[0][...] + fold3(a * scale, fx[2][...]) + fx[0][...]
            lane = spread_lanes()
            z = jnp.where(lane < 3 * SPREAD, z, -1e30)
            top = jnp.max(z, axis=1, keepdims=True)
            e = jnp.where(lane < SPREAD, jnp.exp(z - top), 0.0)
            lse = top + jnp.log(jnp.sum(e, axis=1, keepdims=True))
            t = bl[2][...].astype(F32)
            hit = t > 1.5
            d = jnp.where(t > 0.5, jnp.exp(z - lse) - jnp.where(hit, 1.0, 0.0), 0.0) * fx[1][...]
            db = d.astype(BF16)
            out[0][...] = db
            out[1][...] = split3(db.astype(F32) * scale)
            add_rows(out[2], d)
            add_rows(out[3], jnp.where(hit & (lane < SPREAD), lse - z, 0.0))

        d_bf_3, scaled_3, g_b3, loss_parts = edge_call(
            'layer_3', (meta_f, far_at, src_far, seg_far), 1, halo, n, win_e, [(halo, LANES)], rows_of(1), [got_3, near_3],
            [logits_self, inv, target], [b3, jnp.broadcast_to(inv_total, (1, LANES)), folder],
            [((n, LANES), BF16, False), ((n, LANES), BF16, False), ((8, LANES), F32, True), ((8, LANES), F32, True)],
            n, tile, epi_3, 30, init=1)

        def epi_b3h(a, bl, fx, out):
            out[0][...] = split3(fold3(a, fx[0][...]))

        tile_h = next(t for t in (4096, 512) if halo % t == 0)
        back_3 = edge_call('back_3_halo', (meta_b, halo_at, dst_s, seg_h), 1, n, halo, win_h, [(n, LANES)], rows_of(1),
                           [scaled_3], [], [folder], [((halo, LANES), BF16, False)], halo, tile_h, epi_b3h, 15)[0]
        ret_3 = exchange(back_3.reshape(peers, slots, LANES)).reshape(halo, LANES)
        own_3 = edge_call('back_3_own', (meta_b, own_at, dst_s, seg_o), 1, n, n, win_e, [(n, LANES)], rows_of(1),
                          [scaled_3], [], [], [((n, LANES), F32, False)], n, tile, None, 20)[0]

        def epi_o3(a, bl, fx, out):
            tb = fold3(a, fx[2][...]).astype(BF16)
            d_h = mm(jnp.concatenate([bl[0][...], tb], axis=1), fx[0][...])
            d_pre = jnp.where(bl[1][...].astype(F32) > 0, d_h, 0.0)
            db = d_pre.astype(BF16)
            scale = bl[2][...]
            out[0][...] = tb
            out[1][...] = db
            out[2][...] = (mm(db, fx[1][...]) * jnp.concatenate([scale, scale], axis=1)).astype(BF16)
            add_rows(out[3], d_pre)

        tb_3, d_bf_2, scaled_2, g_b2 = edge_call(
            'owner_3', (meta_b, owner_at, slot_s, seg_r), 1, halo, n, win_r, [(halo, LANES)], rows_of(1), [ret_3, own_3],
            [d_bf_3, hidden_2, inv], [jnp.concatenate([ws3_t, wn3_t], axis=0), w_neigh_2.T, folder],
            [((n, LANES), BF16, False), ((n, hidden), BF16, False), ((n, hidden), BF16, False), ((8, hidden), F32, True)],
            n, tile, epi_o3, 30, init=1, sub=512)

        def epi_b2h(a, bl, fx, out):
            out[0][...] = a.astype(BF16)

        def epi_b2o(a, bl, fx, out):
            out[0][...] = a + mm(bl[0][...], fx[0][...])

        back_2 = edge_call('back_2_halo', (meta_b, halo_at, dst_wide, seg_h), 2, n, halo, win_h, [(n, hidden)], rows_of(2),
                           [scaled_2], [], [], [((halo, hidden), BF16, False)], halo, tile_h, epi_b2h, 20)[0]
        ret_2 = exchange(back_2.reshape(peers, slots, hidden)).reshape(halo, hidden)
        own_2 = edge_call('back_2_own', (meta_b, own_at, dst_wide, seg_o), 2, n, n, win_e, [(n, hidden)], rows_of(2),
                          [scaled_2], [d_bf_2], [w_self_2.T], [((n, hidden), F32, False)], n, tile, epi_b2o, 30)[0]

        def epi_o2(a, bl, fx, out):
            d_pre = jnp.where(bl[0][...].astype(F32) > 0, a, 0.0)
            out[0][...] = d_pre.astype(BF16)
            add_rows(out[1], d_pre)

        d_bf_1, g_b1 = edge_call(
            'owner_2', (meta_b, owner_at, tile_linear(slot_s), seg_r), 2, halo, n, win_r, [(halo, hidden)], rows_of(2),
            [ret_2, own_2], [hidden_1], [], [((n, hidden), BF16, False), ((8, hidden), F32, True)], n, tile, epi_o2, 25,
            init=1)

        def contract(a, b):
            return jnp.einsum('nd,ne->de', a, b, preferred_element_type=F32)

        parts = [contract(features, d_bf_1), contract(mean_1, d_bf_1), jnp.sum(g_b1, axis=0),
                 contract(hidden_1, d_bf_2), contract(mean_2, d_bf_2), jnp.sum(g_b2, axis=0),
                 contract(hidden_2, d_bf_3)[:, :classes], contract(hidden_2, tb_3)[:, :classes],
                 jnp.sum(g_b3, axis=0)[:classes], jnp.sum(loss_parts).reshape(1)]
        sizes = [p.size for p in parts]
        whole = sum(sizes)
        rows = -(-whole // (peers * LANES * 8)) * 8
        flat = jnp.concatenate([p.reshape(-1) for p in parts] + [jnp.zeros((peers * rows * LANES - whole,), F32)])
        full = sum_over_devices(flat.reshape(2, peers // 2, rows, LANES), peers).reshape(-1)
        outs, at = [], 0
        for p, size in zip(parts, sizes):
            outs.append(full[at:at + size].reshape(p.shape))
            at += size
        return (outs[-1][0] / total,) + tuple(outs[:-1])

    sharded = P(GROUP_AXIS)
    whole = P()
    return jax.shard_map(device_step, mesh=mesh,
                         in_specs=(sharded,) * 7 + (whole,) * 9,
                         out_specs=(whole,) * 10, check_vma=False)
```

```python
import math

import jax
import jax.numpy as jnp
from jax import lax
from jax.experimental import pallas as pl
from jax.experimental.pallas import tpu as pltpu
from jax.sharding import PartitionSpec as P

GROUP_AXIS = 'gp'
LANES = 128
SPREAD = 40
BLOCK = 128
GROUP = 8
TAIL = 8
F32 = jnp.float32
BF16 = jnp.bfloat16
VMEM_LIMIT = 60 * 2 ** 20

SMEM_SPEC = pl.BlockSpec(memory_space=pltpu.SMEM)
HBM_SPEC = pl.BlockSpec(memory_space=pltpu.HBM)


def whole_spec(shape):
    return pl.BlockSpec(shape, lambda i: (0,) * len(shape))


def row_spec(rows, width):
    return pl.BlockSpec((rows, width), lambda i: (i, 0))


def params():
    return pltpu.CompilerParams(vmem_limit_bytes=VMEM_LIMIT, dimension_semantics=('arbitrary',))


def cost(micros):
    return pl.CostEstimate(flops=int(micros * 4e6), bytes_accessed=int(micros * 1e6), transcendentals=0)


def mm(a, b):
    return jnp.dot(a, b, preferred_element_type=F32)


def tile_linear(row):
    return ((row >> 3) << 4) | (row & 7)


def put_rows(tab, row0, x, nc):
    rows = x.shape[0]
    if nc == 1:
        tab[pl.ds(pl.multiple_of(row0, 8), rows), :] = x
    else:
        for g in range(rows // 8):
            for c in range(nc):
                at = pl.multiple_of((row0 + g * 8) * nc + c * 8, 8)
                tab[pl.ds(at, 8), :] = x[g * 8:g * 8 + 8, c * LANES:(c + 1) * LANES]


def fetch(src, stage, sem, parts):
    rows = src.shape[0] // parts
    copies = [pltpu.make_async_copy(src.at[pl.ds(k * rows, rows)], stage.at[pl.ds(k * rows, rows)], sem.at[k])
              for k in range(parts)]
    for c in copies:
        c.start()
    return copies


def unpack(copies, stage, tab, row0, nc):
    rows = stage.shape[0] // len(copies)
    step = next(d for d in (128, 96, 64, 32, 16) if rows % d == 0)
    for p, c in enumerate(copies):
        c.wait()

        def body(k, carry):
            at = pl.multiple_of(p * rows + k * step, step)
            put_rows(tab, row0 + at, stage[pl.ds(at, step), :].astype(F32), nc)
            return carry
        lax.fori_loop(0, rows // step, body, 0)


def group_of(blocks):
    return next(u for u in (GROUP, 4, 2) if blocks % u == 0)


def zero_rows(acc):
    rows = acc.shape[0]
    step = next(s for s in (256, 128, 64, 32, 16, 8) if rows % s == 0)

    def body(k, carry):
        acc[pl.ds(pl.multiple_of(k * step, step), step), :] = jnp.zeros((step, acc.shape[1]), F32)
        return carry
    lax.fori_loop(0, rows // step, body, 0)


def gather_16(idx, first, tab, nc):
    sub = lax.broadcasted_iota(jnp.int32, (8, LANES), 0)
    halves = [[None, None] for _ in range(nc)]
    for h in range(2):
        for k in range(8):
            at = idx[first + h * 8 + k]
            for c in range(nc):
                row = jnp.broadcast_to(tab[pl.ds(at + 8 * c, 1), :], (8, LANES))
                halves[c][h] = row if k == 0 else jnp.where(sub == k, row, halves[c][h])
    return [jnp.concatenate(halves[c], axis=0).astype(BF16) for c in range(nc)]


def segment_sums(meta, meta_at, idx, seg, tab, acc, bufs, nc, window, blocks):
    unroll = group_of(blocks)
    first_trip, end_trip, most = [meta[meta_at + 2 * blocks + k] for k in range(3)]

    def fill(b, buf):
        for g in range(BLOCK // 16):
            parts = gather_16(idx, b * BLOCK + g * 16, tab, nc)
            for c in range(nc):
                buf[g * 16:g * 16 + 16, c * LANES:(c + 1) * LANES] = parts[c]

    def sums(b, at, buf):
        rows = lax.broadcasted_iota(jnp.int32, (window, BLOCK), 0) + at
        return mm(jnp.where(rows == seg[b], 1.0, 0.0).astype(BF16), buf[...])

    def add(at, x):
        acc[pl.ds(pl.multiple_of(at, 8), window), :] += x

    fill(jnp.minimum(first_trip * unroll, blocks - 1), bufs[0])

    def body(t, carry):
        before = None
        for u in range(unroll):
            b = t * unroll + u
            now = (meta[meta_at + b], sums(b, meta[meta_at + b], bufs[u % 2]))
            fill(jnp.minimum(b + 1, blocks - 1), bufs[(u + 1) % 2])
            if before is not None:
                add(*before)
            before = now
        add(*before)
        return carry
    lax.fori_loop(first_trip, end_trip, body, 0)

    @pl.when(most > 1)
    def _():
        def again(b, carry):
            count = meta[meta_at + blocks + b]

            @pl.when(count > 1)
            def _():
                fill(b, bufs[0])

                def more(w, c):
                    at = meta[meta_at + b] + w * window
                    add(at, sums(b, at, bufs[0]))
                    return c
                lax.fori_loop(1, count, more, 0)
            return carry
        lax.fori_loop(first_trip * unroll, end_trip * unroll, again, 0)


def spread_lanes():
    return lax.broadcasted_iota(jnp.int32, (1, LANES), 1)


def split3(x):
    hi = x.astype(BF16).astype(F32)
    rest = x - hi
    mid = rest.astype(BF16).astype(F32)
    low = rest - mid
    lane = spread_lanes()
    out = jnp.where(lane < SPREAD, hi, jnp.where(lane < 2 * SPREAD, mid, low))
    return jnp.where(lane < 3 * SPREAD, out, 0.0).astype(BF16)


def pieces3(a):
    hi = a.astype(BF16)
    rest = a - hi.astype(F32)
    mid = rest.astype(BF16)
    low = (rest - mid.astype(F32)).astype(BF16)
    return jnp.concatenate([hi, mid, low], axis=1)


def fold3(a, folder):
    return mm(pieces3(a), folder)


def add_rows(ref, x):
    ref[...] += jnp.sum(x.reshape(x.shape[0] // 8, 8, x.shape[1]), axis=0)


def pick_rows(name, src, idx, peers, slots, mask):
    n = src.shape[0]
    per = math.gcd(peers, 16)
    extra = 0 if mask is None else TAIL
    parts = math.gcd(n // 128, 4)

    def kern(idx_ref, src_ref, *refs):
        if extra:
            mask_ref, out, tab, stage, sem, tail = refs
        else:
            out, tab, stage, sem = refs

        @pl.when(pl.program_id(0) == 0)
        def _():
            copies = fetch(src_ref, stage, sem, parts)
            if extra:
                total = jnp.sum(mask_ref[...], axis=(0, 1), keepdims=True)
                high = jnp.floor(total * (1.0 / LANES))
                first = lax.broadcasted_iota(jnp.int32, (TAIL, LANES), 0) == 0
                lane = lax.broadcasted_iota(jnp.int32, (TAIL, LANES), 1)
                digits = jnp.where(lane == 0, high, jnp.where(lane == 1, total - high * LANES, 0.0))
                tail[...] = jnp.where(first, digits, 0.0).astype(BF16)
            unpack(copies, stage, tab, 0, 1)

        def body(p, carry):
            for g in range(slots // 16):
                out[p, g * 16:g * 16 + 16, :] = gather_16(idx_ref, p * slots + g * 16, tab, 1)[0]
            if extra:
                out[p, slots:slots + extra, :] = tail[...]
            return carry
        lax.fori_loop(0, per, body, 0)

    operands = [idx, src] + ([mask] if extra else [])
    specs = [pl.BlockSpec((per * slots,), lambda i: (i,), memory_space=pltpu.SMEM), HBM_SPEC] + ([whole_spec(mask.shape)] if extra else [])
    return pl.pallas_call(
        kern, name=name, grid=(peers // per,),
        out_shape=jax.ShapeDtypeStruct((peers, slots + extra, LANES), BF16),
        in_specs=specs,
        out_specs=pl.BlockSpec((per, slots + extra, LANES), lambda i: (i, 0, 0)),
        scratch_shapes=([pltpu.VMEM((n, LANES), F32), pltpu.VMEM((n, LANES), BF16), pltpu.SemaphoreType.DMA((parts,))]
                        + ([pltpu.VMEM((TAIL, LANES), BF16)] if extra else [])),
        compiler_params=params(), cost_estimate=cost(10))(*operands)


def pick_into(idx, tab, stage, peers, slots):
    def body(p, carry):
        for g in range(slots // 16):
            stage[p, g * 16:g * 16 + 16, :] = gather_16(idx, p * slots + g * 16, tab, 1)[0]
        return carry
    lax.fori_loop(0, peers, body, 0)


def send_out(stage, out, sem):
    done = pltpu.make_async_copy(stage, out, sem)
    done.start()
    done.wait()


def edge_call(name, edges, nc, table_rows, acc_rows, window, sources, build, hbm_in, blocked, fixed, outs, rows_out,
              tile, epilogue, micros, init=None, sub=1024, keep=0, pick=None, then=None):
    meta, meta_at, idx, seg = edges
    blocks = seg.shape[0]
    width = nc * LANES
    nh, nb, nf, no, ns = len(hbm_in), len(blocked), len(fixed), len(outs), len(sources)
    acc_total = -(-(acc_rows + window) // 256) * 256
    parts = 4
    steps = 1 if epilogue is None else rows_out // tile
    sub = math.gcd(sub, tile)
    more_in, more_specs, more_out, more_scratch = [], [], [], []
    if keep:
        more_scratch.append(pltpu.VMEM((rows_out * keep, LANES), F32))
    if pick:
        p_idx, peers, slots = pick
        more_in.append(p_idx)
        more_specs.append(SMEM_SPEC)
        more_out.append(jax.ShapeDtypeStruct((peers, slots, LANES), BF16))
        more_scratch.append(pltpu.VMEM((peers, slots, LANES), BF16))
    if then:
        (t_meta, t_at, t_idx, t_seg), t_nc, t_rows, t_window, finish = then
        t_width = t_nc * LANES
        t_total = -(-(t_rows + t_window) // 256) * 256
        more_in += [t_meta, t_idx, t_seg]
        more_specs += [SMEM_SPEC, SMEM_SPEC, whole_spec(t_seg.shape)]
        more_out.append(jax.ShapeDtypeStruct((t_rows, t_width), BF16))
        more_scratch += [pltpu.VMEM((t_total, t_width), F32), pltpu.VMEM((BLOCK, t_width), BF16),
                         pltpu.VMEM((BLOCK, t_width), BF16), pltpu.VMEM((t_rows, t_width), BF16)]
    nm = len(more_in)

    def kern(meta_ref, idx_ref, seg_ref, *refs):
        hb, refs = refs[:nh], refs[nh:]
        bl, refs = refs[:nb], refs[nb:]
        fx, refs = refs[:nf], refs[nf:]
        extra, refs = refs[:nm], refs[nm:]
        out, refs = refs[:no], refs[no:]
        last_out, refs = refs[:len(more_out)], refs[len(more_out):]
        tab, acc, buf_0, buf_1, isem = refs[:5]
        stages, sems, scratch = refs[5:5 + ns], refs[5 + ns:5 + 2 * ns], refs[5 + 2 * ns:]
        i = pl.program_id(0)

        @pl.when(i == 0)
        def _():
            copies = [fetch(h, st, sm, parts) for h, st, sm in zip(hb, stages, sems)]
            if init is None:
                zero_rows(acc)
            else:
                start = pltpu.make_async_copy(hb[init], acc.at[pl.ds(0, acc_rows), :], isem)
                start.start()
            for o, (_, _, sums) in zip(out, outs):
                if sums:
                    o[...] = jnp.zeros_like(o)
            if then:
                zero_rows(scratch[1])
            build(copies, stages, tab, fx)
            if init is not None:
                start.wait()
            segment_sums(meta_ref, meta_at, idx_ref, seg_ref, tab, acc, (buf_0, buf_1), nc, window, blocks)
            if epilogue is None:
                send_out(acc.at[pl.ds(0, acc_rows), :], out[0], isem)
        if epilogue is not None:
            def part(j, carry):
                at = pl.multiple_of(j * sub, sub)
                row0 = pl.multiple_of(i * tile + at, sub)

                def put(x):
                    put_rows(scratch[0], row0, x, keep)
                epilogue(acc[pl.ds(row0, sub), :], [r.at[pl.ds(at, sub), :] for r in bl], fx,
                         [o if sums else o.at[pl.ds(at, sub), :] for o, (_, _, sums) in zip(out, outs)], put)
                return carry
            lax.fori_loop(0, tile // sub, part, 0)

        if pick:
            @pl.when(i == steps - 1)
            def _():
                pick_into(extra[0], scratch[0], scratch[1], peers, slots)
                send_out(scratch[1], last_out[0], isem)
        if then:
            @pl.when(i == steps - 1)
            def _():
                kept, acc_2, buf_2, buf_3, stage = scratch
                segment_sums(extra[0], t_at, extra[1], extra[2], kept, acc_2, (buf_2, buf_3), t_nc, t_window,
                             t_seg.shape[0])
                step = math.gcd(1024, t_rows)

                def part(j, carry):
                    at = pl.multiple_of(j * step, step)
                    stage[pl.ds(at, step), :] = finish(acc_2[pl.ds(at, step), :], fx)
                    return carry
                lax.fori_loop(0, t_rows // step, part, 0)
                send_out(stage, last_out[0], isem)

    out_shape, out_specs = [], []
    for shape, dtype, sums in outs:
        out_shape.append(jax.ShapeDtypeStruct(shape, dtype))
        out_specs.append(HBM_SPEC if epilogue is None else whole_spec(shape) if sums else row_spec(tile, shape[1]))
    return pl.pallas_call(
        kern, name=name, grid=(steps,), out_shape=out_shape + more_out,
        in_specs=([SMEM_SPEC, SMEM_SPEC, whole_spec(seg.shape)] + [HBM_SPEC] * nh
                  + [row_spec(tile, x.shape[1]) for x in blocked] + [whole_spec(x.shape) for x in fixed] + more_specs),
        out_specs=out_specs + [HBM_SPEC] * len(more_out),
        scratch_shapes=([pltpu.VMEM((table_rows * nc, LANES), F32), pltpu.VMEM((acc_total, width), F32),
                         pltpu.VMEM((BLOCK, width), BF16), pltpu.VMEM((BLOCK, width), BF16),
                         pltpu.SemaphoreType.DMA(())]
                        + [pltpu.VMEM(shape, BF16) for shape in sources]
                        + [pltpu.SemaphoreType.DMA((parts,)) for _ in sources] + more_scratch),
        compiler_params=params(), cost_estimate=cost(micros))(meta, idx, seg, *hbm_in, *blocked, *fixed, *more_in)


SHARE = 16


def grad_places(shapes):
    places, at = [], 0
    for rows, width in shapes:
        columns = []
        for _ in range(width // LANES):
            columns.append(at)
            at += -(-rows // SHARE)
        places.append(columns)
    return places, at


def sum_over_devices(grads, sums, peers):
    chips = peers // 2
    places, used = grad_places([g.shape for g in grads] + [(SHARE, LANES)])
    rounds = -(-used // peers)
    rows = SHARE * rounds
    widths = [x.shape[1] for x in sums]

    def device(chip, core):
        return chip * 2 + core

    def kern(*refs):
        ng, ns = len(grads), len(sums)
        g_refs, s_refs, out_ref = refs[:ng], refs[ng:ng + ns], refs[ng + ns]
        x_ref, half, mine, got, pair_sem, send_sem, recv_sem, send_2, recv_2 = refs[ng + ns + 1:]
        me = lax.axis_index(GROUP_AXIS)
        chip, core = me // 2, me % 2
        mate = device(chip, 1 - core)

        def at(q):
            unit = q // rounds
            return unit // chips, unit % chips, (q % rounds) * SHARE

        def put(q, value):
            h, c, r = at(q)
            x_ref[h, c, r:r + SHARE, :] = value
        for g, columns in zip(g_refs, places):
            for w, first in enumerate(columns):
                for k in range(g.shape[0] // SHARE):
                    put(first + k, g[k * SHARE:(k + 1) * SHARE, w * LANES:(w + 1) * LANES])
        row = lax.broadcasted_iota(jnp.int32, (SHARE, LANES), 0)
        small, line = jnp.zeros((SHARE, LANES), F32), 0
        for s_ref, width in zip(s_refs, widths):
            for w in range(width // LANES):
                total = jnp.sum(s_ref[:, w * LANES:(w + 1) * LANES], axis=0, keepdims=True)
                small = jnp.where(row == line, total, small)
                line += 1
        put(places[-1][0], small)
        for q in range(used, peers * rounds):
            put(q, jnp.zeros((SHARE, LANES), F32))

        def pair(src, dst, k):
            return pltpu.make_async_remote_copy(src_ref=src, dst_ref=dst, send_sem=pair_sem.at[2 * k],
                                                recv_sem=pair_sem.at[2 * k + 1], device_id=(mate,),
                                                device_id_type=pl.DeviceIdType.MESH)
        first = pair(x_ref.at[1 - core], half, 0)
        first.start()
        first.wait()

        def add(c, carry):
            mine[c] = x_ref[core, c] + half[c]
            return carry
        lax.fori_loop(0, chips, add, 0)

        def share(k):
            to = (chip + k) % chips
            return pltpu.make_async_remote_copy(src_ref=mine.at[to], dst_ref=got.at[chip], send_sem=send_sem.at[k],
                                                recv_sem=recv_sem.at[chip], device_id=(device(to, core),),
                                                device_id_type=pl.DeviceIdType.MESH)

        def landed(k):
            frm = (chip + k) % chips
            return pltpu.make_async_remote_copy(src_ref=mine.at[frm], dst_ref=got.at[frm], send_sem=send_sem.at[k],
                                                recv_sem=recv_sem.at[frm], device_id=(me,),
                                                device_id_type=pl.DeviceIdType.MESH)

        def start(k, carry):
            share(k).start()
            return carry
        lax.fori_loop(1, chips, start, 0)
        got[chip] = mine[chip]

        def settle(k, carry):
            landed(k).wait_recv()
            return carry
        lax.fori_loop(1, chips, settle, 0)

        def more(c, total):
            return total + got[c]
        out_ref[core, chip] = lax.fori_loop(0, chips, more, jnp.zeros((rows, LANES), F32))

        def drain(k, carry):
            share(k).wait_send()
            return carry
        lax.fori_loop(1, chips, drain, 0)

        def give(k):
            return pltpu.make_async_remote_copy(src_ref=out_ref.at[core, chip], dst_ref=out_ref.at[core, chip],
                                                send_sem=send_2.at[k], recv_sem=recv_2.at[chip],
                                                device_id=(device((chip + k) % chips, core),),
                                                device_id_type=pl.DeviceIdType.MESH)

        def given(k):
            frm = (chip + k) % chips
            return pltpu.make_async_remote_copy(src_ref=out_ref.at[core, frm], dst_ref=out_ref.at[core, frm],
                                                send_sem=send_2.at[k], recv_sem=recv_2.at[frm], device_id=(me,),
                                                device_id_type=pl.DeviceIdType.MESH)

        def start_2(k, carry):
            give(k).start()
            return carry
        lax.fori_loop(1, chips, start_2, 0)

        def settle_2(k, carry):
            given(k).wait_recv()
            return carry
        lax.fori_loop(1, chips, settle_2, 0)

        def drain_2(k, carry):
            give(k).wait_send()
            return carry
        lax.fori_loop(1, chips, drain_2, 0)
        last = pair(out_ref.at[core], out_ref.at[core], 1)
        last.start()
        last.wait()

    vmem = pl.BlockSpec(memory_space=pltpu.VMEM)
    shape = (2, chips, rows, LANES)
    full = pl.pallas_call(
        kern, name='sum_all', out_shape=jax.ShapeDtypeStruct(shape, F32),
        in_specs=[vmem] * (len(grads) + len(sums)), out_specs=vmem,
        scratch_shapes=[pltpu.VMEM(shape, F32), pltpu.VMEM(shape[1:], F32), pltpu.VMEM(shape[1:], F32),
                        pltpu.VMEM(shape[1:], F32), pltpu.SemaphoreType.DMA((4,)),
                        pltpu.SemaphoreType.DMA((chips,)), pltpu.SemaphoreType.DMA((chips,)),
                        pltpu.SemaphoreType.DMA((chips,)), pltpu.SemaphoreType.DMA((chips,))],
        compiler_params=pltpu.CompilerParams(has_side_effects=True), cost_estimate=cost(25))(*grads, *sums)

    def unpack_kern(full_ref, *outs):
        def at(q):
            unit = q // rounds
            return unit // chips, unit % chips, (q % rounds) * SHARE
        for o, columns in zip(outs, places):
            for w, first in enumerate(columns):
                for k in range(o.shape[0] // SHARE):
                    h, c, r = at(first + k)
                    o[k * SHARE:(k + 1) * SHARE, w * LANES:(w + 1) * LANES] = full_ref[h, c, r:r + SHARE, :]
        h, c, r = at(places[-1][0])
        small, line = full_ref[h, c, r:r + SHARE, :], 0
        for o, width in zip(outs[len(grads):], widths):
            for w in range(width // LANES):
                o[:, w * LANES:(w + 1) * LANES] = small[line:line + 1, :]
                line += 1
    outs = [jax.ShapeDtypeStruct(g.shape, F32) for g in grads] + [jax.ShapeDtypeStruct((1, w), F32) for w in widths]
    got = pl.pallas_call(unpack_kern, name='unpack_sums', out_shape=outs, in_specs=[vmem], out_specs=[vmem] * len(outs),
                         cost_estimate=cost(3))(full)
    return got[:len(grads)], got[len(grads):]


def edge_meta(seg_first, seg_last, window, first_block, end_block):
    blocks = seg_first.shape[0]
    unroll = group_of(blocks)
    at = jnp.arange(blocks, dtype=jnp.int32)
    base = seg_first & ~7
    count = jnp.where((at >= first_block) & (at < end_block), (seg_last - base) // window + 1, 1)
    tail = jnp.stack([first_block // unroll, (end_block + unroll - 1) // unroll, jnp.max(count)])
    return [base, count, tail]


def join_meta(*metas):
    offsets, at = [], 0
    for m in metas:
        offsets.append(at)
        at += sum(x.shape[0] for x in m)
    return jnp.concatenate([x for m in metas for x in m]).astype(jnp.int32), offsets


def bits_for(n):
    return max(1, (n - 1).bit_length())


def spread3(w):
    w = jnp.pad(w, ((0, 0), (0, SPREAD - w.shape[1])))
    return jnp.pad(jnp.concatenate([w, w, w], axis=1), ((0, 0), (0, LANES - 3 * SPREAD)))


def lanes_pad(w):
    return jnp.pad(w, ((0, 0), (0, LANES - w.shape[1])))


def solution(mesh):
    peers = mesh.shape[GROUP_AXIS]

    def exchange(x):
        return lax.all_to_all(x, GROUP_AXIS, 0, 0, tiled=True)

    def device_step(features, labels, train_mask, send_idx, src_idx, dst_idx, inv_deg,
                    w_self_1, w_neigh_1, bias_1, w_self_2, w_neigh_2, bias_2,
                    w_self_3, w_neigh_3, bias_3):
        n = features.shape[0]
        slots = send_idx.shape[1]
        halo = peers * slots
        edges = src_idx.shape[0]
        hidden = w_self_1.shape[1]
        classes = w_self_3.shape[1]
        send_flat = send_idx.reshape(-1)
        tile = next(t for t in (4096, 1024) if n % t == 0)
        half_tile = tile // 2
        slot_bits = bits_for(halo)
        dst_bits = bits_for(n)
        table = n + halo

        blocks = edges // BLOCK
        halo_blocks = halo // BLOCK
        zero = jnp.int32(0)
        win_e, win_h, win_r = 176, 192, 240
        owned = jnp.sum((src_idx < n).astype(jnp.int32))
        near_end = (owned + BLOCK - 1) // BLOCK
        far_start = owned // BLOCK

        src_bits = bits_for(table)
        far_bit = dst_bits + src_bits
        by_dst = lax.sort(((src_idx >= n).astype(jnp.int32) << far_bit) | (dst_idx << src_bits) | src_idx, is_stable=False)
        src_f = by_dst & ((1 << src_bits) - 1)
        dst_f = (by_dst >> src_bits) & ((1 << dst_bits) - 1)
        is_far = src_f >= n
        src_near = jnp.minimum(src_f, n - 1)
        src_far = jnp.maximum(src_f - n, 0)
        seg_near = jnp.where(is_far, -1, dst_f).reshape(blocks, 1, BLOCK)
        seg_far = jnp.where(is_far, dst_f, -1).reshape(blocks, 1, BLOCK)
        first, last = dst_f[::BLOCK], dst_f[BLOCK - 1::BLOCK]
        meta_f, (near_at, far_at) = join_meta(
            edge_meta(first, jnp.where(is_far[BLOCK - 1::BLOCK], n - 1, last), win_e, zero, near_end),
            edge_meta(jnp.where(is_far[::BLOCK], first, 0), last, win_e, far_start, jnp.int32(blocks)))

        inv = jnp.broadcast_to(inv_deg[:, None], (n, LANES))
        b1 = bias_1.reshape(1, -1)
        b2 = bias_2.reshape(1, -1)
        lane = jnp.arange(LANES, dtype=jnp.int32)
        used = lane < 3 * SPREAD
        folder = jnp.tile(((lane[:, None] % SPREAD == lane[None, :] % SPREAD) & used[:, None] & used[None, :]).astype(BF16),
                          (3, 1))
        b3 = jnp.where(lane < 3 * SPREAD, spread3(bias_3.reshape(1, -1)), -1e30)
        if classes < SPREAD:
            b3 = jnp.where(lane % SPREAD < classes, b3, -1e30)
        target = jnp.where(lane[None, :] < 3 * SPREAD,
                           train_mask[:, None] * (1.0 + (labels[:, None] == lane[None, :] % SPREAD)), 0.0).astype(BF16)
        ws3, wn3 = spread3(w_self_3), spread3(w_neigh_3)
        ws3_t, wn3_t = lanes_pad(w_self_3).T, lanes_pad(w_neigh_3).T

        def rows_of(nc):
            def build(copies, stages, tab, fx):
                unpack(copies[0], stages[0], tab, 0, nc)
            return build

        def near_sums(name, nc, idx, rows, also):
            return edge_call(name, (meta_f, near_at, idx, seg_near), nc, n, n, win_e, [rows.shape], rows_of(nc),
                             [rows] + also, [], [], [((n, nc * LANES), F32, False)], n, tile, None, 20)[0]

        out_1 = pick_rows('send_1', features, send_flat, peers, slots, train_mask.reshape(-1, LANES))
        got_1 = exchange(out_1)
        near_1 = near_sums('near_1', 1, src_near, features, [inv])
        counts = got_1[:, slots, :2].astype(F32)
        total = jnp.sum(counts[:, 0]) * LANES + jnp.sum(counts[:, 1])

        def build_1(copies, stages, tab, fx):
            per = peers // len(copies[0])
            some = math.gcd(per, 8)
            for p in range(len(copies[0])):
                copies[0][p].wait()

                def body(k, carry):
                    q = p * per + k * some
                    rows = stages[0][pl.ds(q, some), :slots, :].reshape(some * slots, LANES)
                    put_rows(tab, q * slots, rows.astype(F32), 1)
                    return carry
                lax.fori_loop(0, per // some, body, 0)

        def epi_1(a, bl, fx, out, put):
            mean = (a * bl[1][...]).astype(BF16)
            z = mm(bl[0][...], fx[0][...]) + mm(mean, fx[1][...]) + fx[2][...]
            out[0][...] = mean
            out[1][...] = jnp.maximum(z, 0.0).astype(BF16)
            put(mean.astype(F32))

        mean_1, hidden_1, out_2 = edge_call(
            'layer_1', (meta_f, far_at, src_far, seg_far), 1, halo, n, win_e, [(peers, slots + TAIL, LANES)], build_1,
            [got_1, near_1], [features, inv], [w_self_1, w_neigh_1, b1],
            [((n, LANES), BF16, False), ((n, hidden), BF16, False)], n, tile, epi_1, 25, init=1,
            keep=1, pick=(send_flat, peers, slots))

        keys = jnp.concatenate([(src_idx << dst_bits) | dst_idx,
                                (1 << 30) | (send_flat << slot_bits) | jnp.arange(halo, dtype=jnp.int32)])
        keys = lax.optimization_barrier((keys, mean_1))[0]
        ordered = lax.sort(keys, is_stable=False)
        by_src, by_row = ordered[:edges], ordered[edges:] & ((1 << 30) - 1)
        src_s = by_src >> dst_bits
        dst_s = by_src & ((1 << dst_bits) - 1)
        row_s = by_row >> slot_bits
        slot_s = by_row & ((1 << slot_bits) - 1)
        first, last = src_s[::BLOCK], src_s[BLOCK - 1::BLOCK]
        meta_b, (own_at, halo_at, owner_at) = join_meta(
            edge_meta(jnp.minimum(first, n - 1), jnp.minimum(last, n - 1), win_e, zero, near_end),
            edge_meta(jnp.maximum(first - n, 0), jnp.maximum(last - n, 0), win_h, far_start, jnp.int32(blocks)),
            edge_meta(row_s[::BLOCK], row_s[BLOCK - 1::BLOCK], win_r, zero, jnp.int32(halo_blocks)))
        seg_o = src_s.reshape(blocks, 1, BLOCK)
        seg_h = seg_o - n
        seg_r = row_s.reshape(halo_blocks, 1, BLOCK)
        dst_wide = tile_linear(dst_s)

        got_2 = exchange(out_2)
        near_2 = near_sums('near_2', 2, tile_linear(src_near), hidden_1, [])

        def build_2(copies, stages, tab, fx):
            per = peers // len(copies[0])
            some = math.gcd(per, 8)
            for p in range(len(copies[0])):
                copies[0][p].wait()
                copies[1][p].wait()

                def body(k, carry):
                    q = p * per + k * some
                    f = stages[0][pl.ds(q, some), :slots, :].reshape(some * slots, LANES)
                    m = stages[1][pl.ds(q, some)].reshape(some * slots, LANES)
                    z = mm(f, fx[3][...]) + mm(m, fx[4][...]) + fx[5][...]
                    put_rows(tab, q * slots, jnp.maximum(z, 0.0).astype(BF16).astype(F32), 2)
                    return carry
                lax.fori_loop(0, per // some, body, 0)

        def epi_2(a, bl, fx, out, put):
            scale = bl[1][...]
            mean = (a * jnp.concatenate([scale, scale], axis=1)).astype(BF16)
            z = mm(bl[0][...], fx[0][...]) + mm(mean, fx[1][...]) + fx[2][...]
            h = jnp.maximum(z, 0.0).astype(BF16)
            out[0][...] = mean
            out[1][...] = h
            both = mm(h, fx[6][...])
            pieces = split3(both[:, :LANES])
            out[2][...] = pieces
            out[3][...] = both[:, LANES:]
            put(pieces.astype(F32))

        mean_2, hidden_2, proj, logits_self, out_3 = edge_call(
            'layer_2', (meta_f, far_at, tile_linear(src_far), seg_far), 2, halo, n, win_e,
            [(peers, slots + TAIL, LANES), (peers, slots, LANES)], build_2, [got_1, got_2, near_2],
            [hidden_1, inv], [w_self_2, w_neigh_2, b2, w_self_1, w_neigh_1, b1, jnp.concatenate([wn3, ws3], axis=1)],
            [((n, hidden), BF16, False), ((n, hidden), BF16, False), ((n, LANES), BF16, False),
             ((n, LANES), F32, False)], n, half_tile, epi_2, 40, init=2, keep=1, pick=(send_flat, peers, slots))

        got_3 = exchange(out_3).reshape(halo, LANES)
        near_3 = near_sums('near_3', 1, src_near, proj, [target])
        inv_total = (1.0 / total).reshape(1, 1)

        def epi_3(a, bl, fx, out, put):
            scale = bl[1][...]
            z = bl[0][...] + fold3(a * scale, fx[2][...]) + fx[0][...]
            lane = spread_lanes()
            z = jnp.where(lane < 3 * SPREAD, z, -1e30)
            top = jnp.max(z, axis=1, keepdims=True)
            e = jnp.where(lane < SPREAD, jnp.exp(z - top), 0.0)
            lse = top + jnp.log(jnp.sum(e, axis=1, keepdims=True))
            t = bl[2][...].astype(F32)
            hit = t > 1.5
            d = jnp.where(t > 0.5, jnp.exp(z - lse) - jnp.where(hit, 1.0, 0.0), 0.0) * fx[1][...]
            db = d.astype(BF16)
            out[0][...] = db
            pieces = split3(db.astype(F32) * scale)
            out[1][...] = pieces
            put(pieces.astype(F32))
            add_rows(out[2], d)
            add_rows(out[3], jnp.where(hit & (lane < SPREAD), lse - z, 0.0))

        def finish_3(a, fx):
            return split3(fold3(a, fx[2][...]))

        d_bf_3, scaled_3, g_b3, loss_parts, back_3 = edge_call(
            'layer_3', (meta_f, far_at, src_far, seg_far), 1, halo, n, win_e, [(halo, LANES)], rows_of(1), [got_3, near_3],
            [logits_self, inv, target], [b3, jnp.broadcast_to(inv_total, (1, LANES)), folder],
            [((n, LANES), BF16, False), ((n, LANES), BF16, False), ((8, LANES), F32, True), ((8, LANES), F32, True)],
            n, tile, epi_3, 30, init=1, keep=1, then=((meta_b, halo_at, dst_s, seg_h), 1, halo, win_h, finish_3))

        ret_3 = exchange(back_3.reshape(peers, slots, LANES)).reshape(halo, LANES)
        own_3 = edge_call('back_3_own', (meta_b, own_at, dst_s, seg_o), 1, n, n, win_e, [(n, LANES)], rows_of(1),
                          [scaled_3], [], [], [((n, LANES), F32, False)], n, tile, None, 20)[0]

        def epi_o3(a, bl, fx, out, put):
            tb = fold3(a, fx[2][...]).astype(BF16)
            d_h = mm(jnp.concatenate([bl[0][...], tb], axis=1), fx[0][...])
            d_pre = jnp.where(bl[1][...].astype(F32) > 0, d_h, 0.0)
            db = d_pre.astype(BF16)
            scale = bl[2][...]
            out[0][...] = tb
            out[1][...] = db
            scaled = (mm(db, fx[1][...]) * jnp.concatenate([scale, scale], axis=1)).astype(BF16)
            out[2][...] = scaled
            put(scaled.astype(F32))
            add_rows(out[3], d_pre)

        def finish_2(a, fx):
            return a.astype(BF16)

        tb_3, d_bf_2, scaled_2, g_b2, back_2 = edge_call(
            'owner_3', (meta_b, owner_at, slot_s, seg_r), 1, halo, n, win_r, [(halo, LANES)], rows_of(1), [ret_3, own_3],
            [d_bf_3, hidden_2, inv], [jnp.concatenate([ws3_t, wn3_t], axis=0), w_neigh_2.T, folder],
            [((n, LANES), BF16, False), ((n, hidden), BF16, False), ((n, hidden), BF16, False), ((8, hidden), F32, True)],
            n, half_tile, epi_o3, 30, init=1, sub=512, keep=2,
            then=((meta_b, halo_at, dst_wide, seg_h), 2, halo, win_h, finish_2))

        def epi_b2o(a, bl, fx, out, put):
            out[0][...] = a + mm(bl[0][...], fx[0][...])

        ret_2 = exchange(back_2.reshape(peers, slots, hidden)).reshape(halo, hidden)
        own_2 = edge_call('back_2_own', (meta_b, own_at, dst_wide, seg_o), 2, n, n, win_e, [(n, hidden)], rows_of(2),
                          [scaled_2], [d_bf_2], [w_self_2.T], [((n, hidden), F32, False)], n, tile, epi_b2o, 30)[0]

        def epi_o2(a, bl, fx, out, put):
            d_pre = jnp.where(bl[0][...].astype(F32) > 0, a, 0.0)
            out[0][...] = d_pre.astype(BF16)
            add_rows(out[1], d_pre)

        d_bf_1, g_b1 = edge_call(
            'owner_2', (meta_b, owner_at, tile_linear(slot_s), seg_r), 2, halo, n, win_r, [(halo, hidden)], rows_of(2),
            [ret_2, own_2], [hidden_1], [], [((n, hidden), BF16, False), ((8, hidden), F32, True)], n, tile, epi_o2, 25,
            init=1)

        def contract(a, b):
            return jnp.einsum('nd,ne->de', a, b, preferred_element_type=F32)

        at = jnp.arange(LANES, dtype=jnp.int32)[None, :]
        g_3 = jnp.where(at < SPREAD, contract(hidden_2, d_bf_3), contract(hidden_2, tb_3))
        g, sums = sum_over_devices([contract(features, d_bf_1), contract(mean_1, d_bf_1), contract(hidden_1, d_bf_2),
                                    contract(mean_2, d_bf_2), g_3], [g_b1, g_b2, g_b3, loss_parts], peers)
        loss = jnp.sum(sums[3]) / total
        return (loss, g[0], g[1], sums[0].reshape(-1), g[2], g[3], sums[1].reshape(-1), g[4][:, :classes],
                g[4][:, SPREAD:SPREAD + classes], sums[2].reshape(-1)[:classes])

    sharded = P(GROUP_AXIS)
    whole = P()
    return jax.shard_map(device_step, mesh=mesh,
                         in_specs=(sharded,) * 7 + (whole,) * 9,
                         out_specs=(whole,) * 10, check_vma=False)
```

```python
import math

import jax
import jax.numpy as jnp
from jax import lax
from jax.experimental import pallas as pl
from jax.experimental.pallas import tpu as pltpu
from jax.sharding import PartitionSpec as P

GROUP_AXIS = 'gp'
LANES = 128
SPREAD = 40
BLOCK = 128
GROUP = 8
TAIL = 8
F32 = jnp.float32
BF16 = jnp.bfloat16
VMEM_LIMIT = 60 * 2 ** 20

SMEM_SPEC = pl.BlockSpec(memory_space=pltpu.SMEM)
HBM_SPEC = pl.BlockSpec(memory_space=pltpu.HBM)


def whole_spec(shape):
    return pl.BlockSpec(shape, lambda i: (0,) * len(shape))


def row_spec(rows, width):
    return pl.BlockSpec((rows, width), lambda i: (i, 0))


def params():
    return pltpu.CompilerParams(vmem_limit_bytes=VMEM_LIMIT, dimension_semantics=('arbitrary',))


def cost(micros):
    return pl.CostEstimate(flops=int(micros * 4e6), bytes_accessed=int(micros * 1e6), transcendentals=0)


def mm(a, b):
    return jnp.dot(a, b, preferred_element_type=F32)


def tile_linear(row):
    return ((row >> 3) << 4) | (row & 7)


def put_rows(tab, row0, x, nc):
    rows = x.shape[0]
    if nc == 1:
        tab[pl.ds(pl.multiple_of(row0, 8), rows), :] = x
    else:
        for g in range(rows // 8):
            for c in range(nc):
                at = pl.multiple_of((row0 + g * 8) * nc + c * 8, 8)
                tab[pl.ds(at, 8), :] = x[g * 8:g * 8 + 8, c * LANES:(c + 1) * LANES]


def fetch(src, stage, sem, parts):
    rows = src.shape[0] // parts
    copies = [pltpu.make_async_copy(src.at[pl.ds(k * rows, rows)], stage.at[pl.ds(k * rows, rows)], sem.at[k])
              for k in range(parts)]
    for c in copies:
        c.start()
    return copies


def unpack(copies, stage, tab, row0, nc):
    rows = stage.shape[0] // len(copies)
    step = next(d for d in (128, 96, 64, 32, 16) if rows % d == 0)
    for p, c in enumerate(copies):
        c.wait()

        def body(k, carry):
            at = pl.multiple_of(p * rows + k * step, step)
            put_rows(tab, row0 + at, stage[pl.ds(at, step), :].astype(F32), nc)
            return carry
        lax.fori_loop(0, rows // step, body, 0)


def group_of(blocks):
    return next(u for u in (GROUP, 4, 2) if blocks % u == 0)


def zero_rows(acc):
    rows = acc.shape[0]
    step = next(s for s in (256, 128, 64, 32, 16, 8) if rows % s == 0)

    def body(k, carry):
        acc[pl.ds(pl.multiple_of(k * step, step), step), :] = jnp.zeros((step, acc.shape[1]), F32)
        return carry
    lax.fori_loop(0, rows // step, body, 0)


def gather_16(idx, base, first, reach, tab, nc, stride=1):
    sub = lax.broadcasted_iota(jnp.int32, (8, LANES), 0)
    room = idx.shape[0] - (reach - 1) * stride
    halves = [[None, None] for _ in range(nc)]
    for h in range(2):
        for k in range(8):
            at = idx.at[pl.ds((first + h * 8 + k) * stride, room)][base]
            for c in range(nc):
                row = jnp.broadcast_to(tab[pl.ds(at + 8 * c, 1), :], (8, LANES))
                halves[c][h] = row if k == 0 else jnp.where(sub == k, row, halves[c][h])
    return [jnp.concatenate(halves[c], axis=0).astype(BF16) for c in range(nc)]


def segment_sums(meta, meta_at, idx, seg, tab, acc, bufs, nc, window, blocks):
    unroll = group_of(blocks)
    first_trip, end_trip, most = [meta[meta_at + 2 * blocks + k] for k in range(3)]

    def fill(base, first, reach, buf):
        for g in range(BLOCK // 16):
            parts = gather_16(idx, base, first + g * 16, reach, tab, nc)
            for c in range(nc):
                buf[g * 16:g * 16 + 16, c * LANES:(c + 1) * LANES] = parts[c]

    def sums(b, at, buf):
        rows = lax.broadcasted_iota(jnp.int32, (window, BLOCK), 0) + at
        return mm(jnp.where(rows == seg[b], 1.0, 0.0).astype(BF16), buf[...])

    def add(at, x):
        acc[pl.ds(pl.multiple_of(at, 8), window), :] += x

    span = unroll * BLOCK
    last_trip = blocks // unroll - 1
    fill(jnp.minimum(first_trip, last_trip) * span, 0, span, bufs[0])

    def body(t, carry):
        before = None
        for u in range(unroll):
            b = t * unroll + u
            now = (meta[meta_at + b], sums(b, meta[meta_at + b], bufs[u % 2]))
            if u + 1 < unroll:
                fill(t * span, (u + 1) * BLOCK, span, bufs[(u + 1) % 2])
            else:
                fill(jnp.minimum(t + 1, last_trip) * span, 0, span, bufs[0])
            if before is not None:
                add(*before)
            before = now
        add(*before)
        return carry
    lax.fori_loop(first_trip, end_trip, body, 0)

    @pl.when(most > 1)
    def _():
        def again(b, carry):
            count = meta[meta_at + blocks + b]

            @pl.when(count > 1)
            def _():
                fill(b * BLOCK, 0, BLOCK, bufs[0])

                def more(w, c):
                    at = meta[meta_at + b] + w * window
                    add(at, sums(b, at, bufs[0]))
                    return c
                lax.fori_loop(1, count, more, 0)
            return carry
        lax.fori_loop(first_trip * unroll, end_trip * unroll, again, 0)


def spread_lanes():
    return lax.broadcasted_iota(jnp.int32, (1, LANES), 1)


def split3(x):
    hi = x.astype(BF16).astype(F32)
    rest = x - hi
    mid = rest.astype(BF16).astype(F32)
    low = rest - mid
    lane = spread_lanes()
    out = jnp.where(lane < SPREAD, hi, jnp.where(lane < 2 * SPREAD, mid, low))
    return jnp.where(lane < 3 * SPREAD, out, 0.0).astype(BF16)


def pieces3(a):
    hi = a.astype(BF16)
    rest = a - hi.astype(F32)
    mid = rest.astype(BF16)
    low = (rest - mid.astype(F32)).astype(BF16)
    return jnp.concatenate([hi, mid, low], axis=1)


def fold3(a, folder):
    return mm(pieces3(a), folder)


def add_rows(ref, x):
    ref[...] += jnp.sum(x.reshape(x.shape[0] // 8, 8, x.shape[1]), axis=0)


def pick_rows(name, src, idx, peers, slots, mask):
    n = src.shape[0]
    per = math.gcd(peers, 16)
    extra = 0 if mask is None else TAIL
    parts = math.gcd(n // 128, 4)

    def kern(idx_ref, src_ref, *refs):
        if extra:
            mask_ref, out, tab, stage, sem, tail = refs
        else:
            out, tab, stage, sem = refs

        @pl.when(pl.program_id(0) == 0)
        def _():
            copies = fetch(src_ref, stage, sem, parts)
            if extra:
                total = jnp.sum(mask_ref[...], axis=(0, 1), keepdims=True)
                high = jnp.floor(total * (1.0 / LANES))
                first = lax.broadcasted_iota(jnp.int32, (TAIL, LANES), 0) == 0
                lane = lax.broadcasted_iota(jnp.int32, (TAIL, LANES), 1)
                digits = jnp.where(lane == 0, high, jnp.where(lane == 1, total - high * LANES, 0.0))
                tail[...] = jnp.where(first, digits, 0.0).astype(BF16)
            unpack(copies, stage, tab, 0, 1)
        first = pl.program_id(0) * per

        def body(p, carry):
            for g in range(slots // 16):
                out[p, g * 16:g * 16 + 16, :] = gather_16(idx_ref, first + p, g * 16, slots, tab, 1, peers)[0]
            if extra:
                out[p, slots:slots + extra, :] = tail[...]
            return carry
        lax.fori_loop(0, per, body, 0)

    operands = [idx, src] + ([mask] if extra else [])
    specs = [SMEM_SPEC, HBM_SPEC] + ([whole_spec(mask.shape)] if extra else [])
    return pl.pallas_call(
        kern, name=name, grid=(peers // per,),
        out_shape=jax.ShapeDtypeStruct((peers, slots + extra, LANES), BF16),
        in_specs=specs,
        out_specs=pl.BlockSpec((per, slots + extra, LANES), lambda i: (i, 0, 0)),
        scratch_shapes=([pltpu.VMEM((n, LANES), F32), pltpu.VMEM((n, LANES), BF16), pltpu.SemaphoreType.DMA((parts,))]
                        + ([pltpu.VMEM((TAIL, LANES), BF16)] if extra else [])),
        compiler_params=params(), cost_estimate=cost(10))(*operands)


def pick_into(idx, tab, stage, peers, slots):
    def body(p, carry):
        for g in range(slots // 16):
            stage[p, g * 16:g * 16 + 16, :] = gather_16(idx, p, g * 16, slots, tab, 1, peers)[0]
        return carry
    lax.fori_loop(0, peers, body, 0)


def send_out(stage, out, sem):
    done = pltpu.make_async_copy(stage, out, sem)
    done.start()
    done.wait()


def edge_call(name, edges, nc, table_rows, acc_rows, window, sources, build, hbm_in, blocked, fixed, outs, rows_out,
              tile, epilogue, micros, init=None, late=False, sub=1024, keep=0, pick=None, then=None):
    meta, meta_at, idx, seg = edges
    blocks = seg.shape[0]
    width = nc * LANES
    nh, nb, nf, no, ns = len(hbm_in), len(blocked), len(fixed), len(outs), len(sources)
    acc_total = -(-(acc_rows + window) // 256) * 256
    parts = 4
    steps = 1 if epilogue is None else rows_out // tile
    sub = math.gcd(sub, tile)
    more_in, more_specs, more_out, more_scratch = [], [], [], []
    late_scratch = [pltpu.VMEM((acc_rows, width), F32)] if late else []
    if keep:
        more_scratch.append(pltpu.VMEM((rows_out * keep, LANES), F32))
    if pick:
        p_idx, peers, slots = pick
        more_in.append(p_idx)
        more_specs.append(SMEM_SPEC)
        more_out.append(jax.ShapeDtypeStruct((peers, slots, LANES), BF16))
        more_scratch.append(pltpu.VMEM((peers, slots, LANES), BF16))
    if then:
        (t_meta, t_at, t_idx, t_seg), t_nc, t_rows, t_window, finish = then
        t_width = t_nc * LANES
        t_total = -(-(t_rows + t_window) // 256) * 256
        more_in += [t_meta, t_idx, t_seg]
        more_specs += [SMEM_SPEC, SMEM_SPEC, whole_spec(t_seg.shape)]
        more_out.append(jax.ShapeDtypeStruct((t_rows, t_width), BF16))
        more_scratch += [pltpu.VMEM((t_total, t_width), F32), pltpu.VMEM((BLOCK, t_width), BF16),
                         pltpu.VMEM((BLOCK, t_width), BF16), pltpu.VMEM((t_rows, t_width), BF16)]
    nm = len(more_in)

    def kern(meta_ref, idx_ref, seg_ref, *refs):
        hb, refs = refs[:nh], refs[nh:]
        bl, refs = refs[:nb], refs[nb:]
        fx, refs = refs[:nf], refs[nf:]
        extra, refs = refs[:nm], refs[nm:]
        out, refs = refs[:no], refs[no:]
        last_out, refs = refs[:len(more_out)], refs[len(more_out):]
        tab, acc, buf_0, buf_1, isem = refs[:5]
        stages, sems, scratch = refs[5:5 + ns], refs[5 + ns:5 + 2 * ns], refs[5 + 2 * ns:]
        if late:
            begin, scratch = scratch[0], scratch[1:]
        i = pl.program_id(0)

        @pl.when(i == 0)
        def _():
            copies = [fetch(h, st, sm, parts) for h, st, sm in zip(hb, stages, sems)]
            if init is not None:
                start = pltpu.make_async_copy(hb[init], begin if late else acc.at[pl.ds(0, acc_rows), :], isem)
                start.start()
            if init is None or late:
                zero_rows(acc)
            for o, (_, _, sums) in zip(out, outs):
                if sums:
                    o[...] = jnp.zeros_like(o)
            if then:
                zero_rows(scratch[1])
            build(copies, stages, tab, fx)
            if init is not None and not late:
                start.wait()
            segment_sums(meta_ref, meta_at, idx_ref, seg_ref, tab, acc, (buf_0, buf_1), nc, window, blocks)
            if late:
                start.wait()
            if epilogue is None:
                send_out(acc.at[pl.ds(0, acc_rows), :], out[0], isem)
        if epilogue is not None:
            def part(j, carry):
                at = pl.multiple_of(j * sub, sub)
                row0 = pl.multiple_of(i * tile + at, sub)

                def put(x):
                    put_rows(scratch[0], row0, x, keep)
                a = acc[pl.ds(row0, sub), :]
                if late:
                    a = a + begin[pl.ds(row0, sub), :]
                epilogue(a, [r.at[pl.ds(at, sub), :] for r in bl], fx,
                         [o if sums else o.at[pl.ds(at, sub), :] for o, (_, _, sums) in zip(out, outs)], put)
                return carry
            lax.fori_loop(0, tile // sub, part, 0)

        if pick:
            @pl.when(i == steps - 1)
            def _():
                pick_into(extra[0], scratch[0], scratch[1], peers, slots)
                send_out(scratch[1], last_out[0], isem)
        if then:
            @pl.when(i == steps - 1)
            def _():
                kept, acc_2, buf_2, buf_3, stage = scratch
                segment_sums(extra[0], t_at, extra[1], extra[2], kept, acc_2, (buf_2, buf_3), t_nc, t_window,
                             t_seg.shape[0])
                step = math.gcd(1024, t_rows)

                def part(j, carry):
                    at = pl.multiple_of(j * step, step)
                    stage[pl.ds(at, step), :] = finish(acc_2[pl.ds(at, step), :], fx)
                    return carry
                lax.fori_loop(0, t_rows // step, part, 0)
                send_out(stage, last_out[0], isem)

    out_shape, out_specs = [], []
    for shape, dtype, sums in outs:
        out_shape.append(jax.ShapeDtypeStruct(shape, dtype))
        out_specs.append(HBM_SPEC if epilogue is None else whole_spec(shape) if sums else row_spec(tile, shape[1]))
    return pl.pallas_call(
        kern, name=name, grid=(steps,), out_shape=out_shape + more_out,
        in_specs=([SMEM_SPEC, SMEM_SPEC, whole_spec(seg.shape)] + [HBM_SPEC] * nh
                  + [row_spec(tile, x.shape[1]) for x in blocked] + [whole_spec(x.shape) for x in fixed] + more_specs),
        out_specs=out_specs + [HBM_SPEC] * len(more_out),
        scratch_shapes=([pltpu.VMEM((table_rows * nc, LANES), F32), pltpu.VMEM((acc_total, width), F32),
                         pltpu.VMEM((BLOCK, width), BF16), pltpu.VMEM((BLOCK, width), BF16),
                         pltpu.SemaphoreType.DMA(())]
                        + [pltpu.VMEM(shape, BF16) for shape in sources]
                        + [pltpu.SemaphoreType.DMA((parts,)) for _ in sources] + late_scratch + more_scratch),
        compiler_params=params(), cost_estimate=cost(micros))(meta, idx, seg, *hbm_in, *blocked, *fixed, *more_in)


SHARE = 16


def grad_places(shapes):
    places, at = [], 0
    for rows, width in shapes:
        columns = []
        for _ in range(width // LANES):
            columns.append(at)
            at += -(-rows // SHARE)
        places.append(columns)
    return places, at


def sum_over_devices(grads, sums, total, classes, peers):
    chips = peers // 2
    places, used = grad_places([g.shape for g in grads] + [(SHARE, LANES)])
    rounds = -(-used // peers)
    rows = SHARE * rounds
    widths = [x.shape[1] for x in sums]

    def device(chip, core):
        return chip * 2 + core

    def kern(*refs):
        ng, ns = len(grads), len(sums)
        g_refs, s_refs, out_ref = refs[:ng], refs[ng:ng + ns], refs[ng + ns]
        x_ref, half, mine, got, pair_sem, send_sem, recv_sem, send_2, recv_2 = refs[ng + ns + 1:]
        me = lax.axis_index(GROUP_AXIS)
        chip, core = me // 2, me % 2
        mate = device(chip, 1 - core)

        def at(q):
            unit = q // rounds
            return unit // chips, unit % chips, (q % rounds) * SHARE

        def put(q, value):
            h, c, r = at(q)
            x_ref[h, c, r:r + SHARE, :] = value
        for g, columns in zip(g_refs, places):
            for w, first in enumerate(columns):
                for k in range(g.shape[0] // SHARE):
                    put(first + k, g[k * SHARE:(k + 1) * SHARE, w * LANES:(w + 1) * LANES])
        row = lax.broadcasted_iota(jnp.int32, (SHARE, LANES), 0)
        small, line = jnp.zeros((SHARE, LANES), F32), 0
        for s_ref, width in zip(s_refs, widths):
            for w in range(width // LANES):
                total = jnp.sum(s_ref[:, w * LANES:(w + 1) * LANES], axis=0, keepdims=True)
                small = jnp.where(row == line, total, small)
                line += 1
        put(places[-1][0], small)
        for q in range(used, peers * rounds):
            put(q, jnp.zeros((SHARE, LANES), F32))

        def pair(src, dst, k):
            return pltpu.make_async_remote_copy(src_ref=src, dst_ref=dst, send_sem=pair_sem.at[2 * k],
                                                recv_sem=pair_sem.at[2 * k + 1], device_id=(mate,),
                                                device_id_type=pl.DeviceIdType.MESH)
        first = pair(x_ref.at[1 - core], half, 0)
        first.start()
        first.wait()

        def add(c, carry):
            mine[c] = x_ref[core, c] + half[c]
            return carry
        lax.fori_loop(0, chips, add, 0)

        def share(k):
            to = (chip + k) % chips
            return pltpu.make_async_remote_copy(src_ref=mine.at[to], dst_ref=got.at[chip], send_sem=send_sem.at[k],
                                                recv_sem=recv_sem.at[chip], device_id=(device(to, core),),
                                                device_id_type=pl.DeviceIdType.MESH)

        def landed(k):
            frm = (chip + k) % chips
            return pltpu.make_async_remote_copy(src_ref=mine.at[frm], dst_ref=got.at[frm], send_sem=send_sem.at[k],
                                                recv_sem=recv_sem.at[frm], device_id=(me,),
                                                device_id_type=pl.DeviceIdType.MESH)

        def start(k, carry):
            share(k).start()
            return carry
        lax.fori_loop(1, chips, start, 0)
        got[chip] = mine[chip]

        def settle(k, carry):
            landed(k).wait_recv()
            return carry
        lax.fori_loop(1, chips, settle, 0)

        def more(c, total):
            return total + got[c]
        out_ref[core, chip] = lax.fori_loop(0, chips, more, jnp.zeros((rows, LANES), F32))

        def drain(k, carry):
            share(k).wait_send()
            return carry
        lax.fori_loop(1, chips, drain, 0)

        def give(k):
            return pltpu.make_async_remote_copy(src_ref=out_ref.at[core, chip], dst_ref=out_ref.at[core, chip],
                                                send_sem=send_2.at[k], recv_sem=recv_2.at[chip],
                                                device_id=(device((chip + k) % chips, core),),
                                                device_id_type=pl.DeviceIdType.MESH)

        def given(k):
            frm = (chip + k) % chips
            return pltpu.make_async_remote_copy(src_ref=out_ref.at[core, frm], dst_ref=out_ref.at[core, frm],
                                                send_sem=send_2.at[k], recv_sem=recv_2.at[frm], device_id=(me,),
                                                device_id_type=pl.DeviceIdType.MESH)

        def start_2(k, carry):
            give(k).start()
            return carry
        lax.fori_loop(1, chips, start_2, 0)

        def settle_2(k, carry):
            given(k).wait_recv()
            return carry
        lax.fori_loop(1, chips, settle_2, 0)

        def drain_2(k, carry):
            give(k).wait_send()
            return carry
        lax.fori_loop(1, chips, drain_2, 0)
        last = pair(out_ref.at[core], out_ref.at[core], 1)
        last.start()
        last.wait()

    vmem = pl.BlockSpec(memory_space=pltpu.VMEM)
    shape = (2, chips, rows, LANES)
    full = pl.pallas_call(
        kern, name='sum_all', out_shape=jax.ShapeDtypeStruct(shape, F32),
        in_specs=[vmem] * (len(grads) + len(sums)), out_specs=vmem,
        scratch_shapes=[pltpu.VMEM(shape, F32), pltpu.VMEM(shape[1:], F32), pltpu.VMEM(shape[1:], F32),
                        pltpu.VMEM(shape[1:], F32), pltpu.SemaphoreType.DMA((4,)),
                        pltpu.SemaphoreType.DMA((chips,)), pltpu.SemaphoreType.DMA((chips,)),
                        pltpu.SemaphoreType.DMA((chips,)), pltpu.SemaphoreType.DMA((chips,))],
        compiler_params=pltpu.CompilerParams(has_side_effects=True), cost_estimate=cost(25))(*grads, *sums)

    def unpack_kern(full_ref, total_ref, *outs):
        def part(q):
            unit = q // rounds
            r = (q % rounds) * SHARE
            return full_ref[unit // chips, unit % chips, r:r + SHARE, :]
        for o, columns in zip(outs, places[:-2]):
            for w, first in enumerate(columns):
                for k in range(o.shape[0] // SHARE):
                    o[k * SHARE:(k + 1) * SHARE, w * LANES:(w + 1) * LANES] = part(first + k)
        o_self, o_neigh = outs[len(grads) - 1], outs[len(grads)]
        for k in range(o_self.shape[0] // SHARE):
            both = part(places[-2][0] + k)
            o_self[k * SHARE:(k + 1) * SHARE, :] = both[:, :classes]
            o_neigh[k * SHARE:(k + 1) * SHARE, :] = pltpu.roll(both, LANES - SPREAD, 1)[:, :classes]
        small, line = part(places[-1][0]), 0
        for o, width in zip(outs[len(grads) + 1:-1], widths):
            for w in range(width // LANES):
                wide = min(LANES, o.shape[1] - w * LANES)
                o[:, w * LANES:w * LANES + wide] = small[line:line + 1, :wide]
                line += 1
        outs[-1][...] = jnp.sum(small[line:line + 1, :], axis=1, keepdims=True) / total_ref[...]
    rows_3 = grads[-1].shape[0]
    outs = ([g.shape for g in grads[:-1]] + [(rows_3, classes)] * 2
            + [(1, w) for w in widths[:-2]] + [(1, classes), (1, 1)])
    return pl.pallas_call(unpack_kern, name='unpack_sums', out_shape=[jax.ShapeDtypeStruct(o, F32) for o in outs],
                          in_specs=[vmem, vmem], out_specs=[vmem] * len(outs), cost_estimate=cost(3))(full, total)


def edge_meta(seg_first, seg_last, window, first_block, end_block):
    blocks = seg_first.shape[0]
    unroll = group_of(blocks)
    at = jnp.arange(blocks, dtype=jnp.int32)
    base = seg_first & ~7
    count = jnp.where((at >= first_block) & (at < end_block), (seg_last - base) // window + 1, 1)
    tail = jnp.stack([first_block // unroll, (end_block + unroll - 1) // unroll, jnp.max(count)])
    return [base, count, tail]


def join_meta(*metas):
    offsets, at = [], 0
    for m in metas:
        offsets.append(at)
        at += sum(x.shape[0] for x in m)
    return jnp.concatenate([x for m in metas for x in m]).astype(jnp.int32), offsets


def bits_for(n):
    return max(1, (n - 1).bit_length())


def spread3(w):
    w = jnp.pad(w, ((0, 0), (0, SPREAD - w.shape[1])))
    return jnp.pad(jnp.concatenate([w, w, w], axis=1), ((0, 0), (0, LANES - 3 * SPREAD)))


def lanes_pad(w):
    return jnp.pad(w, ((0, 0), (0, LANES - w.shape[1])))


def solution(mesh):
    peers = mesh.shape[GROUP_AXIS]

    def exchange(x):
        return lax.all_to_all(x, GROUP_AXIS, 0, 0, tiled=True)

    def device_step(features, labels, train_mask, send_idx, src_idx, dst_idx, inv_deg,
                    w_self_1, w_neigh_1, bias_1, w_self_2, w_neigh_2, bias_2,
                    w_self_3, w_neigh_3, bias_3):
        n = features.shape[0]
        slots = send_idx.shape[1]
        halo = peers * slots
        edges = src_idx.shape[0]
        hidden = w_self_1.shape[1]
        classes = w_self_3.shape[1]
        send_flat = send_idx.T.reshape(-1)
        tile = next(t for t in (4096, 1024) if n % t == 0)
        half_tile = tile // 2
        slot_bits = bits_for(halo)
        dst_bits = bits_for(n)
        table = n + halo

        blocks = edges // BLOCK
        halo_blocks = halo // BLOCK
        zero = jnp.int32(0)
        win_e, win_h, win_r = 176, 192, 240
        owned = jnp.sum((src_idx < n).astype(jnp.int32))
        near_end = (owned + BLOCK - 1) // BLOCK
        far_start = owned // BLOCK

        src_bits = bits_for(table)
        far_bit = dst_bits + src_bits
        by_dst = lax.sort(((src_idx >= n).astype(jnp.int32) << far_bit) | (dst_idx << src_bits) | src_idx, is_stable=False)
        src_f = by_dst & ((1 << src_bits) - 1)
        dst_f = (by_dst >> src_bits) & ((1 << dst_bits) - 1)
        is_far = src_f >= n
        src_near = jnp.minimum(src_f, n - 1)
        src_far = jnp.maximum(src_f - n, 0)
        seg_near = jnp.where(is_far, -1, dst_f).reshape(blocks, 1, BLOCK)
        seg_far = jnp.where(is_far, dst_f, -1).reshape(blocks, 1, BLOCK)
        first, last = dst_f[::BLOCK], dst_f[BLOCK - 1::BLOCK]
        meta_f, (near_at, far_at) = join_meta(
            edge_meta(first, jnp.where(is_far[BLOCK - 1::BLOCK], n - 1, last), win_e, zero, near_end),
            edge_meta(jnp.where(is_far[::BLOCK], first, 0), last, win_e, far_start, jnp.int32(blocks)))

        inv = jnp.broadcast_to(inv_deg[:, None], (n, LANES))
        b1 = bias_1.reshape(1, -1)
        b2 = bias_2.reshape(1, -1)
        lane = jnp.arange(LANES, dtype=jnp.int32)
        used = lane < 3 * SPREAD
        folder = jnp.tile(((lane[:, None] % SPREAD == lane[None, :] % SPREAD) & used[:, None] & used[None, :]).astype(BF16),
                          (3, 1))
        b3 = jnp.where(lane < 3 * SPREAD, spread3(bias_3.reshape(1, -1)), -1e30)
        if classes < SPREAD:
            b3 = jnp.where(lane % SPREAD < classes, b3, -1e30)
        target = jnp.where(lane[None, :] < 3 * SPREAD,
                           train_mask[:, None] * (1.0 + (labels[:, None] == lane[None, :] % SPREAD)), 0.0).astype(BF16)
        ws3, wn3 = spread3(w_self_3), spread3(w_neigh_3)
        ws3_t, wn3_t = lanes_pad(w_self_3).T, lanes_pad(w_neigh_3).T

        def rows_of(nc):
            def build(copies, stages, tab, fx):
                unpack(copies[0], stages[0], tab, 0, nc)
            return build

        def near_sums(name, nc, idx, rows, also):
            return edge_call(name, (meta_f, near_at, idx, seg_near), nc, n, n, win_e, [rows.shape], rows_of(nc),
                             [rows] + also, [], [], [((n, nc * LANES), F32, False)], n, tile, None, 20)[0]

        out_1 = pick_rows('send_1', features, send_flat, peers, slots, train_mask.reshape(-1, LANES))
        got_1 = exchange(out_1)
        near_1 = near_sums('near_1', 1, src_near, features, [inv])
        counts = got_1[:, slots, :2].astype(F32)
        total = jnp.sum(counts[:, 0]) * LANES + jnp.sum(counts[:, 1])

        def build_1(copies, stages, tab, fx):
            per = peers // len(copies[0])
            some = math.gcd(per, 8)
            for p in range(len(copies[0])):
                copies[0][p].wait()

                def body(k, carry):
                    q = p * per + k * some
                    rows = stages[0][pl.ds(q, some), :slots, :].reshape(some * slots, LANES)
                    put_rows(tab, q * slots, rows.astype(F32), 1)
                    return carry
                lax.fori_loop(0, per // some, body, 0)

        def epi_1(a, bl, fx, out, put):
            mean = (a * bl[1][...]).astype(BF16)
            z = mm(bl[0][...], fx[0][...]) + mm(mean, fx[1][...]) + fx[2][...]
            out[0][...] = mean
            out[1][...] = jnp.maximum(z, 0.0).astype(BF16)
            put(mean.astype(F32))

        mean_1, hidden_1, out_2 = edge_call(
            'layer_1', (meta_f, far_at, src_far, seg_far), 1, halo, n, win_e, [(peers, slots + TAIL, LANES)], build_1,
            [got_1, near_1], [features, inv], [w_self_1, w_neigh_1, b1],
            [((n, LANES), BF16, False), ((n, hidden), BF16, False)], n, tile, epi_1, 25, init=1, late=True,
            keep=1, pick=(send_flat, peers, slots))

        place = jnp.arange(halo, dtype=jnp.int32)
        keys = jnp.concatenate([(src_idx << dst_bits) | dst_idx,
                                (1 << 30) | (send_flat << slot_bits) | (place % peers * slots + place // peers)])
        keys = lax.optimization_barrier((keys, mean_1))[0]
        ordered = lax.sort(keys, is_stable=False)
        by_src, by_row = ordered[:edges], ordered[edges:] & ((1 << 30) - 1)
        src_s = by_src >> dst_bits
        dst_s = by_src & ((1 << dst_bits) - 1)
        row_s = by_row >> slot_bits
        slot_s = by_row & ((1 << slot_bits) - 1)
        first, last = src_s[::BLOCK], src_s[BLOCK - 1::BLOCK]
        meta_b, (own_at, halo_at, owner_at) = join_meta(
            edge_meta(jnp.minimum(first, n - 1), jnp.minimum(last, n - 1), win_e, zero, near_end),
            edge_meta(jnp.maximum(first - n, 0), jnp.maximum(last - n, 0), win_h, far_start, jnp.int32(blocks)),
            edge_meta(row_s[::BLOCK], row_s[BLOCK - 1::BLOCK], win_r, zero, jnp.int32(halo_blocks)))
        seg_o = src_s.reshape(blocks, 1, BLOCK)
        seg_h = seg_o - n
        seg_r = row_s.reshape(halo_blocks, 1, BLOCK)
        dst_wide = tile_linear(dst_s)

        got_2 = exchange(out_2)
        near_2 = near_sums('near_2', 2, tile_linear(src_near), hidden_1, [])

        def build_2(copies, stages, tab, fx):
            per = peers // len(copies[0])
            some = math.gcd(per, 8)
            for p in range(len(copies[0])):
                copies[0][p].wait()
                copies[1][p].wait()

                def body(k, carry):
                    q = p * per + k * some
                    f = stages[0][pl.ds(q, some), :slots, :].reshape(some * slots, LANES)
                    m = stages[1][pl.ds(q, some)].reshape(some * slots, LANES)
                    z = mm(f, fx[3][...]) + mm(m, fx[4][...]) + fx[5][...]
                    put_rows(tab, q * slots, jnp.maximum(z, 0.0).astype(BF16).astype(F32), 2)
                    return carry
                lax.fori_loop(0, per // some, body, 0)

        def epi_2(a, bl, fx, out, put):
            scale = bl[1][...]
            mean = (a * jnp.concatenate([scale, scale], axis=1)).astype(BF16)
            z = mm(bl[0][...], fx[0][...]) + mm(mean, fx[1][...]) + fx[2][...]
            h = jnp.maximum(z, 0.0).astype(BF16)
            out[0][...] = mean
            out[1][...] = h
            both = mm(h, fx[6][...])
            pieces = split3(both[:, :LANES])
            out[2][...] = pieces
            out[3][...] = both[:, LANES:]
            put(pieces.astype(F32))

        mean_2, hidden_2, proj, logits_self, out_3 = edge_call(
            'layer_2', (meta_f, far_at, tile_linear(src_far), seg_far), 2, halo, n, win_e,
            [(peers, slots + TAIL, LANES), (peers, slots, LANES)], build_2, [got_1, got_2, near_2],
            [hidden_1, inv], [w_self_2, w_neigh_2, b2, w_self_1, w_neigh_1, b1, jnp.concatenate([wn3, ws3], axis=1)],
            [((n, hidden), BF16, False), ((n, hidden), BF16, False), ((n, LANES), BF16, False),
             ((n, LANES), F32, False)], n, half_tile, epi_2, 40, init=2, keep=1, pick=(send_flat, peers, slots))

        got_3 = exchange(out_3).reshape(halo, LANES)
        near_3 = near_sums('near_3', 1, src_near, proj, [target])
        inv_total = (1.0 / total).reshape(1, 1)

        def epi_3(a, bl, fx, out, put):
            scale = bl[1][...]
            z = bl[0][...] + fold3(a * scale, fx[2][...]) + fx[0][...]
            lane = spread_lanes()
            z = jnp.where(lane < 3 * SPREAD, z, -1e30)
            top = jnp.max(z, axis=1, keepdims=True)
            e = jnp.where(lane < SPREAD, jnp.exp(z - top), 0.0)
            lse = top + jnp.log(jnp.sum(e, axis=1, keepdims=True))
            t = bl[2][...].astype(F32)
            hit = t > 1.5
            d = jnp.where(t > 0.5, jnp.exp(z - lse) - jnp.where(hit, 1.0, 0.0), 0.0) * fx[1][...]
            db = d.astype(BF16)
            out[0][...] = db
            pieces = split3(db.astype(F32) * scale)
            out[1][...] = pieces
            put(pieces.astype(F32))
            add_rows(out[2], d)
            add_rows(out[3], jnp.where(hit & (lane < SPREAD), lse - z, 0.0))

        def finish_3(a, fx):
            return split3(fold3(a, fx[2][...]))

        d_bf_3, scaled_3, g_b3, loss_parts, back_3 = edge_call(
            'layer_3', (meta_f, far_at, src_far, seg_far), 1, halo, n, win_e, [(halo, LANES)], rows_of(1), [got_3, near_3],
            [logits_self, inv, target], [b3, jnp.broadcast_to(inv_total, (1, LANES)), folder],
            [((n, LANES), BF16, False), ((n, LANES), BF16, False), ((8, LANES), F32, True), ((8, LANES), F32, True)],
            n, half_tile, epi_3, 30, init=1, late=True, keep=1,
            then=((meta_b, halo_at, dst_s, seg_h), 1, halo, win_h, finish_3))

        ret_3 = exchange(back_3.reshape(peers, slots, LANES)).reshape(halo, LANES)
        own_3 = edge_call('back_3_own', (meta_b, own_at, dst_s, seg_o), 1, n, n, win_e, [(n, LANES)], rows_of(1),
                          [scaled_3], [], [], [((n, LANES), F32, False)], n, tile, None, 20)[0]

        def epi_o3(a, bl, fx, out, put):
            tb = fold3(a, fx[2][...]).astype(BF16)
            d_h = mm(jnp.concatenate([bl[0][...], tb], axis=1), fx[0][...])
            d_pre = jnp.where(bl[1][...].astype(F32) > 0, d_h, 0.0)
            db = d_pre.astype(BF16)
            scale = bl[2][...]
            out[0][...] = tb
            out[1][...] = db
            scaled = (mm(db, fx[1][...]) * jnp.concatenate([scale, scale], axis=1)).astype(BF16)
            out[2][...] = scaled
            put(scaled.astype(F32))
            add_rows(out[3], d_pre)

        def finish_2(a, fx):
            return a.astype(BF16)

        tb_3, d_bf_2, scaled_2, g_b2, back_2 = edge_call(
            'owner_3', (meta_b, owner_at, slot_s, seg_r), 1, halo, n, win_r, [(halo, LANES)], rows_of(1), [ret_3, own_3],
            [d_bf_3, hidden_2, inv], [jnp.concatenate([ws3_t, wn3_t], axis=0), w_neigh_2.T, folder],
            [((n, LANES), BF16, False), ((n, hidden), BF16, False), ((n, hidden), BF16, False), ((8, hidden), F32, True)],
            n, half_tile, epi_o3, 30, init=1, late=True, sub=512, keep=2,
            then=((meta_b, halo_at, dst_wide, seg_h), 2, halo, win_h, finish_2))

        def epi_b2o(a, bl, fx, out, put):
            out[0][...] = a + mm(bl[0][...], fx[0][...])

        ret_2 = exchange(back_2.reshape(peers, slots, hidden)).reshape(halo, hidden)
        own_2 = edge_call('back_2_own', (meta_b, own_at, dst_wide, seg_o), 2, n, n, win_e, [(n, hidden)], rows_of(2),
                          [scaled_2], [d_bf_2], [w_self_2.T], [((n, hidden), F32, False)], n, tile, epi_b2o, 30)[0]

        def epi_o2(a, bl, fx, out, put):
            d_pre = jnp.where(bl[0][...].astype(F32) > 0, a, 0.0)
            out[0][...] = d_pre.astype(BF16)
            add_rows(out[1], d_pre)

        d_bf_1, g_b1 = edge_call(
            'owner_2', (meta_b, owner_at, tile_linear(slot_s), seg_r), 2, halo, n, win_r, [(halo, hidden)], rows_of(2),
            [ret_2, own_2], [hidden_1], [], [((n, hidden), BF16, False), ((8, hidden), F32, True)], n, tile, epi_o2, 25,
            init=1, late=True)

        def contract(a, b):
            return jnp.einsum('nd,ne->de', a, b, preferred_element_type=F32)

        at = jnp.arange(LANES, dtype=jnp.int32)[None, :]
        g_3 = jnp.where(at < SPREAD, contract(hidden_2, d_bf_3), contract(hidden_2, tb_3))
        g1s, g1n, g2s, g2n, g3s, g3n, s1, s2, s3, loss = sum_over_devices(
            [contract(features, d_bf_1), contract(mean_1, d_bf_1), contract(hidden_1, d_bf_2), contract(mean_2, d_bf_2), g_3],
            [g_b1, g_b2, g_b3, loss_parts], total.reshape(1, 1), classes, peers)
        return (loss.reshape(()), g1s, g1n, s1.reshape(-1), g2s, g2n, s2.reshape(-1), g3s, g3n, s3.reshape(-1))

    sharded = P(GROUP_AXIS)
    whole = P()
    return jax.shard_map(device_step, mesh=mesh,
                         in_specs=(sharded,) * 7 + (whole,) * 9,
                         out_specs=(whole,) * 10, check_vma=False)
```

```python
import math

import jax
import jax.numpy as jnp
from jax import lax
from jax.experimental import pallas as pl
from jax.experimental.pallas import tpu as pltpu
from jax.sharding import PartitionSpec as P

GROUP_AXIS = 'gp'
LANES = 128
SPREAD = 40
BLOCK = 128
GROUP = 8
TAIL = 8
F32 = jnp.float32
BF16 = jnp.bfloat16
VMEM_LIMIT = 60 * 2 ** 20

SMEM_SPEC = pl.BlockSpec(memory_space=pltpu.SMEM)
HBM_SPEC = pl.BlockSpec(memory_space=pltpu.HBM)


def whole_spec(shape):
    return pl.BlockSpec(shape, lambda i: (0,) * len(shape))


def row_spec(rows, width):
    return pl.BlockSpec((rows, width), lambda i: (i, 0))


def params():
    return pltpu.CompilerParams(vmem_limit_bytes=VMEM_LIMIT, dimension_semantics=('arbitrary',))


def cost(micros):
    return pl.CostEstimate(flops=int(micros * 4e6), bytes_accessed=int(micros * 1e6), transcendentals=0)


def mm(a, b):
    return jnp.dot(a, b, preferred_element_type=F32)


def tile_linear(row):
    return ((row >> 3) << 4) | (row & 7)


def put_rows(tab, row0, x, nc):
    rows = x.shape[0]
    if nc == 1:
        tab[pl.ds(pl.multiple_of(row0, 8), rows), :] = x
    else:
        for g in range(rows // 8):
            for c in range(nc):
                at = pl.multiple_of((row0 + g * 8) * nc + c * 8, 8)
                tab[pl.ds(at, 8), :] = x[g * 8:g * 8 + 8, c * LANES:(c + 1) * LANES]


def fetch(src, stage, sem, parts):
    rows = src.shape[0] // parts
    copies = [pltpu.make_async_copy(src.at[pl.ds(k * rows, rows)], stage.at[pl.ds(k * rows, rows)], sem.at[k])
              for k in range(parts)]
    for c in copies:
        c.start()
    return copies


def unpack(copies, stage, tab, row0, nc):
    rows = stage.shape[0] // len(copies)
    step = next(d for d in (128, 96, 64, 32, 16) if rows % d == 0)
    for p, c in enumerate(copies):
        c.wait()

        def body(k, carry):
            at = pl.multiple_of(p * rows + k * step, step)
            put_rows(tab, row0 + at, stage[pl.ds(at, step), :].astype(F32), nc)
            return carry
        lax.fori_loop(0, rows // step, body, 0)


def group_of(blocks):
    return next(u for u in (GROUP, 4, 2) if blocks % u == 0)


def zero_rows(acc):
    rows = acc.shape[0]
    step = next(s for s in (256, 128, 64, 32, 16, 8) if rows % s == 0)

    def body(k, carry):
        acc[pl.ds(pl.multiple_of(k * step, step), step), :] = jnp.zeros((step, acc.shape[1]), F32)
        return carry
    lax.fori_loop(0, rows // step, body, 0)


def gather_16(idx, base, first, reach, tab, nc, stride=1):
    sub = lax.broadcasted_iota(jnp.int32, (8, LANES), 0)
    room = idx.shape[0] - (reach - 1) * stride
    halves = [[None, None] for _ in range(nc)]
    for h in range(2):
        for k in range(8):
            at = idx.at[pl.ds((first + h * 8 + k) * stride, room)][base]
            for c in range(nc):
                row = jnp.broadcast_to(tab[pl.ds(at + 8 * c, 1), :], (8, LANES))
                halves[c][h] = row if k == 0 else jnp.where(sub == k, row, halves[c][h])
    return [jnp.concatenate(halves[c], axis=0).astype(BF16) for c in range(nc)]


def segment_sums(meta, meta_at, idx, seg, tab, acc, bufs, nc, window, blocks):
    unroll = group_of(blocks)
    first_trip, end_trip, most = [meta[meta_at + 2 * blocks + k] for k in range(3)]

    def fill(base, first, reach, buf):
        for g in range(BLOCK // 16):
            parts = gather_16(idx, base, first + g * 16, reach, tab, nc)
            for c in range(nc):
                buf[g * 16:g * 16 + 16, c * LANES:(c + 1) * LANES] = parts[c]

    def sums(b, at, buf):
        rows = lax.broadcasted_iota(jnp.int32, (window, BLOCK), 0) + at
        return mm(jnp.where(rows == seg[b], 1.0, 0.0).astype(BF16), buf[...])

    def add(at, x):
        acc[pl.ds(pl.multiple_of(at, 8), window), :] += x

    span = unroll * BLOCK
    last_trip = blocks // unroll - 1
    fill(jnp.minimum(first_trip, last_trip) * span, 0, span, bufs[0])

    def body(t, carry):
        before = None
        for u in range(unroll):
            b = t * unroll + u
            now = (meta[meta_at + b], sums(b, meta[meta_at + b], bufs[u % 2]))
            if u + 1 < unroll:
                fill(t * span, (u + 1) * BLOCK, span, bufs[(u + 1) % 2])
            else:
                fill(jnp.minimum(t + 1, last_trip) * span, 0, span, bufs[0])
            if before is not None:
                add(*before)
            before = now
        add(*before)
        return carry
    lax.fori_loop(first_trip, end_trip, body, 0)

    @pl.when(most > 1)
    def _():
        def again(b, carry):
            count = meta[meta_at + blocks + b]

            @pl.when(count > 1)
            def _():
                fill(b * BLOCK, 0, BLOCK, bufs[0])

                def more(w, c):
                    at = meta[meta_at + b] + w * window
                    add(at, sums(b, at, bufs[0]))
                    return c
                lax.fori_loop(1, count, more, 0)
            return carry
        lax.fori_loop(first_trip * unroll, end_trip * unroll, again, 0)


def spread_lanes():
    return lax.broadcasted_iota(jnp.int32, (1, LANES), 1)


def split3(x):
    hi = x.astype(BF16).astype(F32)
    rest = x - hi
    mid = rest.astype(BF16).astype(F32)
    low = rest - mid
    lane = spread_lanes()
    out = jnp.where(lane < SPREAD, hi, jnp.where(lane < 2 * SPREAD, mid, low))
    return jnp.where(lane < 3 * SPREAD, out, 0.0).astype(BF16)


def pieces3(a):
    hi = a.astype(BF16)
    rest = a - hi.astype(F32)
    mid = rest.astype(BF16)
    low = (rest - mid.astype(F32)).astype(BF16)
    return jnp.concatenate([hi, mid, low], axis=1)


def fold3(a, folder):
    return mm(pieces3(a), folder)


def add_rows(ref, x):
    ref[...] += jnp.sum(x.reshape(x.shape[0] // 8, 8, x.shape[1]), axis=0)


def pick_rows(name, src, idx, peers, slots, mask):
    n = src.shape[0]
    per = math.gcd(peers, 16)
    extra = 0 if mask is None else TAIL
    parts = math.gcd(n // 128, 4)

    def kern(idx_ref, src_ref, *refs):
        if extra:
            mask_ref, out, tab, stage, sem, tail = refs
        else:
            out, tab, stage, sem = refs

        @pl.when(pl.program_id(0) == 0)
        def _():
            copies = fetch(src_ref, stage, sem, parts)
            if extra:
                total = jnp.sum(mask_ref[...], axis=(0, 1), keepdims=True)
                high = jnp.floor(total * (1.0 / LANES))
                first = lax.broadcasted_iota(jnp.int32, (TAIL, LANES), 0) == 0
                lane = lax.broadcasted_iota(jnp.int32, (TAIL, LANES), 1)
                digits = jnp.where(lane == 0, high, jnp.where(lane == 1, total - high * LANES, 0.0))
                tail[...] = jnp.where(first, digits, 0.0).astype(BF16)
            unpack(copies, stage, tab, 0, 1)
        first = pl.program_id(0) * per

        def body(p, carry):
            for g in range(slots // 16):
                out[p, g * 16:g * 16 + 16, :] = gather_16(idx_ref, first + p, g * 16, slots, tab, 1, peers)[0]
            if extra:
                out[p, slots:slots + extra, :] = tail[...]
            return carry
        lax.fori_loop(0, per, body, 0)

    operands = [idx, src] + ([mask] if extra else [])
    specs = [SMEM_SPEC, HBM_SPEC] + ([whole_spec(mask.shape)] if extra else [])
    return pl.pallas_call(
        kern, name=name, grid=(peers // per,),
        out_shape=jax.ShapeDtypeStruct((peers, slots + extra, LANES), BF16),
        in_specs=specs,
        out_specs=pl.BlockSpec((per, slots + extra, LANES), lambda i: (i, 0, 0)),
        scratch_shapes=([pltpu.VMEM((n, LANES), F32), pltpu.VMEM((n, LANES), BF16), pltpu.SemaphoreType.DMA((parts,))]
                        + ([pltpu.VMEM((TAIL, LANES), BF16)] if extra else [])),
        compiler_params=params(), cost_estimate=cost(10))(*operands)


def pick_into(idx, tab, stage, peers, slots):
    def body(p, carry):
        for g in range(slots // 16):
            stage[p, g * 16:g * 16 + 16, :] = gather_16(idx, p, g * 16, slots, tab, 1, peers)[0]
        return carry
    lax.fori_loop(0, peers, body, 0)


def send_out(stage, out, sem):
    done = pltpu.make_async_copy(stage, out, sem)
    done.start()
    done.wait()


def edge_call(name, edges, nc, table_rows, acc_rows, window, sources, build, hbm_in, blocked, fixed, outs, rows_out,
              tile, epilogue, micros, init=None, late=False, sub=1024, keep=0, pick=None, then=None):
    meta, meta_at, idx, seg = edges
    blocks = seg.shape[0]
    width = nc * LANES
    nh, nb, nf, no, ns = len(hbm_in), len(blocked), len(fixed), len(outs), len(sources)
    acc_total = -(-(acc_rows + window) // 256) * 256
    parts = 4
    steps = 1 if epilogue is None else rows_out // tile
    sub = math.gcd(sub, tile)
    more_in, more_specs, more_out, more_scratch = [], [], [], []
    late_scratch = [pltpu.VMEM((acc_rows, width), F32)] if late else []
    if keep:
        more_scratch.append(pltpu.VMEM((rows_out * keep, LANES), F32))
    if pick:
        p_idx, peers, slots = pick
        more_in.append(p_idx)
        more_specs.append(SMEM_SPEC)
        more_out.append(jax.ShapeDtypeStruct((peers, slots, LANES), BF16))
        more_scratch.append(pltpu.VMEM((peers, slots, LANES), BF16))
    if then:
        (t_meta, t_at, t_idx, t_seg), t_nc, t_rows, t_window, finish = then
        t_width = t_nc * LANES
        t_total = -(-(t_rows + t_window) // 256) * 256
        more_in += [t_meta, t_idx, t_seg]
        more_specs += [SMEM_SPEC, SMEM_SPEC, whole_spec(t_seg.shape)]
        more_out.append(jax.ShapeDtypeStruct((t_rows, t_width), BF16))
        more_scratch += [pltpu.VMEM((t_total, t_width), F32), pltpu.VMEM((BLOCK, t_width), BF16),
                         pltpu.VMEM((BLOCK, t_width), BF16), pltpu.VMEM((t_rows, t_width), BF16)]
    nm = len(more_in)

    def kern(meta_ref, idx_ref, seg_ref, *refs):
        hb, refs = refs[:nh], refs[nh:]
        bl, refs = refs[:nb], refs[nb:]
        fx, refs = refs[:nf], refs[nf:]
        extra, refs = refs[:nm], refs[nm:]
        out, refs = refs[:no], refs[no:]
        last_out, refs = refs[:len(more_out)], refs[len(more_out):]
        tab, acc, buf_0, buf_1, isem = refs[:5]
        stages, sems, scratch = refs[5:5 + ns], refs[5 + ns:5 + 2 * ns], refs[5 + 2 * ns:]
        if late:
            begin, scratch = scratch[0], scratch[1:]
        i = pl.program_id(0)

        @pl.when(i == 0)
        def _():
            copies = [fetch(h, st, sm, parts) for h, st, sm in zip(hb, stages, sems)]
            if init is not None:
                start = pltpu.make_async_copy(hb[init], begin if late else acc.at[pl.ds(0, acc_rows), :], isem)
                start.start()
            if init is None or late:
                zero_rows(acc)
            for o, (_, _, sums) in zip(out, outs):
                if sums:
                    o[...] = jnp.zeros_like(o)
            if then:
                zero_rows(scratch[1])
            build(copies, stages, tab, fx)
            if init is not None and not late:
                start.wait()
            segment_sums(meta_ref, meta_at, idx_ref, seg_ref, tab, acc, (buf_0, buf_1), nc, window, blocks)
            if late:
                start.wait()
            if epilogue is None:
                send_out(acc.at[pl.ds(0, acc_rows), :], out[0], isem)
        if epilogue is not None:
            def part(j, carry):
                at = pl.multiple_of(j * sub, sub)
                row0 = pl.multiple_of(i * tile + at, sub)

                def put(x):
                    put_rows(scratch[0], row0, x, keep)
                a = acc[pl.ds(row0, sub), :]
                if late:
                    a = a + begin[pl.ds(row0, sub), :]
                epilogue(a, [r.at[pl.ds(at, sub), :] for r in bl], fx,
                         [o if sums else o.at[pl.ds(at, sub), :] for o, (_, _, sums) in zip(out, outs)], put)
                return carry
            lax.fori_loop(0, tile // sub, part, 0)

        if pick:
            @pl.when(i == steps - 1)
            def _():
                pick_into(extra[0], scratch[0], scratch[1], peers, slots)
                send_out(scratch[1], last_out[0], isem)
        if then:
            @pl.when(i == steps - 1)
            def _():
                kept, acc_2, buf_2, buf_3, stage = scratch
                segment_sums(extra[0], t_at, extra[1], extra[2], kept, acc_2, (buf_2, buf_3), t_nc, t_window,
                             t_seg.shape[0])
                step = math.gcd(1024, t_rows)

                def part(j, carry):
                    at = pl.multiple_of(j * step, step)
                    stage[pl.ds(at, step), :] = finish(acc_2[pl.ds(at, step), :], fx)
                    return carry
                lax.fori_loop(0, t_rows // step, part, 0)
                send_out(stage, last_out[0], isem)

    out_shape, out_specs = [], []
    for shape, dtype, sums in outs:
        out_shape.append(jax.ShapeDtypeStruct(shape, dtype))
        out_specs.append(HBM_SPEC if epilogue is None else whole_spec(shape) if sums else row_spec(tile, shape[1]))
    return pl.pallas_call(
        kern, name=name, grid=(steps,), out_shape=out_shape + more_out,
        in_specs=([SMEM_SPEC, SMEM_SPEC, whole_spec(seg.shape)] + [HBM_SPEC] * nh
                  + [row_spec(tile, x.shape[1]) for x in blocked] + [whole_spec(x.shape) for x in fixed] + more_specs),
        out_specs=out_specs + [HBM_SPEC] * len(more_out),
        scratch_shapes=([pltpu.VMEM((table_rows * nc, LANES), F32), pltpu.VMEM((acc_total, width), F32),
                         pltpu.VMEM((BLOCK, width), BF16), pltpu.VMEM((BLOCK, width), BF16),
                         pltpu.SemaphoreType.DMA(())]
                        + [pltpu.VMEM(shape, BF16) for shape in sources]
                        + [pltpu.SemaphoreType.DMA((parts,)) for _ in sources] + late_scratch + more_scratch),
        compiler_params=params(), cost_estimate=cost(micros))(meta, idx, seg, *hbm_in, *blocked, *fixed, *more_in)


SHARE = 16


def grad_places(shapes):
    places, at = [], 0
    for rows, width in shapes:
        columns = []
        for _ in range(width // LANES):
            columns.append(at)
            at += -(-rows // SHARE)
        places.append(columns)
    return places, at


def sum_over_devices(grads, sums, total, classes, peers):
    chips = peers // 2
    places, used = grad_places([g.shape for g in grads] + [(SHARE, LANES)])
    rounds = -(-used // peers)
    rows = SHARE * rounds
    widths = [x.shape[1] for x in sums]

    def device(chip, core):
        return chip * 2 + core

    def kern(*refs):
        ng, ns = len(grads), len(sums)
        g_refs, s_refs, out_ref = refs[:ng], refs[ng:ng + ns], refs[ng + ns]
        x_ref, half, mine, got, pair_sem, send_sem, recv_sem, send_2, recv_2 = refs[ng + ns + 1:]
        me = lax.axis_index(GROUP_AXIS)
        chip, core = me // 2, me % 2
        mate = device(chip, 1 - core)
        barrier = pltpu.get_barrier_semaphore()

        def hello(to):
            pl.semaphore_signal(barrier, inc=1, device_id=(to,), device_id_type=pl.DeviceIdType.MESH)

        def greet(k, carry):
            hello(device((chip + k) % chips, core))
            return carry
        lax.fori_loop(1, chips, greet, 0)
        hello(mate)

        def at(q):
            unit = q // rounds
            return unit // chips, unit % chips, (q % rounds) * SHARE

        def put(q, value):
            h, c, r = at(q)
            x_ref[h, c, r:r + SHARE, :] = value
        for g, columns in zip(g_refs, places):
            for w, first in enumerate(columns):
                for k in range(g.shape[0] // SHARE):
                    put(first + k, g[k * SHARE:(k + 1) * SHARE, w * LANES:(w + 1) * LANES])
        row = lax.broadcasted_iota(jnp.int32, (SHARE, LANES), 0)
        small, line = jnp.zeros((SHARE, LANES), F32), 0
        for s_ref, width in zip(s_refs, widths):
            for w in range(width // LANES):
                total = jnp.sum(s_ref[:, w * LANES:(w + 1) * LANES], axis=0, keepdims=True)
                small = jnp.where(row == line, total, small)
                line += 1
        put(places[-1][0], small)
        for q in range(used, peers * rounds):
            put(q, jnp.zeros((SHARE, LANES), F32))

        def pair(src, dst, k):
            return pltpu.make_async_remote_copy(src_ref=src, dst_ref=dst, send_sem=pair_sem.at[2 * k],
                                                recv_sem=pair_sem.at[2 * k + 1], device_id=(mate,),
                                                device_id_type=pl.DeviceIdType.MESH)
        pl.semaphore_wait(barrier, chips)
        first = pair(x_ref.at[1 - core], half, 0)
        first.start()
        first.wait()

        def add(c, carry):
            mine[c] = x_ref[core, c] + half[c]
            return carry
        lax.fori_loop(0, chips, add, 0)

        def share(k):
            to = (chip + k) % chips
            return pltpu.make_async_remote_copy(src_ref=mine.at[to], dst_ref=got.at[chip], send_sem=send_sem.at[k],
                                                recv_sem=recv_sem.at[chip], device_id=(device(to, core),),
                                                device_id_type=pl.DeviceIdType.MESH)

        def landed(k):
            frm = (chip + k) % chips
            return pltpu.make_async_remote_copy(src_ref=mine.at[frm], dst_ref=got.at[frm], send_sem=send_sem.at[k],
                                                recv_sem=recv_sem.at[frm], device_id=(me,),
                                                device_id_type=pl.DeviceIdType.MESH)

        def start(k, carry):
            share(k).start()
            return carry
        lax.fori_loop(1, chips, start, 0)
        got[chip] = mine[chip]

        def settle(k, carry):
            landed(k).wait_recv()
            return carry
        lax.fori_loop(1, chips, settle, 0)

        def more(c, total):
            return total + got[c]
        out_ref[core, chip] = lax.fori_loop(0, chips, more, jnp.zeros((rows, LANES), F32))

        def drain(k, carry):
            share(k).wait_send()
            return carry
        lax.fori_loop(1, chips, drain, 0)

        def give(k):
            return pltpu.make_async_remote_copy(src_ref=out_ref.at[core, chip], dst_ref=out_ref.at[core, chip],
                                                send_sem=send_2.at[k], recv_sem=recv_2.at[chip],
                                                device_id=(device((chip + k) % chips, core),),
                                                device_id_type=pl.DeviceIdType.MESH)

        def given(k):
            frm = (chip + k) % chips
            return pltpu.make_async_remote_copy(src_ref=out_ref.at[core, frm], dst_ref=out_ref.at[core, frm],
                                                send_sem=send_2.at[k], recv_sem=recv_2.at[frm], device_id=(me,),
                                                device_id_type=pl.DeviceIdType.MESH)

        def start_2(k, carry):
            give(k).start()
            return carry
        lax.fori_loop(1, chips, start_2, 0)

        def settle_2(k, carry):
            given(k).wait_recv()
            return carry
        lax.fori_loop(1, chips, settle_2, 0)

        def drain_2(k, carry):
            give(k).wait_send()
            return carry
        lax.fori_loop(1, chips, drain_2, 0)
        last = pair(out_ref.at[core], out_ref.at[core], 1)
        last.start()
        last.wait()

    vmem = pl.BlockSpec(memory_space=pltpu.VMEM)
    shape = (2, chips, rows, LANES)
    full = pl.pallas_call(
        kern, name='sum_all', out_shape=jax.ShapeDtypeStruct(shape, F32),
        in_specs=[vmem] * (len(grads) + len(sums)), out_specs=vmem,
        scratch_shapes=[pltpu.VMEM(shape, F32), pltpu.VMEM(shape[1:], F32), pltpu.VMEM(shape[1:], F32),
                        pltpu.VMEM(shape[1:], F32), pltpu.SemaphoreType.DMA((4,)),
                        pltpu.SemaphoreType.DMA((chips,)), pltpu.SemaphoreType.DMA((chips,)),
                        pltpu.SemaphoreType.DMA((chips,)), pltpu.SemaphoreType.DMA((chips,))],
        compiler_params=pltpu.CompilerParams(collective_id=0, has_side_effects=True), cost_estimate=cost(25))(*grads, *sums)

    def unpack_kern(full_ref, total_ref, *outs):
        def part(q):
            unit = q // rounds
            r = (q % rounds) * SHARE
            return full_ref[unit // chips, unit % chips, r:r + SHARE, :]

        def move(o, columns, skip):
            for w, first in enumerate(columns):
                for k in range(o.shape[0] // SHARE):
                    o[k * SHARE:(k + 1) * SHARE, w * LANES:(w + 1) * LANES] = part(first + skip + k)
        move(outs[0], places[0], 0)
        move(outs[1], places[0], outs[0].shape[0] // SHARE)
        for o, columns in zip(outs[2:], places[1:-2]):
            move(o, columns, 0)
        both = jnp.concatenate([part(places[-2][0] + k) for k in range(rows_3 // SHARE)], axis=0).T
        outs[ng][...] = both[:classes, :]
        outs[ng + 1][...] = both[SPREAD:SPREAD + classes, :]
        small, line = part(places[-1][0]), 0
        for o, width in zip(outs[ng + 2:-1], widths):
            for w in range(width // LANES):
                wide = min(LANES, o.shape[1] - w * LANES)
                o[:, w * LANES:w * LANES + wide] = small[line:line + 1, :wide]
                line += 1
        outs[-1][...] = jnp.sum(small[line:line + 1, :], axis=1, keepdims=True) / total_ref[...]
    ng = len(grads)
    rows_3 = grads[-1].shape[0]
    rows_1, width_1 = grads[0].shape
    outs = ([(rows_1 // 2, width_1)] * 2 + [g.shape for g in grads[1:-1]] + [(classes, rows_3)] * 2
            + [(1, w) for w in widths[:-2]] + [(1, classes), (1, 1)])
    return pl.pallas_call(unpack_kern, name='unpack_sums', out_shape=[jax.ShapeDtypeStruct(o, F32) for o in outs],
                          in_specs=[vmem, vmem], out_specs=[vmem] * len(outs), cost_estimate=cost(3))(full, total)


def edge_meta(seg_first, seg_last, window, first_block, end_block):
    blocks = seg_first.shape[0]
    unroll = group_of(blocks)
    at = jnp.arange(blocks, dtype=jnp.int32)
    base = seg_first & ~7
    count = jnp.where((at >= first_block) & (at < end_block), (seg_last - base) // window + 1, 1)
    tail = jnp.stack([first_block // unroll, (end_block + unroll - 1) // unroll, jnp.max(count)])
    return [base, count, tail]


def join_meta(*metas):
    offsets, at = [], 0
    for m in metas:
        offsets.append(at)
        at += sum(x.shape[0] for x in m)
    return jnp.concatenate([x for m in metas for x in m]).astype(jnp.int32), offsets


def bits_for(n):
    return max(1, (n - 1).bit_length())


def spread3(w):
    w = jnp.pad(w, ((0, 0), (0, SPREAD - w.shape[1])))
    return jnp.pad(jnp.concatenate([w, w, w], axis=1), ((0, 0), (0, LANES - 3 * SPREAD)))


def lanes_pad(w):
    return jnp.pad(w, ((0, 0), (0, LANES - w.shape[1])))


def solution(mesh):
    peers = mesh.shape[GROUP_AXIS]

    def exchange(x):
        return lax.all_to_all(x, GROUP_AXIS, 0, 0, tiled=True)

    def device_step(features, labels, train_mask, send_idx, src_idx, dst_idx, inv_deg,
                    w_self_1, w_neigh_1, bias_1, w_self_2, w_neigh_2, bias_2,
                    w_self_3, w_neigh_3, bias_3):
        n = features.shape[0]
        slots = send_idx.shape[1]
        halo = peers * slots
        edges = src_idx.shape[0]
        hidden = w_self_1.shape[1]
        classes = w_self_3.shape[1]
        send_flat = send_idx.T.reshape(-1)
        tile = next(t for t in (4096, 1024) if n % t == 0)
        half_tile = tile // 2
        slot_bits = bits_for(halo)
        dst_bits = bits_for(n)
        table = n + halo

        blocks = edges // BLOCK
        halo_blocks = halo // BLOCK
        zero = jnp.int32(0)
        win_e, win_h, win_r = 176, 192, 240
        owned = jnp.sum((src_idx < n).astype(jnp.int32))
        near_end = (owned + BLOCK - 1) // BLOCK
        far_start = owned // BLOCK

        src_bits = bits_for(table)
        far_bit = dst_bits + src_bits
        by_dst = lax.sort(((src_idx >= n).astype(jnp.int32) << far_bit) | (dst_idx << src_bits) | src_idx, is_stable=False)
        src_f = by_dst & ((1 << src_bits) - 1)
        dst_f = (by_dst >> src_bits) & ((1 << dst_bits) - 1)
        is_far = src_f >= n
        src_near = jnp.minimum(src_f, n - 1)
        src_far = jnp.maximum(src_f - n, 0)
        seg_near = jnp.where(is_far, -1, dst_f).reshape(blocks, 1, BLOCK)
        seg_far = jnp.where(is_far, dst_f, -1).reshape(blocks, 1, BLOCK)
        first, last = dst_f[::BLOCK], dst_f[BLOCK - 1::BLOCK]
        meta_f, (near_at, far_at) = join_meta(
            edge_meta(first, jnp.where(is_far[BLOCK - 1::BLOCK], n - 1, last), win_e, zero, near_end),
            edge_meta(jnp.where(is_far[::BLOCK], first, 0), last, win_e, far_start, jnp.int32(blocks)))

        inv = jnp.broadcast_to(inv_deg[:, None], (n, LANES))
        b1 = bias_1.reshape(1, -1)
        b2 = bias_2.reshape(1, -1)
        lane = jnp.arange(LANES, dtype=jnp.int32)
        used = lane < 3 * SPREAD
        folder = jnp.tile(((lane[:, None] % SPREAD == lane[None, :] % SPREAD) & used[:, None] & used[None, :]).astype(BF16),
                          (3, 1))
        b3 = jnp.where(lane < 3 * SPREAD, spread3(bias_3.reshape(1, -1)), -1e30)
        if classes < SPREAD:
            b3 = jnp.where(lane % SPREAD < classes, b3, -1e30)
        target = jnp.where(lane[None, :] < 3 * SPREAD,
                           train_mask[:, None] * (1.0 + (labels[:, None] == lane[None, :] % SPREAD)), 0.0).astype(BF16)
        ws3, wn3 = spread3(w_self_3), spread3(w_neigh_3)
        ws3_t, wn3_t = lanes_pad(w_self_3).T, lanes_pad(w_neigh_3).T

        def rows_of(nc):
            def build(copies, stages, tab, fx):
                unpack(copies[0], stages[0], tab, 0, nc)
            return build

        def near_sums(name, nc, idx, rows, also):
            return edge_call(name, (meta_f, near_at, idx, seg_near), nc, n, n, win_e, [rows.shape], rows_of(nc),
                             [rows] + also, [], [], [((n, nc * LANES), F32, False)], n, tile, None, 20)[0]

        out_1 = pick_rows('send_1', features, send_flat, peers, slots, train_mask.reshape(-1, LANES))
        got_1 = exchange(out_1)
        near_1 = near_sums('near_1', 1, src_near, features, [inv])
        counts = got_1[:, slots, :2].astype(F32)
        total = jnp.sum(counts[:, 0]) * LANES + jnp.sum(counts[:, 1])

        def build_1(copies, stages, tab, fx):
            per = peers // len(copies[0])
            some = math.gcd(per, 8)
            for p in range(len(copies[0])):
                copies[0][p].wait()

                def body(k, carry):
                    q = p * per + k * some
                    rows = stages[0][pl.ds(q, some), :slots, :].reshape(some * slots, LANES)
                    put_rows(tab, q * slots, rows.astype(F32), 1)
                    return carry
                lax.fori_loop(0, per // some, body, 0)

        def epi_1(a, bl, fx, out, put):
            mean = (a * bl[1][...]).astype(BF16)
            z = mm(bl[0][...], fx[0][...]) + mm(mean, fx[1][...]) + fx[2][...]
            out[0][...] = mean
            out[1][...] = jnp.maximum(z, 0.0).astype(BF16)
            put(mean.astype(F32))

        mean_1, hidden_1, out_2 = edge_call(
            'layer_1', (meta_f, far_at, src_far, seg_far), 1, halo, n, win_e, [(peers, slots + TAIL, LANES)], build_1,
            [got_1, near_1], [features, inv], [w_self_1, w_neigh_1, b1],
            [((n, LANES), BF16, False), ((n, hidden), BF16, False)], n, tile, epi_1, 25, init=1, late=True,
            keep=1, pick=(send_flat, peers, slots))

        place = jnp.arange(halo, dtype=jnp.int32)
        keys = jnp.concatenate([(src_idx << dst_bits) | dst_idx,
                                (1 << 30) | (send_flat << slot_bits) | (place % peers * slots + place // peers)])
        keys = lax.optimization_barrier((keys, mean_1))[0]
        ordered = lax.sort(keys, is_stable=False)
        by_src, by_row = ordered[:edges], ordered[edges:] & ((1 << 30) - 1)
        src_s = by_src >> dst_bits
        dst_s = by_src & ((1 << dst_bits) - 1)
        row_s = by_row >> slot_bits
        slot_s = by_row & ((1 << slot_bits) - 1)
        first, last = src_s[::BLOCK], src_s[BLOCK - 1::BLOCK]
        meta_b, (own_at, halo_at, owner_at) = join_meta(
            edge_meta(jnp.minimum(first, n - 1), jnp.minimum(last, n - 1), win_e, zero, near_end),
            edge_meta(jnp.maximum(first - n, 0), jnp.maximum(last - n, 0), win_h, far_start, jnp.int32(blocks)),
            edge_meta(row_s[::BLOCK], row_s[BLOCK - 1::BLOCK], win_r, zero, jnp.int32(halo_blocks)))
        seg_o = src_s.reshape(blocks, 1, BLOCK)
        seg_h = seg_o - n
        seg_r = row_s.reshape(halo_blocks, 1, BLOCK)
        dst_wide = tile_linear(dst_s)

        got_2 = exchange(out_2)
        near_2 = near_sums('near_2', 2, tile_linear(src_near), hidden_1, [])

        def build_2(copies, stages, tab, fx):
            per = peers // len(copies[0])
            some = math.gcd(per, 8)
            for p in range(len(copies[0])):
                copies[0][p].wait()
                copies[1][p].wait()

                def body(k, carry):
                    q = p * per + k * some
                    f = stages[0][pl.ds(q, some), :slots, :].reshape(some * slots, LANES)
                    m = stages[1][pl.ds(q, some)].reshape(some * slots, LANES)
                    z = mm(f, fx[3][...]) + mm(m, fx[4][...]) + fx[5][...]
                    put_rows(tab, q * slots, jnp.maximum(z, 0.0).astype(BF16).astype(F32), 2)
                    return carry
                lax.fori_loop(0, per // some, body, 0)

        def epi_2(a, bl, fx, out, put):
            scale = bl[1][...]
            mean = (a * jnp.concatenate([scale, scale], axis=1)).astype(BF16)
            z = mm(bl[0][...], fx[0][...]) + mm(mean, fx[1][...]) + fx[2][...]
            h = jnp.maximum(z, 0.0).astype(BF16)
            out[0][...] = mean
            out[1][...] = h
            both = mm(h, fx[6][...])
            pieces = split3(both[:, :LANES])
            out[2][...] = pieces
            out[3][...] = both[:, LANES:]
            put(pieces.astype(F32))

        mean_2, hidden_2, proj, logits_self, out_3 = edge_call(
            'layer_2', (meta_f, far_at, tile_linear(src_far), seg_far), 2, halo, n, win_e,
            [(peers, slots + TAIL, LANES), (peers, slots, LANES)], build_2, [got_1, got_2, near_2],
            [hidden_1, inv], [w_self_2, w_neigh_2, b2, w_self_1, w_neigh_1, b1, jnp.concatenate([wn3, ws3], axis=1)],
            [((n, hidden), BF16, False), ((n, hidden), BF16, False), ((n, LANES), BF16, False),
             ((n, LANES), F32, False)], n, half_tile, epi_2, 40, init=2, keep=1, pick=(send_flat, peers, slots))

        got_3 = exchange(out_3).reshape(halo, LANES)
        near_3 = near_sums('near_3', 1, src_near, proj, [target])
        inv_total = (1.0 / total).reshape(1, 1)

        def epi_3(a, bl, fx, out, put):
            scale = bl[1][...]
            z = bl[0][...] + fold3(a * scale, fx[2][...]) + fx[0][...]
            lane = spread_lanes()
            z = jnp.where(lane < 3 * SPREAD, z, -1e30)
            top = jnp.max(z, axis=1, keepdims=True)
            e = jnp.where(lane < SPREAD, jnp.exp(z - top), 0.0)
            lse = top + jnp.log(jnp.sum(e, axis=1, keepdims=True))
            t = bl[2][...].astype(F32)
            hit = t > 1.5
            d = jnp.where(t > 0.5, jnp.exp(z - lse) - jnp.where(hit, 1.0, 0.0), 0.0) * fx[1][...]
            db = d.astype(BF16)
            out[0][...] = db
            pieces = split3(db.astype(F32) * scale)
            out[1][...] = pieces
            put(pieces.astype(F32))
            add_rows(out[2], d)
            add_rows(out[3], jnp.where(hit & (lane < SPREAD), lse - z, 0.0))

        def finish_3(a, fx):
            return split3(fold3(a, fx[2][...]))

        d_bf_3, scaled_3, g_b3, loss_parts, back_3 = edge_call(
            'layer_3', (meta_f, far_at, src_far, seg_far), 1, halo, n, win_e, [(halo, LANES)], rows_of(1), [got_3, near_3],
            [logits_self, inv, target], [b3, jnp.broadcast_to(inv_total, (1, LANES)), folder],
            [((n, LANES), BF16, False), ((n, LANES), BF16, False), ((8, LANES), F32, True), ((8, LANES), F32, True)],
            n, half_tile, epi_3, 30, init=1, late=True, keep=1,
            then=((meta_b, halo_at, dst_s, seg_h), 1, halo, win_h, finish_3))

        ret_3 = exchange(back_3.reshape(peers, slots, LANES)).reshape(halo, LANES)
        own_3 = edge_call('back_3_own', (meta_b, own_at, dst_s, seg_o), 1, n, n, win_e, [(n, LANES)], rows_of(1),
                          [scaled_3], [], [], [((n, LANES), F32, False)], n, tile, None, 20)[0]

        def epi_o3(a, bl, fx, out, put):
            tb = fold3(a, fx[2][...]).astype(BF16)
            d_h = mm(jnp.concatenate([bl[0][...], tb], axis=1), fx[0][...])
            d_pre = jnp.where(bl[1][...].astype(F32) > 0, d_h, 0.0)
            db = d_pre.astype(BF16)
            scale = bl[2][...]
            out[0][...] = tb
            out[1][...] = db
            scaled = (mm(db, fx[1][...]) * jnp.concatenate([scale, scale], axis=1)).astype(BF16)
            out[2][...] = scaled
            put(scaled.astype(F32))
            add_rows(out[3], d_pre)

        def finish_2(a, fx):
            return a.astype(BF16)

        tb_3, d_bf_2, scaled_2, g_b2, back_2 = edge_call(
            'owner_3', (meta_b, owner_at, slot_s, seg_r), 1, halo, n, win_r, [(halo, LANES)], rows_of(1), [ret_3, own_3],
            [d_bf_3, hidden_2, inv], [jnp.concatenate([ws3_t, wn3_t], axis=0), w_neigh_2.T, folder],
            [((n, LANES), BF16, False), ((n, hidden), BF16, False), ((n, hidden), BF16, False), ((8, hidden), F32, True)],
            n, half_tile, epi_o3, 30, init=1, late=True, sub=512, keep=2,
            then=((meta_b, halo_at, dst_wide, seg_h), 2, halo, win_h, finish_2))

        def epi_b2o(a, bl, fx, out, put):
            out[0][...] = a + mm(bl[0][...], fx[0][...])

        ret_2 = exchange(back_2.reshape(peers, slots, hidden)).reshape(halo, hidden)
        own_2 = edge_call('back_2_own', (meta_b, own_at, dst_wide, seg_o), 2, n, n, win_e, [(n, hidden)], rows_of(2),
                          [scaled_2], [d_bf_2], [w_self_2.T], [((n, hidden), F32, False)], n, tile, epi_b2o, 30)[0]

        def epi_o2(a, bl, fx, out, put):
            d_pre = jnp.where(bl[0][...].astype(F32) > 0, a, 0.0)
            inputs = jnp.concatenate([bl[1][...], bl[2][...]], axis=1)
            out[0][...] += lax.dot_general(inputs, d_pre.astype(BF16), (((0,), (0,)), ((), ())),
                                           preferred_element_type=F32)
            add_rows(out[1], d_pre)

        g_1, g_b1 = edge_call(
            'owner_2', (meta_b, owner_at, tile_linear(slot_s), seg_r), 2, halo, n, win_r, [(halo, hidden)], rows_of(2),
            [ret_2, own_2], [hidden_1, features, mean_1], [],
            [((2 * LANES, hidden), F32, True), ((8, hidden), F32, True)], n, half_tile, epi_o2, 25, init=1, late=True)

        def contract(a, b):
            return jnp.einsum('nd,ne->de', a, b, preferred_element_type=F32)

        at = jnp.arange(LANES, dtype=jnp.int32)[None, :]
        g_3 = jnp.where(at < SPREAD, contract(hidden_2, d_bf_3), contract(hidden_2, tb_3))
        g1s, g1n, g2s, g2n, g3s, g3n, s1, s2, s3, loss = sum_over_devices(
            [g_1, contract(hidden_1, d_bf_2), contract(mean_2, d_bf_2), g_3],
            [g_b1, g_b2, g_b3, loss_parts], total.reshape(1, 1), classes, peers)
        return (loss.reshape(()), g1s, g1n, s1.reshape(-1), g2s, g2n, s2.reshape(-1), g3s.T, g3n.T, s3.reshape(-1))

    sharded = P(GROUP_AXIS)
    whole = P()
    return jax.shard_map(device_step, mesh=mesh,
                         in_specs=(sharded,) * 7 + (whole,) * 9,
                         out_specs=(whole,) * 10, check_vma=False)
```

```python
import math

import jax
import jax.numpy as jnp
from jax import lax
from jax.experimental import pallas as pl
from jax.experimental.pallas import tpu as pltpu
from jax.sharding import PartitionSpec as P

GROUP_AXIS = 'gp'
LANES = 128
SPREAD = 40
BLOCK = 128
GROUP = 8
TAIL = 8
F32 = jnp.float32
BF16 = jnp.bfloat16
VMEM_LIMIT = 60 * 2 ** 20

SMEM_SPEC = pl.BlockSpec(memory_space=pltpu.SMEM)
HBM_SPEC = pl.BlockSpec(memory_space=pltpu.HBM)


def whole_spec(shape):
    return pl.BlockSpec(shape, lambda i: (0,) * len(shape))


def row_spec(rows, width):
    return pl.BlockSpec((rows, width), lambda i: (i, 0))


def params():
    return pltpu.CompilerParams(vmem_limit_bytes=VMEM_LIMIT, dimension_semantics=('arbitrary',))


def cost(micros):
    return pl.CostEstimate(flops=int(micros * 4e6), bytes_accessed=int(micros * 1e6), transcendentals=0)


def mm(a, b):
    return jnp.dot(a, b, preferred_element_type=F32)


def tile_linear(row):
    return ((row >> 3) << 4) | (row & 7)


def put_rows(tab, row0, x, nc):
    rows = x.shape[0]
    if nc == 1:
        tab[pl.ds(pl.multiple_of(row0, 8), rows), :] = x
    else:
        for g in range(rows // 8):
            for c in range(nc):
                at = pl.multiple_of((row0 + g * 8) * nc + c * 8, 8)
                tab[pl.ds(at, 8), :] = x[g * 8:g * 8 + 8, c * LANES:(c + 1) * LANES]


def fetch(src, stage, sem, parts):
    rows = src.shape[0] // parts
    copies = [pltpu.make_async_copy(src.at[pl.ds(k * rows, rows)], stage.at[pl.ds(k * rows, rows)], sem.at[k])
              for k in range(parts)]
    for c in copies:
        c.start()
    return copies


def unpack(copies, stage, tab, row0, nc):
    rows = stage.shape[0] // len(copies)
    step = next(d for d in (128, 96, 64, 32, 16) if rows % d == 0)
    for p, c in enumerate(copies):
        c.wait()

        def body(k, carry):
            at = pl.multiple_of(p * rows + k * step, step)
            put_rows(tab, row0 + at, stage[pl.ds(at, step), :].astype(F32), nc)
            return carry
        lax.fori_loop(0, rows // step, body, 0)


def group_of(blocks):
    return next(u for u in (GROUP, 4, 2) if blocks % u == 0)


def zero_rows(acc):
    rows = acc.shape[0]
    step = next(s for s in (256, 128, 64, 32, 16, 8) if rows % s == 0)

    def body(k, carry):
        acc[pl.ds(pl.multiple_of(k * step, step), step), :] = jnp.zeros((step, acc.shape[1]), F32)
        return carry
    lax.fori_loop(0, rows // step, body, 0)


def gather_16(idx, base, first, reach, tab, nc, stride=1):
    sub = lax.broadcasted_iota(jnp.int32, (8, LANES), 0)
    room = idx.shape[0] - (reach - 1) * stride
    halves = [[None, None] for _ in range(nc)]
    for h in range(2):
        for k in range(8):
            at = idx.at[pl.ds((first + h * 8 + k) * stride, room)][base]
            for c in range(nc):
                row = jnp.broadcast_to(tab[pl.ds(at + 8 * c, 1), :], (8, LANES))
                halves[c][h] = row if k == 0 else jnp.where(sub == k, row, halves[c][h])
    return [jnp.concatenate(halves[c], axis=0).astype(BF16) for c in range(nc)]


def segment_sums(meta, meta_at, idx, seg, tab, acc, bufs, nc, window, blocks):
    unroll = group_of(blocks)
    first_trip, end_trip, most = [meta[meta_at + 2 * blocks + k] for k in range(3)]

    def fill(base, first, reach, buf):
        for g in range(BLOCK // 16):
            parts = gather_16(idx, base, first + g * 16, reach, tab, nc)
            for c in range(nc):
                buf[g * 16:g * 16 + 16, c * LANES:(c + 1) * LANES] = parts[c]

    def sums(b, at, buf):
        rows = lax.broadcasted_iota(jnp.int32, (window, BLOCK), 0) + at
        return mm(jnp.where(rows == seg[b], 1.0, 0.0).astype(BF16), buf[...])

    def add(at, x):
        acc[pl.ds(pl.multiple_of(at, 8), window), :] += x

    span = unroll * BLOCK
    last_trip = blocks // unroll - 1
    fill(jnp.minimum(first_trip, last_trip) * span, 0, span, bufs[0])

    def body(t, carry):
        before = None
        for u in range(unroll):
            b = t * unroll + u
            now = (meta[meta_at + b], sums(b, meta[meta_at + b], bufs[u % 2]))
            if u + 1 < unroll:
                fill(t * span, (u + 1) * BLOCK, span, bufs[(u + 1) % 2])
            else:
                fill(jnp.minimum(t + 1, last_trip) * span, 0, span, bufs[0])
            if before is not None:
                add(*before)
            before = now
        add(*before)
        return carry
    lax.fori_loop(first_trip, end_trip, body, 0)

    @pl.when(most > 1)
    def _():
        def again(b, carry):
            count = meta[meta_at + blocks + b]

            @pl.when(count > 1)
            def _():
                fill(b * BLOCK, 0, BLOCK, bufs[0])

                def more(w, c):
                    at = meta[meta_at + b] + w * window
                    add(at, sums(b, at, bufs[0]))
                    return c
                lax.fori_loop(1, count, more, 0)
            return carry
        lax.fori_loop(first_trip * unroll, end_trip * unroll, again, 0)


def spread_lanes():
    return lax.broadcasted_iota(jnp.int32, (1, LANES), 1)


def split3(x):
    hi = x.astype(BF16).astype(F32)
    rest = x - hi
    mid = rest.astype(BF16).astype(F32)
    low = rest - mid
    lane = spread_lanes()
    out = jnp.where(lane < SPREAD, hi, jnp.where(lane < 2 * SPREAD, mid, low))
    return jnp.where(lane < 3 * SPREAD, out, 0.0).astype(BF16)


def pieces3(a):
    hi = a.astype(BF16)
    rest = a - hi.astype(F32)
    mid = rest.astype(BF16)
    low = (rest - mid.astype(F32)).astype(BF16)
    return jnp.concatenate([hi, mid, low], axis=1)


def fold3(a, folder):
    return mm(pieces3(a), folder)


def add_rows(ref, x):
    ref[...] += jnp.sum(x.reshape(x.shape[0] // 8, 8, x.shape[1]), axis=0)


def pick_rows(name, src, idx, peers, slots, mask):
    n = src.shape[0]
    per = math.gcd(peers, 16)
    extra = 0 if mask is None else TAIL
    parts = math.gcd(n // 128, 4)

    def kern(idx_ref, src_ref, *refs):
        if extra:
            mask_ref, out, tab, stage, sem, tail = refs
        else:
            out, tab, stage, sem = refs

        @pl.when(pl.program_id(0) == 0)
        def _():
            copies = fetch(src_ref, stage, sem, parts)
            if extra:
                total = jnp.sum(mask_ref[...], axis=(0, 1), keepdims=True)
                high = jnp.floor(total * (1.0 / LANES))
                first = lax.broadcasted_iota(jnp.int32, (TAIL, LANES), 0) == 0
                lane = lax.broadcasted_iota(jnp.int32, (TAIL, LANES), 1)
                digits = jnp.where(lane == 0, high, jnp.where(lane == 1, total - high * LANES, 0.0))
                tail[...] = jnp.where(first, digits, 0.0).astype(BF16)
            unpack(copies, stage, tab, 0, 1)
        first = pl.program_id(0) * per

        def body(p, carry):
            for g in range(slots // 16):
                out[p, g * 16:g * 16 + 16, :] = gather_16(idx_ref, first + p, g * 16, slots, tab, 1, peers)[0]
            if extra:
                out[p, slots:slots + extra, :] = tail[...]
            return carry
        lax.fori_loop(0, per, body, 0)

    operands = [idx, src] + ([mask] if extra else [])
    specs = [SMEM_SPEC, HBM_SPEC] + ([whole_spec(mask.shape)] if extra else [])
    return pl.pallas_call(
        kern, name=name, grid=(peers // per,),
        out_shape=jax.ShapeDtypeStruct((peers, slots + extra, LANES), BF16),
        in_specs=specs,
        out_specs=pl.BlockSpec((per, slots + extra, LANES), lambda i: (i, 0, 0)),
        scratch_shapes=([pltpu.VMEM((n, LANES), F32), pltpu.VMEM((n, LANES), BF16), pltpu.SemaphoreType.DMA((parts,))]
                        + ([pltpu.VMEM((TAIL, LANES), BF16)] if extra else [])),
        compiler_params=params(), cost_estimate=cost(10))(*operands)


PIECES = 4


def send_part(stage, out, sem, k):
    size = stage.shape[0] // PIECES
    at = pl.multiple_of(k * size, size)
    return pltpu.make_async_copy(stage.at[pl.ds(at, size)], out.at[pl.ds(at, size)], sem.at[k])


def send_out(src, out, sem):
    done = pltpu.make_async_copy(src, out, sem)
    done.start()
    done.wait()


def edge_call(name, edges, nc, table_rows, acc_rows, window, sources, build, hbm_in, blocked, fixed, outs, rows_out,
              tile, epilogue, micros, init=None, late=False, sub=1024, keep=0, pick=None, then=None):
    meta, meta_at, idx, seg = edges
    blocks = seg.shape[0]
    width = nc * LANES
    nh, nb, nf, no, ns = len(hbm_in), len(blocked), len(fixed), len(outs), len(sources)
    acc_total = -(-(acc_rows + window) // 256) * 256
    parts = 4
    steps = 1 if epilogue is None else rows_out // tile
    sub = math.gcd(sub, tile)
    more_in, more_specs, more_out, more_scratch = [], [], [], []
    late_scratch = [pltpu.VMEM((acc_rows, width), F32)] if late else []
    if keep:
        more_scratch.append(pltpu.VMEM((rows_out * keep, LANES), F32))
    if pick:
        p_idx, peers, slots = pick
        more_in.append(p_idx)
        more_specs.append(SMEM_SPEC)
        more_out.append(jax.ShapeDtypeStruct((peers, slots, LANES), BF16))
        more_scratch += [pltpu.VMEM((peers, slots, LANES), BF16), pltpu.SemaphoreType.DMA((PIECES,))]
    if then:
        (t_meta, t_at, t_idx, t_seg), t_nc, t_rows, t_window, finish = then
        t_width = t_nc * LANES
        t_total = -(-(t_rows + t_window) // 256) * 256
        more_in += [t_meta, t_idx, t_seg]
        more_specs += [SMEM_SPEC, SMEM_SPEC, whole_spec(t_seg.shape)]
        more_out.append(jax.ShapeDtypeStruct((t_rows, t_width), BF16))
        more_scratch += [pltpu.VMEM((t_total, t_width), F32), pltpu.VMEM((BLOCK, t_width), BF16),
                         pltpu.VMEM((BLOCK, t_width), BF16), pltpu.VMEM((t_rows, t_width), BF16),
                         pltpu.SemaphoreType.DMA((PIECES,))]
    nm = len(more_in)

    def kern(meta_ref, idx_ref, seg_ref, *refs):
        hb, refs = refs[:nh], refs[nh:]
        bl, refs = refs[:nb], refs[nb:]
        fx, refs = refs[:nf], refs[nf:]
        extra, refs = refs[:nm], refs[nm:]
        out, refs = refs[:no], refs[no:]
        last_out, refs = refs[:len(more_out)], refs[len(more_out):]
        tab, acc, buf_0, buf_1, isem = refs[:5]
        stages, sems, scratch = refs[5:5 + ns], refs[5 + ns:5 + 2 * ns], refs[5 + 2 * ns:]
        if late:
            begin, scratch = scratch[0], scratch[1:]
        i = pl.program_id(0)

        @pl.when(i == 0)
        def _():
            copies = [fetch(h, st, sm, parts) for h, st, sm in zip(hb, stages, sems)]
            if init is not None:
                start = pltpu.make_async_copy(hb[init], begin if late else acc.at[pl.ds(0, acc_rows), :], isem)
                if not late:
                    start.start()
            if init is None or late:
                zero_rows(acc)
            for o, (_, _, sums) in zip(out, outs):
                if sums:
                    o[...] = jnp.zeros_like(o)
            if then:
                zero_rows(scratch[1])
            build(copies, stages, tab, fx)
            if late:
                start.start()
            if init is not None and not late:
                start.wait()
            segment_sums(meta_ref, meta_at, idx_ref, seg_ref, tab, acc, (buf_0, buf_1), nc, window, blocks)
            if late:
                start.wait()
            if epilogue is None:
                send_out(acc.at[pl.ds(0, acc_rows), :], out[0], isem)
        if epilogue is not None:
            def part(j, carry):
                at = pl.multiple_of(j * sub, sub)
                row0 = pl.multiple_of(i * tile + at, sub)

                def put(x):
                    put_rows(scratch[0], row0, x, keep)
                a = acc[pl.ds(row0, sub), :]
                if late:
                    a = a + begin[pl.ds(row0, sub), :]
                epilogue(a, [r.at[pl.ds(at, sub), :] for r in bl], fx,
                         [o if sums else o.at[pl.ds(at, sub), :] for o, (_, _, sums) in zip(out, outs)], put)
                return carry
            lax.fori_loop(0, tile // sub, part, 0)

        if pick:
            @pl.when(i == steps - 1)
            def _():
                kept, stage, out_sem = scratch
                size = peers // PIECES

                def piece(k, c):
                    def body(p, carry):
                        for g in range(slots // 16):
                            rows = gather_16(extra[0], k * size + p, g * 16, slots, kept, 1, peers)[0]
                            stage[k * size + p, g * 16:g * 16 + 16, :] = rows
                        return carry
                    lax.fori_loop(0, size, body, 0)
                    send_part(stage, last_out[0], out_sem, k).start()
                    return c
                lax.fori_loop(0, PIECES, piece, 0)
                for k in range(PIECES):
                    send_part(stage, last_out[0], out_sem, k).wait()
        if then:
            @pl.when(i == steps - 1)
            def _():
                kept, acc_2, buf_2, buf_3, stage, out_sem = scratch
                segment_sums(extra[0], t_at, extra[1], extra[2], kept, acc_2, (buf_2, buf_3), t_nc, t_window,
                             t_seg.shape[0])
                size = t_rows // PIECES
                step = math.gcd(1024, size)

                def piece(k, c):
                    def part(j, carry):
                        at = pl.multiple_of(k * size + j * step, step)
                        stage[pl.ds(at, step), :] = finish(acc_2[pl.ds(at, step), :], fx)
                        return carry
                    lax.fori_loop(0, size // step, part, 0)
                    send_part(stage, last_out[0], out_sem, k).start()
                    return c
                lax.fori_loop(0, PIECES, piece, 0)
                for k in range(PIECES):
                    send_part(stage, last_out[0], out_sem, k).wait()

    out_shape, out_specs = [], []
    for shape, dtype, sums in outs:
        out_shape.append(jax.ShapeDtypeStruct(shape, dtype))
        out_specs.append(HBM_SPEC if epilogue is None else whole_spec(shape) if sums else row_spec(tile, shape[1]))
    return pl.pallas_call(
        kern, name=name, grid=(steps,), out_shape=out_shape + more_out,
        in_specs=([SMEM_SPEC, SMEM_SPEC, whole_spec(seg.shape)] + [HBM_SPEC] * nh
                  + [row_spec(tile, x.shape[1]) for x in blocked] + [whole_spec(x.shape) for x in fixed] + more_specs),
        out_specs=out_specs + [HBM_SPEC] * len(more_out),
        scratch_shapes=([pltpu.VMEM((table_rows * nc, LANES), F32), pltpu.VMEM((acc_total, width), F32),
                         pltpu.VMEM((BLOCK, width), BF16), pltpu.VMEM((BLOCK, width), BF16),
                         pltpu.SemaphoreType.DMA(())]
                        + [pltpu.VMEM(shape, BF16) for shape in sources]
                        + [pltpu.SemaphoreType.DMA((parts,)) for _ in sources] + late_scratch + more_scratch),
        compiler_params=params(), cost_estimate=cost(micros))(meta, idx, seg, *hbm_in, *blocked, *fixed, *more_in)


SHARE = 16


def grad_places(shapes):
    places, at = [], 0
    for rows, width in shapes:
        columns = []
        for _ in range(width // LANES):
            columns.append(at)
            at += -(-rows // SHARE)
        places.append(columns)
    return places, at


def sum_over_devices(grads, sums, total, classes, peers):
    chips = peers // 2
    places, used = grad_places([g.shape for g in grads] + [(SHARE, LANES)])
    rounds = -(-used // peers)
    rows = SHARE * rounds
    widths = [x.shape[1] for x in sums]

    def device(chip, core):
        return chip * 2 + core

    def kern(*refs):
        ng, ns = len(grads), len(sums)
        g_refs, s_refs, out_ref = refs[:ng], refs[ng:ng + ns], refs[ng + ns]
        x_ref, half, mine, got, pair_sem, send_sem, recv_sem, send_2, recv_2 = refs[ng + ns + 1:]
        me = lax.axis_index(GROUP_AXIS)
        chip, core = me // 2, me % 2
        mate = device(chip, 1 - core)
        barrier = pltpu.get_barrier_semaphore()

        def hello(to):
            pl.semaphore_signal(barrier, inc=1, device_id=(to,), device_id_type=pl.DeviceIdType.MESH)

        def greet(k, carry):
            hello(device((chip + k) % chips, core))
            return carry
        lax.fori_loop(1, chips, greet, 0)
        hello(mate)

        def at(q):
            unit = q // rounds
            return unit // chips, unit % chips, (q % rounds) * SHARE

        def put(q, value):
            h, c, r = at(q)
            x_ref[h, c, r:r + SHARE, :] = value
        for g, columns in zip(g_refs, places):
            for w, first in enumerate(columns):
                for k in range(g.shape[0] // SHARE):
                    put(first + k, g[k * SHARE:(k + 1) * SHARE, w * LANES:(w + 1) * LANES])
        row = lax.broadcasted_iota(jnp.int32, (SHARE, LANES), 0)
        small, line = jnp.zeros((SHARE, LANES), F32), 0
        for s_ref, width in zip(s_refs, widths):
            for w in range(width // LANES):
                total = jnp.sum(s_ref[:, w * LANES:(w + 1) * LANES], axis=0, keepdims=True)
                small = jnp.where(row == line, total, small)
                line += 1
        put(places[-1][0], small)
        for q in range(used, peers * rounds):
            put(q, jnp.zeros((SHARE, LANES), F32))

        def pair(src, dst, k):
            return pltpu.make_async_remote_copy(src_ref=src, dst_ref=dst, send_sem=pair_sem.at[2 * k],
                                                recv_sem=pair_sem.at[2 * k + 1], device_id=(mate,),
                                                device_id_type=pl.DeviceIdType.MESH)
        pl.semaphore_wait(barrier, chips)
        first = pair(x_ref.at[1 - core], half, 0)
        first.start()
        first.wait()

        def add(c, carry):
            mine[c] = x_ref[core, c] + half[c]
            return carry
        lax.fori_loop(0, chips, add, 0)

        def share(k):
            to = (chip + k) % chips
            return pltpu.make_async_remote_copy(src_ref=mine.at[to], dst_ref=got.at[chip], send_sem=send_sem.at[k],
                                                recv_sem=recv_sem.at[chip], device_id=(device(to, core),),
                                                device_id_type=pl.DeviceIdType.MESH)

        def landed(k):
            frm = (chip + k) % chips
            return pltpu.make_async_remote_copy(src_ref=mine.at[frm], dst_ref=got.at[frm], send_sem=send_sem.at[k],
                                                recv_sem=recv_sem.at[frm], device_id=(me,),
                                                device_id_type=pl.DeviceIdType.MESH)

        def start(k, carry):
            share(k).start()
            return carry
        lax.fori_loop(1, chips, start, 0)
        got[chip] = mine[chip]

        def settle(k, carry):
            landed(k).wait_recv()
            return carry
        lax.fori_loop(1, chips, settle, 0)

        def more(c, total):
            return total + got[c]
        out_ref[core, chip] = lax.fori_loop(0, chips, more, jnp.zeros((rows, LANES), F32))

        def drain(k, carry):
            share(k).wait_send()
            return carry
        lax.fori_loop(1, chips, drain, 0)

        def give(k):
            return pltpu.make_async_remote_copy(src_ref=out_ref.at[core, chip], dst_ref=out_ref.at[core, chip],
                                                send_sem=send_2.at[k], recv_sem=recv_2.at[chip],
                                                device_id=(device((chip + k) % chips, core),),
                                                device_id_type=pl.DeviceIdType.MESH)

        def given(k):
            frm = (chip + k) % chips
            return pltpu.make_async_remote_copy(src_ref=out_ref.at[core, frm], dst_ref=out_ref.at[core, frm],
                                                send_sem=send_2.at[k], recv_sem=recv_2.at[frm], device_id=(me,),
                                                device_id_type=pl.DeviceIdType.MESH)

        def start_2(k, carry):
            give(k).start()
            return carry
        lax.fori_loop(1, chips, start_2, 0)

        def settle_2(k, carry):
            given(k).wait_recv()
            return carry
        lax.fori_loop(1, chips, settle_2, 0)

        def drain_2(k, carry):
            give(k).wait_send()
            return carry
        lax.fori_loop(1, chips, drain_2, 0)
        last = pair(out_ref.at[core], out_ref.at[core], 1)
        last.start()
        last.wait()

    vmem = pl.BlockSpec(memory_space=pltpu.VMEM)
    shape = (2, chips, rows, LANES)
    full = pl.pallas_call(
        kern, name='sum_all', out_shape=jax.ShapeDtypeStruct(shape, F32),
        in_specs=[vmem] * (len(grads) + len(sums)), out_specs=vmem,
        scratch_shapes=[pltpu.VMEM(shape, F32), pltpu.VMEM(shape[1:], F32), pltpu.VMEM(shape[1:], F32),
                        pltpu.VMEM(shape[1:], F32), pltpu.SemaphoreType.DMA((4,)),
                        pltpu.SemaphoreType.DMA((chips,)), pltpu.SemaphoreType.DMA((chips,)),
                        pltpu.SemaphoreType.DMA((chips,)), pltpu.SemaphoreType.DMA((chips,))],
        compiler_params=pltpu.CompilerParams(collective_id=0, has_side_effects=True), cost_estimate=cost(25))(*grads, *sums)

    def unpack_kern(full_ref, total_ref, *outs):
        def part(q):
            unit = q // rounds
            r = (q % rounds) * SHARE
            return full_ref[unit // chips, unit % chips, r:r + SHARE, :]

        def move(o, columns, skip):
            for w, first in enumerate(columns):
                for k in range(o.shape[0] // SHARE):
                    o[k * SHARE:(k + 1) * SHARE, w * LANES:(w + 1) * LANES] = part(first + skip + k)
        move(outs[0], places[0], 0)
        move(outs[1], places[0], outs[0].shape[0] // SHARE)
        for o, columns in zip(outs[2:], places[1:-2]):
            move(o, columns, 0)
        both = jnp.concatenate([part(places[-2][0] + k) for k in range(rows_3 // SHARE)], axis=0).T
        outs[ng][...] = both[:classes, :]
        outs[ng + 1][...] = both[SPREAD:SPREAD + classes, :]
        small, line = part(places[-1][0]), 0
        for o, width in zip(outs[ng + 2:-1], widths):
            for w in range(width // LANES):
                wide = min(LANES, o.shape[1] - w * LANES)
                o[:, w * LANES:w * LANES + wide] = small[line:line + 1, :wide]
                line += 1
        outs[-1][...] = jnp.sum(small[line:line + 1, :], axis=1, keepdims=True) / total_ref[...]
    ng = len(grads)
    rows_3 = grads[-1].shape[0]
    rows_1, width_1 = grads[0].shape
    outs = ([(rows_1 // 2, width_1)] * 2 + [g.shape for g in grads[1:-1]] + [(classes, rows_3)] * 2
            + [(1, w) for w in widths[:-2]] + [(1, classes), (1, 1)])
    return pl.pallas_call(unpack_kern, name='unpack_sums', out_shape=[jax.ShapeDtypeStruct(o, F32) for o in outs],
                          in_specs=[vmem, vmem], out_specs=[vmem] * len(outs), cost_estimate=cost(3))(full, total)


def edge_meta(seg_first, seg_last, window, first_block, end_block):
    blocks = seg_first.shape[0]
    unroll = group_of(blocks)
    at = jnp.arange(blocks, dtype=jnp.int32)
    base = seg_first & ~7
    count = jnp.where((at >= first_block) & (at < end_block), (seg_last - base) // window + 1, 1)
    tail = jnp.stack([first_block // unroll, (end_block + unroll - 1) // unroll, jnp.max(count)])
    return [base, count, tail]


def join_meta(*metas):
    offsets, at = [], 0
    for m in metas:
        offsets.append(at)
        at += sum(x.shape[0] for x in m)
    return jnp.concatenate([x for m in metas for x in m]).astype(jnp.int32), offsets


def bits_for(n):
    return max(1, (n - 1).bit_length())


def spread3(w):
    w = jnp.pad(w, ((0, 0), (0, SPREAD - w.shape[1])))
    return jnp.pad(jnp.concatenate([w, w, w], axis=1), ((0, 0), (0, LANES - 3 * SPREAD)))


def lanes_pad(w):
    return jnp.pad(w, ((0, 0), (0, LANES - w.shape[1])))


def solution(mesh):
    peers = mesh.shape[GROUP_AXIS]

    def exchange(x):
        return lax.all_to_all(x, GROUP_AXIS, 0, 0, tiled=True)

    def device_step(features, labels, train_mask, send_idx, src_idx, dst_idx, inv_deg,
                    w_self_1, w_neigh_1, bias_1, w_self_2, w_neigh_2, bias_2,
                    w_self_3, w_neigh_3, bias_3):
        n = features.shape[0]
        slots = send_idx.shape[1]
        halo = peers * slots
        edges = src_idx.shape[0]
        hidden = w_self_1.shape[1]
        classes = w_self_3.shape[1]
        send_flat = send_idx.T.reshape(-1)
        tile = next(t for t in (4096, 1024) if n % t == 0)
        half_tile = tile // 2
        slot_bits = bits_for(halo)
        dst_bits = bits_for(n)
        table = n + halo

        blocks = edges // BLOCK
        halo_blocks = halo // BLOCK
        zero = jnp.int32(0)
        win_e, win_h, win_r = 192, 208, 272
        owned = jnp.sum((src_idx < n).astype(jnp.int32))
        near_end = (owned + BLOCK - 1) // BLOCK
        far_start = owned // BLOCK

        src_bits = bits_for(table)
        far_bit = dst_bits + src_bits
        by_dst = lax.sort(((src_idx >= n).astype(jnp.int32) << far_bit) | (dst_idx << src_bits) | src_idx, is_stable=False)
        src_f = by_dst & ((1 << src_bits) - 1)
        dst_f = (by_dst >> src_bits) & ((1 << dst_bits) - 1)
        is_far = src_f >= n
        src_near = jnp.minimum(src_f, n - 1)
        src_far = jnp.maximum(src_f - n, 0)
        seg_near = jnp.where(is_far, -1, dst_f).reshape(blocks, 1, BLOCK)
        seg_far = jnp.where(is_far, dst_f, -1).reshape(blocks, 1, BLOCK)
        first, last = dst_f[::BLOCK], dst_f[BLOCK - 1::BLOCK]
        meta_f, (near_at, far_at) = join_meta(
            edge_meta(first, jnp.where(is_far[BLOCK - 1::BLOCK], n - 1, last), win_e, zero, near_end),
            edge_meta(jnp.where(is_far[::BLOCK], first, 0), last, win_e, far_start, jnp.int32(blocks)))

        inv = jnp.broadcast_to(inv_deg[:, None], (n, LANES))
        b1 = bias_1.reshape(1, -1)
        b2 = bias_2.reshape(1, -1)
        lane = jnp.arange(LANES, dtype=jnp.int32)
        used = lane < 3 * SPREAD
        folder = jnp.tile(((lane[:, None] % SPREAD == lane[None, :] % SPREAD) & used[:, None] & used[None, :]).astype(BF16),
                          (3, 1))
        b3 = jnp.where(lane < 3 * SPREAD, spread3(bias_3.reshape(1, -1)), -1e30)
        if classes < SPREAD:
            b3 = jnp.where(lane % SPREAD < classes, b3, -1e30)
        target = jnp.where(lane[None, :] < 3 * SPREAD,
                           train_mask[:, None] * (1.0 + (labels[:, None] == lane[None, :] % SPREAD)), 0.0).astype(BF16)
        ws3, wn3 = spread3(w_self_3), spread3(w_neigh_3)
        ws3_t, wn3_t = lanes_pad(w_self_3).T, lanes_pad(w_neigh_3).T

        def rows_of(nc):
            def build(copies, stages, tab, fx):
                unpack(copies[0], stages[0], tab, 0, nc)
            return build

        def near_sums(name, nc, idx, rows, also):
            return edge_call(name, (meta_f, near_at, idx, seg_near), nc, n, n, win_e, [rows.shape], rows_of(nc),
                             [rows] + also, [], [], [((n, nc * LANES), F32, False)], n, tile, None, 20)[0]

        out_1 = pick_rows('send_1', features, send_flat, peers, slots, train_mask.reshape(-1, LANES))
        got_1 = exchange(out_1)
        near_1 = near_sums('near_1', 1, src_near, features, [inv])
        counts = got_1[:, slots, :2].astype(F32)
        total = jnp.sum(counts[:, 0]) * LANES + jnp.sum(counts[:, 1])

        def build_1(copies, stages, tab, fx):
            per = peers // len(copies[0])
            some = math.gcd(per, 8)
            for p in range(len(copies[0])):
                copies[0][p].wait()

                def body(k, carry):
                    q = p * per + k * some
                    rows = stages[0][pl.ds(q, some), :slots, :].reshape(some * slots, LANES)
                    put_rows(tab, q * slots, rows.astype(F32), 1)
                    return carry
                lax.fori_loop(0, per // some, body, 0)

        def epi_1(a, bl, fx, out, put):
            mean = (a * bl[1][...]).astype(BF16)
            z = mm(bl[0][...], fx[0][...]) + mm(mean, fx[1][...]) + fx[2][...]
            out[0][...] = mean
            out[1][...] = jnp.maximum(z, 0.0).astype(BF16)
            put(mean.astype(F32))

        mean_1, hidden_1, out_2 = edge_call(
            'layer_1', (meta_f, far_at, src_far, seg_far), 1, halo, n, win_e, [(peers, slots + TAIL, LANES)], build_1,
            [got_1, near_1], [features, inv], [w_self_1, w_neigh_1, b1],
            [((n, LANES), BF16, False), ((n, hidden), BF16, False)], n, tile, epi_1, 25, init=1, late=True,
            keep=1, pick=(send_flat, peers, slots))

        place = jnp.arange(halo, dtype=jnp.int32)
        keys = jnp.concatenate([(src_idx << dst_bits) | dst_idx,
                                (1 << 30) | (send_flat << slot_bits) | (place % peers * slots + place // peers)])
        keys = lax.optimization_barrier((keys, mean_1))[0]
        ordered = lax.sort(keys, is_stable=False)
        by_src, by_row = ordered[:edges], ordered[edges:] & ((1 << 30) - 1)
        src_s = by_src >> dst_bits
        dst_s = by_src & ((1 << dst_bits) - 1)
        row_s = by_row >> slot_bits
        slot_s = by_row & ((1 << slot_bits) - 1)
        first, last = src_s[::BLOCK], src_s[BLOCK - 1::BLOCK]
        meta_b, (own_at, halo_at, owner_at) = join_meta(
            edge_meta(jnp.minimum(first, n - 1), jnp.minimum(last, n - 1), win_e, zero, near_end),
            edge_meta(jnp.maximum(first - n, 0), jnp.maximum(last - n, 0), win_h, far_start, jnp.int32(blocks)),
            edge_meta(row_s[::BLOCK], row_s[BLOCK - 1::BLOCK], win_r, zero, jnp.int32(halo_blocks)))
        seg_o = src_s.reshape(blocks, 1, BLOCK)
        seg_h = seg_o - n
        seg_r = row_s.reshape(halo_blocks, 1, BLOCK)
        dst_wide = tile_linear(dst_s)

        got_2 = exchange(out_2)
        near_2 = near_sums('near_2', 2, tile_linear(src_near), hidden_1, [])

        def build_2(copies, stages, tab, fx):
            per = peers // len(copies[0])
            some = math.gcd(per, 8)
            for p in range(len(copies[0])):
                copies[0][p].wait()
                copies[1][p].wait()

                def body(k, carry):
                    q = p * per + k * some
                    f = stages[0][pl.ds(q, some), :slots, :].reshape(some * slots, LANES)
                    m = stages[1][pl.ds(q, some)].reshape(some * slots, LANES)
                    z = mm(f, fx[3][...]) + mm(m, fx[4][...]) + fx[5][...]
                    put_rows(tab, q * slots, jnp.maximum(z, 0.0).astype(BF16).astype(F32), 2)
                    return carry
                lax.fori_loop(0, per // some, body, 0)

        def epi_2(a, bl, fx, out, put):
            scale = bl[1][...]
            mean = (a * jnp.concatenate([scale, scale], axis=1)).astype(BF16)
            z = mm(bl[0][...], fx[0][...]) + mm(mean, fx[1][...]) + fx[2][...]
            h = jnp.maximum(z, 0.0).astype(BF16)
            out[0][...] = mean
            out[1][...] = h
            both = mm(h, fx[6][...])
            pieces = split3(both[:, :LANES])
            out[2][...] = pieces
            out[3][...] = both[:, LANES:]
            put(pieces.astype(F32))

        mean_2, hidden_2, proj, logits_self, out_3 = edge_call(
            'layer_2', (meta_f, far_at, tile_linear(src_far), seg_far), 2, halo, n, win_e,
            [(peers, slots + TAIL, LANES), (peers, slots, LANES)], build_2, [got_1, got_2, near_2],
            [hidden_1, inv], [w_self_2, w_neigh_2, b2, w_self_1, w_neigh_1, b1, jnp.concatenate([wn3, ws3], axis=1)],
            [((n, hidden), BF16, False), ((n, hidden), BF16, False), ((n, LANES), BF16, False),
             ((n, LANES), F32, False)], n, tile, epi_2, 40, init=2, keep=1, pick=(send_flat, peers, slots))

        got_3 = exchange(out_3).reshape(halo, LANES)
        near_3 = near_sums('near_3', 1, src_near, proj, [target])
        inv_total = (1.0 / total).reshape(1, 1)

        def epi_3(a, bl, fx, out, put):
            scale = bl[1][...]
            z = bl[0][...] + fold3(a * scale, fx[2][...]) + fx[0][...]
            lane = spread_lanes()
            z = jnp.where(lane < 3 * SPREAD, z, -1e30)
            top = jnp.max(z, axis=1, keepdims=True)
            e = jnp.where(lane < SPREAD, jnp.exp(z - top), 0.0)
            lse = top + jnp.log(jnp.sum(e, axis=1, keepdims=True))
            t = bl[2][...].astype(F32)
            hit = t > 1.5
            d = jnp.where(t > 0.5, jnp.exp(z - lse) - jnp.where(hit, 1.0, 0.0), 0.0) * fx[1][...]
            db = d.astype(BF16)
            out[0][...] = db
            pieces = split3(db.astype(F32) * scale)
            out[1][...] = pieces
            put(pieces.astype(F32))
            add_rows(out[2], d)
            add_rows(out[3], jnp.where(hit & (lane < SPREAD), lse - z, 0.0))

        def finish_3(a, fx):
            return split3(fold3(a, fx[2][...]))

        d_bf_3, scaled_3, g_b3, loss_parts, back_3 = edge_call(
            'layer_3', (meta_f, far_at, src_far, seg_far), 1, halo, n, win_e, [(halo, LANES)], rows_of(1), [got_3, near_3],
            [logits_self, inv, target], [b3, jnp.broadcast_to(inv_total, (1, LANES)), folder],
            [((n, LANES), BF16, False), ((n, LANES), BF16, False), ((8, LANES), F32, True), ((8, LANES), F32, True)],
            n, tile, epi_3, 30, init=1, late=True, keep=1,
            then=((meta_b, halo_at, dst_s, seg_h), 1, halo, win_h, finish_3))

        ret_3 = exchange(back_3.reshape(peers, slots, LANES)).reshape(halo, LANES)
        own_3 = edge_call('back_3_own', (meta_b, own_at, dst_s, seg_o), 1, n, n, win_e, [(n, LANES)], rows_of(1),
                          [scaled_3], [], [], [((n, LANES), F32, False)], n, tile, None, 20)[0]

        def epi_o3(a, bl, fx, out, put):
            tb = fold3(a, fx[2][...]).astype(BF16)
            d_h = mm(jnp.concatenate([bl[0][...], tb], axis=1), fx[0][...])
            d_pre = jnp.where(bl[1][...].astype(F32) > 0, d_h, 0.0)
            db = d_pre.astype(BF16)
            scale = bl[2][...]
            out[0][...] = tb
            out[1][...] = db
            scaled = (mm(db, fx[1][...]) * jnp.concatenate([scale, scale], axis=1)).astype(BF16)
            out[2][...] = scaled
            put(scaled.astype(F32))
            add_rows(out[3], d_pre)

        def finish_2(a, fx):
            return a.astype(BF16)

        tb_3, d_bf_2, scaled_2, g_b2, back_2 = edge_call(
            'owner_3', (meta_b, owner_at, slot_s, seg_r), 1, halo, n, win_r, [(halo, LANES)], rows_of(1), [ret_3, own_3],
            [d_bf_3, hidden_2, inv], [jnp.concatenate([ws3_t, wn3_t], axis=0), w_neigh_2.T, folder],
            [((n, LANES), BF16, False), ((n, hidden), BF16, False), ((n, hidden), BF16, False), ((8, hidden), F32, True)],
            n, half_tile, epi_o3, 30, init=1, late=True, sub=512, keep=2,
            then=((meta_b, halo_at, dst_wide, seg_h), 2, halo, win_h, finish_2))

        def epi_b2o(a, bl, fx, out, put):
            out[0][...] = a + mm(bl[0][...], fx[0][...])

        ret_2 = exchange(back_2.reshape(peers, slots, hidden)).reshape(halo, hidden)
        own_2 = edge_call('back_2_own', (meta_b, own_at, dst_wide, seg_o), 2, n, n, win_e, [(n, hidden)], rows_of(2),
                          [scaled_2], [d_bf_2], [w_self_2.T], [((n, hidden), F32, False)], n, tile, epi_b2o, 30)[0]

        def epi_o2(a, bl, fx, out, put):
            d_pre = jnp.where(bl[0][...].astype(F32) > 0, a, 0.0)
            inputs = jnp.concatenate([bl[1][...], bl[2][...]], axis=1)
            out[0][...] += lax.dot_general(inputs, d_pre.astype(BF16), (((0,), (0,)), ((), ())),
                                           preferred_element_type=F32)
            add_rows(out[1], d_pre)

        g_1, g_b1 = edge_call(
            'owner_2', (meta_b, owner_at, tile_linear(slot_s), seg_r), 2, halo, n, win_r, [(halo, hidden)], rows_of(2),
            [ret_2, own_2], [hidden_1, features, mean_1], [],
            [((2 * LANES, hidden), F32, True), ((8, hidden), F32, True)], n, half_tile, epi_o2, 25, init=1, late=True)

        def contract(a, b):
            return jnp.einsum('nd,ne->de', a, b, preferred_element_type=F32)

        at = jnp.arange(LANES, dtype=jnp.int32)[None, :]
        g_3 = jnp.where(at < SPREAD, contract(hidden_2, d_bf_3), contract(hidden_2, tb_3))
        g1s, g1n, g2s, g2n, g3s, g3n, s1, s2, s3, loss = sum_over_devices(
            [g_1, contract(hidden_1, d_bf_2), contract(mean_2, d_bf_2), g_3],
            [g_b1, g_b2, g_b3, loss_parts], total.reshape(1, 1), classes, peers)
        return (loss.reshape(()), g1s, g1n, s1.reshape(-1), g2s, g2n, s2.reshape(-1), g3s.T, g3n.T, s3.reshape(-1))

    sharded = P(GROUP_AXIS)
    whole = P()
    return jax.shard_map(device_step, mesh=mesh,
                         in_specs=(sharded,) * 7 + (whole,) * 9,
                         out_specs=(whole,) * 10, check_vma=False)
```

```python
import math

import jax
import jax.numpy as jnp
from jax import lax
from jax.experimental import pallas as pl
from jax.experimental.pallas import tpu as pltpu
from jax.sharding import PartitionSpec as P

GROUP_AXIS = 'gp'
LANES = 128
SPREAD = 40
BLOCK = 128
GROUP = 8
TAIL = 8
F32 = jnp.float32
BF16 = jnp.bfloat16
VMEM_LIMIT = 60 * 2 ** 20

SMEM_SPEC = pl.BlockSpec(memory_space=pltpu.SMEM)
HBM_SPEC = pl.BlockSpec(memory_space=pltpu.HBM)


def whole_spec(shape):
    return pl.BlockSpec(shape, lambda i: (0,) * len(shape))


def row_spec(rows, width):
    return pl.BlockSpec((rows, width), lambda i: (i, 0))


def params():
    return pltpu.CompilerParams(vmem_limit_bytes=VMEM_LIMIT, dimension_semantics=('arbitrary',))


def cost(micros):
    return pl.CostEstimate(flops=int(micros * 4e6), bytes_accessed=int(micros * 1e6), transcendentals=0)


def mm(a, b):
    return jnp.dot(a, b, preferred_element_type=F32)


def tile_linear(row):
    return ((row >> 3) << 4) | (row & 7)


def put_rows(tab, row0, x, nc):
    rows = x.shape[0]
    if nc == 1:
        tab[pl.ds(pl.multiple_of(row0, 8), rows), :] = x
    else:
        for g in range(rows // 8):
            for c in range(nc):
                at = pl.multiple_of((row0 + g * 8) * nc + c * 8, 8)
                tab[pl.ds(at, 8), :] = x[g * 8:g * 8 + 8, c * LANES:(c + 1) * LANES]


def fetch(src, stage, sem, parts):
    rows = src.shape[0] // parts
    copies = [pltpu.make_async_copy(src.at[pl.ds(k * rows, rows)], stage.at[pl.ds(k * rows, rows)], sem.at[k])
              for k in range(parts)]
    for c in copies:
        c.start()
    return copies


def unpack(copies, stage, tab, row0, nc):
    rows = stage.shape[0] // len(copies)
    step = next(d for d in (128, 96, 64, 32, 16) if rows % d == 0)
    for p, c in enumerate(copies):
        c.wait()

        def body(k, carry):
            at = pl.multiple_of(p * rows + k * step, step)
            put_rows(tab, row0 + at, stage[pl.ds(at, step), :].astype(F32), nc)
            return carry
        lax.fori_loop(0, rows // step, body, 0)


def group_of(blocks):
    return next(u for u in (GROUP, 4, 2) if blocks % u == 0)


def zero_rows(acc):
    rows = acc.shape[0]
    step = next(s for s in (256, 128, 64, 32, 16, 8) if rows % s == 0)

    def body(k, carry):
        acc[pl.ds(pl.multiple_of(k * step, step), step), :] = jnp.zeros((step, acc.shape[1]), F32)
        return carry
    lax.fori_loop(0, rows // step, body, 0)


def gather_16(idx, base, first, reach, tab, nc, stride=1):
    sub = lax.broadcasted_iota(jnp.int32, (8, LANES), 0)
    room = idx.shape[0] - (reach - 1) * stride
    halves = [[None, None] for _ in range(nc)]
    for h in range(2):
        for k in range(8):
            at = idx.at[pl.ds((first + h * 8 + k) * stride, room)][base]
            for c in range(nc):
                row = jnp.broadcast_to(tab[pl.ds(at + 8 * c, 1), :], (8, LANES))
                halves[c][h] = row if k == 0 else jnp.where(sub == k, row, halves[c][h])
    return [jnp.concatenate(halves[c], axis=0).astype(BF16) for c in range(nc)]


def segment_sums(meta, idx, seg, tab, acc, bufs, nc, window, blocks):
    unroll = group_of(blocks)
    base, counts = meta[:2]
    first_trip, end_trip, most = [m[0] for m in meta[2:]]

    def fill(start, first, reach, buf):
        for g in range(BLOCK // 16):
            parts = gather_16(idx, start, first + g * 16, reach, tab, nc)
            for c in range(nc):
                buf[g * 16:g * 16 + 16, c * LANES:(c + 1) * LANES] = parts[c]

    def sums(b, at, buf):
        rows = lax.broadcasted_iota(jnp.int32, (window, BLOCK), 0) + at
        return mm(jnp.where(rows == seg[b], 1.0, 0.0).astype(BF16), buf[...])

    def add(at, x):
        acc[pl.ds(pl.multiple_of(at, 8), window), :] += x

    span = unroll * BLOCK
    last_trip = blocks // unroll - 1
    fill(jnp.minimum(first_trip, last_trip) * span, 0, span, bufs[0])

    def body(t, carry):
        before = None
        for u in range(unroll):
            b = t * unroll + u
            now = (base[b], sums(b, base[b], bufs[u % 2]))
            if u + 1 < unroll:
                fill(t * span, (u + 1) * BLOCK, span, bufs[(u + 1) % 2])
            else:
                fill(jnp.minimum(t + 1, last_trip) * span, 0, span, bufs[0])
            if before is not None:
                add(*before)
            before = now
        add(*before)
        return carry
    lax.fori_loop(first_trip, end_trip, body, 0)

    @pl.when(most > 1)
    def _():
        def again(b, carry):
            count = counts[b]

            @pl.when(count > 1)
            def _():
                fill(b * BLOCK, 0, BLOCK, bufs[0])

                def more(w, c):
                    at = base[b] + w * window
                    add(at, sums(b, at, bufs[0]))
                    return c
                lax.fori_loop(1, count, more, 0)
            return carry
        lax.fori_loop(first_trip * unroll, end_trip * unroll, again, 0)


def spread_lanes():
    return lax.broadcasted_iota(jnp.int32, (1, LANES), 1)


def split3(x):
    hi = x.astype(BF16).astype(F32)
    rest = x - hi
    mid = rest.astype(BF16).astype(F32)
    low = rest - mid
    lane = spread_lanes()
    out = jnp.where(lane < SPREAD, hi, jnp.where(lane < 2 * SPREAD, mid, low))
    return jnp.where(lane < 3 * SPREAD, out, 0.0).astype(BF16)


def pieces3(a):
    hi = a.astype(BF16)
    rest = a - hi.astype(F32)
    mid = rest.astype(BF16)
    low = (rest - mid.astype(F32)).astype(BF16)
    return jnp.concatenate([hi, mid, low], axis=1)


def fold3(a, folder):
    return mm(pieces3(a), folder)


def add_rows(ref, x):
    ref[...] += jnp.sum(x.reshape(x.shape[0] // 8, 8, x.shape[1]), axis=0)


def pick_rows(name, src, idx, peers, slots, mask):
    n = src.shape[0]
    per = math.gcd(peers, 16)
    extra = 0 if mask is None else TAIL
    parts = math.gcd(n // 128, 4)

    def kern(idx_ref, src_ref, *refs):
        if extra:
            mask_ref, out, tab, stage, sem, tail = refs
        else:
            out, tab, stage, sem = refs

        @pl.when(pl.program_id(0) == 0)
        def _():
            copies = fetch(src_ref, stage, sem, parts)
            if extra:
                total = jnp.sum(mask_ref[...], axis=(0, 1), keepdims=True)
                high = jnp.floor(total * (1.0 / LANES))
                first = lax.broadcasted_iota(jnp.int32, (TAIL, LANES), 0) == 0
                lane = lax.broadcasted_iota(jnp.int32, (TAIL, LANES), 1)
                digits = jnp.where(lane == 0, high, jnp.where(lane == 1, total - high * LANES, 0.0))
                tail[...] = jnp.where(first, digits, 0.0).astype(BF16)
            unpack(copies, stage, tab, 0, 1)
        first = pl.program_id(0) * per

        def body(p, carry):
            for g in range(slots // 16):
                out[p, g * 16:g * 16 + 16, :] = gather_16(idx_ref, first + p, g * 16, slots, tab, 1, peers)[0]
            if extra:
                out[p, slots:slots + extra, :] = tail[...]
            return carry
        lax.fori_loop(0, per, body, 0)

    operands = [idx, src] + ([mask] if extra else [])
    specs = [SMEM_SPEC, HBM_SPEC] + ([whole_spec(mask.shape)] if extra else [])
    return pl.pallas_call(
        kern, name=name, grid=(peers // per,),
        out_shape=jax.ShapeDtypeStruct((peers, slots + extra, LANES), BF16),
        in_specs=specs,
        out_specs=pl.BlockSpec((per, slots + extra, LANES), lambda i: (i, 0, 0)),
        scratch_shapes=([pltpu.VMEM((n, LANES), F32), pltpu.VMEM((n, LANES), BF16), pltpu.SemaphoreType.DMA((parts,))]
                        + ([pltpu.VMEM((TAIL, LANES), BF16)] if extra else [])),
        compiler_params=params(), cost_estimate=cost(10))(*operands)


PIECES = 4


def send_part(stage, out, sem, k):
    size = stage.shape[0] // PIECES
    at = pl.multiple_of(k * size, size)
    return pltpu.make_async_copy(stage.at[pl.ds(at, size)], out.at[pl.ds(at, size)], sem.at[k])


def send_out(src, out, sem):
    done = pltpu.make_async_copy(src, out, sem)
    done.start()
    done.wait()


def edge_call(name, edges, nc, table_rows, acc_rows, window, sources, build, hbm_in, blocked, fixed, outs, rows_out,
              tile, epilogue, micros, init=None, late=False, sub=2048, keep=0, pick=None, then=None):
    meta, idx, seg = edges
    blocks = seg.shape[0]
    width = nc * LANES
    nh, nb, nf, no, ns = len(hbm_in), len(blocked), len(fixed), len(outs), len(sources)
    acc_total = -(-(acc_rows + window) // 256) * 256
    parts = 4
    steps = 1 if epilogue is None else rows_out // tile
    sub = math.gcd(sub, tile)
    more_in, more_specs, more_out, more_scratch = [], [], [], []
    late_scratch = [pltpu.VMEM((acc_rows, width), F32)] if late else []
    if keep:
        more_scratch.append(pltpu.VMEM((rows_out * keep, LANES), F32))
    if pick:
        p_idx, peers, slots = pick
        more_in.append(p_idx)
        more_specs.append(SMEM_SPEC)
        more_out.append(jax.ShapeDtypeStruct((peers, slots, LANES), BF16))
        more_scratch += [pltpu.VMEM((peers, slots, LANES), BF16), pltpu.SemaphoreType.DMA((PIECES,))]
    if then:
        (t_meta, t_idx, t_seg), t_nc, t_rows, t_window, finish = then
        t_width = t_nc * LANES
        t_total = -(-(t_rows + t_window) // 256) * 256
        more_in += [*t_meta, t_idx, t_seg]
        more_specs += [SMEM_SPEC] * 6 + [whole_spec(t_seg.shape)]
        more_out.append(jax.ShapeDtypeStruct((t_rows, t_width), BF16))
        more_scratch += [pltpu.VMEM((t_total, t_width), F32), pltpu.VMEM((BLOCK, t_width), BF16),
                         pltpu.VMEM((BLOCK, t_width), BF16), pltpu.VMEM((t_rows, t_width), BF16),
                         pltpu.SemaphoreType.DMA((PIECES,))]
    nm = len(more_in)

    def kern(*refs):
        meta_refs, (idx_ref, seg_ref), refs = refs[:5], refs[5:7], refs[7:]
        hb, refs = refs[:nh], refs[nh:]
        bl, refs = refs[:nb], refs[nb:]
        fx, refs = refs[:nf], refs[nf:]
        extra, refs = refs[:nm], refs[nm:]
        out, refs = refs[:no], refs[no:]
        last_out, refs = refs[:len(more_out)], refs[len(more_out):]
        tab, acc, buf_0, buf_1, isem = refs[:5]
        stages, sems, scratch = refs[5:5 + ns], refs[5 + ns:5 + 2 * ns], refs[5 + 2 * ns:]
        if late:
            begin, scratch = scratch[0], scratch[1:]
        i = pl.program_id(0)

        @pl.when(i == 0)
        def _():
            copies = [fetch(h, st, sm, parts) for h, st, sm in zip(hb, stages, sems)]
            if init is not None:
                start = pltpu.make_async_copy(hb[init], begin if late else acc.at[pl.ds(0, acc_rows), :], isem)
                if not late:
                    start.start()
            if init is None or late:
                zero_rows(acc)
            for o, (_, _, sums) in zip(out, outs):
                if sums:
                    o[...] = jnp.zeros_like(o)
            if then:
                zero_rows(scratch[1])
            build(copies, stages, tab, fx)
            if late:
                start.start()
            if init is not None and not late:
                start.wait()
            segment_sums(meta_refs, idx_ref, seg_ref, tab, acc, (buf_0, buf_1), nc, window, blocks)
            if late:
                start.wait()
            if epilogue is None:
                send_out(acc.at[pl.ds(0, acc_rows), :], out[0], isem)
        if epilogue is not None:
            def part(j, carry):
                at = pl.multiple_of(j * sub, sub)
                row0 = pl.multiple_of(i * tile + at, sub)

                def put(x):
                    put_rows(scratch[0], row0, x, keep)
                a = acc[pl.ds(row0, sub), :]
                if late:
                    a = a + begin[pl.ds(row0, sub), :]
                epilogue(a, [r.at[pl.ds(at, sub), :] for r in bl], fx,
                         [o if sums else o.at[pl.ds(at, sub), :] for o, (_, _, sums) in zip(out, outs)], put)
                return carry
            lax.fori_loop(0, tile // sub, part, 0)

        if pick:
            @pl.when(i == steps - 1)
            def _():
                kept, stage, out_sem = scratch
                size = peers // PIECES

                def piece(k, c):
                    def body(p, carry):
                        for g in range(slots // 16):
                            rows = gather_16(extra[0], k * size + p, g * 16, slots, kept, 1, peers)[0]
                            stage[k * size + p, g * 16:g * 16 + 16, :] = rows
                        return carry
                    lax.fori_loop(0, size, body, 0)
                    send_part(stage, last_out[0], out_sem, k).start()
                    return c
                lax.fori_loop(0, PIECES, piece, 0)
                for k in range(PIECES):
                    send_part(stage, last_out[0], out_sem, k).wait()
        if then:
            @pl.when(i == steps - 1)
            def _():
                kept, acc_2, buf_2, buf_3, stage, out_sem = scratch
                segment_sums(extra[:5], extra[5], extra[6], kept, acc_2, (buf_2, buf_3), t_nc, t_window,
                             t_seg.shape[0])
                size = t_rows // PIECES
                step = math.gcd(1024, size)

                def piece(k, c):
                    def part(j, carry):
                        at = pl.multiple_of(k * size + j * step, step)
                        stage[pl.ds(at, step), :] = finish(acc_2[pl.ds(at, step), :], fx)
                        return carry
                    lax.fori_loop(0, size // step, part, 0)
                    send_part(stage, last_out[0], out_sem, k).start()
                    return c
                lax.fori_loop(0, PIECES, piece, 0)
                for k in range(PIECES):
                    send_part(stage, last_out[0], out_sem, k).wait()

    out_shape, out_specs = [], []
    for shape, dtype, sums in outs:
        out_shape.append(jax.ShapeDtypeStruct(shape, dtype))
        out_specs.append(HBM_SPEC if epilogue is None else whole_spec(shape) if sums else row_spec(tile, shape[1]))
    return pl.pallas_call(
        kern, name=name, grid=(steps,), out_shape=out_shape + more_out,
        in_specs=([SMEM_SPEC] * 6 + [whole_spec(seg.shape)] + [HBM_SPEC] * nh
                  + [row_spec(tile, x.shape[1]) for x in blocked] + [whole_spec(x.shape) for x in fixed] + more_specs),
        out_specs=out_specs + [HBM_SPEC] * len(more_out),
        scratch_shapes=([pltpu.VMEM((table_rows * nc, LANES), F32), pltpu.VMEM((acc_total, width), F32),
                         pltpu.VMEM((BLOCK, width), BF16), pltpu.VMEM((BLOCK, width), BF16),
                         pltpu.SemaphoreType.DMA(())]
                        + [pltpu.VMEM(shape, BF16) for shape in sources]
                        + [pltpu.SemaphoreType.DMA((parts,)) for _ in sources] + late_scratch + more_scratch),
        compiler_params=params(), cost_estimate=cost(micros))(*meta, idx, seg, *hbm_in, *blocked, *fixed, *more_in)


SHARE = 16


def grad_places(shapes):
    places, at = [], 0
    for rows, width in shapes:
        columns = []
        for _ in range(width // LANES):
            columns.append(at)
            at += -(-rows // SHARE)
        places.append(columns)
    return places, at


def sum_over_devices(grads, sums, total, classes, peers):
    chips = peers // 2
    places, used = grad_places([g.shape for g in grads] + [(SHARE, LANES)])
    rounds = -(-used // peers)
    rows = SHARE * rounds
    widths = [x.shape[1] for x in sums]

    def device(chip, core):
        return chip * 2 + core

    def kern(*refs):
        ng, ns = len(grads), len(sums)
        g_refs, s_refs, out_ref = refs[:ng], refs[ng:ng + ns], refs[ng + ns]
        x_ref, half, mine, got, pair_sem, send_sem, recv_sem, send_2, recv_2 = refs[ng + ns + 1:]
        me = lax.axis_index(GROUP_AXIS)
        chip, core = me // 2, me % 2
        mate = device(chip, 1 - core)
        barrier = pltpu.get_barrier_semaphore()

        def hello(to):
            pl.semaphore_signal(barrier, inc=1, device_id=(to,), device_id_type=pl.DeviceIdType.MESH)

        def greet(k, carry):
            hello(device((chip + k) % chips, core))
            return carry
        lax.fori_loop(1, chips, greet, 0)
        hello(mate)

        def at(q):
            unit = q // rounds
            return unit // chips, unit % chips, (q % rounds) * SHARE

        def put(q, value):
            h, c, r = at(q)
            x_ref[h, c, r:r + SHARE, :] = value
        for g, columns in zip(g_refs, places):
            for w, first in enumerate(columns):
                for k in range(g.shape[0] // SHARE):
                    put(first + k, g[k * SHARE:(k + 1) * SHARE, w * LANES:(w + 1) * LANES])
        row = lax.broadcasted_iota(jnp.int32, (SHARE, LANES), 0)
        small, line = jnp.zeros((SHARE, LANES), F32), 0
        for s_ref, width in zip(s_refs, widths):
            for w in range(width // LANES):
                total = jnp.sum(s_ref[:, w * LANES:(w + 1) * LANES], axis=0, keepdims=True)
                small = jnp.where(row == line, total, small)
                line += 1
        put(places[-1][0], small)
        for q in range(used, peers * rounds):
            put(q, jnp.zeros((SHARE, LANES), F32))

        def pair(src, dst, k):
            return pltpu.make_async_remote_copy(src_ref=src, dst_ref=dst, send_sem=pair_sem.at[2 * k],
                                                recv_sem=pair_sem.at[2 * k + 1], device_id=(mate,),
                                                device_id_type=pl.DeviceIdType.MESH)
        pl.semaphore_wait(barrier, chips)
        first = pair(x_ref.at[1 - core], half, 0)
        first.start()
        first.wait()

        def add(c, carry):
            mine[c] = x_ref[core, c] + half[c]
            return carry
        lax.fori_loop(0, chips, add, 0)

        def share(k):
            to = (chip + k) % chips
            return pltpu.make_async_remote_copy(src_ref=mine.at[to], dst_ref=got.at[chip], send_sem=send_sem.at[k],
                                                recv_sem=recv_sem.at[chip], device_id=(device(to, core),),
                                                device_id_type=pl.DeviceIdType.MESH)

        def landed(k):
            frm = (chip + k) % chips
            return pltpu.make_async_remote_copy(src_ref=mine.at[frm], dst_ref=got.at[frm], send_sem=send_sem.at[k],
                                                recv_sem=recv_sem.at[frm], device_id=(me,),
                                                device_id_type=pl.DeviceIdType.MESH)

        def start(k, carry):
            share(k).start()
            return carry
        lax.fori_loop(1, chips, start, 0)
        got[chip] = mine[chip]

        def settle(k, carry):
            landed(k).wait_recv()
            return carry
        lax.fori_loop(1, chips, settle, 0)

        def more(c, total):
            return total + got[c]
        out_ref[core, chip] = lax.fori_loop(0, chips, more, jnp.zeros((rows, LANES), F32))

        def drain(k, carry):
            share(k).wait_send()
            return carry
        lax.fori_loop(1, chips, drain, 0)

        def give(k):
            return pltpu.make_async_remote_copy(src_ref=out_ref.at[core, chip], dst_ref=out_ref.at[core, chip],
                                                send_sem=send_2.at[k], recv_sem=recv_2.at[chip],
                                                device_id=(device((chip + k) % chips, core),),
                                                device_id_type=pl.DeviceIdType.MESH)

        def given(k):
            frm = (chip + k) % chips
            return pltpu.make_async_remote_copy(src_ref=out_ref.at[core, frm], dst_ref=out_ref.at[core, frm],
                                                send_sem=send_2.at[k], recv_sem=recv_2.at[frm], device_id=(me,),
                                                device_id_type=pl.DeviceIdType.MESH)

        def start_2(k, carry):
            give(k).start()
            return carry
        lax.fori_loop(1, chips, start_2, 0)

        def settle_2(k, carry):
            given(k).wait_recv()
            return carry
        lax.fori_loop(1, chips, settle_2, 0)

        def drain_2(k, carry):
            give(k).wait_send()
            return carry
        lax.fori_loop(1, chips, drain_2, 0)
        last = pair(out_ref.at[core], out_ref.at[core], 1)
        last.start()
        last.wait()

    vmem = pl.BlockSpec(memory_space=pltpu.VMEM)
    shape = (2, chips, rows, LANES)
    full = pl.pallas_call(
        kern, name='sum_all', out_shape=jax.ShapeDtypeStruct(shape, F32),
        in_specs=[vmem] * (len(grads) + len(sums)), out_specs=vmem,
        scratch_shapes=[pltpu.VMEM(shape, F32), pltpu.VMEM(shape[1:], F32), pltpu.VMEM(shape[1:], F32),
                        pltpu.VMEM(shape[1:], F32), pltpu.SemaphoreType.DMA((4,)),
                        pltpu.SemaphoreType.DMA((chips,)), pltpu.SemaphoreType.DMA((chips,)),
                        pltpu.SemaphoreType.DMA((chips,)), pltpu.SemaphoreType.DMA((chips,))],
        compiler_params=pltpu.CompilerParams(collective_id=0, has_side_effects=True), cost_estimate=cost(25))(*grads, *sums)

    def unpack_kern(full_ref, total_ref, *outs):
        def part(q):
            unit = q // rounds
            r = (q % rounds) * SHARE
            return full_ref[unit // chips, unit % chips, r:r + SHARE, :]

        def move(o, columns, skip):
            for w, first in enumerate(columns):
                for k in range(o.shape[0] // SHARE):
                    o[k * SHARE:(k + 1) * SHARE, w * LANES:(w + 1) * LANES] = part(first + skip + k)
        move(outs[0], places[0], 0)
        move(outs[1], places[0], outs[0].shape[0] // SHARE)
        for o, columns in zip(outs[2:], places[1:-2]):
            move(o, columns, 0)
        both = jnp.concatenate([part(places[-2][0] + k) for k in range(rows_3 // SHARE)], axis=0).T
        outs[ng][...] = both[:classes, :]
        outs[ng + 1][...] = both[SPREAD:SPREAD + classes, :]
        small, line = part(places[-1][0]), 0
        for o, width in zip(outs[ng + 2:-1], widths):
            for w in range(width // LANES):
                wide = min(LANES, o.shape[1] - w * LANES)
                o[:, w * LANES:w * LANES + wide] = small[line:line + 1, :wide]
                line += 1
        outs[-1][...] = jnp.sum(small[line:line + 1, :SPREAD], axis=1, keepdims=True) / total_ref[...]
    ng = len(grads)
    rows_3 = grads[-1].shape[0]
    rows_1, width_1 = grads[0].shape
    outs = ([(rows_1 // 2, width_1)] * 2 + [g.shape for g in grads[1:-1]] + [(classes, rows_3)] * 2
            + [(1, w) for w in widths[:-2]] + [(1, classes), (1, 1)])
    return pl.pallas_call(unpack_kern, name='unpack_sums', out_shape=[jax.ShapeDtypeStruct(o, F32) for o in outs],
                          in_specs=[vmem, vmem], out_specs=[vmem] * len(outs), cost_estimate=cost(3))(full, total)


def edge_meta(seg_first, seg_last, window, first_block, end_block):
    blocks = seg_first.shape[0]
    shift = group_of(blocks).bit_length() - 1
    at = jnp.arange(blocks, dtype=jnp.int32)
    base = seg_first & ~7
    inside = (at >= first_block) & (at < end_block)
    count = jnp.where(inside, lax.div(jnp.maximum(seg_last - base, 0), jnp.int32(window)) + 1, 1)
    scalars = [first_block >> shift, (end_block + (1 << shift) - 1) >> shift, jnp.max(count)]
    return [base, count] + [x.reshape(1) for x in scalars]


def bits_for(n):
    return max(1, (n - 1).bit_length())


def spread3(w):
    w = jnp.pad(w, ((0, 0), (0, SPREAD - w.shape[1])))
    return jnp.pad(jnp.concatenate([w, w, w], axis=1), ((0, 0), (0, LANES - 3 * SPREAD)))


def lanes_pad(w):
    return jnp.pad(w, ((0, 0), (0, LANES - w.shape[1])))


def solution(mesh):
    peers = mesh.shape[GROUP_AXIS]

    def exchange(x):
        return lax.all_to_all(x, GROUP_AXIS, 0, 0, tiled=True)

    def device_step(features, labels, train_mask, send_idx, src_idx, dst_idx, inv_deg,
                    w_self_1, w_neigh_1, bias_1, w_self_2, w_neigh_2, bias_2,
                    w_self_3, w_neigh_3, bias_3):
        n = features.shape[0]
        slots = send_idx.shape[1]
        halo = peers * slots
        edges = src_idx.shape[0]
        hidden = w_self_1.shape[1]
        classes = w_self_3.shape[1]
        send_flat = send_idx.T.reshape(-1)
        tile = next(t for t in (4096, 1024) if n % t == 0)
        half_tile = tile // 2
        slot_bits = bits_for(halo)
        dst_bits = bits_for(n)
        table = n + halo

        blocks = edges // BLOCK
        halo_blocks = halo // BLOCK
        zero = jnp.int32(0)
        win_e, win_h, win_r = 192, 208, 272
        owned = jnp.sum((src_idx < n).astype(jnp.int32))
        block_shift = BLOCK.bit_length() - 1
        near_end = (owned + BLOCK - 1) >> block_shift
        far_start = owned >> block_shift

        src_bits = bits_for(table)
        far_bit = dst_bits + src_bits
        by_dst = lax.sort(((src_idx >= n).astype(jnp.int32) << far_bit) | (dst_idx << src_bits) | src_idx, is_stable=False)
        src_f = by_dst & ((1 << src_bits) - 1)
        dst_f = (by_dst >> src_bits) & ((1 << dst_bits) - 1)
        is_far = src_f >= n
        src_near = jnp.minimum(src_f, n - 1)
        src_far = jnp.maximum(src_f - n, 0)
        seg_near = jnp.where(is_far, -1, dst_f).reshape(blocks, 1, BLOCK)
        seg_far = jnp.where(is_far, dst_f, -1).reshape(blocks, 1, BLOCK)
        first, last = dst_f[::BLOCK], dst_f[BLOCK - 1::BLOCK]
        meta_near = edge_meta(first, jnp.where(is_far[BLOCK - 1::BLOCK], n - 1, last), win_e, zero, near_end)
        meta_far = edge_meta(jnp.where(is_far[::BLOCK], first, 0), last, win_e, far_start, jnp.int32(blocks))

        inv = jnp.broadcast_to(inv_deg[:, None], (n, LANES))
        b1 = bias_1.reshape(1, -1)
        b2 = bias_2.reshape(1, -1)
        lane = jnp.arange(LANES, dtype=jnp.int32)
        used = lane < 3 * SPREAD
        folder = jnp.tile(((lane[:, None] % SPREAD == lane[None, :] % SPREAD) & used[:, None] & used[None, :]).astype(BF16),
                          (3, 1))
        b3 = jnp.where(lane < 3 * SPREAD, spread3(bias_3.reshape(1, -1)), -1e30)
        if classes < SPREAD:
            b3 = jnp.where(lane % SPREAD < classes, b3, -1e30)
        target = jnp.where(lane[None, :] < 3 * SPREAD,
                           train_mask[:, None] * (1.0 + (labels[:, None] == lane[None, :] % SPREAD)), 0.0).astype(BF16)
        ws3, wn3 = spread3(w_self_3), spread3(w_neigh_3)
        ws3_t, wn3_t = lanes_pad(w_self_3).T, lanes_pad(w_neigh_3).T

        def rows_of(nc):
            def build(copies, stages, tab, fx):
                unpack(copies[0], stages[0], tab, 0, nc)
            return build

        def near_sums(name, nc, idx, rows, also):
            return edge_call(name, (meta_near, idx, seg_near), nc, n, n, win_e, [rows.shape], rows_of(nc),
                             [rows] + also, [], [], [((n, nc * LANES), F32, False)], n, tile, None, 20)[0]

        out_1 = pick_rows('send_1', features, send_flat, peers, slots, train_mask.reshape(-1, LANES))
        got_1 = exchange(out_1)
        near_1 = near_sums('near_1', 1, src_near, features, [inv])
        counts = got_1[:, slots, :2].astype(F32)
        total = jnp.sum(counts[:, 0]) * LANES + jnp.sum(counts[:, 1])

        def build_1(copies, stages, tab, fx):
            per = peers // len(copies[0])
            some = math.gcd(per, 8)
            for p in range(len(copies[0])):
                copies[0][p].wait()

                def body(k, carry):
                    q = p * per + k * some
                    rows = stages[0][pl.ds(q, some), :slots, :].reshape(some * slots, LANES)
                    put_rows(tab, q * slots, rows.astype(F32), 1)
                    return carry
                lax.fori_loop(0, per // some, body, 0)

        def epi_1(a, bl, fx, out, put):
            mean = (a * bl[1][...]).astype(BF16)
            z = mm(bl[0][...], fx[0][...]) + mm(mean, fx[1][...]) + fx[2][...]
            out[0][...] = mean
            out[1][...] = jnp.maximum(z, 0.0).astype(BF16)
            put(mean.astype(F32))

        mean_1, hidden_1, out_2 = edge_call(
            'layer_1', (meta_far, src_far, seg_far), 1, halo, n, win_e, [(peers, slots + TAIL, LANES)], build_1,
            [got_1, near_1], [features, inv], [w_self_1, w_neigh_1, b1],
            [((n, LANES), BF16, False), ((n, hidden), BF16, False)], n, tile, epi_1, 25, init=1, late=True,
            keep=1, pick=(send_flat, peers, slots))

        place = jnp.arange(halo, dtype=jnp.int32)
        keys = jnp.concatenate([(src_idx << dst_bits) | dst_idx,
                                (1 << 30) | (send_flat << slot_bits) | (place % peers * slots + place // peers)])
        keys = lax.optimization_barrier((keys, mean_1))[0]
        ordered = lax.sort(keys, is_stable=False)
        by_src, by_row = ordered[:edges], ordered[edges:] & ((1 << 30) - 1)
        src_s = by_src >> dst_bits
        dst_s = by_src & ((1 << dst_bits) - 1)
        row_s = by_row >> slot_bits
        slot_s = by_row & ((1 << slot_bits) - 1)
        first, last = src_s[::BLOCK], src_s[BLOCK - 1::BLOCK]
        meta_own = edge_meta(jnp.minimum(first, n - 1), jnp.minimum(last, n - 1), win_e, zero, near_end)
        meta_halo = edge_meta(jnp.maximum(first - n, 0), jnp.maximum(last - n, 0), win_h, far_start, jnp.int32(blocks))
        meta_owner = edge_meta(row_s[::BLOCK], row_s[BLOCK - 1::BLOCK], win_r, zero, jnp.int32(halo_blocks))
        seg_o = src_s.reshape(blocks, 1, BLOCK)
        seg_h = seg_o - n
        seg_r = row_s.reshape(halo_blocks, 1, BLOCK)
        dst_wide = tile_linear(dst_s)

        got_2 = exchange(out_2)
        near_2 = near_sums('near_2', 2, tile_linear(src_near), hidden_1, [])

        def build_2(copies, stages, tab, fx):
            per = peers // len(copies[0])
            some = math.gcd(per, 8)
            for p in range(len(copies[0])):
                copies[0][p].wait()
                copies[1][p].wait()

                def body(k, carry):
                    q = p * per + k * some
                    f = stages[0][pl.ds(q, some), :slots, :].reshape(some * slots, LANES)
                    m = stages[1][pl.ds(q, some)].reshape(some * slots, LANES)
                    z = mm(f, fx[3][...]) + mm(m, fx[4][...]) + fx[5][...]
                    put_rows(tab, q * slots, jnp.maximum(z, 0.0).astype(BF16).astype(F32), 2)
                    return carry
                lax.fori_loop(0, per // some, body, 0)

        def epi_2(a, bl, fx, out, put):
            scale = bl[1][...]
            mean = (a * jnp.concatenate([scale, scale], axis=1)).astype(BF16)
            z = mm(bl[0][...], fx[0][...]) + mm(mean, fx[1][...]) + fx[2][...]
            h = jnp.maximum(z, 0.0).astype(BF16)
            out[0][...] = mean
            out[1][...] = h
            both = mm(h, fx[6][...])
            pieces = split3(both[:, :LANES])
            out[2][...] = pieces
            out[3][...] = both[:, LANES:]
            put(pieces.astype(F32))

        mean_2, hidden_2, proj, logits_self, out_3 = edge_call(
            'layer_2', (meta_far, tile_linear(src_far), seg_far), 2, halo, n, win_e,
            [(peers, slots + TAIL, LANES), (peers, slots, LANES)], build_2, [got_1, got_2, near_2],
            [hidden_1, inv], [w_self_2, w_neigh_2, b2, w_self_1, w_neigh_1, b1, jnp.concatenate([wn3, ws3], axis=1)],
            [((n, hidden), BF16, False), ((n, hidden), BF16, False), ((n, LANES), BF16, False),
             ((n, LANES), F32, False)], n, tile, epi_2, 40, init=2, keep=1, pick=(send_flat, peers, slots))

        got_3 = exchange(out_3).reshape(halo, LANES)
        near_3 = near_sums('near_3', 1, src_near, proj, [target])
        inv_total = (1.0 / total).reshape(1, 1)

        def epi_3(a, bl, fx, out, put):
            scale = bl[1][...]
            z = bl[0][...] + fold3(a * scale, fx[2][...]) + fx[0][...]
            top = jnp.max(z, axis=1, keepdims=True)
            e = jnp.exp(z - top)
            each = jnp.sum(e, axis=1, keepdims=True) * (1.0 / 3.0)
            lse = top + jnp.log(each)
            t = bl[2][...].astype(F32)
            inside = jnp.minimum(t, 1.0)
            hit = t - inside
            d = (e * (1.0 / each) * inside - hit) * fx[1][...]
            db = d.astype(BF16)
            out[0][...] = db
            pieces = split3(db.astype(F32) * scale)
            out[1][...] = pieces
            put(pieces.astype(F32))
            add_rows(out[2], d)
            add_rows(out[3], hit * (lse - z))

        def finish_3(a, fx):
            return split3(fold3(a, fx[2][...]))

        d_bf_3, scaled_3, g_b3, loss_parts, back_3 = edge_call(
            'layer_3', (meta_far, src_far, seg_far), 1, halo, n, win_e, [(halo, LANES)], rows_of(1), [got_3, near_3],
            [logits_self, inv, target], [b3, jnp.broadcast_to(inv_total, (1, LANES)), folder],
            [((n, LANES), BF16, False), ((n, LANES), BF16, False), ((8, LANES), F32, True), ((8, LANES), F32, True)],
            n, tile, epi_3, 30, init=1, late=True, keep=1,
            then=((meta_halo, dst_s, seg_h), 1, halo, win_h, finish_3))

        ret_3 = exchange(back_3.reshape(peers, slots, LANES)).reshape(halo, LANES)
        own_3 = edge_call('back_3_own', (meta_own, dst_s, seg_o), 1, n, n, win_e, [(n, LANES)], rows_of(1),
                          [scaled_3], [], [], [((n, LANES), F32, False)], n, tile, None, 20)[0]

        def epi_o3(a, bl, fx, out, put):
            tb = fold3(a, fx[2][...]).astype(BF16)
            d_h = mm(jnp.concatenate([bl[0][...], tb], axis=1), fx[0][...])
            d_pre = jnp.where(bl[1][...].astype(F32) > 0, d_h, 0.0)
            db = d_pre.astype(BF16)
            scale = bl[2][...]
            out[0][...] = tb
            out[1][...] = db
            scaled = (mm(db, fx[1][...]) * jnp.concatenate([scale, scale], axis=1)).astype(BF16)
            out[2][...] = scaled
            put(scaled.astype(F32))
            add_rows(out[3], d_pre)

        def finish_2(a, fx):
            return a.astype(BF16)

        tb_3, d_bf_2, scaled_2, g_b2, back_2 = edge_call(
            'owner_3', (meta_owner, slot_s, seg_r), 1, halo, n, win_r, [(halo, LANES)], rows_of(1), [ret_3, own_3],
            [d_bf_3, hidden_2, inv], [jnp.concatenate([ws3_t, wn3_t], axis=0), w_neigh_2.T, folder],
            [((n, LANES), BF16, False), ((n, hidden), BF16, False), ((n, hidden), BF16, False), ((8, hidden), F32, True)],
            n, half_tile, epi_o3, 30, init=1, late=True, keep=2,
            then=((meta_halo, dst_wide, seg_h), 2, halo, win_h, finish_2))

        def epi_b2o(a, bl, fx, out, put):
            out[0][...] = a + mm(bl[0][...], fx[0][...])

        ret_2 = exchange(back_2.reshape(peers, slots, hidden)).reshape(halo, hidden)
        own_2 = edge_call('back_2_own', (meta_own, dst_wide, seg_o), 2, n, n, win_e, [(n, hidden)], rows_of(2),
                          [scaled_2], [d_bf_2], [w_self_2.T], [((n, hidden), F32, False)], n, tile, epi_b2o, 30)[0]

        def epi_o2(a, bl, fx, out, put):
            d_pre = jnp.where(bl[0][...].astype(F32) > 0, a, 0.0)
            inputs = jnp.concatenate([bl[1][...], bl[2][...]], axis=1)
            out[0][...] += lax.dot_general(inputs, d_pre.astype(BF16), (((0,), (0,)), ((), ())),
                                           preferred_element_type=F32)
            add_rows(out[1], d_pre)

        g_1, g_b1 = edge_call(
            'owner_2', (meta_owner, tile_linear(slot_s), seg_r), 2, halo, n, win_r, [(halo, hidden)], rows_of(2),
            [ret_2, own_2], [hidden_1, features, mean_1], [],
            [((2 * LANES, hidden), F32, True), ((8, hidden), F32, True)], n, half_tile, epi_o2, 25, init=1, late=True)

        def contract(a, b):
            return jnp.einsum('nd,ne->de', a, b, preferred_element_type=F32)

        at = jnp.arange(LANES, dtype=jnp.int32)[None, :]
        g_3 = jnp.where(at < SPREAD, contract(hidden_2, d_bf_3), contract(hidden_2, tb_3))
        g1s, g1n, g2s, g2n, g3s, g3n, s1, s2, s3, loss = sum_over_devices(
            [g_1, contract(hidden_1, d_bf_2), contract(mean_2, d_bf_2), g_3],
            [g_b1, g_b2, g_b3, loss_parts], total.reshape(1, 1), classes, peers)
        return (loss.reshape(()), g1s, g1n, s1.reshape(-1), g2s, g2n, s2.reshape(-1), g3s.T, g3n.T, s3.reshape(-1))

    sharded = P(GROUP_AXIS)
    whole = P()
    return jax.shard_map(device_step, mesh=mesh,
                         in_specs=(sharded,) * 7 + (whole,) * 9,
                         out_specs=(whole,) * 10, check_vma=False)
```

```python
import math

import jax
import jax.numpy as jnp
from jax import lax
from jax.experimental import pallas as pl
from jax.experimental.pallas import tpu as pltpu
from jax.sharding import PartitionSpec as P

GROUP_AXIS = 'gp'
LANES = 128
SPREAD = 40
BLOCK = 128
GROUP = 8
TAIL = 8
F32 = jnp.float32
BF16 = jnp.bfloat16
VMEM_LIMIT = 63 * 2 ** 20

SMEM_SPEC = pl.BlockSpec(memory_space=pltpu.SMEM)
HBM_SPEC = pl.BlockSpec(memory_space=pltpu.HBM)


def whole_spec(shape):
    return pl.BlockSpec(shape, lambda i: (0,) * len(shape))


def row_spec(rows, width):
    return pl.BlockSpec((rows, width), lambda i: (i, 0))


def params():
    return pltpu.CompilerParams(vmem_limit_bytes=VMEM_LIMIT, dimension_semantics=('arbitrary',))


def cost(micros):
    return pl.CostEstimate(flops=int(micros * 4e6), bytes_accessed=int(micros * 1e6), transcendentals=0)


def mm(a, b):
    return jnp.dot(a, b, preferred_element_type=F32)


def tile_linear(row):
    return ((row >> 3) << 4) | (row & 7)


def put_rows(tab, row0, x, nc):
    rows = x.shape[0]
    if nc == 1:
        tab[pl.ds(pl.multiple_of(row0, 8), rows), :] = x
    else:
        for g in range(rows // 8):
            for c in range(nc):
                at = pl.multiple_of((row0 + g * 8) * nc + c * 8, 8)
                tab[pl.ds(at, 8), :] = x[g * 8:g * 8 + 8, c * LANES:(c + 1) * LANES]


def fetch(src, stage, sem, parts):
    rows = src.shape[0] // parts
    copies = [pltpu.make_async_copy(src.at[pl.ds(k * rows, rows)], stage.at[pl.ds(k * rows, rows)], sem.at[k])
              for k in range(parts)]
    for c in copies:
        c.start()
    return copies


def unpack(copies, stage, tab, row0, nc):
    rows = stage.shape[0] // len(copies)
    step = next(d for d in (128, 96, 64, 32, 16) if rows % d == 0)
    for p, c in enumerate(copies):
        c.wait()

        def body(k, carry):
            at = pl.multiple_of(p * rows + k * step, step)
            put_rows(tab, row0 + at, stage[pl.ds(at, step), :].astype(F32), nc)
            return carry
        lax.fori_loop(0, rows // step, body, 0)


def group_of(blocks):
    return next(u for u in (GROUP, 4, 2) if blocks % u == 0)


def zero_rows(acc):
    rows = acc.shape[0]
    step = next(s for s in (256, 128, 64, 32, 16, 8) if rows % s == 0)

    def body(k, carry):
        acc[pl.ds(pl.multiple_of(k * step, step), step), :] = jnp.zeros((step, acc.shape[1]), F32)
        return carry
    lax.fori_loop(0, rows // step, body, 0)


def gather_16(idx, base, first, reach, tab, nc, stride=1):
    sub = lax.broadcasted_iota(jnp.int32, (8, LANES), 0)
    room = idx.shape[0] - (reach - 1) * stride
    halves = [[None, None] for _ in range(nc)]
    for h in range(2):
        for k in range(8):
            at = idx.at[pl.ds((first + h * 8 + k) * stride, room)][base]
            for c in range(nc):
                row = jnp.broadcast_to(tab[pl.ds(at + 8 * c, 1), :], (8, LANES))
                halves[c][h] = row if k == 0 else jnp.where(sub == k, row, halves[c][h])
    return [jnp.concatenate(halves[c], axis=0).astype(BF16) for c in range(nc)]


def segment_sums(meta, idx, seg, tab, acc, bufs, nc, window, blocks):
    unroll = group_of(blocks)
    base, counts = meta[:2]
    first_trip, end_trip, most = [m[0] for m in meta[2:]]

    def fill(start, first, reach, buf):
        for g in range(BLOCK // 16):
            parts = gather_16(idx, start, first + g * 16, reach, tab, nc)
            for c in range(nc):
                buf[g * 16:g * 16 + 16, c * LANES:(c + 1) * LANES] = parts[c]

    def sums(b, at, buf):
        rows = lax.broadcasted_iota(jnp.int32, (window, BLOCK), 0) + at
        return mm(jnp.where(rows == seg[b], 1.0, 0.0).astype(BF16), buf[...])

    def add(at, x):
        acc[pl.ds(pl.multiple_of(at, 8), window), :] += x

    span = unroll * BLOCK
    last_trip = blocks // unroll - 1
    fill(jnp.minimum(first_trip, last_trip) * span, 0, span, bufs[0])

    def body(t, carry):
        before = None
        for u in range(unroll):
            b = t * unroll + u
            now = (base[b], sums(b, base[b], bufs[u % 2]))
            if u + 1 < unroll:
                fill(t * span, (u + 1) * BLOCK, span, bufs[(u + 1) % 2])
            else:
                fill(jnp.minimum(t + 1, last_trip) * span, 0, span, bufs[0])
            if before is not None:
                add(*before)
            before = now
        add(*before)
        return carry
    lax.fori_loop(first_trip, end_trip, body, 0)

    @pl.when(most > 1)
    def _():
        def again(b, carry):
            count = counts[b]

            @pl.when(count > 1)
            def _():
                fill(b * BLOCK, 0, BLOCK, bufs[0])

                def more(w, c):
                    at = base[b] + w * window
                    add(at, sums(b, at, bufs[0]))
                    return c
                lax.fori_loop(1, count, more, 0)
            return carry
        lax.fori_loop(first_trip * unroll, end_trip * unroll, again, 0)


def spread_lanes():
    return lax.broadcasted_iota(jnp.int32, (1, LANES), 1)


def split3(x):
    hi = x.astype(BF16).astype(F32)
    rest = x - hi
    mid = rest.astype(BF16).astype(F32)
    low = rest - mid
    lane = spread_lanes()
    out = jnp.where(lane < SPREAD, hi, jnp.where(lane < 2 * SPREAD, mid, low))
    return jnp.where(lane < 3 * SPREAD, out, 0.0).astype(BF16)


def pieces3(a):
    hi = a.astype(BF16)
    rest = a - hi.astype(F32)
    mid = rest.astype(BF16)
    low = (rest - mid.astype(F32)).astype(BF16)
    return jnp.concatenate([hi, mid, low], axis=1)


def fold3(a, folder):
    return mm(pieces3(a), folder)


def add_rows(ref, x):
    ref[...] += jnp.sum(x.reshape(x.shape[0] // 8, 8, x.shape[1]), axis=0)


PIECES = 4


def send_part(stage, out, sem, k):
    size = stage.shape[0] // PIECES
    at = pl.multiple_of(k * size, size)
    return pltpu.make_async_copy(stage.at[pl.ds(at, size)], out.at[pl.ds(at, size)], sem.at[k])


def send_out(src, out, sem):
    done = pltpu.make_async_copy(src, out, sem)
    done.start()
    done.wait()


def pick_pieces(idx, tab, stage, out, sem, peers, slots):
    size = peers // PIECES

    def piece(k, c):
        def body(p, carry):
            for g in range(slots // 16):
                stage[k * size + p, g * 16:g * 16 + 16, :] = gather_16(idx, k * size + p, g * 16, slots, tab, 1, peers)[0]
            return carry
        lax.fori_loop(0, size, body, 0)
        send_part(stage, out, sem, k).start()
        return c
    lax.fori_loop(0, PIECES, piece, 0)
    for k in range(PIECES):
        send_part(stage, out, sem, k).wait()


def pick_rows(name, src, idx, peers, slots, mask):
    n = src.shape[0]
    parts = math.gcd(n // 128, 4)

    def kern(idx_ref, src_ref, mask_ref, out, tab, stage, sem, rows, out_sem):
        copies = fetch(src_ref, stage, sem, parts)
        total = jnp.sum(mask_ref[...], axis=(0, 1), keepdims=True)
        high = jnp.floor(total * (1.0 / LANES))
        first = lax.broadcasted_iota(jnp.int32, (TAIL, LANES), 0) == 0
        lane = lax.broadcasted_iota(jnp.int32, (TAIL, LANES), 1)
        digits = jnp.where(lane == 0, high, jnp.where(lane == 1, total - high * LANES, 0.0))
        tail = jnp.where(first, digits, 0.0).astype(BF16)

        def put_tail(p, c):
            rows[p, slots:slots + TAIL, :] = tail
            return c
        lax.fori_loop(0, peers, put_tail, 0)
        unpack(copies, stage, tab, 0, 1)
        pick_pieces(idx_ref, tab, rows, out, out_sem, peers, slots)

    return pl.pallas_call(
        kern, name=name, out_shape=jax.ShapeDtypeStruct((peers, slots + TAIL, LANES), BF16),
        in_specs=[SMEM_SPEC, HBM_SPEC, pl.BlockSpec(memory_space=pltpu.VMEM)], out_specs=HBM_SPEC,
        scratch_shapes=[pltpu.VMEM((n, LANES), F32), pltpu.VMEM((n, LANES), BF16), pltpu.SemaphoreType.DMA((parts,)),
                        pltpu.VMEM((peers, slots + TAIL, LANES), BF16), pltpu.SemaphoreType.DMA((PIECES,))],
        compiler_params=pltpu.CompilerParams(vmem_limit_bytes=VMEM_LIMIT), cost_estimate=cost(10))(idx, src, mask)


def edge_call(name, edges, nc, table_rows, acc_rows, window, sources, build, hbm_in, blocked, fixed, outs, rows_out,
              tile, epilogue, micros, init=None, late=False, sub=2048, keep=0, pick=None, then=None):
    meta, idx, seg = edges
    blocks = seg.shape[0]
    width = nc * LANES
    nh, nb, nf, no, ns = len(hbm_in), len(blocked), len(fixed), len(outs), len(sources)
    acc_total = -(-(acc_rows + window) // 256) * 256
    parts = 4
    steps = 1 if epilogue is None else rows_out // tile
    sub = math.gcd(sub, tile)
    more_in, more_specs, more_out, more_scratch = [], [], [], []
    late_scratch = [pltpu.VMEM((acc_rows, width), F32)] if late else []
    if keep:
        more_scratch.append(pltpu.VMEM((rows_out * keep, LANES), F32))
    if pick:
        p_idx, peers, slots = pick
        more_in.append(p_idx)
        more_specs.append(SMEM_SPEC)
        more_out.append(jax.ShapeDtypeStruct((peers, slots, LANES), BF16))
        more_scratch += [pltpu.VMEM((peers, slots, LANES), BF16), pltpu.SemaphoreType.DMA((PIECES,))]
    if then:
        (t_meta, t_idx, t_seg), t_nc, t_rows, t_window, finish = then
        t_width = t_nc * LANES
        t_total = -(-(t_rows + t_window) // 256) * 256
        more_in += [*t_meta, t_idx, t_seg]
        more_specs += [SMEM_SPEC] * 6 + [whole_spec(t_seg.shape)]
        more_out.append(jax.ShapeDtypeStruct((t_rows, t_width), BF16))
        more_scratch += [pltpu.VMEM((t_total, t_width), F32), pltpu.VMEM((BLOCK, t_width), BF16),
                         pltpu.VMEM((BLOCK, t_width), BF16), pltpu.VMEM((t_rows, t_width), BF16),
                         pltpu.SemaphoreType.DMA((PIECES,))]
    nm = len(more_in)

    def kern(*refs):
        meta_refs, (idx_ref, seg_ref), refs = refs[:5], refs[5:7], refs[7:]
        hb, refs = refs[:nh], refs[nh:]
        bl, refs = refs[:nb], refs[nb:]
        fx, refs = refs[:nf], refs[nf:]
        extra, refs = refs[:nm], refs[nm:]
        out, refs = refs[:no], refs[no:]
        last_out, refs = refs[:len(more_out)], refs[len(more_out):]
        tab, acc, buf_0, buf_1, isem = refs[:5]
        stages, sems, scratch = refs[5:5 + ns], refs[5 + ns:5 + 2 * ns], refs[5 + 2 * ns:]
        if late:
            begin, scratch = scratch[0], scratch[1:]
        i = pl.program_id(0)

        @pl.when(i == 0)
        def _():
            copies = [fetch(h, st, sm, parts) for h, st, sm in zip(hb, stages, sems)]
            if init is not None:
                start = pltpu.make_async_copy(hb[init], begin if late else acc.at[pl.ds(0, acc_rows), :], isem)
                if not late:
                    start.start()
            if init is None or late:
                zero_rows(acc)
            for o, (_, _, sums) in zip(out, outs):
                if sums:
                    o[...] = jnp.zeros_like(o)
            if then:
                zero_rows(scratch[1])
            build(copies, stages, tab, fx)
            if late:
                start.start()
            if init is not None and not late:
                start.wait()
            segment_sums(meta_refs, idx_ref, seg_ref, tab, acc, (buf_0, buf_1), nc, window, blocks)
            if late:
                start.wait()
            if epilogue is None:
                send_out(acc.at[pl.ds(0, acc_rows), :], out[0], isem)
        if epilogue is not None:
            def part(j, carry):
                at = pl.multiple_of(j * sub, sub)
                row0 = pl.multiple_of(i * tile + at, sub)

                def put(x):
                    put_rows(scratch[0], row0, x, keep)
                a = acc[pl.ds(row0, sub), :]
                if late:
                    a = a + begin[pl.ds(row0, sub), :]
                epilogue(a, [r.at[pl.ds(at, sub), :] for r in bl], fx,
                         [o if sums else o.at[pl.ds(at, sub), :] for o, (_, _, sums) in zip(out, outs)], put)
                return carry
            lax.fori_loop(0, tile // sub, part, 0)

        if pick:
            @pl.when(i == steps - 1)
            def _():
                kept, stage, out_sem = scratch
                pick_pieces(extra[0], kept, stage, last_out[0], out_sem, peers, slots)
        if then:
            @pl.when(i == steps - 1)
            def _():
                kept, acc_2, buf_2, buf_3, stage, out_sem = scratch
                segment_sums(extra[:5], extra[5], extra[6], kept, acc_2, (buf_2, buf_3), t_nc, t_window,
                             t_seg.shape[0])
                size = t_rows // PIECES
                step = math.gcd(1024, size)

                def piece(k, c):
                    def part(j, carry):
                        at = pl.multiple_of(k * size + j * step, step)
                        stage[pl.ds(at, step), :] = finish(acc_2[pl.ds(at, step), :], fx)
                        return carry
                    lax.fori_loop(0, size // step, part, 0)
                    send_part(stage, last_out[0], out_sem, k).start()
                    return c
                lax.fori_loop(0, PIECES, piece, 0)
                for k in range(PIECES):
                    send_part(stage, last_out[0], out_sem, k).wait()

    out_shape, out_specs = [], []
    for shape, dtype, sums in outs:
        out_shape.append(jax.ShapeDtypeStruct(shape, dtype))
        out_specs.append(HBM_SPEC if epilogue is None else whole_spec(shape) if sums else row_spec(tile, shape[1]))
    return pl.pallas_call(
        kern, name=name, grid=(steps,), out_shape=out_shape + more_out,
        in_specs=([SMEM_SPEC] * 6 + [whole_spec(seg.shape)] + [HBM_SPEC] * nh
                  + [row_spec(tile, x.shape[1]) for x in blocked] + [whole_spec(x.shape) for x in fixed] + more_specs),
        out_specs=out_specs + [HBM_SPEC] * len(more_out),
        scratch_shapes=([pltpu.VMEM((table_rows * nc, LANES), F32), pltpu.VMEM((acc_total, width), F32),
                         pltpu.VMEM((BLOCK, width), BF16), pltpu.VMEM((BLOCK, width), BF16),
                         pltpu.SemaphoreType.DMA(())]
                        + [pltpu.VMEM(shape, BF16) for shape in sources]
                        + [pltpu.SemaphoreType.DMA((parts,)) for _ in sources] + late_scratch + more_scratch),
        compiler_params=params(), cost_estimate=cost(micros))(*meta, idx, seg, *hbm_in, *blocked, *fixed, *more_in)


SHARE = 16


def grad_places(shapes):
    places, at = [], 0
    for rows, width in shapes:
        columns = []
        for _ in range(width // LANES):
            columns.append(at)
            at += -(-rows // SHARE)
        places.append(columns)
    return places, at


def sum_over_devices(grads, sums, total, classes, peers):
    chips = peers // 2
    places, used = grad_places([g.shape for g in grads] + [(SHARE, LANES)])
    rounds = -(-used // peers)
    rows = SHARE * rounds
    widths = [x.shape[1] for x in sums]

    def device(chip, core):
        return chip * 2 + core

    def kern(*refs):
        ng, ns = len(grads), len(sums)
        g_refs, s_refs, out_ref = refs[:ng], refs[ng:ng + ns], refs[ng + ns]
        x_ref, half, mine, got, pair_sem, send_sem, recv_sem, send_2, recv_2 = refs[ng + ns + 1:]
        me = lax.axis_index(GROUP_AXIS)
        chip, core = me // 2, me % 2
        mate = device(chip, 1 - core)
        barrier = pltpu.get_barrier_semaphore()

        def hello(to):
            pl.semaphore_signal(barrier, inc=1, device_id=(to,), device_id_type=pl.DeviceIdType.MESH)

        def greet(k, carry):
            hello(device((chip + k) % chips, core))
            return carry
        lax.fori_loop(1, chips, greet, 0)
        hello(mate)

        def at(q):
            unit = q // rounds
            return unit // chips, unit % chips, (q % rounds) * SHARE

        def put(q, value):
            h, c, r = at(q)
            x_ref[h, c, r:r + SHARE, :] = value
        for g, columns in zip(g_refs, places):
            for w, first in enumerate(columns):
                for k in range(g.shape[0] // SHARE):
                    put(first + k, g[k * SHARE:(k + 1) * SHARE, w * LANES:(w + 1) * LANES])
        row = lax.broadcasted_iota(jnp.int32, (SHARE, LANES), 0)
        small, line = jnp.zeros((SHARE, LANES), F32), 0
        for s_ref, width in zip(s_refs, widths):
            for w in range(width // LANES):
                total = jnp.sum(s_ref[:, w * LANES:(w + 1) * LANES], axis=0, keepdims=True)
                small = jnp.where(row == line, total, small)
                line += 1
        put(places[-1][0], small)
        for q in range(used, peers * rounds):
            put(q, jnp.zeros((SHARE, LANES), F32))

        def pair(src, dst, k):
            return pltpu.make_async_remote_copy(src_ref=src, dst_ref=dst, send_sem=pair_sem.at[2 * k],
                                                recv_sem=pair_sem.at[2 * k + 1], device_id=(mate,),
                                                device_id_type=pl.DeviceIdType.MESH)
        pl.semaphore_wait(barrier, chips)
        first = pair(x_ref.at[1 - core], half, 0)
        first.start()
        first.wait()

        def add(c, carry):
            mine[c] = x_ref[core, c] + half[c]
            return carry
        lax.fori_loop(0, chips, add, 0)

        def share(k):
            to = (chip + k) % chips
            return pltpu.make_async_remote_copy(src_ref=mine.at[to], dst_ref=got.at[chip], send_sem=send_sem.at[k],
                                                recv_sem=recv_sem.at[chip], device_id=(device(to, core),),
                                                device_id_type=pl.DeviceIdType.MESH)

        def landed(k):
            frm = (chip + k) % chips
            return pltpu.make_async_remote_copy(src_ref=mine.at[frm], dst_ref=got.at[frm], send_sem=send_sem.at[k],
                                                recv_sem=recv_sem.at[frm], device_id=(me,),
                                                device_id_type=pl.DeviceIdType.MESH)

        def start(k, carry):
            share(k).start()
            return carry
        lax.fori_loop(1, chips, start, 0)
        got[chip] = mine[chip]

        def settle(k, carry):
            landed(k).wait_recv()
            return carry
        lax.fori_loop(1, chips, settle, 0)

        def more(c, total):
            return total + got[c]
        out_ref[core, chip] = lax.fori_loop(0, chips, more, jnp.zeros((rows, LANES), F32))

        def drain(k, carry):
            share(k).wait_send()
            return carry
        lax.fori_loop(1, chips, drain, 0)

        def give(k):
            return pltpu.make_async_remote_copy(src_ref=out_ref.at[core, chip], dst_ref=out_ref.at[core, chip],
                                                send_sem=send_2.at[k], recv_sem=recv_2.at[chip],
                                                device_id=(device((chip + k) % chips, core),),
                                                device_id_type=pl.DeviceIdType.MESH)

        def given(k):
            frm = (chip + k) % chips
            return pltpu.make_async_remote_copy(src_ref=out_ref.at[core, frm], dst_ref=out_ref.at[core, frm],
                                                send_sem=send_2.at[k], recv_sem=recv_2.at[frm], device_id=(me,),
                                                device_id_type=pl.DeviceIdType.MESH)

        def start_2(k, carry):
            give(k).start()
            return carry
        lax.fori_loop(1, chips, start_2, 0)

        def settle_2(k, carry):
            given(k).wait_recv()
            return carry
        lax.fori_loop(1, chips, settle_2, 0)

        def drain_2(k, carry):
            give(k).wait_send()
            return carry
        lax.fori_loop(1, chips, drain_2, 0)
        last = pair(out_ref.at[core], out_ref.at[core], 1)
        last.start()
        last.wait()

    vmem = pl.BlockSpec(memory_space=pltpu.VMEM)
    shape = (2, chips, rows, LANES)
    full = pl.pallas_call(
        kern, name='sum_all', out_shape=jax.ShapeDtypeStruct(shape, F32),
        in_specs=[vmem] * (len(grads) + len(sums)), out_specs=vmem,
        scratch_shapes=[pltpu.VMEM(shape, F32), pltpu.VMEM(shape[1:], F32), pltpu.VMEM(shape[1:], F32),
                        pltpu.VMEM(shape[1:], F32), pltpu.SemaphoreType.DMA((4,)),
                        pltpu.SemaphoreType.DMA((chips,)), pltpu.SemaphoreType.DMA((chips,)),
                        pltpu.SemaphoreType.DMA((chips,)), pltpu.SemaphoreType.DMA((chips,))],
        compiler_params=pltpu.CompilerParams(collective_id=0, has_side_effects=True), cost_estimate=cost(25))(*grads, *sums)

    def unpack_kern(full_ref, total_ref, *outs):
        def part(q):
            unit = q // rounds
            r = (q % rounds) * SHARE
            return full_ref[unit // chips, unit % chips, r:r + SHARE, :]

        def move(o, columns, skip):
            for w, first in enumerate(columns):
                for k in range(o.shape[0] // SHARE):
                    o[k * SHARE:(k + 1) * SHARE, w * LANES:(w + 1) * LANES] = part(first + skip + k)
        move(outs[0], places[0], 0)
        move(outs[1], places[0], outs[0].shape[0] // SHARE)
        for o, columns in zip(outs[2:], places[1:-2]):
            move(o, columns, 0)
        both = jnp.concatenate([part(places[-2][0] + k) for k in range(rows_3 // SHARE)], axis=0).T
        outs[ng][...] = both[:classes, :]
        outs[ng + 1][...] = both[SPREAD:SPREAD + classes, :]
        small, line = part(places[-1][0]), 0
        for o, width in zip(outs[ng + 2:-1], widths):
            for w in range(width // LANES):
                wide = min(LANES, o.shape[1] - w * LANES)
                o[:, w * LANES:w * LANES + wide] = small[line:line + 1, :wide]
                line += 1
        outs[-1][...] = jnp.sum(small[line:line + 1, :SPREAD], axis=1, keepdims=True) / total_ref[...]
    ng = len(grads)
    rows_3 = grads[-1].shape[0]
    rows_1, width_1 = grads[0].shape
    outs = ([(rows_1 // 2, width_1)] * 2 + [g.shape for g in grads[1:-1]] + [(classes, rows_3)] * 2
            + [(1, w) for w in widths[:-2]] + [(1, classes), (1, 1)])
    return pl.pallas_call(unpack_kern, name='unpack_sums', out_shape=[jax.ShapeDtypeStruct(o, F32) for o in outs],
                          in_specs=[vmem, vmem], out_specs=[vmem] * len(outs), cost_estimate=cost(3))(full, total)


def edge_meta(seg_first, seg_last, window, first_block, end_block):
    blocks = seg_first.shape[0]
    shift = group_of(blocks).bit_length() - 1
    at = jnp.arange(blocks, dtype=jnp.int32)
    base = seg_first & ~7
    inside = (at >= first_block) & (at < end_block)
    count = jnp.where(inside, lax.div(jnp.maximum(seg_last - base, 0), jnp.int32(window)) + 1, 1)
    scalars = [first_block >> shift, (end_block + (1 << shift) - 1) >> shift, jnp.max(count)]
    return [base, count] + [x.reshape(1) for x in scalars]


def bits_for(n):
    return max(1, (n - 1).bit_length())


def spread3(w):
    w = jnp.pad(w, ((0, 0), (0, SPREAD - w.shape[1])))
    return jnp.pad(jnp.concatenate([w, w, w], axis=1), ((0, 0), (0, LANES - 3 * SPREAD)))


def lanes_pad(w):
    return jnp.pad(w, ((0, 0), (0, LANES - w.shape[1])))


def solution(mesh):
    peers = mesh.shape[GROUP_AXIS]

    def exchange(x):
        return lax.all_to_all(x, GROUP_AXIS, 0, 0, tiled=True)

    def device_step(features, labels, train_mask, send_idx, src_idx, dst_idx, inv_deg,
                    w_self_1, w_neigh_1, bias_1, w_self_2, w_neigh_2, bias_2,
                    w_self_3, w_neigh_3, bias_3):
        n = features.shape[0]
        slots = send_idx.shape[1]
        halo = peers * slots
        edges = src_idx.shape[0]
        hidden = w_self_1.shape[1]
        classes = w_self_3.shape[1]
        send_flat = send_idx.T.reshape(-1)
        tile = next(t for t in (4096, 1024) if n % t == 0)
        half_tile = tile // 2
        slot_bits = bits_for(halo)
        dst_bits = bits_for(n)
        table = n + halo

        blocks = edges // BLOCK
        halo_blocks = halo // BLOCK
        zero = jnp.int32(0)
        win_e, win_h, win_r = 192, 208, 272
        owned = jnp.sum((src_idx < n).astype(jnp.int32))
        block_shift = BLOCK.bit_length() - 1
        near_end = (owned + BLOCK - 1) >> block_shift
        far_start = owned >> block_shift

        src_bits = bits_for(table)
        far_bit = dst_bits + src_bits
        by_dst = lax.sort(((src_idx >= n).astype(jnp.int32) << far_bit) | (dst_idx << src_bits) | src_idx, is_stable=False)
        src_f = by_dst & ((1 << src_bits) - 1)
        dst_f = (by_dst >> src_bits) & ((1 << dst_bits) - 1)
        is_far = src_f >= n
        src_near = jnp.minimum(src_f, n - 1)
        src_far = jnp.maximum(src_f - n, 0)
        seg_near = jnp.where(is_far, -1, dst_f).reshape(blocks, 1, BLOCK)
        seg_far = jnp.where(is_far, dst_f, -1).reshape(blocks, 1, BLOCK)
        first, last = dst_f[::BLOCK], dst_f[BLOCK - 1::BLOCK]
        meta_near = edge_meta(first, jnp.where(is_far[BLOCK - 1::BLOCK], n - 1, last), win_e, zero, near_end)
        meta_far = edge_meta(jnp.where(is_far[::BLOCK], first, 0), last, win_e, far_start, jnp.int32(blocks))

        inv = jnp.broadcast_to(inv_deg[:, None], (n, LANES))
        b1 = bias_1.reshape(1, -1)
        b2 = bias_2.reshape(1, -1)
        lane = jnp.arange(LANES, dtype=jnp.int32)
        used = lane < 3 * SPREAD
        folder = jnp.tile(((lane[:, None] % SPREAD == lane[None, :] % SPREAD) & used[:, None] & used[None, :]).astype(BF16),
                          (3, 1))
        b3 = jnp.where(lane < 3 * SPREAD, spread3(bias_3.reshape(1, -1)), -1e30)
        if classes < SPREAD:
            b3 = jnp.where(lane % SPREAD < classes, b3, -1e30)
        target = jnp.where(lane[None, :] < 3 * SPREAD,
                           train_mask[:, None] * (1.0 + (labels[:, None] == lane[None, :] % SPREAD)), 0.0).astype(BF16)
        ws3, wn3 = spread3(w_self_3), spread3(w_neigh_3)
        ws3_t, wn3_t = lanes_pad(w_self_3).T, lanes_pad(w_neigh_3).T

        def rows_of(nc):
            def build(copies, stages, tab, fx):
                unpack(copies[0], stages[0], tab, 0, nc)
            return build

        def near_sums(name, nc, idx, rows, also):
            return edge_call(name, (meta_near, idx, seg_near), nc, n, n, win_e, [rows.shape], rows_of(nc),
                             [rows] + also, [], [], [((n, nc * LANES), F32, False)], n, tile, None, 20)[0]

        out_1 = pick_rows('send_1', features, send_flat, peers, slots, train_mask.reshape(-1, LANES))
        got_1 = exchange(out_1)
        near_1 = near_sums('near_1', 1, src_near, features, [inv])
        counts = got_1[:, slots, :2].astype(F32)
        total = jnp.sum(counts[:, 0]) * LANES + jnp.sum(counts[:, 1])

        def build_1(copies, stages, tab, fx):
            per = peers // len(copies[0])
            some = math.gcd(per, 8)
            for p in range(len(copies[0])):
                copies[0][p].wait()

                def body(k, carry):
                    q = p * per + k * some
                    rows = stages[0][pl.ds(q, some), :slots, :].reshape(some * slots, LANES)
                    put_rows(tab, q * slots, rows.astype(F32), 1)
                    return carry
                lax.fori_loop(0, per // some, body, 0)

        def epi_1(a, bl, fx, out, put):
            mean = (a * bl[1][...]).astype(BF16)
            z = mm(bl[0][...], fx[0][...]) + mm(mean, fx[1][...]) + fx[2][...]
            out[0][...] = mean
            out[1][...] = jnp.maximum(z, 0.0).astype(BF16)
            put(mean.astype(F32))

        mean_1, hidden_1, out_2 = edge_call(
            'layer_1', (meta_far, src_far, seg_far), 1, halo, n, win_e, [(peers, slots + TAIL, LANES)], build_1,
            [got_1, near_1], [features, inv], [w_self_1, w_neigh_1, b1],
            [((n, LANES), BF16, False), ((n, hidden), BF16, False)], n, tile, epi_1, 25, init=1, late=True,
            keep=1, pick=(send_flat, peers, slots))

        place = jnp.arange(halo, dtype=jnp.int32)
        keys = jnp.concatenate([(src_idx << dst_bits) | dst_idx,
                                (1 << 30) | (send_flat << slot_bits) | (place % peers * slots + place // peers)])
        keys = lax.optimization_barrier((keys, mean_1))[0]
        ordered = lax.sort(keys, is_stable=False)
        by_src, by_row = ordered[:edges], ordered[edges:] & ((1 << 30) - 1)
        src_s = by_src >> dst_bits
        dst_s = by_src & ((1 << dst_bits) - 1)
        row_s = by_row >> slot_bits
        slot_s = by_row & ((1 << slot_bits) - 1)
        first, last = src_s[::BLOCK], src_s[BLOCK - 1::BLOCK]
        meta_own = edge_meta(jnp.minimum(first, n - 1), jnp.minimum(last, n - 1), win_e, zero, near_end)
        meta_halo = edge_meta(jnp.maximum(first - n, 0), jnp.maximum(last - n, 0), win_h, far_start, jnp.int32(blocks))
        meta_owner = edge_meta(row_s[::BLOCK], row_s[BLOCK - 1::BLOCK], win_r, zero, jnp.int32(halo_blocks))
        seg_o = src_s.reshape(blocks, 1, BLOCK)
        seg_h = seg_o - n
        seg_r = row_s.reshape(halo_blocks, 1, BLOCK)
        dst_wide = tile_linear(dst_s)

        got_2 = exchange(out_2)
        near_2 = near_sums('near_2', 2, tile_linear(src_near), hidden_1, [])

        def build_2(copies, stages, tab, fx):
            per = peers // len(copies[0])
            some = math.gcd(per, 8)
            for p in range(len(copies[0])):
                copies[0][p].wait()
                copies[1][p].wait()

                def body(k, carry):
                    q = p * per + k * some
                    f = stages[0][pl.ds(q, some), :slots, :].reshape(some * slots, LANES)
                    m = stages[1][pl.ds(q, some)].reshape(some * slots, LANES)
                    z = mm(f, fx[3][...]) + mm(m, fx[4][...]) + fx[5][...]
                    put_rows(tab, q * slots, jnp.maximum(z, 0.0).astype(BF16).astype(F32), 2)
                    return carry
                lax.fori_loop(0, per // some, body, 0)

        def epi_2(a, bl, fx, out, put):
            scale = bl[1][...]
            mean = (a * jnp.concatenate([scale, scale], axis=1)).astype(BF16)
            z = mm(bl[0][...], fx[0][...]) + mm(mean, fx[1][...]) + fx[2][...]
            h = jnp.maximum(z, 0.0).astype(BF16)
            out[0][...] = mean
            out[1][...] = h
            both = mm(h, fx[6][...])
            pieces = split3(both[:, :LANES])
            out[2][...] = pieces
            out[3][...] = both[:, LANES:]
            put(pieces.astype(F32))

        mean_2, hidden_2, proj, logits_self, out_3 = edge_call(
            'layer_2', (meta_far, tile_linear(src_far), seg_far), 2, halo, n, win_e,
            [(peers, slots + TAIL, LANES), (peers, slots, LANES)], build_2, [got_1, got_2, near_2],
            [hidden_1, inv], [w_self_2, w_neigh_2, b2, w_self_1, w_neigh_1, b1, jnp.concatenate([wn3, ws3], axis=1)],
            [((n, hidden), BF16, False), ((n, hidden), BF16, False), ((n, LANES), BF16, False),
             ((n, LANES), F32, False)], n, tile, epi_2, 40, init=2, keep=1, pick=(send_flat, peers, slots))

        got_3 = exchange(out_3).reshape(halo, LANES)
        near_3 = near_sums('near_3', 1, src_near, proj, [target])
        inv_total = (1.0 / total).reshape(1, 1)

        def epi_3(a, bl, fx, out, put):
            scale = bl[1][...]
            z = bl[0][...] + fold3(a * scale, fx[2][...]) + fx[0][...]
            top = jnp.max(z, axis=1, keepdims=True)
            e = jnp.exp(z - top)
            each = jnp.sum(e, axis=1, keepdims=True) * (1.0 / 3.0)
            lse = top + jnp.log(each)
            t = bl[2][...].astype(F32)
            inside = jnp.minimum(t, 1.0)
            hit = t - inside
            d = (e * (1.0 / each) * inside - hit) * fx[1][...]
            db = d.astype(BF16)
            out[0][...] = db
            pieces = split3(db.astype(F32) * scale)
            out[1][...] = pieces
            put(pieces.astype(F32))
            add_rows(out[2], d)
            add_rows(out[3], hit * (lse - z))

        def finish_3(a, fx):
            return split3(fold3(a, fx[2][...]))

        d_bf_3, scaled_3, g_b3, loss_parts, back_3 = edge_call(
            'layer_3', (meta_far, src_far, seg_far), 1, halo, n, win_e, [(halo, LANES)], rows_of(1), [got_3, near_3],
            [logits_self, inv, target], [b3, jnp.broadcast_to(inv_total, (1, LANES)), folder],
            [((n, LANES), BF16, False), ((n, LANES), BF16, False), ((8, LANES), F32, True), ((8, LANES), F32, True)],
            n, tile, epi_3, 30, init=1, late=True, keep=1,
            then=((meta_halo, dst_s, seg_h), 1, halo, win_h, finish_3))

        ret_3 = exchange(back_3.reshape(peers, slots, LANES)).reshape(halo, LANES)
        own_3 = edge_call('back_3_own', (meta_own, dst_s, seg_o), 1, n, n, win_e, [(n, LANES)], rows_of(1),
                          [scaled_3], [], [], [((n, LANES), F32, False)], n, tile, None, 20)[0]

        def epi_o3(a, bl, fx, out, put):
            tb = fold3(a, fx[2][...]).astype(BF16)
            d_h = mm(jnp.concatenate([bl[0][...], tb], axis=1), fx[0][...])
            d_pre = jnp.where(bl[1][...].astype(F32) > 0, d_h, 0.0)
            db = d_pre.astype(BF16)
            scale = bl[2][...]
            out[0][...] = tb
            out[1][...] = db
            scaled = (mm(db, fx[1][...]) * jnp.concatenate([scale, scale], axis=1)).astype(BF16)
            out[2][...] = scaled
            put(scaled.astype(F32))
            add_rows(out[3], d_pre)

        def finish_2(a, fx):
            return a.astype(BF16)

        tb_3, d_bf_2, scaled_2, g_b2, back_2 = edge_call(
            'owner_3', (meta_owner, slot_s, seg_r), 1, halo, n, win_r, [(halo, LANES)], rows_of(1), [ret_3, own_3],
            [d_bf_3, hidden_2, inv], [jnp.concatenate([ws3_t, wn3_t], axis=0), w_neigh_2.T, folder],
            [((n, LANES), BF16, False), ((n, hidden), BF16, False), ((n, hidden), BF16, False), ((8, hidden), F32, True)],
            n, half_tile, epi_o3, 30, init=1, late=True, keep=2,
            then=((meta_halo, dst_wide, seg_h), 2, halo, win_h, finish_2))

        def epi_b2o(a, bl, fx, out, put):
            out[0][...] = a + mm(bl[0][...], fx[0][...])

        ret_2 = exchange(back_2.reshape(peers, slots, hidden)).reshape(halo, hidden)
        own_2 = edge_call('back_2_own', (meta_own, dst_wide, seg_o), 2, n, n, win_e, [(n, hidden)], rows_of(2),
                          [scaled_2], [d_bf_2], [w_self_2.T], [((n, hidden), F32, False)], n, tile, epi_b2o, 30)[0]

        def epi_o2(a, bl, fx, out, put):
            d_pre = jnp.where(bl[0][...].astype(F32) > 0, a, 0.0)
            inputs = jnp.concatenate([bl[1][...], bl[2][...]], axis=1)
            out[0][...] += lax.dot_general(inputs, d_pre.astype(BF16), (((0,), (0,)), ((), ())),
                                           preferred_element_type=F32)
            add_rows(out[1], d_pre)

        g_1, g_b1 = edge_call(
            'owner_2', (meta_owner, tile_linear(slot_s), seg_r), 2, halo, n, win_r, [(halo, hidden)], rows_of(2),
            [ret_2, own_2], [hidden_1, features, mean_1], [],
            [((2 * LANES, hidden), F32, True), ((8, hidden), F32, True)], n, half_tile, epi_o2, 25, init=1, late=True)

        def contract(a, b):
            return jnp.einsum('nd,ne->de', a, b, preferred_element_type=F32)

        at = jnp.arange(LANES, dtype=jnp.int32)[None, :]
        g_3 = jnp.where(at < SPREAD, contract(hidden_2, d_bf_3), contract(hidden_2, tb_3))
        g1s, g1n, g2s, g2n, g3s, g3n, s1, s2, s3, loss = sum_over_devices(
            [g_1, contract(hidden_1, d_bf_2), contract(mean_2, d_bf_2), g_3],
            [g_b1, g_b2, g_b3, loss_parts], total.reshape(1, 1), classes, peers)
        return (loss.reshape(()), g1s, g1n, s1.reshape(-1), g2s, g2n, s2.reshape(-1), g3s.T, g3n.T, s3.reshape(-1))

    sharded = P(GROUP_AXIS)
    whole = P()
    return jax.shard_map(device_step, mesh=mesh,
                         in_specs=(sharded,) * 7 + (whole,) * 9,
                         out_specs=(whole,) * 10, check_vma=False)
```

```python
import math

import jax
import jax.numpy as jnp
from jax import lax
from jax.experimental import pallas as pl
from jax.experimental.pallas import tpu as pltpu
from jax.sharding import PartitionSpec as P

GROUP_AXIS = 'gp'
LANES = 128
SPREAD = 40
BLOCK = 128
GROUP = 8
TAIL = 8
F32 = jnp.float32
BF16 = jnp.bfloat16
VMEM_LIMIT = 63 * 2 ** 20

SMEM_SPEC = pl.BlockSpec(memory_space=pltpu.SMEM)
HBM_SPEC = pl.BlockSpec(memory_space=pltpu.HBM)


def whole_spec(shape):
    return pl.BlockSpec(shape, lambda i: (0,) * len(shape))


def row_spec(rows, width):
    return pl.BlockSpec((rows, width), lambda i: (i, 0))


def params():
    return pltpu.CompilerParams(vmem_limit_bytes=VMEM_LIMIT, dimension_semantics=('arbitrary',))


def cost(micros):
    return pl.CostEstimate(flops=int(micros * 4e6), bytes_accessed=int(micros * 1e6), transcendentals=0)


def mm(a, b):
    return jnp.dot(a, b, preferred_element_type=F32)


def tile_linear(row):
    return ((row >> 3) << 4) | (row & 7)


def put_rows(tab, row0, x, nc):
    rows = x.shape[0]
    if nc == 1:
        tab[pl.ds(pl.multiple_of(row0, 8), rows), :] = x
    else:
        for g in range(rows // 8):
            for c in range(nc):
                at = pl.multiple_of((row0 + g * 8) * nc + c * 8, 8)
                tab[pl.ds(at, 8), :] = x[g * 8:g * 8 + 8, c * LANES:(c + 1) * LANES]


def fetch(src, stage, sem, parts):
    rows = src.shape[0] // parts
    copies = [pltpu.make_async_copy(src.at[pl.ds(k * rows, rows)], stage.at[pl.ds(k * rows, rows)], sem.at[k])
              for k in range(parts)]
    for c in copies:
        c.start()
    return copies


def unpack(copies, stage, tab, row0, nc):
    rows = stage.shape[0] // len(copies)
    step = next(d for d in (128, 96, 64, 32, 16) if rows % d == 0)
    for p, c in enumerate(copies):
        c.wait()

        def body(k, carry):
            at = pl.multiple_of(p * rows + k * step, step)
            put_rows(tab, row0 + at, stage[pl.ds(at, step), :].astype(F32), nc)
            return carry
        lax.fori_loop(0, rows // step, body, 0)


def group_of(blocks):
    return next(u for u in (GROUP, 4, 2) if blocks % u == 0)


def zero_rows(acc):
    rows = acc.shape[0]
    step = next(s for s in (256, 128, 64, 32, 16, 8) if rows % s == 0)

    def body(k, carry):
        acc[pl.ds(pl.multiple_of(k * step, step), step), :] = jnp.zeros((step, acc.shape[1]), F32)
        return carry
    lax.fori_loop(0, rows // step, body, 0)


def gather_16(idx, base, first, reach, tab, nc, stride=1):
    sub = lax.broadcasted_iota(jnp.int32, (8, LANES), 0)
    room = idx.shape[0] - (reach - 1) * stride
    halves = [[None, None] for _ in range(nc)]
    for h in range(2):
        for k in range(8):
            at = idx.at[pl.ds((first + h * 8 + k) * stride, room)][base]
            for c in range(nc):
                row = jnp.broadcast_to(tab[pl.ds(at + 8 * c, 1), :], (8, LANES))
                halves[c][h] = row if k == 0 else jnp.where(sub == k, row, halves[c][h])
    return [jnp.concatenate(halves[c], axis=0).astype(BF16) for c in range(nc)]


def segment_sums(meta, idx, seg, tab, acc, bufs, nc, window, blocks):
    unroll = group_of(blocks)
    base, counts = meta[:2]
    first_trip, end_trip, most = [m[0] for m in meta[2:]]

    def fill(start, first, reach, buf):
        for g in range(BLOCK // 16):
            parts = gather_16(idx, start, first + g * 16, reach, tab, nc)
            for c in range(nc):
                buf[g * 16:g * 16 + 16, c * LANES:(c + 1) * LANES] = parts[c]

    def sums(b, at, buf):
        rows = lax.broadcasted_iota(jnp.int32, (window, BLOCK), 0) + at
        return mm(jnp.where(rows == seg[b], 1.0, 0.0).astype(BF16), buf[...])

    def add(at, x):
        acc[pl.ds(pl.multiple_of(at, 8), window), :] += x

    span = unroll * BLOCK
    last_trip = blocks // unroll - 1
    fill(jnp.minimum(first_trip, last_trip) * span, 0, span, bufs[0])

    def body(t, carry):
        before = None
        for u in range(unroll):
            b = t * unroll + u
            now = (base[b], sums(b, base[b], bufs[u % 2]))
            if u + 1 < unroll:
                fill(t * span, (u + 1) * BLOCK, span, bufs[(u + 1) % 2])
            else:
                fill(jnp.minimum(t + 1, last_trip) * span, 0, span, bufs[0])
            if before is not None:
                add(*before)
            before = now
        add(*before)
        return carry
    lax.fori_loop(first_trip, end_trip, body, 0)

    @pl.when(most > 1)
    def _():
        def again(b, carry):
            count = counts[b]

            @pl.when(count > 1)
            def _():
                fill(b * BLOCK, 0, BLOCK, bufs[0])

                def more(w, c):
                    at = base[b] + w * window
                    add(at, sums(b, at, bufs[0]))
                    return c
                lax.fori_loop(1, count, more, 0)
            return carry
        lax.fori_loop(first_trip * unroll, end_trip * unroll, again, 0)


def spread_lanes():
    return lax.broadcasted_iota(jnp.int32, (1, LANES), 1)


def split3(x):
    hi = x.astype(BF16).astype(F32)
    rest = x - hi
    mid = rest.astype(BF16).astype(F32)
    low = rest - mid
    lane = spread_lanes()
    out = jnp.where(lane < SPREAD, hi, jnp.where(lane < 2 * SPREAD, mid, low))
    return jnp.where(lane < 3 * SPREAD, out, 0.0).astype(BF16)


def pieces3(a):
    hi = a.astype(BF16)
    rest = a - hi.astype(F32)
    mid = rest.astype(BF16)
    low = (rest - mid.astype(F32)).astype(BF16)
    return jnp.concatenate([hi, mid, low], axis=1)


def fold3(a, folder):
    return mm(pieces3(a), folder)


def add_rows(ref, x):
    ref[...] += jnp.sum(x.reshape(x.shape[0] // 8, 8, x.shape[1]), axis=0)


PIECES = 4


def send_part(stage, out, sem, k):
    size = stage.shape[0] // PIECES
    at = pl.multiple_of(k * size, size)
    return pltpu.make_async_copy(stage.at[pl.ds(at, size)], out.at[pl.ds(at, size)], sem.at[k])


def send_out(src, out, sem):
    done = pltpu.make_async_copy(src, out, sem)
    done.start()
    done.wait()


def pick_pieces(idx, tab, stage, out, sem, peers, slots):
    size = peers // PIECES

    def piece(k, c):
        def body(p, carry):
            for g in range(slots // 16):
                stage[k * size + p, g * 16:g * 16 + 16, :] = gather_16(idx, k * size + p, g * 16, slots, tab, 1, peers)[0]
            return carry
        lax.fori_loop(0, size, body, 0)
        send_part(stage, out, sem, k).start()
        return c
    lax.fori_loop(0, PIECES, piece, 0)
    for k in range(PIECES):
        send_part(stage, out, sem, k).wait()


def pick_rows(name, src, idx, peers, slots, mask):
    n = src.shape[0]
    parts = math.gcd(n // 128, 4)

    def kern(idx_ref, src_ref, mask_ref, out, tab, stage, sem, rows, out_sem):
        copies = fetch(src_ref, stage, sem, parts)
        total = jnp.sum(mask_ref[...], axis=(0, 1), keepdims=True)
        high = jnp.floor(total * (1.0 / LANES))
        first = lax.broadcasted_iota(jnp.int32, (TAIL, LANES), 0) == 0
        lane = lax.broadcasted_iota(jnp.int32, (TAIL, LANES), 1)
        digits = jnp.where(lane == 0, high, jnp.where(lane == 1, total - high * LANES, 0.0))
        tail = jnp.where(first, digits, 0.0).astype(BF16)

        def put_tail(p, c):
            rows[p, slots:slots + TAIL, :] = tail
            return c
        lax.fori_loop(0, peers, put_tail, 0)
        unpack(copies, stage, tab, 0, 1)
        pick_pieces(idx_ref, tab, rows, out, out_sem, peers, slots)

    return pl.pallas_call(
        kern, name=name, out_shape=jax.ShapeDtypeStruct((peers, slots + TAIL, LANES), BF16),
        in_specs=[SMEM_SPEC, HBM_SPEC, pl.BlockSpec(memory_space=pltpu.VMEM)], out_specs=HBM_SPEC,
        scratch_shapes=[pltpu.VMEM((n, LANES), F32), pltpu.VMEM((n, LANES), BF16), pltpu.SemaphoreType.DMA((parts,)),
                        pltpu.VMEM((peers, slots + TAIL, LANES), BF16), pltpu.SemaphoreType.DMA((PIECES,))],
        compiler_params=pltpu.CompilerParams(vmem_limit_bytes=VMEM_LIMIT), cost_estimate=cost(10))(idx, src, mask)


def edge_call(name, edges, nc, table_rows, acc_rows, window, sources, build, hbm_in, blocked, fixed, outs, rows_out,
              tile, epilogue, micros, init=None, late=False, sub=2048, keep=0, pick=None, then=None,
              ahead=0):
    meta, idx, seg = edges
    blocks = seg.shape[0]
    width = nc * LANES
    nh, nb, nf, no, ns = len(hbm_in), len(blocked), len(fixed), len(outs), len(sources)
    acc_total = -(-(acc_rows + window) // 256) * 256
    parts = 4
    steps = 1 if epilogue is None else rows_out // tile
    sub = math.gcd(sub, tile)
    more_in, more_specs, more_out, more_scratch = [], [], [], []
    late_scratch = [pltpu.VMEM((acc_rows, width), F32)] if late else []
    if ahead:
        late_scratch += [pltpu.VMEM(x.shape, x.dtype) for x in blocked[:ahead]] + [pltpu.SemaphoreType.DMA((ahead,))]
    if keep:
        more_scratch.append(pltpu.VMEM((rows_out * keep, LANES), F32))
    if pick:
        p_idx, peers, slots = pick
        more_in.append(p_idx)
        more_specs.append(SMEM_SPEC)
        more_out.append(jax.ShapeDtypeStruct((peers, slots, LANES), BF16))
        more_scratch += [pltpu.VMEM((peers, slots, LANES), BF16), pltpu.SemaphoreType.DMA((PIECES,))]
    if then:
        (t_meta, t_idx, t_seg), t_nc, t_rows, t_window, finish = then
        t_width = t_nc * LANES
        t_total = -(-(t_rows + t_window) // 256) * 256
        more_in += [*t_meta, t_idx, t_seg]
        more_specs += [SMEM_SPEC] * 6 + [whole_spec(t_seg.shape)]
        more_out.append(jax.ShapeDtypeStruct((t_rows, t_width), BF16))
        more_scratch += [pltpu.VMEM((t_total, t_width), F32), pltpu.VMEM((BLOCK, t_width), BF16),
                         pltpu.VMEM((BLOCK, t_width), BF16), pltpu.VMEM((t_rows, t_width), BF16),
                         pltpu.SemaphoreType.DMA((PIECES,))]
    nm = len(more_in)

    def kern(*refs):
        meta_refs, (idx_ref, seg_ref), refs = refs[:5], refs[5:7], refs[7:]
        hb, refs = refs[:nh], refs[nh:]
        bl, refs = refs[:nb], refs[nb:]
        fx, refs = refs[:nf], refs[nf:]
        extra, refs = refs[:nm], refs[nm:]
        out, refs = refs[:no], refs[no:]
        last_out, refs = refs[:len(more_out)], refs[len(more_out):]
        tab, acc, buf_0, buf_1, isem = refs[:5]
        stages, sems, scratch = refs[5:5 + ns], refs[5 + ns:5 + 2 * ns], refs[5 + 2 * ns:]
        if late:
            begin, scratch = scratch[0], scratch[1:]
        if ahead:
            whole, whole_sem, scratch = scratch[:ahead], scratch[ahead], scratch[ahead + 1:]
        i = pl.program_id(0)

        @pl.when(i == 0)
        def _():
            copies = [fetch(h, st, sm, parts) for h, st, sm in zip(hb, stages, sems)]
            if init is not None:
                start = pltpu.make_async_copy(hb[init], begin if late else acc.at[pl.ds(0, acc_rows), :], isem)
                if not late:
                    start.start()
            if init is None or late:
                zero_rows(acc)
            for o, (_, _, sums) in zip(out, outs):
                if sums:
                    o[...] = jnp.zeros_like(o)
            if then:
                zero_rows(scratch[1])
            build(copies, stages, tab, fx)
            if late:
                start.start()
            wholes = [pltpu.make_async_copy(bl[k], whole[k], whole_sem.at[k]) for k in range(ahead)]
            for c in wholes:
                c.start()
            if init is not None and not late:
                start.wait()
            segment_sums(meta_refs, idx_ref, seg_ref, tab, acc, (buf_0, buf_1), nc, window, blocks)
            if late:
                start.wait()
            for c in wholes:
                c.wait()
            if epilogue is None:
                send_out(acc.at[pl.ds(0, acc_rows), :], out[0], isem)
        if epilogue is not None:
            def part(j, carry):
                at = pl.multiple_of(j * sub, sub)
                row0 = pl.multiple_of(i * tile + at, sub)

                def put(x):
                    put_rows(scratch[0], row0, x, keep)
                a = acc[pl.ds(row0, sub), :]
                if late:
                    a = a + begin[pl.ds(row0, sub), :]
                epilogue(a, [whole[k].at[pl.ds(row0, sub), :] for k in range(ahead)]
                         + [r.at[pl.ds(at, sub), :] for r in bl[ahead:]], fx,
                         [o if sums else o.at[pl.ds(at, sub), :] for o, (_, _, sums) in zip(out, outs)], put)
                return carry
            lax.fori_loop(0, tile // sub, part, 0)

        if pick:
            @pl.when(i == steps - 1)
            def _():
                kept, stage, out_sem = scratch
                pick_pieces(extra[0], kept, stage, last_out[0], out_sem, peers, slots)
        if then:
            @pl.when(i == steps - 1)
            def _():
                kept, acc_2, buf_2, buf_3, stage, out_sem = scratch
                segment_sums(extra[:5], extra[5], extra[6], kept, acc_2, (buf_2, buf_3), t_nc, t_window,
                             t_seg.shape[0])
                size = t_rows // PIECES
                step = math.gcd(1024, size)

                def piece(k, c):
                    def part(j, carry):
                        at = pl.multiple_of(k * size + j * step, step)
                        stage[pl.ds(at, step), :] = finish(acc_2[pl.ds(at, step), :], fx)
                        return carry
                    lax.fori_loop(0, size // step, part, 0)
                    send_part(stage, last_out[0], out_sem, k).start()
                    return c
                lax.fori_loop(0, PIECES, piece, 0)
                for k in range(PIECES):
                    send_part(stage, last_out[0], out_sem, k).wait()

    out_shape, out_specs = [], []
    for shape, dtype, sums in outs:
        out_shape.append(jax.ShapeDtypeStruct(shape, dtype))
        out_specs.append(HBM_SPEC if epilogue is None else whole_spec(shape) if sums else row_spec(tile, shape[1]))
    return pl.pallas_call(
        kern, name=name, grid=(steps,), out_shape=out_shape + more_out,
        in_specs=([SMEM_SPEC] * 6 + [whole_spec(seg.shape)] + [HBM_SPEC] * nh
                  + [HBM_SPEC] * ahead + [row_spec(tile, x.shape[1]) for x in blocked[ahead:]]
                  + [whole_spec(x.shape) for x in fixed] + more_specs),
        out_specs=out_specs + [HBM_SPEC] * len(more_out),
        scratch_shapes=([pltpu.VMEM((table_rows * nc, LANES), F32), pltpu.VMEM((acc_total, width), F32),
                         pltpu.VMEM((BLOCK, width), BF16), pltpu.VMEM((BLOCK, width), BF16),
                         pltpu.SemaphoreType.DMA(())]
                        + [pltpu.VMEM(shape, BF16) for shape in sources]
                        + [pltpu.SemaphoreType.DMA((parts,)) for _ in sources] + late_scratch + more_scratch),
        compiler_params=params(), cost_estimate=cost(micros))(*meta, idx, seg, *hbm_in, *blocked, *fixed, *more_in)


SHARE = 16


def grad_places(shapes):
    places, at = [], 0
    for rows, width in shapes:
        columns = []
        for _ in range(width // LANES):
            columns.append(at)
            at += -(-rows // SHARE)
        places.append(columns)
    return places, at


def sum_over_devices(grads, sums, total, classes, peers):
    chips = peers // 2
    places, used = grad_places([g.shape for g in grads] + [(SHARE, LANES)])
    rounds = -(-used // peers)
    rows = SHARE * rounds
    widths = [x.shape[1] for x in sums]

    def device(chip, core):
        return chip * 2 + core

    def kern(*refs):
        ng, ns = len(grads), len(sums)
        g_refs, s_refs, out_ref = refs[:ng], refs[ng:ng + ns], refs[ng + ns]
        x_ref, half, mine, got, pair_sem, send_sem, recv_sem, send_2, recv_2 = refs[ng + ns + 1:]
        me = lax.axis_index(GROUP_AXIS)
        chip, core = me // 2, me % 2
        mate = device(chip, 1 - core)
        barrier = pltpu.get_barrier_semaphore()

        def hello(to):
            pl.semaphore_signal(barrier, inc=1, device_id=(to,), device_id_type=pl.DeviceIdType.MESH)

        def greet(k, carry):
            hello(device((chip + k) % chips, core))
            return carry
        lax.fori_loop(1, chips, greet, 0)
        hello(mate)

        def at(q):
            unit = q // rounds
            return unit // chips, unit % chips, (q % rounds) * SHARE

        def put(q, value):
            h, c, r = at(q)
            x_ref[h, c, r:r + SHARE, :] = value
        for g, columns in zip(g_refs, places):
            for w, first in enumerate(columns):
                for k in range(g.shape[0] // SHARE):
                    put(first + k, g[k * SHARE:(k + 1) * SHARE, w * LANES:(w + 1) * LANES])
        row = lax.broadcasted_iota(jnp.int32, (SHARE, LANES), 0)
        small, line = jnp.zeros((SHARE, LANES), F32), 0
        for s_ref, width in zip(s_refs, widths):
            for w in range(width // LANES):
                total = jnp.sum(s_ref[:, w * LANES:(w + 1) * LANES], axis=0, keepdims=True)
                small = jnp.where(row == line, total, small)
                line += 1
        put(places[-1][0], small)
        for q in range(used, peers * rounds):
            put(q, jnp.zeros((SHARE, LANES), F32))

        def pair(src, dst, k):
            return pltpu.make_async_remote_copy(src_ref=src, dst_ref=dst, send_sem=pair_sem.at[2 * k],
                                                recv_sem=pair_sem.at[2 * k + 1], device_id=(mate,),
                                                device_id_type=pl.DeviceIdType.MESH)
        pl.semaphore_wait(barrier, chips)
        first = pair(x_ref.at[1 - core], half, 0)
        first.start()
        first.wait()

        def add(c, carry):
            mine[c] = x_ref[core, c] + half[c]
            return carry
        lax.fori_loop(0, chips, add, 0)

        def share(k):
            to = (chip + k) % chips
            return pltpu.make_async_remote_copy(src_ref=mine.at[to], dst_ref=got.at[chip], send_sem=send_sem.at[k],
                                                recv_sem=recv_sem.at[chip], device_id=(device(to, core),),
                                                device_id_type=pl.DeviceIdType.MESH)

        def landed(k):
            frm = (chip + k) % chips
            return pltpu.make_async_remote_copy(src_ref=mine.at[frm], dst_ref=got.at[frm], send_sem=send_sem.at[k],
                                                recv_sem=recv_sem.at[frm], device_id=(me,),
                                                device_id_type=pl.DeviceIdType.MESH)

        def start(k, carry):
            share(k).start()
            return carry
        lax.fori_loop(1, chips, start, 0)
        got[chip] = mine[chip]

        def settle(k, carry):
            landed(k).wait_recv()
            return carry
        lax.fori_loop(1, chips, settle, 0)

        def more(c, total):
            return total + got[c]
        out_ref[core, chip] = lax.fori_loop(0, chips, more, jnp.zeros((rows, LANES), F32))

        def drain(k, carry):
            share(k).wait_send()
            return carry
        lax.fori_loop(1, chips, drain, 0)

        def give(k):
            return pltpu.make_async_remote_copy(src_ref=out_ref.at[core, chip], dst_ref=out_ref.at[core, chip],
                                                send_sem=send_2.at[k], recv_sem=recv_2.at[chip],
                                                device_id=(device((chip + k) % chips, core),),
                                                device_id_type=pl.DeviceIdType.MESH)

        def given(k):
            frm = (chip + k) % chips
            return pltpu.make_async_remote_copy(src_ref=out_ref.at[core, frm], dst_ref=out_ref.at[core, frm],
                                                send_sem=send_2.at[k], recv_sem=recv_2.at[frm], device_id=(me,),
                                                device_id_type=pl.DeviceIdType.MESH)

        def start_2(k, carry):
            give(k).start()
            return carry
        lax.fori_loop(1, chips, start_2, 0)

        def settle_2(k, carry):
            given(k).wait_recv()
            return carry
        lax.fori_loop(1, chips, settle_2, 0)

        def drain_2(k, carry):
            give(k).wait_send()
            return carry
        lax.fori_loop(1, chips, drain_2, 0)
        last = pair(out_ref.at[core], out_ref.at[core], 1)
        last.start()
        last.wait()

    vmem = pl.BlockSpec(memory_space=pltpu.VMEM)
    shape = (2, chips, rows, LANES)
    full = pl.pallas_call(
        kern, name='sum_all', out_shape=jax.ShapeDtypeStruct(shape, F32),
        in_specs=[vmem] * (len(grads) + len(sums)), out_specs=vmem,
        scratch_shapes=[pltpu.VMEM(shape, F32), pltpu.VMEM(shape[1:], F32), pltpu.VMEM(shape[1:], F32),
                        pltpu.VMEM(shape[1:], F32), pltpu.SemaphoreType.DMA((4,)),
                        pltpu.SemaphoreType.DMA((chips,)), pltpu.SemaphoreType.DMA((chips,)),
                        pltpu.SemaphoreType.DMA((chips,)), pltpu.SemaphoreType.DMA((chips,))],
        compiler_params=pltpu.CompilerParams(collective_id=0, has_side_effects=True), cost_estimate=cost(25))(*grads, *sums)

    def unpack_kern(full_ref, total_ref, *outs):
        def part(q):
            unit = q // rounds
            r = (q % rounds) * SHARE
            return full_ref[unit // chips, unit % chips, r:r + SHARE, :]

        def move(o, columns, skip):
            for w, first in enumerate(columns):
                for k in range(o.shape[0] // SHARE):
                    o[k * SHARE:(k + 1) * SHARE, w * LANES:(w + 1) * LANES] = part(first + skip + k)
        move(outs[0], places[0], 0)
        move(outs[1], places[0], outs[0].shape[0] // SHARE)
        for o, columns in zip(outs[2:], places[1:-2]):
            move(o, columns, 0)
        both = jnp.concatenate([part(places[-2][0] + k) for k in range(rows_3 // SHARE)], axis=0).T
        outs[ng][...] = both[:classes, :]
        outs[ng + 1][...] = both[SPREAD:SPREAD + classes, :]
        small, line = part(places[-1][0]), 0
        for o, width in zip(outs[ng + 2:-1], widths):
            for w in range(width // LANES):
                wide = min(LANES, o.shape[1] - w * LANES)
                o[:, w * LANES:w * LANES + wide] = small[line:line + 1, :wide]
                line += 1
        outs[-1][...] = jnp.sum(small[line:line + 1, :SPREAD], axis=1, keepdims=True) / total_ref[...]
    ng = len(grads)
    rows_3 = grads[-1].shape[0]
    rows_1, width_1 = grads[0].shape
    outs = ([(rows_1 // 2, width_1)] * 2 + [g.shape for g in grads[1:-1]] + [(classes, rows_3)] * 2
            + [(1, w) for w in widths[:-2]] + [(1, classes), (1, 1)])
    return pl.pallas_call(unpack_kern, name='unpack_sums', out_shape=[jax.ShapeDtypeStruct(o, F32) for o in outs],
                          in_specs=[vmem, vmem], out_specs=[vmem] * len(outs), cost_estimate=cost(3))(full, total)


def edge_meta(seg_first, seg_last, window, first_block, end_block):
    blocks = seg_first.shape[0]
    shift = group_of(blocks).bit_length() - 1
    at = jnp.arange(blocks, dtype=jnp.int32)
    base = seg_first & ~7
    inside = (at >= first_block) & (at < end_block)
    count = jnp.where(inside, lax.div(jnp.maximum(seg_last - base, 0), jnp.int32(window)) + 1, 1)
    scalars = [first_block >> shift, (end_block + (1 << shift) - 1) >> shift, jnp.max(count)]
    return [base, count] + [x.reshape(1) for x in scalars]


def bits_for(n):
    return max(1, (n - 1).bit_length())


def spread3(w):
    w = jnp.pad(w, ((0, 0), (0, SPREAD - w.shape[1])))
    return jnp.pad(jnp.concatenate([w, w, w], axis=1), ((0, 0), (0, LANES - 3 * SPREAD)))


def lanes_pad(w):
    return jnp.pad(w, ((0, 0), (0, LANES - w.shape[1])))


def solution(mesh):
    peers = mesh.shape[GROUP_AXIS]

    def exchange(x):
        return lax.all_to_all(x, GROUP_AXIS, 0, 0, tiled=True)

    def device_step(features, labels, train_mask, send_idx, src_idx, dst_idx, inv_deg,
                    w_self_1, w_neigh_1, bias_1, w_self_2, w_neigh_2, bias_2,
                    w_self_3, w_neigh_3, bias_3):
        n = features.shape[0]
        slots = send_idx.shape[1]
        halo = peers * slots
        edges = src_idx.shape[0]
        hidden = w_self_1.shape[1]
        classes = w_self_3.shape[1]
        send_flat = send_idx.T.reshape(-1)
        tile = next(t for t in (4096, 1024) if n % t == 0)
        half_tile = tile // 2
        slot_bits = bits_for(halo)
        dst_bits = bits_for(n)
        table = n + halo

        blocks = edges // BLOCK
        halo_blocks = halo // BLOCK
        zero = jnp.int32(0)
        win_e, win_h, win_r = 192, 208, 272
        owned = jnp.sum((src_idx < n).astype(jnp.int32))
        block_shift = BLOCK.bit_length() - 1
        near_end = (owned + BLOCK - 1) >> block_shift
        far_start = owned >> block_shift

        src_bits = bits_for(table)
        far_bit = dst_bits + src_bits
        by_dst = lax.sort(((src_idx >= n).astype(jnp.int32) << far_bit) | (dst_idx << src_bits) | src_idx, is_stable=False)
        src_f = by_dst & ((1 << src_bits) - 1)
        dst_f = (by_dst >> src_bits) & ((1 << dst_bits) - 1)
        is_far = src_f >= n
        src_near = jnp.minimum(src_f, n - 1)
        src_far = jnp.maximum(src_f - n, 0)
        seg_near = jnp.where(is_far, -1, dst_f).reshape(blocks, 1, BLOCK)
        seg_far = jnp.where(is_far, dst_f, -1).reshape(blocks, 1, BLOCK)
        first, last = dst_f[::BLOCK], dst_f[BLOCK - 1::BLOCK]
        meta_near = edge_meta(first, jnp.where(is_far[BLOCK - 1::BLOCK], n - 1, last), win_e, zero, near_end)
        meta_far = edge_meta(jnp.where(is_far[::BLOCK], first, 0), last, win_e, far_start, jnp.int32(blocks))

        inv = jnp.broadcast_to(inv_deg[:, None], (n, LANES))
        b1 = bias_1.reshape(1, -1)
        b2 = bias_2.reshape(1, -1)
        lane = jnp.arange(LANES, dtype=jnp.int32)
        used = lane < 3 * SPREAD
        folder = jnp.tile(((lane[:, None] % SPREAD == lane[None, :] % SPREAD) & used[:, None] & used[None, :]).astype(BF16),
                          (3, 1))
        b3 = jnp.where(lane < 3 * SPREAD, spread3(bias_3.reshape(1, -1)), -1e30)
        if classes < SPREAD:
            b3 = jnp.where(lane % SPREAD < classes, b3, -1e30)
        target = jnp.where(lane[None, :] < 3 * SPREAD,
                           train_mask[:, None] * (1.0 + (labels[:, None] == lane[None, :] % SPREAD)), 0.0).astype(BF16)
        ws3, wn3 = spread3(w_self_3), spread3(w_neigh_3)
        ws3_t, wn3_t = lanes_pad(w_self_3).T, lanes_pad(w_neigh_3).T

        def rows_of(nc):
            def build(copies, stages, tab, fx):
                unpack(copies[0], stages[0], tab, 0, nc)
            return build

        def near_sums(name, nc, idx, rows, also):
            return edge_call(name, (meta_near, idx, seg_near), nc, n, n, win_e, [rows.shape], rows_of(nc),
                             [rows] + also, [], [], [((n, nc * LANES), F32, False)], n, tile, None, 20)[0]

        out_1 = pick_rows('send_1', features, send_flat, peers, slots, train_mask.reshape(-1, LANES))
        got_1 = exchange(out_1)
        near_1 = near_sums('near_1', 1, src_near, features, [inv])
        counts = got_1[:, slots, :2].astype(F32)
        total = jnp.sum(counts[:, 0]) * LANES + jnp.sum(counts[:, 1])

        def build_1(copies, stages, tab, fx):
            per = peers // len(copies[0])
            some = math.gcd(per, 8)
            for p in range(len(copies[0])):
                copies[0][p].wait()

                def body(k, carry):
                    q = p * per + k * some
                    rows = stages[0][pl.ds(q, some), :slots, :].reshape(some * slots, LANES)
                    put_rows(tab, q * slots, rows.astype(F32), 1)
                    return carry
                lax.fori_loop(0, per // some, body, 0)

        def epi_1(a, bl, fx, out, put):
            mean = (a * bl[1][...]).astype(BF16)
            z = mm(bl[0][...], fx[0][...]) + mm(mean, fx[1][...]) + fx[2][...]
            out[0][...] = mean
            out[1][...] = jnp.maximum(z, 0.0).astype(BF16)
            put(mean.astype(F32))

        mean_1, hidden_1, out_2 = edge_call(
            'layer_1', (meta_far, src_far, seg_far), 1, halo, n, win_e, [(peers, slots + TAIL, LANES)], build_1,
            [got_1, near_1], [features, inv], [w_self_1, w_neigh_1, b1],
            [((n, LANES), BF16, False), ((n, hidden), BF16, False)], n, tile, epi_1, 25, init=1, late=True, ahead=2,
            keep=1, pick=(send_flat, peers, slots))

        place = jnp.arange(halo, dtype=jnp.int32)
        keys = jnp.concatenate([(src_idx << dst_bits) | dst_idx,
                                (1 << 30) | (send_flat << slot_bits) | (place % peers * slots + place // peers)])
        keys = lax.optimization_barrier((keys, mean_1))[0]
        ordered = lax.sort(keys, is_stable=False)
        by_src, by_row = ordered[:edges], ordered[edges:] & ((1 << 30) - 1)
        src_s = by_src >> dst_bits
        dst_s = by_src & ((1 << dst_bits) - 1)
        row_s = by_row >> slot_bits
        slot_s = by_row & ((1 << slot_bits) - 1)
        first, last = src_s[::BLOCK], src_s[BLOCK - 1::BLOCK]
        meta_own = edge_meta(jnp.minimum(first, n - 1), jnp.minimum(last, n - 1), win_e, zero, near_end)
        meta_halo = edge_meta(jnp.maximum(first - n, 0), jnp.maximum(last - n, 0), win_h, far_start, jnp.int32(blocks))
        meta_owner = edge_meta(row_s[::BLOCK], row_s[BLOCK - 1::BLOCK], win_r, zero, jnp.int32(halo_blocks))
        seg_o = src_s.reshape(blocks, 1, BLOCK)
        seg_h = seg_o - n
        seg_r = row_s.reshape(halo_blocks, 1, BLOCK)
        dst_wide = tile_linear(dst_s)

        got_2 = exchange(out_2)
        near_2 = near_sums('near_2', 2, tile_linear(src_near), hidden_1, [])

        def build_2(copies, stages, tab, fx):
            per = peers // len(copies[0])
            some = math.gcd(per, 8)
            for p in range(len(copies[0])):
                copies[0][p].wait()
                copies[1][p].wait()

                def body(k, carry):
                    q = p * per + k * some
                    f = stages[0][pl.ds(q, some), :slots, :].reshape(some * slots, LANES)
                    m = stages[1][pl.ds(q, some)].reshape(some * slots, LANES)
                    z = mm(f, fx[3][...]) + mm(m, fx[4][...]) + fx[5][...]
                    put_rows(tab, q * slots, jnp.maximum(z, 0.0).astype(BF16).astype(F32), 2)
                    return carry
                lax.fori_loop(0, per // some, body, 0)

        def epi_2(a, bl, fx, out, put):
            scale = bl[1][...]
            mean = (a * jnp.concatenate([scale, scale], axis=1)).astype(BF16)
            z = mm(bl[0][...], fx[0][...]) + mm(mean, fx[1][...]) + fx[2][...]
            h = jnp.maximum(z, 0.0).astype(BF16)
            out[0][...] = mean
            out[1][...] = h
            both = mm(h, fx[6][...])
            pieces = split3(both[:, :LANES])
            out[2][...] = pieces
            out[3][...] = both[:, LANES:]
            put(pieces.astype(F32))

        mean_2, hidden_2, proj, logits_self, out_3 = edge_call(
            'layer_2', (meta_far, tile_linear(src_far), seg_far), 2, halo, n, win_e,
            [(peers, slots + TAIL, LANES), (peers, slots, LANES)], build_2, [got_1, got_2, near_2],
            [hidden_1, inv], [w_self_2, w_neigh_2, b2, w_self_1, w_neigh_1, b1, jnp.concatenate([wn3, ws3], axis=1)],
            [((n, hidden), BF16, False), ((n, hidden), BF16, False), ((n, LANES), BF16, False),
             ((n, LANES), F32, False)], n, half_tile, epi_2, 40, init=2, ahead=2, keep=1, pick=(send_flat, peers, slots))

        got_3 = exchange(out_3).reshape(halo, LANES)
        near_3 = near_sums('near_3', 1, src_near, proj, [target])
        inv_total = (1.0 / total).reshape(1, 1)

        def epi_3(a, bl, fx, out, put):
            scale = bl[1][...]
            z = bl[0][...] + fold3(a * scale, fx[2][...]) + fx[0][...]
            top = jnp.max(z, axis=1, keepdims=True)
            e = jnp.exp(z - top)
            each = jnp.sum(e, axis=1, keepdims=True) * (1.0 / 3.0)
            lse = top + jnp.log(each)
            t = bl[2][...].astype(F32)
            inside = jnp.minimum(t, 1.0)
            hit = t - inside
            d = (e * (1.0 / each) * inside - hit) * fx[1][...]
            db = d.astype(BF16)
            out[0][...] = db
            pieces = split3(db.astype(F32) * scale)
            out[1][...] = pieces
            put(pieces.astype(F32))
            add_rows(out[2], d)
            add_rows(out[3], hit * (lse - z))

        def finish_3(a, fx):
            return split3(fold3(a, fx[2][...]))

        d_bf_3, scaled_3, g_b3, loss_parts, back_3 = edge_call(
            'layer_3', (meta_far, src_far, seg_far), 1, halo, n, win_e, [(halo, LANES)], rows_of(1), [got_3, near_3],
            [logits_self, inv, target], [b3, jnp.broadcast_to(inv_total, (1, LANES)), folder],
            [((n, LANES), BF16, False), ((n, LANES), BF16, False), ((8, LANES), F32, True), ((8, LANES), F32, True)],
            n, tile, epi_3, 30, init=1, late=True, ahead=3, keep=1,
            then=((meta_halo, dst_s, seg_h), 1, halo, win_h, finish_3))

        ret_3 = exchange(back_3.reshape(peers, slots, LANES)).reshape(halo, LANES)
        own_3 = edge_call('back_3_own', (meta_own, dst_s, seg_o), 1, n, n, win_e, [(n, LANES)], rows_of(1),
                          [scaled_3], [], [], [((n, LANES), F32, False)], n, tile, None, 20)[0]

        def epi_o3(a, bl, fx, out, put):
            tb = fold3(a, fx[2][...]).astype(BF16)
            d_h = mm(jnp.concatenate([bl[1][...], tb], axis=1), fx[0][...])
            d_pre = jnp.where(bl[0][...].astype(F32) > 0, d_h, 0.0)
            db = d_pre.astype(BF16)
            scale = bl[2][...]
            out[0][...] = tb
            out[1][...] = db
            scaled = (mm(db, fx[1][...]) * jnp.concatenate([scale, scale], axis=1)).astype(BF16)
            out[2][...] = scaled
            put(scaled.astype(F32))
            add_rows(out[3], d_pre)

        def finish_2(a, fx):
            return a.astype(BF16)

        tb_3, d_bf_2, scaled_2, g_b2, back_2 = edge_call(
            'owner_3', (meta_owner, slot_s, seg_r), 1, halo, n, win_r, [(halo, LANES)], rows_of(1), [ret_3, own_3],
            [hidden_2, d_bf_3, inv], [jnp.concatenate([ws3_t, wn3_t], axis=0), w_neigh_2.T, folder],
            [((n, LANES), BF16, False), ((n, hidden), BF16, False), ((n, hidden), BF16, False), ((8, hidden), F32, True)],
            n, half_tile, epi_o3, 30, init=1, late=True, ahead=1, keep=2,
            then=((meta_halo, dst_wide, seg_h), 2, halo, win_h, finish_2))

        def epi_b2o(a, bl, fx, out, put):
            out[0][...] = a + mm(bl[0][...], fx[0][...])

        ret_2 = exchange(back_2.reshape(peers, slots, hidden)).reshape(halo, hidden)
        own_2 = edge_call('back_2_own', (meta_own, dst_wide, seg_o), 2, n, n, win_e, [(n, hidden)], rows_of(2),
                          [scaled_2], [d_bf_2], [w_self_2.T], [((n, hidden), F32, False)], n, tile, epi_b2o, 30)[0]

        def epi_o2(a, bl, fx, out, put):
            d_pre = jnp.where(bl[0][...].astype(F32) > 0, a, 0.0)
            inputs = jnp.concatenate([bl[1][...], bl[2][...]], axis=1)
            out[0][...] += lax.dot_general(inputs, d_pre.astype(BF16), (((0,), (0,)), ((), ())),
                                           preferred_element_type=F32)
            add_rows(out[1], d_pre)

        g_1, g_b1 = edge_call(
            'owner_2', (meta_owner, tile_linear(slot_s), seg_r), 2, halo, n, win_r, [(halo, hidden)], rows_of(2),
            [ret_2, own_2], [hidden_1, features, mean_1], [],
            [((2 * LANES, hidden), F32, True), ((8, hidden), F32, True)], n, n, epi_o2, 25, init=1, late=True, ahead=3)

        def contract(a, b):
            return jnp.einsum('nd,ne->de', a, b, preferred_element_type=F32)

        at = jnp.arange(LANES, dtype=jnp.int32)[None, :]
        g_3 = jnp.where(at < SPREAD, contract(hidden_2, d_bf_3), contract(hidden_2, tb_3))
        g1s, g1n, g2s, g2n, g3s, g3n, s1, s2, s3, loss = sum_over_devices(
            [g_1, contract(hidden_1, d_bf_2), contract(mean_2, d_bf_2), g_3],
            [g_b1, g_b2, g_b3, loss_parts], total.reshape(1, 1), classes, peers)
        return (loss.reshape(()), g1s, g1n, s1.reshape(-1), g2s, g2n, s2.reshape(-1), g3s.T, g3n.T, s3.reshape(-1))

    sharded = P(GROUP_AXIS)
    whole = P()
    return jax.shard_map(device_step, mesh=mesh,
                         in_specs=(sharded,) * 7 + (whole,) * 9,
                         out_specs=(whole,) * 10, check_vma=False)
```

```python
import math

import jax
import jax.numpy as jnp
from jax import lax
from jax.experimental import pallas as pl
from jax.experimental.pallas import tpu as pltpu
from jax.sharding import PartitionSpec as P

GROUP_AXIS = 'gp'
LANES = 128
SPREAD = 40
BLOCK = 128
GROUP = 8
TAIL = 8
F32 = jnp.float32
BF16 = jnp.bfloat16
VMEM_LIMIT = 63 * 2 ** 20

SMEM_SPEC = pl.BlockSpec(memory_space=pltpu.SMEM)
HBM_SPEC = pl.BlockSpec(memory_space=pltpu.HBM)


def whole_spec(shape):
    return pl.BlockSpec(shape, lambda i: (0,) * len(shape))


def row_spec(rows, width):
    return pl.BlockSpec((rows, width), lambda i: (i, 0))


def params():
    return pltpu.CompilerParams(vmem_limit_bytes=VMEM_LIMIT, dimension_semantics=('arbitrary',))


def cost(micros):
    return pl.CostEstimate(flops=int(micros * 4e6), bytes_accessed=int(micros * 1e6), transcendentals=0)


def mm(a, b):
    return jnp.dot(a, b, preferred_element_type=F32)


def tile_linear(row):
    return ((row >> 3) << 4) | (row & 7)


def put_rows(tab, row0, x, nc):
    rows = x.shape[0]
    if nc == 1:
        tab[pl.ds(pl.multiple_of(row0, 8), rows), :] = x
    else:
        for g in range(rows // 8):
            for c in range(nc):
                at = pl.multiple_of((row0 + g * 8) * nc + c * 8, 8)
                tab[pl.ds(at, 8), :] = x[g * 8:g * 8 + 8, c * LANES:(c + 1) * LANES]


def fetch(src, stage, sem, parts):
    rows = src.shape[0] // parts
    copies = [pltpu.make_async_copy(src.at[pl.ds(k * rows, rows)], stage.at[pl.ds(k * rows, rows)], sem.at[k])
              for k in range(parts)]
    for c in copies:
        c.start()
    return copies


def unpack(copies, stage, tab, row0, nc):
    rows = stage.shape[0] // len(copies)
    step = next(d for d in (128, 96, 64, 32, 16) if rows % d == 0)
    for p, c in enumerate(copies):
        c.wait()

        def body(k, carry):
            at = pl.multiple_of(p * rows + k * step, step)
            put_rows(tab, row0 + at, stage[pl.ds(at, step), :].astype(F32), nc)
            return carry
        lax.fori_loop(0, rows // step, body, 0)


def group_of(blocks):
    return next(u for u in (GROUP, 4, 2) if blocks % u == 0)


def zero_rows(acc):
    rows = acc.shape[0]
    step = next(s for s in (256, 128, 64, 32, 16, 8) if rows % s == 0)

    def body(k, carry):
        acc[pl.ds(pl.multiple_of(k * step, step), step), :] = jnp.zeros((step, acc.shape[1]), F32)
        return carry
    lax.fori_loop(0, rows // step, body, 0)


def gather_16(idx, base, first, reach, tab, nc, stride=1):
    sub = lax.broadcasted_iota(jnp.int32, (8, LANES), 0)
    room = idx.shape[0] - (reach - 1) * stride
    halves = [[None, None] for _ in range(nc)]
    for h in range(2):
        for k in range(8):
            at = idx.at[pl.ds((first + h * 8 + k) * stride, room)][base]
            for c in range(nc):
                row = jnp.broadcast_to(tab[pl.ds(at + 8 * c, 1), :], (8, LANES))
                halves[c][h] = row if k == 0 else jnp.where(sub == k, row, halves[c][h])
    return [jnp.concatenate(halves[c], axis=0).astype(BF16) for c in range(nc)]


def segment_sums(meta, part, idx, seg, tab, acc, bufs, nc, window, blocks):
    unroll = group_of(blocks)
    base, counts, most, owned = meta[0], meta[1], meta[2][0], meta[3][0]
    shift = (unroll * BLOCK).bit_length() - 1
    first_trip = owned >> shift if part == 'far' else 0
    end_trip = (owned + (1 << shift) - 1) >> shift if part == 'near' else blocks // unroll

    def fill(start, first, reach, buf):
        for g in range(BLOCK // 16):
            parts = gather_16(idx, start, first + g * 16, reach, tab, nc)
            for c in range(nc):
                buf[g * 16:g * 16 + 16, c * LANES:(c + 1) * LANES] = parts[c]

    def sums(b, at, buf):
        rows = lax.broadcasted_iota(jnp.int32, (window, BLOCK), 0) + at
        return mm(jnp.where(rows == seg[b], 1.0, 0.0).astype(BF16), buf[...])

    def add(at, x):
        acc[pl.ds(pl.multiple_of(at, 8), window), :] += x

    span = unroll * BLOCK
    last_trip = blocks // unroll - 1
    fill(jnp.minimum(first_trip, last_trip) * span, 0, span, bufs[0])

    def body(t, carry):
        before = None
        for u in range(unroll):
            b = t * unroll + u
            now = (base[b], sums(b, base[b], bufs[u % 2]))
            if u + 1 < unroll:
                fill(t * span, (u + 1) * BLOCK, span, bufs[(u + 1) % 2])
            else:
                fill(jnp.minimum(t + 1, last_trip) * span, 0, span, bufs[0])
            if before is not None:
                add(*before)
            before = now
        add(*before)
        return carry
    lax.fori_loop(first_trip, end_trip, body, 0)

    @pl.when(most > 1)
    def _():
        def again(b, carry):
            count = counts[b]

            @pl.when(count > 1)
            def _():
                fill(b * BLOCK, 0, BLOCK, bufs[0])

                def more(w, c):
                    at = base[b] + w * window
                    add(at, sums(b, at, bufs[0]))
                    return c
                lax.fori_loop(1, count, more, 0)
            return carry
        lax.fori_loop(first_trip * unroll, end_trip * unroll, again, 0)


def spread_lanes():
    return lax.broadcasted_iota(jnp.int32, (1, LANES), 1)


def split3(x):
    hi = x.astype(BF16).astype(F32)
    rest = x - hi
    mid = rest.astype(BF16).astype(F32)
    low = rest - mid
    lane = spread_lanes()
    out = jnp.where(lane < SPREAD, hi, jnp.where(lane < 2 * SPREAD, mid, low))
    return jnp.where(lane < 3 * SPREAD, out, 0.0).astype(BF16)


def pieces3(a):
    hi = a.astype(BF16)
    rest = a - hi.astype(F32)
    mid = rest.astype(BF16)
    low = (rest - mid.astype(F32)).astype(BF16)
    return jnp.concatenate([hi, mid, low], axis=1)


def fold3(a, folder):
    return mm(pieces3(a), folder)


def add_rows(ref, x):
    ref[...] += jnp.sum(x.reshape(x.shape[0] // 8, 8, x.shape[1]), axis=0)


PIECES = 4


def send_part(stage, out, sem, k):
    size = stage.shape[0] // PIECES
    at = pl.multiple_of(k * size, size)
    return pltpu.make_async_copy(stage.at[pl.ds(at, size)], out.at[pl.ds(at, size)], sem.at[k])


def send_out(src, out, sem):
    done = pltpu.make_async_copy(src, out, sem)
    done.start()
    done.wait()


def pick_pieces(idx, tab, stage, out, sem, peers, slots):
    size = peers // PIECES

    def piece(k, c):
        def body(p, carry):
            for g in range(slots // 16):
                stage[k * size + p, g * 16:g * 16 + 16, :] = gather_16(idx, k * size + p, g * 16, slots, tab, 1, peers)[0]
            return carry
        lax.fori_loop(0, size, body, 0)
        send_part(stage, out, sem, k).start()
        return c
    lax.fori_loop(0, PIECES, piece, 0)
    for k in range(PIECES):
        send_part(stage, out, sem, k).wait()


def pick_rows(name, src, idx, peers, slots, mask):
    n = src.shape[0]
    parts = math.gcd(n // 128, 4)

    def kern(idx_ref, src_ref, mask_ref, out, tab, stage, sem, rows, out_sem):
        copies = fetch(src_ref, stage, sem, parts)
        total = jnp.sum(mask_ref[...], axis=(0, 1), keepdims=True)
        high = jnp.floor(total * (1.0 / LANES))
        first = lax.broadcasted_iota(jnp.int32, (TAIL, LANES), 0) == 0
        lane = lax.broadcasted_iota(jnp.int32, (TAIL, LANES), 1)
        digits = jnp.where(lane == 0, high, jnp.where(lane == 1, total - high * LANES, 0.0))
        tail = jnp.where(first, digits, 0.0).astype(BF16)

        def put_tail(p, c):
            rows[p, slots:slots + TAIL, :] = tail
            return c
        lax.fori_loop(0, peers, put_tail, 0)
        unpack(copies, stage, tab, 0, 1)
        pick_pieces(idx_ref, tab, rows, out, out_sem, peers, slots)

    return pl.pallas_call(
        kern, name=name, out_shape=jax.ShapeDtypeStruct((peers, slots + TAIL, LANES), BF16),
        in_specs=[SMEM_SPEC, HBM_SPEC, pl.BlockSpec(memory_space=pltpu.VMEM)], out_specs=HBM_SPEC,
        scratch_shapes=[pltpu.VMEM((n, LANES), F32), pltpu.VMEM((n, LANES), BF16), pltpu.SemaphoreType.DMA((parts,)),
                        pltpu.VMEM((peers, slots + TAIL, LANES), BF16), pltpu.SemaphoreType.DMA((PIECES,))],
        compiler_params=pltpu.CompilerParams(vmem_limit_bytes=VMEM_LIMIT), cost_estimate=cost(10))(idx, src, mask)


def edge_call(name, edges, nc, table_rows, acc_rows, window, sources, build, hbm_in, blocked, fixed, outs, rows_out,
              tile, epilogue, micros, init=None, late=False, sub=2048, keep=0, pick=None, then=None,
              ahead=0):
    meta, part, idx, seg = edges
    blocks = seg.shape[0]
    width = nc * LANES
    nh, nb, nf, no, ns = len(hbm_in), len(blocked), len(fixed), len(outs), len(sources)
    acc_total = -(-(acc_rows + window) // 256) * 256
    parts = 4
    steps = 1 if epilogue is None else rows_out // tile
    sub = math.gcd(sub, tile)
    more_in, more_specs, more_out, more_scratch = [], [], [], []
    late_scratch = [pltpu.VMEM((acc_rows, width), F32)] if late else []
    if ahead:
        late_scratch += [pltpu.VMEM(x.shape, x.dtype) for x in blocked[:ahead]] + [pltpu.SemaphoreType.DMA((ahead,))]
    if keep:
        more_scratch.append(pltpu.VMEM((rows_out * keep, LANES), F32))
    if pick:
        p_idx, peers, slots = pick
        more_in.append(p_idx)
        more_specs.append(SMEM_SPEC)
        more_out.append(jax.ShapeDtypeStruct((peers, slots, LANES), BF16))
        more_scratch += [pltpu.VMEM((peers, slots, LANES), BF16), pltpu.SemaphoreType.DMA((PIECES,))]
    if then:
        (t_meta, t_part, t_idx, t_seg), t_nc, t_rows, t_window, finish = then
        t_width = t_nc * LANES
        t_total = -(-(t_rows + t_window) // 256) * 256
        more_in += [*t_meta, t_idx, t_seg]
        more_specs += [SMEM_SPEC] * 5 + [whole_spec(t_seg.shape)]
        more_out.append(jax.ShapeDtypeStruct((t_rows, t_width), BF16))
        more_scratch += [pltpu.VMEM((t_total, t_width), F32), pltpu.VMEM((BLOCK, t_width), BF16),
                         pltpu.VMEM((BLOCK, t_width), BF16), pltpu.VMEM((t_rows, t_width), BF16),
                         pltpu.SemaphoreType.DMA((PIECES,))]
    nm = len(more_in)

    def kern(*refs):
        meta_refs, (idx_ref, seg_ref), refs = refs[:4], refs[4:6], refs[6:]
        hb, refs = refs[:nh], refs[nh:]
        bl, refs = refs[:nb], refs[nb:]
        fx, refs = refs[:nf], refs[nf:]
        extra, refs = refs[:nm], refs[nm:]
        out, refs = refs[:no], refs[no:]
        last_out, refs = refs[:len(more_out)], refs[len(more_out):]
        tab, acc, buf_0, buf_1, isem = refs[:5]
        stages, sems, scratch = refs[5:5 + ns], refs[5 + ns:5 + 2 * ns], refs[5 + 2 * ns:]
        if late:
            begin, scratch = scratch[0], scratch[1:]
        if ahead:
            whole, whole_sem, scratch = scratch[:ahead], scratch[ahead], scratch[ahead + 1:]
        i = pl.program_id(0)

        @pl.when(i == 0)
        def _():
            copies = [fetch(h, st, sm, parts) for h, st, sm in zip(hb, stages, sems)]
            if init is not None:
                start = pltpu.make_async_copy(hb[init], begin if late else acc.at[pl.ds(0, acc_rows), :], isem)
                if not late:
                    start.start()
            if init is None or late:
                zero_rows(acc)
            for o, (_, _, sums) in zip(out, outs):
                if sums:
                    o[...] = jnp.zeros_like(o)
            if then:
                zero_rows(scratch[1])
            build(copies, stages, tab, fx)
            if late:
                start.start()
            wholes = [pltpu.make_async_copy(bl[k], whole[k], whole_sem.at[k]) for k in range(ahead)]
            for c in wholes:
                c.start()
            if init is not None and not late:
                start.wait()
            segment_sums(meta_refs, part, idx_ref, seg_ref, tab, acc, (buf_0, buf_1), nc, window, blocks)
            if late:
                start.wait()
            for c in wholes:
                c.wait()
            if epilogue is None:
                send_out(acc.at[pl.ds(0, acc_rows), :], out[0], isem)
        if epilogue is not None:
            def rows(j, carry):
                at = pl.multiple_of(j * sub, sub)
                row0 = pl.multiple_of(i * tile + at, sub)

                def put(x):
                    put_rows(scratch[0], row0, x, keep)
                a = acc[pl.ds(row0, sub), :]
                if late:
                    a = a + begin[pl.ds(row0, sub), :]
                epilogue(a, [whole[k].at[pl.ds(row0, sub), :] for k in range(ahead)]
                         + [r.at[pl.ds(at, sub), :] for r in bl[ahead:]], fx,
                         [o if sums else o.at[pl.ds(at, sub), :] for o, (_, _, sums) in zip(out, outs)], put)
                return carry
            lax.fori_loop(0, tile // sub, rows, 0)

        if pick:
            @pl.when(i == steps - 1)
            def _():
                kept, stage, out_sem = scratch
                pick_pieces(extra[0], kept, stage, last_out[0], out_sem, peers, slots)
        if then:
            @pl.when(i == steps - 1)
            def _():
                kept, acc_2, buf_2, buf_3, stage, out_sem = scratch
                segment_sums(extra[:4], t_part, extra[4], extra[5], kept, acc_2, (buf_2, buf_3), t_nc, t_window,
                             t_seg.shape[0])
                size = t_rows // PIECES
                step = math.gcd(2048, size)

                def piece(k, c):
                    def rows(j, carry):
                        at = pl.multiple_of(k * size + j * step, step)
                        stage[pl.ds(at, step), :] = finish(acc_2[pl.ds(at, step), :], fx)
                        return carry
                    lax.fori_loop(0, size // step, rows, 0)
                    send_part(stage, last_out[0], out_sem, k).start()
                    return c
                lax.fori_loop(0, PIECES, piece, 0)
                for k in range(PIECES):
                    send_part(stage, last_out[0], out_sem, k).wait()

    out_shape, out_specs = [], []
    for shape, dtype, sums in outs:
        out_shape.append(jax.ShapeDtypeStruct(shape, dtype))
        out_specs.append(HBM_SPEC if epilogue is None else whole_spec(shape) if sums else row_spec(tile, shape[1]))
    return pl.pallas_call(
        kern, name=name, grid=(steps,), out_shape=out_shape + more_out,
        in_specs=([SMEM_SPEC] * 5 + [whole_spec(seg.shape)] + [HBM_SPEC] * nh
                  + [HBM_SPEC] * ahead + [row_spec(tile, x.shape[1]) for x in blocked[ahead:]]
                  + [whole_spec(x.shape) for x in fixed] + more_specs),
        out_specs=out_specs + [HBM_SPEC] * len(more_out),
        scratch_shapes=([pltpu.VMEM((table_rows * nc, LANES), F32), pltpu.VMEM((acc_total, width), F32),
                         pltpu.VMEM((BLOCK, width), BF16), pltpu.VMEM((BLOCK, width), BF16),
                         pltpu.SemaphoreType.DMA(())]
                        + [pltpu.VMEM(shape, BF16) for shape in sources]
                        + [pltpu.SemaphoreType.DMA((parts,)) for _ in sources] + late_scratch + more_scratch),
        compiler_params=params(), cost_estimate=cost(micros))(*meta, idx, seg, *hbm_in, *blocked, *fixed, *more_in)


SHARE = 16


def grad_places(shapes):
    places, at = [], 0
    for rows, width in shapes:
        columns = []
        for _ in range(width // LANES):
            columns.append(at)
            at += -(-rows // SHARE)
        places.append(columns)
    return places, at


def sum_over_devices(grads, sums, total, classes, peers):
    chips = peers // 2
    places, used = grad_places([g.shape for g in grads] + [(SHARE, LANES)])
    rounds = -(-used // peers)
    rows = SHARE * rounds
    widths = [x.shape[1] for x in sums]

    def device(chip, core):
        return chip * 2 + core

    def kern(*refs):
        ng, ns = len(grads), len(sums)
        g_refs, s_refs, out_ref = refs[:ng], refs[ng:ng + ns], refs[ng + ns]
        x_ref, half, mine, got, pair_sem, send_sem, recv_sem, send_2, recv_2 = refs[ng + ns + 1:]
        me = lax.axis_index(GROUP_AXIS)
        chip, core = me // 2, me % 2
        mate = device(chip, 1 - core)
        barrier = pltpu.get_barrier_semaphore()

        def hello(to):
            pl.semaphore_signal(barrier, inc=1, device_id=(to,), device_id_type=pl.DeviceIdType.MESH)

        def greet(k, carry):
            hello(device((chip + k) % chips, core))
            return carry
        lax.fori_loop(1, chips, greet, 0)
        hello(mate)

        def at(q):
            unit = q // rounds
            return unit // chips, unit % chips, (q % rounds) * SHARE

        def put(q, value):
            h, c, r = at(q)
            x_ref[h, c, r:r + SHARE, :] = value
        for g, columns in zip(g_refs, places):
            for w, first in enumerate(columns):
                for k in range(g.shape[0] // SHARE):
                    put(first + k, g[k * SHARE:(k + 1) * SHARE, w * LANES:(w + 1) * LANES])
        row = lax.broadcasted_iota(jnp.int32, (SHARE, LANES), 0)
        small, line = jnp.zeros((SHARE, LANES), F32), 0
        for s_ref, width in zip(s_refs, widths):
            for w in range(width // LANES):
                total = jnp.sum(s_ref[:, w * LANES:(w + 1) * LANES], axis=0, keepdims=True)
                small = jnp.where(row == line, total, small)
                line += 1
        put(places[-1][0], small)
        for q in range(used, peers * rounds):
            put(q, jnp.zeros((SHARE, LANES), F32))

        def pair(src, dst, k):
            return pltpu.make_async_remote_copy(src_ref=src, dst_ref=dst, send_sem=pair_sem.at[2 * k],
                                                recv_sem=pair_sem.at[2 * k + 1], device_id=(mate,),
                                                device_id_type=pl.DeviceIdType.MESH)
        pl.semaphore_wait(barrier, chips)
        first = pair(x_ref.at[1 - core], half, 0)
        first.start()
        first.wait()

        def add(c, carry):
            mine[c] = x_ref[core, c] + half[c]
            return carry
        lax.fori_loop(0, chips, add, 0)

        def share(k):
            to = (chip + k) % chips
            return pltpu.make_async_remote_copy(src_ref=mine.at[to], dst_ref=got.at[chip], send_sem=send_sem.at[k],
                                                recv_sem=recv_sem.at[chip], device_id=(device(to, core),),
                                                device_id_type=pl.DeviceIdType.MESH)

        def landed(k):
            frm = (chip + k) % chips
            return pltpu.make_async_remote_copy(src_ref=mine.at[frm], dst_ref=got.at[frm], send_sem=send_sem.at[k],
                                                recv_sem=recv_sem.at[frm], device_id=(me,),
                                                device_id_type=pl.DeviceIdType.MESH)

        def start(k, carry):
            share(k).start()
            return carry
        lax.fori_loop(1, chips, start, 0)
        got[chip] = mine[chip]

        def settle(k, carry):
            landed(k).wait_recv()
            return carry
        lax.fori_loop(1, chips, settle, 0)

        def more(c, total):
            return total + got[c]
        out_ref[core, chip] = lax.fori_loop(0, chips, more, jnp.zeros((rows, LANES), F32))

        def drain(k, carry):
            share(k).wait_send()
            return carry
        lax.fori_loop(1, chips, drain, 0)

        def give(k):
            return pltpu.make_async_remote_copy(src_ref=out_ref.at[core, chip], dst_ref=out_ref.at[core, chip],
                                                send_sem=send_2.at[k], recv_sem=recv_2.at[chip],
                                                device_id=(device((chip + k) % chips, core),),
                                                device_id_type=pl.DeviceIdType.MESH)

        def given(k):
            frm = (chip + k) % chips
            return pltpu.make_async_remote_copy(src_ref=out_ref.at[core, frm], dst_ref=out_ref.at[core, frm],
                                                send_sem=send_2.at[k], recv_sem=recv_2.at[frm], device_id=(me,),
                                                device_id_type=pl.DeviceIdType.MESH)

        def start_2(k, carry):
            give(k).start()
            return carry
        lax.fori_loop(1, chips, start_2, 0)

        def settle_2(k, carry):
            given(k).wait_recv()
            return carry
        lax.fori_loop(1, chips, settle_2, 0)

        def drain_2(k, carry):
            give(k).wait_send()
            return carry
        lax.fori_loop(1, chips, drain_2, 0)
        last = pair(out_ref.at[core], out_ref.at[core], 1)
        last.start()
        last.wait()

    vmem = pl.BlockSpec(memory_space=pltpu.VMEM)
    shape = (2, chips, rows, LANES)
    full = pl.pallas_call(
        kern, name='sum_all', out_shape=jax.ShapeDtypeStruct(shape, F32),
        in_specs=[vmem] * (len(grads) + len(sums)), out_specs=vmem,
        scratch_shapes=[pltpu.VMEM(shape, F32), pltpu.VMEM(shape[1:], F32), pltpu.VMEM(shape[1:], F32),
                        pltpu.VMEM(shape[1:], F32), pltpu.SemaphoreType.DMA((4,)),
                        pltpu.SemaphoreType.DMA((chips,)), pltpu.SemaphoreType.DMA((chips,)),
                        pltpu.SemaphoreType.DMA((chips,)), pltpu.SemaphoreType.DMA((chips,))],
        compiler_params=pltpu.CompilerParams(collective_id=0, has_side_effects=True), cost_estimate=cost(25))(*grads, *sums)

    def unpack_kern(full_ref, total_ref, *outs):
        def part(q):
            unit = q // rounds
            r = (q % rounds) * SHARE
            return full_ref[unit // chips, unit % chips, r:r + SHARE, :]

        def move(o, columns, skip):
            for w, first in enumerate(columns):
                for k in range(o.shape[0] // SHARE):
                    o[k * SHARE:(k + 1) * SHARE, w * LANES:(w + 1) * LANES] = part(first + skip + k)
        move(outs[0], places[0], 0)
        move(outs[1], places[0], outs[0].shape[0] // SHARE)
        for o, columns in zip(outs[2:], places[1:-2]):
            move(o, columns, 0)
        both = jnp.concatenate([part(places[-2][0] + k) for k in range(rows_3 // SHARE)], axis=0).T
        outs[ng][...] = both[:classes, :]
        outs[ng + 1][...] = both[SPREAD:SPREAD + classes, :]
        small, line = part(places[-1][0]), 0
        for o, width in zip(outs[ng + 2:-1], widths):
            for w in range(width // LANES):
                wide = min(LANES, o.shape[1] - w * LANES)
                o[:, w * LANES:w * LANES + wide] = small[line:line + 1, :wide]
                line += 1
        outs[-1][...] = jnp.sum(small[line:line + 1, :SPREAD], axis=1, keepdims=True) / total_ref[...]
    ng = len(grads)
    rows_3 = grads[-1].shape[0]
    rows_1, width_1 = grads[0].shape
    outs = ([(rows_1 // 2, width_1)] * 2 + [g.shape for g in grads[1:-1]] + [(classes, rows_3)] * 2
            + [(1, w) for w in widths[:-2]] + [(1, classes), (1, 1)])
    return pl.pallas_call(unpack_kern, name='unpack_sums', out_shape=[jax.ShapeDtypeStruct(o, F32) for o in outs],
                          in_specs=[vmem, vmem], out_specs=[vmem] * len(outs), cost_estimate=cost(3))(full, total)


def edge_meta(seg_first, seg_last, window, inside):
    base = seg_first & ~7
    count = jnp.where(inside, lax.div(jnp.maximum(seg_last - base, 0), jnp.int32(window)) + 1, 1)
    return base, count, jnp.max(count).reshape(1)


def bits_for(n):
    return max(1, (n - 1).bit_length())


def spread3(w):
    w = jnp.pad(w, ((0, 0), (0, SPREAD - w.shape[1])))
    return jnp.pad(jnp.concatenate([w, w, w], axis=1), ((0, 0), (0, LANES - 3 * SPREAD)))


def lanes_pad(w):
    return jnp.pad(w, ((0, 0), (0, LANES - w.shape[1])))


def solution(mesh):
    peers = mesh.shape[GROUP_AXIS]

    def exchange(x):
        return lax.all_to_all(x, GROUP_AXIS, 0, 0, tiled=True)

    def device_step(features, labels, train_mask, send_idx, src_idx, dst_idx, inv_deg,
                    w_self_1, w_neigh_1, bias_1, w_self_2, w_neigh_2, bias_2,
                    w_self_3, w_neigh_3, bias_3):
        n = features.shape[0]
        slots = send_idx.shape[1]
        halo = peers * slots
        edges = src_idx.shape[0]
        hidden = w_self_1.shape[1]
        classes = w_self_3.shape[1]
        send_flat = send_idx.T.reshape(-1)
        tile = next(t for t in (4096, 1024) if n % t == 0)
        half_tile = tile // 2
        slot_bits = bits_for(halo)
        dst_bits = bits_for(n)
        table = n + halo

        blocks = edges // BLOCK
        halo_blocks = halo // BLOCK
        win_e, win_h, win_r = 192, 208, 272
        owned = jnp.sum((src_idx < n).astype(jnp.int32))
        start = jnp.arange(blocks, dtype=jnp.int32) * BLOCK
        near_inside, far_inside = start < owned, start + BLOCK > owned
        owned_1 = owned.reshape(1)

        src_bits = bits_for(table)
        far_bit = dst_bits + src_bits
        by_dst = lax.sort(((src_idx >= n).astype(jnp.int32) << far_bit) | (dst_idx << src_bits) | src_idx, is_stable=False)
        src_f = by_dst & ((1 << src_bits) - 1)
        dst_f = (by_dst >> src_bits) & ((1 << dst_bits) - 1)
        is_far = src_f >= n
        src_near = jnp.minimum(src_f, n - 1)
        src_far = jnp.maximum(src_f - n, 0)
        seg_near = jnp.where(is_far, -1, dst_f).reshape(blocks, 1, BLOCK)
        seg_far = jnp.where(is_far, dst_f, -1).reshape(blocks, 1, BLOCK)
        first, last = dst_f[::BLOCK], dst_f[BLOCK - 1::BLOCK]
        meta_near = (*edge_meta(first, jnp.where(is_far[BLOCK - 1::BLOCK], n - 1, last), win_e, near_inside), owned_1)
        meta_far = (*edge_meta(jnp.where(is_far[::BLOCK], first, 0), last, win_e, far_inside), owned_1)

        inv = jnp.broadcast_to(inv_deg[:, None], (n, LANES))
        b1 = bias_1.reshape(1, -1)
        b2 = bias_2.reshape(1, -1)
        lane = jnp.arange(LANES, dtype=jnp.int32)
        used = lane < 3 * SPREAD
        folder = jnp.tile(((lane[:, None] % SPREAD == lane[None, :] % SPREAD) & used[:, None] & used[None, :]).astype(BF16),
                          (3, 1))
        b3 = jnp.where(lane < 3 * SPREAD, spread3(bias_3.reshape(1, -1)), -1e30)
        if classes < SPREAD:
            b3 = jnp.where(lane % SPREAD < classes, b3, -1e30)
        target = jnp.where(lane[None, :] < 3 * SPREAD,
                           train_mask[:, None] * (1.0 + (labels[:, None] == lane[None, :] % SPREAD)), 0.0).astype(BF16)
        ws3, wn3 = spread3(w_self_3), spread3(w_neigh_3)
        ws3_t, wn3_t = lanes_pad(w_self_3).T, lanes_pad(w_neigh_3).T

        def rows_of(nc):
            def build(copies, stages, tab, fx):
                unpack(copies[0], stages[0], tab, 0, nc)
            return build

        def near_sums(name, nc, idx, rows, also):
            return edge_call(name, (meta_near, 'near', idx, seg_near), nc, n, n, win_e, [rows.shape], rows_of(nc),
                             [rows] + also, [], [], [((n, nc * LANES), F32, False)], n, tile, None, 20)[0]

        out_1 = pick_rows('send_1', features, send_flat, peers, slots, train_mask.reshape(-1, LANES))
        got_1 = exchange(out_1)
        near_1 = near_sums('near_1', 1, src_near, features, [inv])
        counts = got_1[:, slots, :2].astype(F32)
        total = jnp.sum(counts[:, 0]) * LANES + jnp.sum(counts[:, 1])

        def build_1(copies, stages, tab, fx):
            per = peers // len(copies[0])
            some = math.gcd(per, 8)
            for p in range(len(copies[0])):
                copies[0][p].wait()

                def body(k, carry):
                    q = p * per + k * some
                    rows = stages[0][pl.ds(q, some), :slots, :].reshape(some * slots, LANES)
                    put_rows(tab, q * slots, rows.astype(F32), 1)
                    return carry
                lax.fori_loop(0, per // some, body, 0)

        def epi_1(a, bl, fx, out, put):
            mean = (a * bl[1][...]).astype(BF16)
            z = mm(bl[0][...], fx[0][...]) + mm(mean, fx[1][...]) + fx[2][...]
            out[0][...] = mean
            out[1][...] = jnp.maximum(z, 0.0).astype(BF16)
            put(mean.astype(F32))

        mean_1, hidden_1, out_2 = edge_call(
            'layer_1', (meta_far, 'far', src_far, seg_far), 1, halo, n, win_e, [(peers, slots + TAIL, LANES)], build_1,
            [got_1, near_1], [features, inv], [w_self_1, w_neigh_1, b1],
            [((n, LANES), BF16, False), ((n, hidden), BF16, False)], n, tile, epi_1, 25, init=1, late=True, ahead=2,
            keep=1, pick=(send_flat, peers, slots))

        place = jnp.arange(halo, dtype=jnp.int32)
        keys = jnp.concatenate([(src_idx << dst_bits) | dst_idx,
                                (1 << 30) | (send_flat << slot_bits) | (place % peers * slots + place // peers)])
        keys = lax.optimization_barrier((keys, mean_1))[0]
        ordered = lax.sort(keys, is_stable=False)
        by_src, by_row = ordered[:edges], ordered[edges:] & ((1 << 30) - 1)
        src_s = by_src >> dst_bits
        dst_s = by_src & ((1 << dst_bits) - 1)
        row_s = by_row >> slot_bits
        slot_s = by_row & ((1 << slot_bits) - 1)
        first, last = src_s[::BLOCK], src_s[BLOCK - 1::BLOCK]
        meta_own = (*edge_meta(jnp.minimum(first, n - 1), jnp.minimum(last, n - 1), win_e, near_inside), owned_1)
        meta_halo = (*edge_meta(jnp.maximum(first - n, 0), jnp.maximum(last - n, 0), win_h, far_inside), owned_1)
        meta_owner = (*edge_meta(row_s[::BLOCK], row_s[BLOCK - 1::BLOCK], win_r, True), owned_1)
        seg_o = src_s.reshape(blocks, 1, BLOCK)
        seg_h = seg_o - n
        seg_r = row_s.reshape(halo_blocks, 1, BLOCK)
        dst_wide = tile_linear(dst_s)

        got_2 = exchange(out_2)
        near_2 = near_sums('near_2', 2, tile_linear(src_near), hidden_1, [])

        def build_2(copies, stages, tab, fx):
            per = peers // len(copies[0])
            some = math.gcd(per, 16)
            for p in range(len(copies[0])):
                copies[0][p].wait()
                copies[1][p].wait()

                def body(k, carry):
                    q = p * per + k * some
                    f = stages[0][pl.ds(q, some), :slots, :].reshape(some * slots, LANES)
                    m = stages[1][pl.ds(q, some)].reshape(some * slots, LANES)
                    z = mm(f, fx[3][...]) + mm(m, fx[4][...]) + fx[5][...]
                    put_rows(tab, q * slots, jnp.maximum(z, 0.0).astype(BF16).astype(F32), 2)
                    return carry
                lax.fori_loop(0, per // some, body, 0)

        def epi_2(a, bl, fx, out, put):
            scale = bl[1][...]
            mean = (a * jnp.concatenate([scale, scale], axis=1)).astype(BF16)
            z = mm(bl[0][...], fx[0][...]) + mm(mean, fx[1][...]) + fx[2][...]
            h = jnp.maximum(z, 0.0).astype(BF16)
            out[0][...] = mean
            out[1][...] = h
            both = mm(h, fx[6][...])
            pieces = split3(both[:, :LANES])
            out[2][...] = pieces
            out[3][...] = both[:, LANES:]
            put(pieces.astype(F32))

        mean_2, hidden_2, proj, logits_self, out_3 = edge_call(
            'layer_2', (meta_far, 'far', tile_linear(src_far), seg_far), 2, halo, n, win_e,
            [(peers, slots + TAIL, LANES), (peers, slots, LANES)], build_2, [got_1, got_2, near_2],
            [hidden_1, inv], [w_self_2, w_neigh_2, b2, w_self_1, w_neigh_1, b1, jnp.concatenate([wn3, ws3], axis=1)],
            [((n, hidden), BF16, False), ((n, hidden), BF16, False), ((n, LANES), BF16, False),
             ((n, LANES), F32, False)], n, half_tile, epi_2, 40, init=2, ahead=2, keep=1, pick=(send_flat, peers, slots))

        got_3 = exchange(out_3).reshape(halo, LANES)
        near_3 = near_sums('near_3', 1, src_near, proj, [target])
        inv_total = (1.0 / total).reshape(1, 1)

        def epi_3(a, bl, fx, out, put):
            scale = bl[1][...]
            z = bl[0][...] + fold3(a * scale, fx[2][...]) + fx[0][...]
            top = jnp.max(z, axis=1, keepdims=True)
            e = jnp.exp(z - top)
            each = jnp.sum(e, axis=1, keepdims=True) * (1.0 / 3.0)
            lse = top + jnp.log(each)
            t = bl[2][...].astype(F32)
            inside = jnp.minimum(t, 1.0)
            hit = t - inside
            d = (e * (1.0 / each) * inside - hit) * fx[1][...]
            db = d.astype(BF16)
            out[0][...] = db
            pieces = split3(db.astype(F32) * scale)
            out[1][...] = pieces
            put(pieces.astype(F32))
            add_rows(out[2], d)
            add_rows(out[3], hit * (lse - z))

        def finish_3(a, fx):
            return split3(fold3(a, fx[2][...]))

        d_bf_3, scaled_3, g_b3, loss_parts, back_3 = edge_call(
            'layer_3', (meta_far, 'far', src_far, seg_far), 1, halo, n, win_e, [(halo, LANES)], rows_of(1), [got_3, near_3],
            [logits_self, inv, target], [b3, jnp.broadcast_to(inv_total, (1, LANES)), folder],
            [((n, LANES), BF16, False), ((n, LANES), BF16, False), ((8, LANES), F32, True), ((8, LANES), F32, True)],
            n, tile, epi_3, 30, init=1, late=True, keep=1,
            then=((meta_halo, 'far', dst_s, seg_h), 1, halo, win_h, finish_3))

        ret_3 = exchange(back_3.reshape(peers, slots, LANES)).reshape(halo, LANES)
        own_3 = edge_call('back_3_own', (meta_own, 'near', dst_s, seg_o), 1, n, n, win_e, [(n, LANES)], rows_of(1),
                          [scaled_3], [], [], [((n, LANES), F32, False)], n, tile, None, 20)[0]

        def epi_o3(a, bl, fx, out, put):
            tb = fold3(a, fx[2][...]).astype(BF16)
            d_h = mm(jnp.concatenate([bl[1][...], tb], axis=1), fx[0][...])
            d_pre = jnp.where(bl[0][...].astype(F32) > 0, d_h, 0.0)
            db = d_pre.astype(BF16)
            scale = bl[2][...]
            out[0][...] = tb
            out[1][...] = db
            scaled = (mm(db, fx[1][...]) * jnp.concatenate([scale, scale], axis=1)).astype(BF16)
            out[2][...] = scaled
            put(scaled.astype(F32))
            add_rows(out[3], d_pre)

        def finish_2(a, fx):
            return a.astype(BF16)

        tb_3, d_bf_2, scaled_2, g_b2, back_2 = edge_call(
            'owner_3', (meta_owner, 'all', slot_s, seg_r), 1, halo, n, win_r, [(halo, LANES)], rows_of(1), [ret_3, own_3],
            [hidden_2, d_bf_3, inv], [jnp.concatenate([ws3_t, wn3_t], axis=0), w_neigh_2.T, folder],
            [((n, LANES), BF16, False), ((n, hidden), BF16, False), ((n, hidden), BF16, False), ((8, hidden), F32, True)],
            n, half_tile, epi_o3, 30, init=1, late=True, ahead=1, keep=2,
            then=((meta_halo, 'far', dst_wide, seg_h), 2, halo, win_h, finish_2))

        def epi_b2o(a, bl, fx, out, put):
            out[0][...] = a + mm(bl[0][...], fx[0][...])

        ret_2 = exchange(back_2.reshape(peers, slots, hidden)).reshape(halo, hidden)
        own_2 = edge_call('back_2_own', (meta_own, 'near', dst_wide, seg_o), 2, n, n, win_e, [(n, hidden)], rows_of(2),
                          [scaled_2], [d_bf_2], [w_self_2.T], [((n, hidden), F32, False)], n, tile, epi_b2o, 30)[0]

        def epi_o2(a, bl, fx, out, put):
            d_pre = jnp.where(bl[0][...].astype(F32) > 0, a, 0.0)
            inputs = jnp.concatenate([bl[1][...], bl[2][...]], axis=1)
            out[0][...] += lax.dot_general(inputs, d_pre.astype(BF16), (((0,), (0,)), ((), ())),
                                           preferred_element_type=F32)
            add_rows(out[1], d_pre)

        g_1, g_b1 = edge_call(
            'owner_2', (meta_owner, 'all', tile_linear(slot_s), seg_r), 2, halo, n, win_r, [(halo, hidden)], rows_of(2),
            [ret_2, own_2], [hidden_1, features, mean_1], [],
            [((2 * LANES, hidden), F32, True), ((8, hidden), F32, True)], n, n, epi_o2, 25, init=1, late=True, ahead=3)

        def contract(a, b):
            return jnp.einsum('nd,ne->de', a, b, preferred_element_type=F32)

        at = jnp.arange(LANES, dtype=jnp.int32)[None, :]
        g_3 = jnp.where(at < SPREAD, contract(hidden_2, d_bf_3), contract(hidden_2, tb_3))
        g1s, g1n, g2s, g2n, g3s, g3n, s1, s2, s3, loss = sum_over_devices(
            [g_1, contract(hidden_1, d_bf_2), contract(mean_2, d_bf_2), g_3],
            [g_b1, g_b2, g_b3, loss_parts], total.reshape(1, 1), classes, peers)
        return (loss.reshape(()), g1s, g1n, s1.reshape(-1), g2s, g2n, s2.reshape(-1), g3s.T, g3n.T, s3.reshape(-1))

    sharded = P(GROUP_AXIS)
    whole = P()
    return jax.shard_map(device_step, mesh=mesh,
                         in_specs=(sharded,) * 7 + (whole,) * 9,
                         out_specs=(whole,) * 10, check_vma=False)
```
